128 devices in a mesh: gz: 4 (over y), gy: 4 (over x_hi, core), gx: 8 (over z, x_lo).
Axes of the slice: x: 4 (x_hi: 2, x_lo: 2; x = x_hi * 2 + x_lo), y: 4, z: 4, core: 2. Of those that a mesh axis runs over, the one named last changes fastest.
Arguments:
- start: float32 [128, 64, 1024], P('gz', 'gy', 'gx'), may hold values from -21 to 21
- measured: float32 [128, 8, 1024], P(('gz', 'gy', 'gx')), may hold values from -18 to 18
- tiles: bfloat16 [8192, 8, 2048], P('gy', None, 'gx'), may hold values from -0.125 to 0.125
- tile_block: int32 [4, 8, 8], replicated, may hold values from 0 to 3
- angle_row: int32 [8], replicated, may hold values from 0 to 7, each once
Outputs:
- estimate: float32 [128, 64, 1024], P('gz', 'gy', 'gx')
- dual_state: float32 [3, 128, 64, 1024], P(None, 'gz', 'gy', 'gx')
The draws below stay inside these ranges and needn't reach their ends.
Inputs may be any that keep to these rules, and one draw needn't show every extreme that they name: `tile_block`: which of the 4 detector blocks of 256 columns each brick's tile covers at each angle. `angle_row`: every row of measured is named once.
All inputs are finite; a program needn't handle non-finite values.
Results may differ from the reference program's by a relative error of at most 0.0008.
Values may be sent and summed in bfloat16 or wider, within the bound.
A program may use at most 128 MiB of HBM per device.

```python
import jax
import jax.numpy as jnp
from jax import lax

CY = 16
CX = 128
ANG = 8
DW = 256
NBLK = 4
RADIUS = 8
ITERS = 2
V = 2048
DET = 1024
BRICKS_Y = 4
BRICKS_X = 8
NZ = 128
NY = 64
NX = 1024
N_GY = 4
N_GX = 8


def draw_start(key, part):
    depth_at = jnp.arange(NZ, dtype=jnp.float32)[:, None, None] / NZ
    height_at = jnp.arange(NY, dtype=jnp.float32)[None, :, None] / NY
    breadth_at = jnp.arange(NX, dtype=jnp.float32)[None, None, :] / NX
    position = depth_at + height_at + breadth_at
    ramp = jnp.exp(jnp.log(3.0) * (position - 1.5))
    rough = jnp.clip(jax.random.normal(key, (NZ, NY, NX), jnp.float32), -4.0, 4.0)
    return ramp * rough


def plant(result, stream_key, low, high):
    shape = result.shape
    index_at = [jax.random.randint(jax.random.fold_in(stream_key, axis), (), 0, shape[axis]) for axis in range(len(shape))]
    result = result.at[tuple(index_at)].set(low)
    longest = shape.index(max(shape))
    index_at[longest] = (index_at[longest] + 1) % shape[longest]
    return result.at[tuple(index_at)].set(high)


def steps_of(stream_key, shape, split, low, top_value):
    def one(axis_at, blocks):
        heights = jax.random.uniform(jax.random.fold_in(jax.random.fold_in(stream_key, 6), axis_at), (blocks,), jnp.float32, low / len(split), top_value / len(split))
        return jnp.repeat(jnp.exp(heights), shape[axis_at] // blocks).reshape((-1,) + (1,) * (len(shape) - axis_at - 1))

    gain = one(*split[0])
    for cut in split[1:]:
        gain = gain * one(*cut)
    return gain


def centred(key, extent, width, reach, shards=(), kind=jnp.bfloat16):
    gain = steps_of(key, extent, shards, -0.22, 0.18) if shards else 1.0
    result = jax.random.normal(key, extent, jnp.float32) * width * gain
    return jnp.minimum(jnp.maximum(result, -reach), reach).astype(kind)


def setup_inputs(seed: int = 0) -> dict:
    key_of = jax.random.split(jax.random.key(seed), 6)
    start = draw_start(jax.random.fold_in(key_of[5], 71), 0)
    measured = centred(key_of[1], (NZ, ANG, DET), 3.0, 18.0, ((0, 128),), jnp.float32)
    tiles = centred(key_of[2], (BRICKS_Y * V, ANG, BRICKS_X * DW), V ** -0.5, 0.125, ((0, 4), (2, 8)))
    tile_block = plant(jax.random.randint(key_of[3], (BRICKS_Y, BRICKS_X, ANG), 0, NBLK), jax.random.fold_in(key_of[3], 1), 0, NBLK - 1).astype(jnp.int32)
    angle_row = jax.random.permutation(key_of[4], ANG).astype(jnp.int32)
    return dict(start=start, measured=measured, tiles=tiles, tile_block=tile_block, angle_row=angle_row)


blur_sigma = 2.5
step_size = 0.5
shrink_weight = 0.2
rho_start = 1.0
eps_norm = 1e-6


def blur_weights():
    offsets = jnp.arange(-RADIUS, RADIUS + 1).astype(jnp.float32)
    raw = jnp.exp(-offsets * offsets / (2.0 * blur_sigma * blur_sigma))
    return raw / jnp.sum(raw)


def blur_valid(padded, weights, axis, length):
    total = weights[0] * lax.slice_in_dim(padded, 0, length, axis=axis)
    for offset in range(1, 2 * RADIUS + 1):
        total = total + weights[offset] * lax.slice_in_dim(padded, offset, offset + length, axis=axis)
    return total


def blur_volume(field, weights):
    for axis in range(3):
        widths = [(0, 0), (0, 0), (0, 0)]
        widths[axis] = (RADIUS, RADIUS)
        field = blur_valid(jnp.pad(field, widths), weights, axis, field.shape[axis])
    return field


def select_blocks(spread, own_blocks):
    chosen = spread[:, :, 0, :]
    for block in range(1, NBLK):
        chosen = jnp.where((own_blocks == block)[None, :, None], spread[:, :, block, :], chosen)
    return chosen


def project(volume, tiles, tile_block):
    sino = jnp.zeros((NZ, ANG, NBLK, DW), jnp.float32)
    blocks = jnp.arange(NBLK, dtype=jnp.int32)
    for brow in range(N_GY):
        for bcol in range(N_GX):
            brick = volume[:, brow * CY:(brow + 1) * CY, bcol * CX:(bcol + 1) * CX].reshape(NZ, V)
            tile = tiles[brow * V:(brow + 1) * V, :, bcol * DW:(bcol + 1) * DW].reshape(V, ANG * DW)
            contrib = jnp.dot(brick, tile, preferred_element_type=jnp.float32).reshape(NZ, ANG, DW)
            onehot = (tile_block[brow, bcol][:, None] == blocks[None, :]).astype(jnp.float32)
            sino = sino + contrib[:, :, None, :] * onehot[None, :, :, None]
    return sino.reshape(NZ, ANG, NBLK * DW)


def backproject(misfit, tiles, tile_block):
    spread = misfit.reshape(NZ, ANG, NBLK, DW)
    slabs = []
    for brow in range(N_GY):
        pieces = []
        for bcol in range(N_GX):
            chosen = select_blocks(spread, tile_block[brow, bcol]).reshape(NZ, ANG * DW)
            tile = tiles[brow * V:(brow + 1) * V, :, bcol * DW:(bcol + 1) * DW].reshape(V, ANG * DW)
            back = lax.dot_general(chosen, tile, (((1,), (1,)), ((), ())), preferred_element_type=jnp.float32)
            pieces.append(back.reshape(NZ, CY, CX))
        slabs.append(jnp.concatenate(pieces, axis=2))
    return jnp.concatenate(slabs, axis=1)


def adjoint_one(values, axis):
    length = values.shape[axis]
    zero_slab = jnp.zeros_like(lax.slice_in_dim(values, 0, 1, axis=axis))
    before = jnp.concatenate([zero_slab, lax.slice_in_dim(values, 0, length - 1, axis=axis)], axis=axis)
    current = jnp.concatenate([lax.slice_in_dim(values, 0, length - 1, axis=axis), zero_slab], axis=axis)
    return before - current


def forward_terms(field):
    diffs = []
    smoothing = None
    for axis in range(3):
        zero_slab = jnp.zeros_like(lax.slice_in_dim(field, 0, 1, axis=axis))
        diff = jnp.concatenate([jnp.diff(field, axis=axis), zero_slab], axis=axis)
        term = adjoint_one(diff, axis)
        smoothing = term if smoothing is None else smoothing + term
        diffs.append(diff)
    return jnp.stack(diffs), smoothing


def adjoint_terms(stack):
    results = []
    for group in range(stack.shape[0] // 3):
        total = None
        for axis in range(3):
            term = adjoint_one(stack[group * 3 + axis], axis)
            total = term if total is None else total + term
        results.append(total)
    return results


def reference(start, measured, tiles, tile_block, angle_row):
    weights = blur_weights()
    observed = jnp.take(measured, angle_row, axis=1)
    cells = float(NZ * NY * NX)
    field = start
    jumps, smoothing = forward_terms(field)
    penalty = jnp.float32(rho_start)
    cutoff = shrink_weight / penalty
    shrunk = jumps - jnp.clip(jumps, -cutoff, cutoff)
    dual = jnp.zeros_like(jumps)
    back_shrunk = adjoint_terms(shrunk)[0]
    back_dual = jnp.zeros_like(field)
    for sweep in range(ITERS):
        blurred = blur_volume(field, weights).astype(jnp.bfloat16)
        sino = project(blurred, tiles, tile_block)
        misfit = (sino - observed).astype(jnp.bfloat16)
        data_grad = blur_volume(backproject(misfit, tiles, tile_block), weights)
        field = field - step_size * (data_grad + penalty * (smoothing + back_dual - back_shrunk))
        jumps, smoothing = forward_terms(field)
        total = jumps + dual
        shrunk_new = total - jnp.clip(total, -cutoff, cutoff)
        dual = total - shrunk_new
        if sweep + 1 < ITERS:
            back_dual, back_new = adjoint_terms(jnp.concatenate([dual, shrunk_new]))
        else:
            back_new = adjoint_terms(shrunk_new)[0]
        primal_sum = jnp.sum(jnp.square(jumps - shrunk_new))
        dual_sum = jnp.sum(jnp.square(back_new - back_shrunk))
        primal_res = primal_sum / (3.0 * cells)
        dual_res = penalty * penalty * dual_sum / cells
        factor = ((primal_res + eps_norm) / (dual_res + eps_norm)) ** 0.25
        penalty = penalty * factor
        cutoff = shrink_weight / penalty
        dual = dual / factor
        back_dual = back_dual / factor
        shrunk = shrunk_new
        back_shrunk = back_new
    return (field, dual)
```

```python
import math

import jax
import jax.numpy as jnp
from jax import lax
from jax.experimental import pallas as pl
from jax.experimental.pallas import tpu as pltpu
from jax.sharding import PartitionSpec as P

CZ, CY, CX = 32, 16, 128
ROWS = CZ * CY
ANG, DW, NBLK = 8, 256, 4
V = CY * CX
R = 8
GZ, GY, GX = 4, 4, 8
BRICKS = GY * GX
CELLS = float(CZ * CY * CX * GZ * BRICKS)
MESH = pl.DeviceIdType.MESH
F32, BF16 = jnp.float32, jnp.bfloat16
STEP = 0.5
SHRINK = 0.2
EPS = 1e-6
CHUNK = 128
NCHUNK = V // CHUNK

RAW = [math.exp(-k * k / 12.5) for k in range(-R, R + 1)]
TAPS = [r / sum(RAW) for r in RAW]


def dot(a, b, dims):
    return lax.dot_general(a, b, (dims, ((), ())), preferred_element_type=F32)


def split(v):
    hi = v.astype(BF16)
    lo = (v - hi.astype(F32)).astype(BF16)
    return hi, lo


def kernel(
    start_ref, meas_ref, tiles_ref, tb_ref, row_ref,
    x_out, dual_out,
    raw, mat, tmp, vol, grad, xa, zbuf, ybuf, tbv, obs, mis,
    zs, zr, ys, yr, xs, xr,
    fzs, fzr, fys, fyr, fxs, fxr,
    stage, sl, snd1, rcv1, snd2, rcv2, rtmp,
    hterm, back, dl, dlm, xlr,
    red0, redz, red1, redx,
    bx, wx, acc,
    load_sem, tile_sem, hs_send, hs_recv, f_send, f_recv,
    a_send, a_recv, rz_send, rz_recv, rx_send, rx_recv, out_sem,
):
    gz, gy, gx = lax.axis_index("gz"), lax.axis_index("gy"), lax.axis_index("gx")
    me = gy * GX + gx

    ld = [
        pltpu.make_async_copy(start_ref, vol, load_sem.at[0]),
        pltpu.make_async_copy(meas_ref, obs, load_sem.at[1]),
    ]
    for c in ld:
        c.start()

    def tile_copy(c):
        rows = pl.ds(pl.multiple_of(c * CHUNK, CHUNK), CHUNK)
        return pltpu.make_async_copy(tiles_ref.at[rows], raw.at[rows], tile_sem.at[c])

    @pl.loop(0, NCHUNK)
    def _(c):
        tile_copy(c).start()

    barrier = pltpu.get_barrier_semaphore()

    def member(t):
        d = lax.rem(me + t, BRICKS)
        return d, (gz, d // GX, lax.rem(d, GX))

    @pl.loop(1, BRICKS)
    def _(t):
        pl.semaphore_signal(barrier, inc=1, device_id=member(t)[1], device_id_type=MESH)

    @pl.loop(1, GZ)
    def _(t):
        pl.semaphore_signal(
            barrier, inc=1, device_id=(lax.rem(gz + t, GZ), gy, gx), device_id_type=MESH
        )

    sides = {
        "z": (gz > 0, gz < GZ - 1, (gz - 1, gy, gx), (gz + 1, gy, gx)),
        "y": (gy > 0, gy < GY - 1, (gz, gy - 1, gx), (gz, gy + 1, gx)),
        "x": (gx > 0, gx < GX - 1, (gz, gy, gx - 1), (gz, gy, gx + 1)),
    }

    class Swap:
        def __init__(self, axis, src, dst, send, recv):
            self.has_lo, self.has_hi, low, high = sides[axis]
            self.lo = pltpu.make_async_remote_copy(
                src.at[0], dst.at[1], send.at[0], recv.at[1], device_id=low, device_id_type=MESH
            )
            self.hi = pltpu.make_async_remote_copy(
                src.at[1], dst.at[0], send.at[1], recv.at[0], device_id=high, device_id_type=MESH
            )
            self.dst = dst

        def clear(self):
            @pl.when(jnp.logical_not(self.has_lo))
            def _():
                self.dst[0] = jnp.zeros(self.dst.shape[1:], self.dst.dtype)

            @pl.when(jnp.logical_not(self.has_hi))
            def _():
                self.dst[1] = jnp.zeros(self.dst.shape[1:], self.dst.dtype)

        def start(self):
            @pl.when(self.has_lo)
            def _():
                self.lo.start()

            @pl.when(self.has_hi)
            def _():
                self.hi.start()

        def wait_recv(self):
            @pl.when(self.has_lo)
            def _():
                self.hi.wait_recv()

            @pl.when(self.has_hi)
            def _():
                self.lo.wait_recv()

        def wait_send(self):
            @pl.when(self.has_lo)
            def _():
                self.lo.wait_send()

            @pl.when(self.has_hi)
            def _():
                self.hi.wait_send()

    zsw = [Swap("z", zs.at[n], zr.at[n], hs_send.at[n, 0], hs_recv.at[n, 0]) for n in range(4)]
    ysw = [Swap("y", ys.at[n], yr.at[n], hs_send.at[n, 1], hs_recv.at[n, 1]) for n in range(4)]
    xsw = [Swap("x", xs.at[n], xr.at[n], hs_send.at[n, 2], hs_recv.at[n, 2]) for n in range(4)]
    fsw = [
        [
            Swap("z", fzs.at[n], fzr.at[n], f_send.at[n, 0], f_recv.at[n, 0]),
            Swap("y", fys.at[n], fyr.at[n], f_send.at[n, 1], f_recv.at[n, 1]),
            Swap("x", fxs.at[n], fxr.at[n], f_send.at[n, 2], f_recv.at[n, 2]),
        ]
        for n in range(3)
    ]
    every = zsw + ysw + xsw + [s for f in fsw for s in f]
    for s in every:
        s.clear()

    def gauss(d):
        df = d.astype(F32)
        w = jnp.exp(df * df * (-1.0 / 12.5)) * (1.0 / sum(RAW))
        return jnp.where(jnp.abs(d) <= R, w, 0.0)

    i0 = lax.broadcasted_iota(jnp.int32, (CX, CX), 0)
    i1 = lax.broadcasted_iota(jnp.int32, (CX, CX), 1)
    bhi, blo = split(gauss(i0 - i1))
    bx[0:CX] = bhi
    bx[CX : 2 * CX] = bhi
    bx[2 * CX : 3 * CX] = blo
    k0 = lax.broadcasted_iota(jnp.int32, (32, CX), 0)
    k1 = lax.broadcasted_iota(jnp.int32, (32, CX), 1)
    pos = jnp.where(k0 < 16, lax.rem(k0, 8) - 8, CX + lax.rem(k0, 8))
    whi, wlo = split(gauss(pos - k1))
    wx[0:32] = whi
    wx[32:64] = wlo
    rim = jnp.where(
        ((k1 == 0) & ((k0 == 7) | (k0 == 15))) | ((k1 == CX - 1) & ((k0 == 16) | (k0 == 24))),
        1.0,
        0.0,
    )
    wx[64:96] = rim.astype(BF16)
    s0 = lax.broadcasted_iota(jnp.int32, (32, 2 * CX), 0)
    s1 = lax.broadcasted_iota(jnp.int32, (32, 2 * CX), 1)
    want = jnp.where(s0 < 16, lax.rem(s0, 8), CX - 8 + lax.rem(s0, 8)) + jnp.where(
        lax.rem(s0, 16) < 8, 0, CX
    )
    pick = jnp.where(s1 == want, 1.0, 0.0).astype(BF16)

    e0 = lax.broadcasted_iota(jnp.int32, (GX, GX * CX), 0)
    e1 = lax.broadcasted_iota(jnp.int32, (GX, GX * CX), 1) // CX
    spread = jnp.where(e0 == e1, 1.0, 0.0).astype(BF16)
    for b in range(GY):
        rows = dot(tb_ref[b].astype(F32).astype(BF16), spread, ((0,), (0,)))
        for c in range(GX):
            tbv[b * GX + c] = rows[:, c * CX : (c + 1) * CX]

    for c in ld:
        c.wait()
    for a in range(ANG):
        acc[pl.ds(a, 1), :] = obs[0, pl.ds(row_ref[a], 1), :]

    pl.semaphore_wait(barrier, BRICKS - 1 + GZ - 1)

    def send_faces(n, src):
        fzs[n, 0] = src[0]
        fzs[n, 1] = src[CZ - 1]
        v = src[...]
        fys[n, 0] = v[:, 0, :]
        fys[n, 1] = v[:, CY - 1, :]
        hi, lo = split(v.reshape(ROWS, CX))
        f = dot(pick, jnp.concatenate([hi, lo], axis=1), ((1,), (1,))).astype(BF16)
        fxs[n, 0] = f[0:16]
        fxs[n, 1] = f[16:32]
        for s in fsw[n]:
            s.start()

    def send_z(n, src):
        zs[n, 0] = src[0:R].reshape(R * CY, CX).astype(BF16)
        zs[n, 1] = src[CZ - R : CZ].reshape(R * CY, CX).astype(BF16)
        zsw[n].start()

    def blur(n, src, between):
        zbuf[R : R + CZ] = src[...]
        between()
        zsw[n].wait_recv()
        zbuf[0:R] = zr[n, 0].astype(F32).reshape(R, CY, CX)
        zbuf[R + CZ :] = zr[n, 1].astype(F32).reshape(R, CY, CX)

        @pl.loop(0, CZ)
        def _(z):
            t = TAPS[R] * zbuf[z + R]
            for k in range(R):
                t += TAPS[k] * (zbuf[z + k] + zbuf[z + 2 * R - k])
            ybuf[z, R : R + CY, :] = t

        ys[n, 0] = ybuf[:, R : 2 * R, :].reshape(CZ * R, CX).astype(BF16)
        ys[n, 1] = ybuf[:, CY : R + CY, :].reshape(CZ * R, CX).astype(BF16)
        ysw[n].start()
        ysw[n].wait_recv()
        ybuf[:, 0:R, :] = yr[n, 0].astype(F32).reshape(CZ, R, CX)
        ybuf[:, R + CY :, :] = yr[n, 1].astype(F32).reshape(CZ, R, CX)

        @pl.loop(0, CZ)
        def _(z):
            t = TAPS[R] * ybuf[z, R : R + CY, :]
            for k in range(R):
                t += TAPS[k] * (ybuf[z, k : k + CY, :] + ybuf[z, 2 * R - k : 2 * R - k + CY, :])
            grad[pl.ds(pl.multiple_of(z * CY, CY), CY), :] = t

        hi, lo = split(grad[...])
        both = jnp.concatenate([hi, lo], axis=1)
        f = dot(pick, both, ((1,), (1,))).astype(BF16)
        xs[n, 0] = f[0:16]
        xs[n, 1] = f[16:32]
        xsw[n].start()
        own = dot(both, bx[0 : 2 * CX], ((1,), (0,))) + dot(hi, bx[2 * CX :], ((1,), (0,)))
        xsw[n].wait_recv()
        halo = xr[n].reshape(32, ROWS)
        return own + dot(halo, wx[0:32], ((0,), (0,))) + dot(halo, wx[32:64], ((0,), (0,)))

    lane = lax.broadcasted_iota(jnp.int32, (CY, CX), 1)
    sub = lax.broadcasted_iota(jnp.int32, (CY, CX), 0)
    first = {
        "z": (gz == 0, gz == GZ - 1),
        "y": (gy == 0, gy == GY - 1),
        "x": (gx == 0, gx == GX - 1),
    }

    def wait_faces(n):
        for s in fsw[n]:
            s.wait_recv()
        xlr[...] = dot(fxr[n].reshape(32, ROWS), wx[64:96], ((0,), (0,))).reshape(CZ, CY, CX)
        xa[0] = fzr[n, 0]
        xa[CZ + 1] = fzr[n, 1]

    def diffs(n, z):
        v = xa[z + 1]
        out = []
        up, low = xa[z + 2], xa[z]
        out.append((
            jnp.where((z == CZ - 1) & first["z"][1], 0.0, up - v),
            jnp.where((z == 0) & first["z"][0], 0.0, v - low),
        ))
        rim = fyr[n, 1, pl.ds(z, 1), :]
        up = jnp.where(sub == CY - 1, rim, pltpu.roll(v, CY - 1, 0))
        rim = fyr[n, 0, pl.ds(z, 1), :]
        low = jnp.where(sub == 0, rim, pltpu.roll(v, 1, 0))
        out.append((
            jnp.where((sub == CY - 1) & first["y"][1], 0.0, up - v),
            jnp.where((sub == 0) & first["y"][0], 0.0, v - low),
        ))
        edge = xlr[z]
        up = jnp.where(lane == CX - 1, edge, pltpu.roll(v, CX - 1, 1))
        low = jnp.where(lane == 0, edge, pltpu.roll(v, 1, 1))
        out.append((
            jnp.where((lane == CX - 1) & first["x"][1], 0.0, up - v),
            jnp.where((lane == 0) & first["x"][0], 0.0, v - low),
        ))
        return out

    def fold(p):
        return p[0:8] + p[8:16]

    def send_sums(n, primal, dualres):
        p = jnp.sum(primal, axis=0, keepdims=True)
        d = jnp.sum(dualres, axis=0, keepdims=True)
        r8 = lax.broadcasted_iota(jnp.int32, (8, CX), 0)
        red0[n] = jnp.where(r8 < 4, p, d)

        for t in range(1, GZ):
            redz_copy(n, t).start()

    def redz_copy(n, t):
        return pltpu.make_async_remote_copy(
            red0.at[n], redz.at[n, t], rz_send.at[n, t], rz_recv.at[n, t],
            device_id=(lax.rem(gz + t, GZ), gy, gx), device_id_type=MESH,
        )

    def redx_copy(n, t):
        return pltpu.make_async_remote_copy(
            red1.at[n], redx.at[n, t], rx_send.at[n], rx_recv.at[n],
            device_id=member(t)[1], device_id_type=MESH,
        )

    def forward_sums(n):
        total = red0[n]
        for t in range(1, GZ):
            redz_copy(n, t).wait_recv()
            total += redz[n, t]
        red1[n] = total

        @pl.loop(1, BRICKS)
        def _(t):
            redx_copy(n, t).start()

    def finish_sums(n):
        total = red1[n]
        got = redx.at[n, pl.ds(1, BRICKS - 1)]
        pltpu.make_async_copy(got, got, rx_recv.at[n]).wait()
        total += jnp.sum(redx[n, 1:BRICKS], axis=0)
        p = jnp.sum(total[0:1], axis=1, keepdims=True)
        d = jnp.sum(total[4:5], axis=1, keepdims=True)
        return jnp.broadcast_to(p, (8, CX)), jnp.broadcast_to(d, (8, CX))

    send_z(0, vol)
    send_faces(0, vol)

    def relayout():
        @pl.loop(0, NCHUNK)
        def _(c):
            tile_copy(c).wait()
            rows = pl.ds(pl.multiple_of(c * CHUNK, CHUNK), CHUNK)
            block = raw[rows].astype(F32).reshape(CHUNK * ANG, DW)
            for h in range(2):
                tmp[h] = block[:, h * 128 : (h + 1) * 128]
            for a in range(ANG):
                for h in range(2):
                    part = tmp[h, pl.ds(a, CHUNK, stride=ANG), :]
                    mat[rows, a * DW + h * 128 : a * DW + (h + 1) * 128] = part.astype(BF16)

    def first_terms():
        wait_faces(0)
        xa[1 : CZ + 1] = vol[...]
        cut = SHRINK

        @pl.loop(0, CZ)
        def _(z):
            smooth = jnp.zeros((CY, CX), F32)
            shrunk = jnp.zeros((CY, CX), F32)
            for j, jm in diffs(0, z):
                s = j - jnp.clip(j, -cut, cut)
                sm = jm - jnp.clip(jm, -cut, cut)
                smooth += jm - j
                shrunk += sm - s
            hterm[z] = smooth - shrunk
            back[z] = shrunk

    def copy1(n, d, dev):
        return pltpu.make_async_remote_copy(
            snd1.at[n, d], rcv1.at[n, me], a_send.at[n, 0], a_recv.at[n, 0],
            device_id=dev, device_id_type=MESH,
        )

    def copy2(n, d, dev):
        return pltpu.make_async_remote_copy(
            snd2.at[n, d], rcv2.at[n, me], a_send.at[n, 1], a_recv.at[n, 1],
            device_id=dev, device_id_type=MESH,
        )

    def arrivals(ref, sem):
        got = ref.at[pl.ds(0, BRICKS - 1)]
        pltpu.make_async_copy(got, got, sem).wait()

    def project(n, blurred, between):
        grad[...] = blurred
        for y in range(CY):
            sl[:, y * CX : (y + 1) * CX] = grad[pl.ds(y, CZ, stride=CY), :].astype(BF16)
        for a in range(ANG):
            c = dot(sl[...], mat[:, a * DW : (a + 1) * DW], ((1,), (0,)))
            for h in range(2):
                stage[h, pl.ds(a, CZ, stride=ANG), :] = c[:, h * 128 : (h + 1) * 128]

        def block_of(d):
            rows = pl.ds(pl.multiple_of(d * ANG, ANG), ANG)
            return jnp.concatenate([stage[0, rows, :], stage[1, rows, :]], axis=1).astype(BF16)

        @pl.loop(1, BRICKS)
        def _(t):
            d, dev = member(t)
            snd1[n, d] = block_of(d)
            copy1(n, d, dev).start()

        rcv1[n, me] = block_of(me)
        between()
        arrivals(rcv1.at[n], a_recv.at[n, 0])

        def add(s, sums):
            x = rcv1[n, s].astype(F32)
            t = tbv[s]
            t = jnp.concatenate([t, t], axis=1)
            return tuple(sums[q] + jnp.where(t == float(q), x, 0.0) for q in range(NBLK))

        sums = lax.fori_loop(
            0, BRICKS, add, tuple(jnp.zeros((ANG, DW), F32) for _ in range(NBLK))
        )
        for q in range(NBLK):
            cols = slice(q * DW, (q + 1) * DW)
            mis[:, cols] = (sums[q] - acc[:, cols]).astype(BF16).astype(F32)

        def chosen(d):
            t = tbv[d]
            t = jnp.concatenate([t, t], axis=1)
            c = mis[:, 0:DW]
            for q in range(1, NBLK):
                c = jnp.where(t == float(q), mis[:, q * DW : (q + 1) * DW], c)
            return c.astype(BF16)

        @pl.loop(1, BRICKS)
        def _(t):
            d, dev = member(t)
            snd2[n, d] = chosen(d)
            copy2(n, d, dev).start()

        rcv2[n, me] = chosen(me)

    def backproject(n):
        arrivals(rcv2.at[n], a_recv.at[n, 1])
        r = rcv2[n].astype(F32).reshape(CZ * ANG, DW)
        for h in range(2):
            stage[h] = r[:, h * 128 : (h + 1) * 128]
        for a in range(ANG):
            for h in range(2):
                sl[:, a * DW + h * 128 : a * DW + (h + 1) * 128] = stage[
                    h, pl.ds(a, CZ, stride=ANG), :
                ].astype(BF16)
        for c in range(ANG):
            b = dot(sl[...], mat[c * DW : (c + 1) * DW, :], ((1,), (1,)))
            for h in range(2):
                grad[pl.ds(2 * c + h, CZ, stride=CY), :] = b[:, h * 128 : (h + 1) * 128]

    def before():
        first_terms()
        relayout()

    project(0, blur(0, vol, before), lambda: None)
    backproject(0)
    vol[...] = grad[...].reshape(CZ, CY, CX)
    send_z(1, vol)
    g = blur(1, vol, lambda: None).reshape(CZ, CY, CX)
    xa[1 : CZ + 1] = xa[1 : CZ + 1] - STEP * (g + hterm[...])
    vol[...] = xa[1 : CZ + 1]
    send_z(2, vol)
    send_faces(1, vol)

    def second_terms():
        wait_faces(1)
        cut = SHRINK

        def one(z, sums):
            primal, dres = sums
            smooth = jnp.zeros((CY, CX), F32)
            shrunk = jnp.zeros((CY, CX), F32)
            bdual = jnp.zeros((CY, CX), F32)
            for axis, (j, jm) in enumerate(diffs(1, z)):
                d = jnp.clip(j, -cut, cut)
                dm = jnp.clip(jm, -cut, cut)
                s = j - d
                sm = jm - dm
                d = j - s
                dm = jm - sm
                smooth += jm - j
                shrunk += sm - s
                bdual += dm - d
                dl[axis, z] = d
                dlm[axis, z] = dm
                primal += fold(jnp.square(j - s))
            dres += fold(jnp.square(shrunk - back[z]))
            hterm[z] = smooth - shrunk
            back[z] = shrunk
            zbuf[z] = bdual
            return primal, dres

        zero = jnp.zeros((8, CX), F32)
        primal, dres = lax.fori_loop(0, CZ, one, (zero, zero))
        send_sums(0, primal, dres)

    def factor_of(n, penalty):
        p, d = finish_sums(n)
        p = p * (1.0 / (3.0 * CELLS))
        d = penalty * penalty * d * (1.0 / CELLS)
        return jnp.sqrt(jnp.sqrt((p + EPS) / (d + EPS)))

    def keep_terms():
        second_terms()

    blurred = blur(2, vol, lambda: None)
    keep_terms()
    bd = zbuf[0:CZ]
    dual_keep = bd
    xlr[...] = dual_keep

    def pass_sums():
        forward_sums(0)

    project(1, blurred, pass_sums)
    factor1 = factor_of(0, jnp.ones((8, CX), F32))
    penalty = factor1
    inv1 = 1.0 / factor1
    pen3 = penalty[0:1].reshape(1, 1, CX)
    inv3 = inv1[0:1].reshape(1, 1, CX)
    hterm[...] = STEP * pen3 * (hterm[...] + xlr[...] * inv3)
    backproject(1)
    vol[...] = grad[...].reshape(CZ, CY, CX)
    send_z(3, vol)
    g = blur(3, vol, lambda: None).reshape(CZ, CY, CX)
    xa[1 : CZ + 1] = xa[1 : CZ + 1] - (STEP * g + hterm[...])
    vol[...] = xa[1 : CZ + 1]
    send_faces(2, vol)
    x_copy = pltpu.make_async_copy(vol, x_out, out_sem.at[0])
    x_copy.start()

    wait_faces(2)
    cut = (SHRINK / penalty)[0:1]
    inv = inv1[0:1]

    def last(z, sums):
        primal, dres = sums
        shrunk = jnp.zeros((CY, CX), F32)
        for axis, (j, jm) in enumerate(diffs(2, z)):
            t = j + dl[axis, z] * inv
            tm = jm + dlm[axis, z] * inv
            s = t - jnp.clip(t, -cut, cut)
            sm = tm - jnp.clip(tm, -cut, cut)
            shrunk += sm - s
            dl[axis, z] = t - s
            primal += fold(jnp.square(j - s))
        dres += fold(jnp.square(shrunk - back[z]))
        return primal, dres

    zero = jnp.zeros((8, CX), F32)
    primal, dres = lax.fori_loop(0, CZ, last, (zero, zero))
    send_sums(1, primal, dres)
    forward_sums(1)
    factor2 = factor_of(1, penalty)
    scale = (1.0 / factor2)[0:1].reshape(1, 1, 1, CX)
    dl[...] = dl[...] * scale
    d_copy = pltpu.make_async_copy(dl, dual_out, out_sem.at[1])
    d_copy.start()

    for s in every:
        s.wait_send()
    for n in range(2):
        for i, ref in enumerate((snd1, snd2)):
            arrivals(ref.at[n], a_send.at[n, i])
        for t in range(1, GZ):
            redz_copy(n, t).wait_send()
        got = redx.at[n, pl.ds(1, BRICKS - 1)]
        pltpu.make_async_copy(got, got, rx_send.at[n]).wait()
    x_copy.wait()
    d_copy.wait()


def body(start, measured, tiles, tile_block, angle_row):
    vm = pltpu.VMEM
    dma = pltpu.SemaphoreType.DMA
    return pl.pallas_call(
        kernel,
        out_shape=(
            jax.ShapeDtypeStruct((CZ, CY, CX), F32),
            jax.ShapeDtypeStruct((3, CZ, CY, CX), F32),
        ),
        in_specs=[
            pl.BlockSpec(memory_space=pl.ANY),
            pl.BlockSpec(memory_space=pl.ANY),
            pl.BlockSpec(memory_space=pl.ANY),
            pl.BlockSpec(memory_space=pltpu.VMEM),
            pl.BlockSpec(memory_space=pltpu.SMEM),
        ],
        out_specs=(pl.BlockSpec(memory_space=pl.ANY), pl.BlockSpec(memory_space=pl.ANY)),
        scratch_shapes=[
            vm((V, ANG, DW), BF16),
            vm((V, ANG * DW), BF16),
            vm((2, CHUNK * ANG, 128), F32),
            vm((CZ, CY, CX), F32),
            vm((ROWS, CX), F32),
            vm((CZ + 2, CY, CX), F32),
            vm((CZ + 2 * R, CY, CX), F32),
            vm((CZ, CY + 2 * R, CX), F32),
            vm((BRICKS, ANG, CX), F32),
            vm((1, ANG, NBLK * DW), F32),
            vm((ANG, NBLK * DW), F32),
            vm((4, 2, R * CY, CX), BF16),
            vm((4, 2, R * CY, CX), BF16),
            vm((4, 2, CZ * R, CX), BF16),
            vm((4, 2, CZ * R, CX), BF16),
            vm((4, 2, 16, ROWS), BF16),
            vm((4, 2, 16, ROWS), BF16),
            vm((3, 2, CY, CX), F32),
            vm((3, 2, CY, CX), F32),
            vm((3, 2, CZ, CX), F32),
            vm((3, 2, CZ, CX), F32),
            vm((3, 2, 16, ROWS), BF16),
            vm((3, 2, 16, ROWS), BF16),
            vm((2, CZ * ANG, 128), F32),
            vm((CZ, V), BF16),
            vm((2, BRICKS, ANG, DW), BF16),
            vm((2, BRICKS, ANG, DW), BF16),
            vm((2, BRICKS, ANG, DW), BF16),
            vm((2, BRICKS, ANG, DW), BF16),
            vm((8, CX), F32),
            vm((CZ, CY, CX), F32),
            vm((CZ, CY, CX), F32),
            vm((3, CZ, CY, CX), F32),
            vm((3, CZ, CY, CX), F32),
            vm((CZ, CY, CX), F32),
            vm((2, 8, CX), F32),
            vm((2, GZ, 8, CX), F32),
            vm((2, 8, CX), F32),
            vm((2, BRICKS, 8, CX), F32),
            vm((3 * CX, CX), BF16),
            vm((96, CX), BF16),
            vm((ANG, NBLK * DW), F32),
            dma((2,)),
            dma((NCHUNK,)),
            dma((4, 3, 2)),
            dma((4, 3, 2)),
            dma((3, 3, 2)),
            dma((3, 3, 2)),
            dma((2, 2)),
            dma((2, 2)),
            dma((2, GZ)),
            dma((2, GZ)),
            dma((2,)),
            dma((2,)),
            dma((2,)),
        ],
        compiler_params=pltpu.CompilerParams(
            collective_id=0, has_side_effects=True, vmem_limit_bytes=60 * 1024 * 1024
        ),
    )(start, measured, tiles, tile_block, angle_row)


def solution(mesh):
    return jax.shard_map(
        body,
        mesh=mesh,
        in_specs=(
            P("gz", "gy", "gx"),
            P(("gz", "gy", "gx"), None, None),
            P("gy", None, "gx"),
            P(),
            P(),
        ),
        out_specs=(P("gz", "gy", "gx"), P(None, "gz", "gy", "gx")),
        check_vma=False,
    )
```

```python
import math

import jax
import jax.numpy as jnp
from jax import lax
from jax.experimental import pallas as pl
from jax.experimental.pallas import tpu as pltpu
from jax.sharding import PartitionSpec as P

CZ, CY, CX = 32, 16, 128
ROWS = CZ * CY
ANG, DW, NBLK = 8, 256, 4
V = CY * CX
R = 8
GZ, GY, GX = 4, 4, 8
BRICKS = GY * GX
CELLS = float(CZ * CY * CX * GZ * BRICKS)
MESH = pl.DeviceIdType.MESH
F32, BF16 = jnp.float32, jnp.bfloat16
STEP = 0.5
SHRINK = 0.2
EPS = 1e-6
CHUNK = 128
NCHUNK = V // CHUNK

RAW = [math.exp(-k * k / 12.5) for k in range(-R, R + 1)]
TAPS = [r / sum(RAW) for r in RAW]


def dot(a, b, dims):
    return lax.dot_general(a, b, (dims, ((), ())), preferred_element_type=F32)


def split(v):
    hi = v.astype(BF16)
    lo = (v - hi.astype(F32)).astype(BF16)
    return hi, lo


def kernel(
    start_ref, meas_ref, tiles_ref, tb_ref, row_ref,
    x_out, dual_out,
    raw, mat, tmp, vol, grad, xa, zbuf, ybuf, tbv, obs, mis,
    zs, zr, ys, yr, xs, xr,
    fzs, fzr, fys, fyr, fxs, fxr,
    stage, sl, snd1, rcv1, snd2, rcv2, rmis,
    hterm, back, dl, dlm, xlr,
    red0, redz, red1, redx,
    bx, wx, acc,
    load_sem, tile_sem, hs_send, hs_recv, f_send, f_recv,
    a_send, a_recv, rz_send, rz_recv, rx_send, rx_recv, out_sem,
):
    gz, gy, gx = lax.axis_index("gz"), lax.axis_index("gy"), lax.axis_index("gx")
    me = gy * GX + gx

    ld = [
        pltpu.make_async_copy(start_ref, vol, load_sem.at[0]),
        pltpu.make_async_copy(meas_ref, obs, load_sem.at[1]),
    ]
    for c in ld:
        c.start()

    def tile_copy(c):
        rows = pl.ds(pl.multiple_of(c * CHUNK, CHUNK), CHUNK)
        return pltpu.make_async_copy(tiles_ref.at[rows], raw.at[rows], tile_sem.at[c])

    @pl.loop(0, NCHUNK)
    def _(c):
        tile_copy(c).start()

    barrier = pltpu.get_barrier_semaphore()

    def member(t):
        d = lax.rem(me + t, BRICKS)
        return d, (gz, d // GX, lax.rem(d, GX))

    @pl.loop(1, BRICKS)
    def _(t):
        pl.semaphore_signal(barrier, inc=1, device_id=member(t)[1], device_id_type=MESH)

    @pl.loop(1, GZ)
    def _(t):
        pl.semaphore_signal(
            barrier, inc=1, device_id=(lax.rem(gz + t, GZ), gy, gx), device_id_type=MESH
        )

    sides = {
        "z": (gz > 0, gz < GZ - 1, (gz - 1, gy, gx), (gz + 1, gy, gx)),
        "y": (gy > 0, gy < GY - 1, (gz, gy - 1, gx), (gz, gy + 1, gx)),
        "x": (gx > 0, gx < GX - 1, (gz, gy, gx - 1), (gz, gy, gx + 1)),
    }

    class Swap:
        def __init__(self, axis, src, dst, send, recv):
            self.has_lo, self.has_hi, low, high = sides[axis]
            self.lo = pltpu.make_async_remote_copy(
                src.at[0], dst.at[1], send.at[0], recv.at[1], device_id=low, device_id_type=MESH
            )
            self.hi = pltpu.make_async_remote_copy(
                src.at[1], dst.at[0], send.at[1], recv.at[0], device_id=high, device_id_type=MESH
            )
            self.dst = dst

        def clear(self):
            @pl.when(jnp.logical_not(self.has_lo))
            def _():
                self.dst[0] = jnp.zeros(self.dst.shape[1:], self.dst.dtype)

            @pl.when(jnp.logical_not(self.has_hi))
            def _():
                self.dst[1] = jnp.zeros(self.dst.shape[1:], self.dst.dtype)

        def start(self):
            @pl.when(self.has_lo)
            def _():
                self.lo.start()

            @pl.when(self.has_hi)
            def _():
                self.hi.start()

        def wait_recv(self):
            @pl.when(self.has_lo)
            def _():
                self.hi.wait_recv()

            @pl.when(self.has_hi)
            def _():
                self.lo.wait_recv()

        def wait_send(self):
            @pl.when(self.has_lo)
            def _():
                self.lo.wait_send()

            @pl.when(self.has_hi)
            def _():
                self.hi.wait_send()

    zsw = [Swap("z", zs.at[n], zr.at[n], hs_send.at[n, 0], hs_recv.at[n, 0]) for n in range(4)]
    ysw = [Swap("y", ys.at[n], yr.at[n], hs_send.at[n, 1], hs_recv.at[n, 1]) for n in range(4)]
    xsw = [Swap("x", xs.at[n], xr.at[n], hs_send.at[n, 2], hs_recv.at[n, 2]) for n in range(4)]
    fsw = [
        [
            Swap("z", fzs.at[n], fzr.at[n], f_send.at[n, 0], f_recv.at[n, 0]),
            Swap("y", fys.at[n], fyr.at[n], f_send.at[n, 1], f_recv.at[n, 1]),
            Swap("x", fxs.at[n], fxr.at[n], f_send.at[n, 2], f_recv.at[n, 2]),
        ]
        for n in range(3)
    ]
    every = zsw + ysw + xsw + [s for f in fsw for s in f]
    for s in every:
        s.clear()

    def gauss(d):
        df = d.astype(F32)
        w = jnp.exp(df * df * (-1.0 / 12.5)) * (1.0 / sum(RAW))
        return jnp.where(jnp.abs(d) <= R, w, 0.0)

    i0 = lax.broadcasted_iota(jnp.int32, (CX, CX), 0)
    i1 = lax.broadcasted_iota(jnp.int32, (CX, CX), 1)
    bhi, blo = split(gauss(i0 - i1))
    bx[0:CX] = bhi
    bx[CX : 2 * CX] = bhi
    bx[2 * CX : 3 * CX] = blo
    k0 = lax.broadcasted_iota(jnp.int32, (32, CX), 0)
    k1 = lax.broadcasted_iota(jnp.int32, (32, CX), 1)
    pos = jnp.where(k0 < 16, lax.rem(k0, 8) - 8, CX + lax.rem(k0, 8))
    whi, wlo = split(gauss(pos - k1))
    wx[0:32] = whi
    wx[32:64] = wlo
    rim = jnp.where(
        ((k1 == 0) & ((k0 == 7) | (k0 == 15))) | ((k1 == CX - 1) & ((k0 == 16) | (k0 == 24))),
        1.0,
        0.0,
    )
    wx[64:96] = rim.astype(BF16)
    s0 = lax.broadcasted_iota(jnp.int32, (32, 2 * CX), 0)
    s1 = lax.broadcasted_iota(jnp.int32, (32, 2 * CX), 1)
    want = jnp.where(s0 < 16, lax.rem(s0, 8), CX - 8 + lax.rem(s0, 8)) + jnp.where(
        lax.rem(s0, 16) < 8, 0, CX
    )
    pick = jnp.where(s1 == want, 1.0, 0.0).astype(BF16)

    e0 = lax.broadcasted_iota(jnp.int32, (GX, GX * CX), 0)
    e1 = lax.broadcasted_iota(jnp.int32, (GX, GX * CX), 1) // CX
    spread = jnp.where(e0 == e1, 1.0, 0.0).astype(BF16)
    for b in range(GY):
        rows = dot(tb_ref[b].astype(F32).astype(BF16), spread, ((0,), (0,)))
        for c in range(GX):
            tbv[b * GX + c] = rows[:, c * CX : (c + 1) * CX]

    def relayout(low, high):
        @pl.loop(low, high)
        def _(c):
            tile_copy(c).wait()
            rows = pl.ds(pl.multiple_of(c * CHUNK, CHUNK), CHUNK)
            block = raw[rows].astype(F32).reshape(CHUNK * ANG, DW)
            for h in range(2):
                tmp[h] = block[:, h * 128 : (h + 1) * 128]
            for a in range(ANG):
                for h in range(2):
                    part = tmp[h, pl.ds(a, CHUNK, stride=ANG), :]
                    mat[rows, a * DW + h * 128 : a * DW + (h + 1) * 128] = part.astype(BF16)

    for c in ld:
        c.wait()
    for a in range(ANG):
        acc[pl.ds(a, 1), :] = obs[0, pl.ds(row_ref[a], 1), :]

    relayout(0, 6)
    with jax.named_scope("wait_barrier"):
        pl.semaphore_wait(barrier, BRICKS - 1 + GZ - 1)

    def send_faces(n, src):
        fzs[n, 0] = src[0]
        fzs[n, 1] = src[CZ - 1]
        v = src[...]
        fys[n, 0] = v[:, 0, :]
        fys[n, 1] = v[:, CY - 1, :]
        hi, lo = split(v.reshape(ROWS, CX))
        f = dot(pick, jnp.concatenate([hi, lo], axis=1), ((1,), (1,))).astype(BF16)
        fxs[n, 0] = f[0:16]
        fxs[n, 1] = f[16:32]
        for s in fsw[n]:
            s.start()

    def nothing():
        pass

    def send_z(n, src):
        zs[n, 0] = src[0:R].reshape(R * CY, CX).astype(BF16)
        zs[n, 1] = src[CZ - R : CZ].reshape(R * CY, CX).astype(BF16)
        zsw[n].start()

    def blur(n, src, between=nothing, in_y=nothing, in_x=nothing):
        zbuf[R : R + CZ] = src[...]
        between()
        with jax.named_scope("wait_z"):
            zsw[n].wait_recv()
        zbuf[0:R] = zr[n, 0].astype(F32).reshape(R, CY, CX)
        zbuf[R + CZ :] = zr[n, 1].astype(F32).reshape(R, CY, CX)

        @pl.loop(0, CZ)
        def _(z):
            t = TAPS[R] * zbuf[z + R]
            for k in range(R):
                t += TAPS[k] * (zbuf[z + k] + zbuf[z + 2 * R - k])
            ybuf[z, R : R + CY, :] = t

        ys[n, 0] = ybuf[:, R : 2 * R, :].reshape(CZ * R, CX).astype(BF16)
        ys[n, 1] = ybuf[:, CY : R + CY, :].reshape(CZ * R, CX).astype(BF16)
        ysw[n].start()
        in_y()
        with jax.named_scope("wait_y"):
            ysw[n].wait_recv()
        ybuf[:, 0:R, :] = yr[n, 0].astype(F32).reshape(CZ, R, CX)
        ybuf[:, R + CY :, :] = yr[n, 1].astype(F32).reshape(CZ, R, CX)

        @pl.loop(0, CZ)
        def _(z):
            t = TAPS[R] * ybuf[z, R : R + CY, :]
            for k in range(R):
                t += TAPS[k] * (ybuf[z, k : k + CY, :] + ybuf[z, 2 * R - k : 2 * R - k + CY, :])
            grad[pl.ds(pl.multiple_of(z * CY, CY), CY), :] = t

        hi, lo = split(grad[...])
        both = jnp.concatenate([hi, lo], axis=1)
        f = dot(pick, both, ((1,), (1,))).astype(BF16)
        xs[n, 0] = f[0:16]
        xs[n, 1] = f[16:32]
        xsw[n].start()
        own = dot(both, bx[0 : 2 * CX], ((1,), (0,))) + dot(hi, bx[2 * CX :], ((1,), (0,)))
        in_x()
        with jax.named_scope("wait_x"):
            xsw[n].wait_recv()
        halo = xr[n].reshape(32, ROWS)
        return own + dot(halo, wx[0:32], ((0,), (0,))) + dot(halo, wx[32:64], ((0,), (0,)))

    lane = lax.broadcasted_iota(jnp.int32, (CY, CX), 1)
    sub = lax.broadcasted_iota(jnp.int32, (CY, CX), 0)
    first = {
        "z": (gz == 0, gz == GZ - 1),
        "y": (gy == 0, gy == GY - 1),
        "x": (gx == 0, gx == GX - 1),
    }

    def wait_faces(n):
        for s in fsw[n]:
            s.wait_recv()
        xlr[...] = dot(fxr[n].reshape(32, ROWS), wx[64:96], ((0,), (0,))).reshape(CZ, CY, CX)
        xa[0] = fzr[n, 0]
        xa[CZ + 1] = fzr[n, 1]

    def diffs(n, z):
        v = xa[z + 1]
        out = []
        up, low = xa[z + 2], xa[z]
        out.append((
            jnp.where((z == CZ - 1) & first["z"][1], 0.0, up - v),
            jnp.where((z == 0) & first["z"][0], 0.0, v - low),
        ))
        rim = fyr[n, 1, pl.ds(z, 1), :]
        up = jnp.where(sub == CY - 1, rim, pltpu.roll(v, CY - 1, 0))
        rim = fyr[n, 0, pl.ds(z, 1), :]
        low = jnp.where(sub == 0, rim, pltpu.roll(v, 1, 0))
        out.append((
            jnp.where((sub == CY - 1) & first["y"][1], 0.0, up - v),
            jnp.where((sub == 0) & first["y"][0], 0.0, v - low),
        ))
        edge = xlr[z]
        up = jnp.where(lane == CX - 1, edge, pltpu.roll(v, CX - 1, 1))
        low = jnp.where(lane == 0, edge, pltpu.roll(v, 1, 1))
        out.append((
            jnp.where((lane == CX - 1) & first["x"][1], 0.0, up - v),
            jnp.where((lane == 0) & first["x"][0], 0.0, v - low),
        ))
        return out

    def fold(p):
        return p[0:8] + p[8:16]

    def send_sums(n, primal, dualres):
        p = jnp.sum(jnp.sum(primal, axis=0, keepdims=True), axis=1, keepdims=True)
        d = jnp.sum(jnp.sum(dualres, axis=0, keepdims=True), axis=1, keepdims=True)
        red0[n] = jnp.where(lane[0:1] < CX // 2, p, d)

        for t in range(1, GZ):
            redz_copy(n, t).start()

    def redz_copy(n, t):
        return pltpu.make_async_remote_copy(
            red0.at[n], redz.at[n, t], rz_send.at[n, t], rz_recv.at[n, t],
            device_id=(lax.rem(gz + t, GZ), gy, gx), device_id_type=MESH,
        )

    def redx_copy(n, t):
        return pltpu.make_async_remote_copy(
            red1.at[n], redx.at[n, t], rx_send.at[n], rx_recv.at[n],
            device_id=member(t)[1], device_id_type=MESH,
        )

    def forward_sums(n):
        total = red0[n]
        for t in range(1, GZ):
            redz_copy(n, t).wait_recv()
            total += redz[n, t]
        red1[n] = total

        @pl.loop(1, BRICKS)
        def _(t):
            redx_copy(n, t).start()

    def finish_sums(n):
        total = red1[n]
        got = redx.at[n, pl.ds(1, BRICKS - 1)]
        pltpu.make_async_copy(got, got, rx_recv.at[n]).wait()
        total += jnp.sum(redx[n, 1:BRICKS], axis=0)
        p, d = total[:, 0:1], total[:, CX - 1 : CX]
        return jnp.broadcast_to(p, (8, CX)), jnp.broadcast_to(d, (8, CX))

    send_z(0, vol)
    send_faces(0, vol)

    def first_terms():
        with jax.named_scope("first_terms"):
            wait_faces(0)
        xa[1 : CZ + 1] = vol[...]
        cut = SHRINK

        @pl.loop(0, CZ)
        def _(z):
            smooth = jnp.zeros((CY, CX), F32)
            shrunk = jnp.zeros((CY, CX), F32)
            for j, jm in diffs(0, z):
                s = j - jnp.clip(j, -cut, cut)
                sm = jm - jnp.clip(jm, -cut, cut)
                smooth += jm - j
                shrunk += sm - s
            hterm[z] = smooth - shrunk
            back[z] = shrunk

    def copy1(n, d, dev):
        return pltpu.make_async_remote_copy(
            snd1.at[n, d], rcv1.at[n, me], a_send.at[n, 0], a_recv.at[n, 0],
            device_id=dev, device_id_type=MESH,
        )

    def copy2(n, d, dev):
        return pltpu.make_async_remote_copy(
            snd2.at[n, d], rcv2.at[n, me], a_send.at[n, 1], a_recv.at[n, 1],
            device_id=dev, device_id_type=MESH,
        )

    def arrivals(ref, sem):
        got = ref.at[pl.ds(0, BRICKS - 1)]
        pltpu.make_async_copy(got, got, sem).wait()

    def project(n, blurred, between):
        grad[...] = blurred
        for y in range(CY):
            sl[:, y * CX : (y + 1) * CX] = grad[pl.ds(y, CZ, stride=CY), :].astype(BF16)
        with jax.named_scope("mm_fwd"):
          for a in range(ANG):
            c = dot(sl[...], mat[:, a * DW : (a + 1) * DW], ((1,), (0,)))
            for h in range(2):
                stage[h, pl.ds(a, CZ, stride=ANG), :] = c[:, h * 128 : (h + 1) * 128]

        def block_of(d):
            rows = pl.ds(pl.multiple_of(d * ANG, ANG), ANG)
            return jnp.concatenate([stage[0, rows, :], stage[1, rows, :]], axis=1).astype(BF16)

        @pl.loop(1, BRICKS)
        def _(t):
            d, dev = member(t)
            snd1[n, d] = block_of(d)
            copy1(n, d, dev).start()

        rcv1[n, me] = block_of(me)
        between()
        with jax.named_scope("wait_a1"):
            arrivals(rcv1.at[n], a_recv.at[n, 0])

        def add(s, sums):
            x = rcv1[n, s].astype(F32)
            t = tbv[s]
            t = jnp.concatenate([t, t], axis=1)
            return tuple(sums[q] + jnp.where(t == float(q), x, 0.0) for q in range(NBLK))

        sums = lax.fori_loop(
            0, BRICKS, add, tuple(jnp.zeros((ANG, DW), F32) for _ in range(NBLK))
        )
        for q in range(NBLK):
            cols = slice(q * DW, (q + 1) * DW)
            mis[:, cols] = (sums[q] - acc[:, cols]).astype(BF16).astype(F32)

        def chosen(d):
            t = tbv[d]
            t = jnp.concatenate([t, t], axis=1)
            c = mis[:, 0:DW]
            for q in range(1, NBLK):
                c = jnp.where(t == float(q), mis[:, q * DW : (q + 1) * DW], c)
            return c.astype(BF16)

        @pl.loop(1, BRICKS)
        def _(t):
            d, dev = member(t)
            snd2[n, d] = chosen(d)
            copy2(n, d, dev).start()

        rcv2[n, me] = chosen(me)

    def backproject(n):
        with jax.named_scope("wait_a2"):
            arrivals(rcv2.at[n], a_recv.at[n, 1])
        r = rcv2[n].astype(F32).reshape(CZ * ANG, DW)
        for h in range(2):
            stage[h] = r[:, h * 128 : (h + 1) * 128]
        for a in range(ANG):
            for h in range(2):
                sl[:, a * DW + h * 128 : a * DW + (h + 1) * 128] = stage[
                    h, pl.ds(a, CZ, stride=ANG), :
                ].astype(BF16)
        with jax.named_scope("mm_bwd"):
          for c in range(ANG):
            b = dot(sl[...], mat[c * DW : (c + 1) * DW, :], ((1,), (1,)))
            for h in range(2):
                grad[pl.ds(2 * c + h, CZ, stride=CY), :] = b[:, h * 128 : (h + 1) * 128]

    blurred = blur(0, vol, lambda: relayout(6, 12), lambda: relayout(12, NCHUNK))
    project(0, blurred, first_terms)
    backproject(0)
    vol[...] = grad[...].reshape(CZ, CY, CX)
    send_z(1, vol)
    g = blur(1, vol).reshape(CZ, CY, CX)
    xa[1 : CZ + 1] = xa[1 : CZ + 1] - STEP * (g + hterm[...])
    vol[...] = xa[1 : CZ + 1]
    send_z(2, vol)
    send_faces(1, vol)

    def second_terms():
        with jax.named_scope("second_terms"):
            wait_faces(1)
        cut = SHRINK

        def one(z, sums):
            primal, dres = sums
            smooth = jnp.zeros((CY, CX), F32)
            shrunk = jnp.zeros((CY, CX), F32)
            bdual = jnp.zeros((CY, CX), F32)
            for axis, (j, jm) in enumerate(diffs(1, z)):
                d = jnp.clip(j, -cut, cut)
                dm = jnp.clip(jm, -cut, cut)
                s = j - d
                sm = jm - dm
                d = j - s
                dm = jm - sm
                smooth += jm - j
                shrunk += sm - s
                bdual += dm - d
                dl[axis, z] = d
                dlm[axis, z] = dm
                primal += fold(jnp.square(j - s))
            dres += fold(jnp.square(shrunk - back[z]))
            hterm[z] = smooth - shrunk
            back[z] = shrunk
            xlr[z] = bdual
            return primal, dres

        zero = jnp.zeros((8, CX), F32)
        primal, dres = lax.fori_loop(0, CZ, one, (zero, zero))
        send_sums(0, primal, dres)

    def factor_of(n, penalty):
        p, d = finish_sums(n)
        p = p * (1.0 / (3.0 * CELLS))
        d = penalty * penalty * d * (1.0 / CELLS)
        return jnp.sqrt(jnp.sqrt((p + EPS) / (d + EPS)))

    project(1, blur(2, vol), second_terms)
    forward_sums(0)
    backproject(1)
    ones = jnp.ones((8, CX), F32)

    def new_penalty():
        factor = factor_of(0, ones)
        pen3 = factor[0:1].reshape(1, 1, CX)
        hterm[...] = STEP * pen3 * (hterm[...] + xlr[...] * (1.0 / pen3))
        rmis[...] = factor

    vol[...] = grad[...].reshape(CZ, CY, CX)
    send_z(3, vol)
    g = blur(3, vol, new_penalty).reshape(CZ, CY, CX)
    penalty = rmis[...]
    inv1 = 1.0 / penalty
    xa[1 : CZ + 1] = xa[1 : CZ + 1] - (STEP * g + hterm[...])
    vol[...] = xa[1 : CZ + 1]
    send_faces(2, vol)
    x_copy = pltpu.make_async_copy(vol, x_out, out_sem.at[0])
    x_copy.start()

    with jax.named_scope("wait_faces"):
        wait_faces(2)
    cut = (SHRINK / penalty)[0:1]
    inv = inv1[0:1]

    def last(z, sums):
        primal, dres = sums
        shrunk = jnp.zeros((CY, CX), F32)
        for axis, (j, jm) in enumerate(diffs(2, z)):
            t = j + dl[axis, z] * inv
            tm = jm + dlm[axis, z] * inv
            s = t - jnp.clip(t, -cut, cut)
            sm = tm - jnp.clip(tm, -cut, cut)
            shrunk += sm - s
            dl[axis, z] = t - s
            primal += fold(jnp.square(j - s))
        dres += fold(jnp.square(shrunk - back[z]))
        return primal, dres

    zero = jnp.zeros((8, CX), F32)
    primal, dres = lax.fori_loop(0, CZ, last, (zero, zero))
    send_sums(1, primal, dres)
    with jax.named_scope("sums_z"):
        forward_sums(1)
    with jax.named_scope("sums_x"):
        factor2 = factor_of(1, penalty)
    scale = (1.0 / factor2)[0:1].reshape(1, 1, 1, CX)
    dl[...] = dl[...] * scale
    d_copy = pltpu.make_async_copy(dl, dual_out, out_sem.at[1])
    d_copy.start()

    with jax.named_scope("wait_sends"):
      for s in every:
        s.wait_send()
    for n in range(2):
        for i, ref in enumerate((snd1, snd2)):
            arrivals(ref.at[n], a_send.at[n, i])
        for t in range(1, GZ):
            redz_copy(n, t).wait_send()
        got = redx.at[n, pl.ds(1, BRICKS - 1)]
        pltpu.make_async_copy(got, got, rx_send.at[n]).wait()
    x_copy.wait()
    d_copy.wait()


def body(start, measured, tiles, tile_block, angle_row):
    vm = pltpu.VMEM
    dma = pltpu.SemaphoreType.DMA
    return pl.pallas_call(
        kernel,
        out_shape=(
            jax.ShapeDtypeStruct((CZ, CY, CX), F32),
            jax.ShapeDtypeStruct((3, CZ, CY, CX), F32),
        ),
        in_specs=[
            pl.BlockSpec(memory_space=pl.ANY),
            pl.BlockSpec(memory_space=pl.ANY),
            pl.BlockSpec(memory_space=pl.ANY),
            pl.BlockSpec(memory_space=pltpu.VMEM),
            pl.BlockSpec(memory_space=pltpu.SMEM),
        ],
        out_specs=(pl.BlockSpec(memory_space=pl.ANY), pl.BlockSpec(memory_space=pl.ANY)),
        scratch_shapes=[
            vm((V, ANG, DW), BF16),
            vm((V, ANG * DW), BF16),
            vm((2, CHUNK * ANG, 128), F32),
            vm((CZ, CY, CX), F32),
            vm((ROWS, CX), F32),
            vm((CZ + 2, CY, CX), F32),
            vm((CZ + 2 * R, CY, CX), F32),
            vm((CZ, CY + 2 * R, CX), F32),
            vm((BRICKS, ANG, CX), F32),
            vm((1, ANG, NBLK * DW), F32),
            vm((ANG, NBLK * DW), F32),
            vm((4, 2, R * CY, CX), BF16),
            vm((4, 2, R * CY, CX), BF16),
            vm((4, 2, CZ * R, CX), BF16),
            vm((4, 2, CZ * R, CX), BF16),
            vm((4, 2, 16, ROWS), BF16),
            vm((4, 2, 16, ROWS), BF16),
            vm((3, 2, CY, CX), F32),
            vm((3, 2, CY, CX), F32),
            vm((3, 2, CZ, CX), F32),
            vm((3, 2, CZ, CX), F32),
            vm((3, 2, 16, ROWS), BF16),
            vm((3, 2, 16, ROWS), BF16),
            vm((2, CZ * ANG, 128), F32),
            vm((CZ, V), BF16),
            vm((2, BRICKS, ANG, DW), BF16),
            vm((2, BRICKS, ANG, DW), BF16),
            vm((2, BRICKS, ANG, DW), BF16),
            vm((2, BRICKS, ANG, DW), BF16),
            vm((8, CX), F32),
            vm((CZ, CY, CX), F32),
            vm((CZ, CY, CX), F32),
            vm((3, CZ, CY, CX), F32),
            vm((3, CZ, CY, CX), F32),
            vm((CZ, CY, CX), F32),
            vm((2, 1, CX), F32),
            vm((2, GZ, 1, CX), F32),
            vm((2, 1, CX), F32),
            vm((2, BRICKS, 1, CX), F32),
            vm((3 * CX, CX), BF16),
            vm((96, CX), BF16),
            vm((ANG, NBLK * DW), F32),
            dma((2,)),
            dma((NCHUNK,)),
            dma((4, 3, 2)),
            dma((4, 3, 2)),
            dma((3, 3, 2)),
            dma((3, 3, 2)),
            dma((2, 2)),
            dma((2, 2)),
            dma((2, GZ)),
            dma((2, GZ)),
            dma((2,)),
            dma((2,)),
            dma((2,)),
        ],
        compiler_params=pltpu.CompilerParams(
            collective_id=0, has_side_effects=True, vmem_limit_bytes=60 * 1024 * 1024
        ),
    )(start, measured, tiles, tile_block, angle_row)


def solution(mesh):
    return jax.shard_map(
        body,
        mesh=mesh,
        in_specs=(
            P("gz", "gy", "gx"),
            P(("gz", "gy", "gx"), None, None),
            P("gy", None, "gx"),
            P(),
            P(),
        ),
        out_specs=(P("gz", "gy", "gx"), P(None, "gz", "gy", "gx")),
        check_vma=False,
    )
```

```python
import math

import jax
import jax.numpy as jnp
from jax import lax
from jax.experimental import pallas as pl
from jax.experimental.pallas import tpu as pltpu
from jax.sharding import PartitionSpec as P

CZ, CY, CX = 32, 16, 128
ROWS = CZ * CY
ANG, DW, NBLK = 8, 256, 4
V = CY * CX
R = 8
GZ, GY, GX = 4, 4, 8
BRICKS = GY * GX
CELLS = float(CZ * CY * CX * GZ * BRICKS)
MESH = pl.DeviceIdType.MESH
F32, BF16 = jnp.float32, jnp.bfloat16
STEP = 0.5
SHRINK = 0.2
EPS = 1e-6
CHUNK = 128
NCHUNK = V // CHUNK

RAW = [math.exp(-k * k / 12.5) for k in range(-R, R + 1)]
TAPS = [r / sum(RAW) for r in RAW]


def dot(a, b, dims):
    return lax.dot_general(a, b, (dims, ((), ())), preferred_element_type=F32)


def split(v):
    hi = v.astype(BF16)
    lo = (v - hi.astype(F32)).astype(BF16)
    return hi, lo


def kernel(
    start_ref, meas_ref, tiles_ref, tb_ref, row_ref,
    x_out, dual_out,
    raw, mat, tmp, x0, w1, w2, res, qbuf, xa, zbuf, zmid, ybuf, ymid, tbv, obs, mis, acc,
    zs, zr, zs2, zr2, ys, yr, ys2, yr2, xs, xr,
    fzs, fzr, fys, fyr, fxs, fxr,
    stage, sl, snd1, rcv1, snd2, rcv2,
    hterm, back, dl, dlm, xlr, bdl, fac,
    red0, redz, red1, redx,
    bx, wx, bx2, wx2,
    load_sem, tile_sem, z_send, z_recv, yx_send, yx_recv, f_send, f_recv,
    a_send, a_recv, rz_send, rz_recv, rx_send, rx_recv, out_sem,
):
    gz, gy, gx = lax.axis_index("gz"), lax.axis_index("gy"), lax.axis_index("gx")
    me = gy * GX + gx
    scope = jax.named_scope

    barrier = pltpu.get_barrier_semaphore()

    def member(t):
        d = lax.rem(me + t, BRICKS)
        return d, (gz, d // GX, lax.rem(d, GX))

    @pl.loop(1, BRICKS)
    def _(t):
        pl.semaphore_signal(barrier, inc=1, device_id=member(t)[1], device_id_type=MESH)

    @pl.loop(1, GZ)
    def _(t):
        pl.semaphore_signal(
            barrier, inc=1, device_id=(lax.rem(gz + t, GZ), gy, gx), device_id_type=MESH
        )

    ld = [
        pltpu.make_async_copy(start_ref, x0, load_sem.at[0]),
        pltpu.make_async_copy(meas_ref, obs, load_sem.at[1]),
    ]
    for c in ld:
        c.start()

    def tile_copy(c):
        rows = pl.ds(pl.multiple_of(c * CHUNK, CHUNK), CHUNK)
        return pltpu.make_async_copy(tiles_ref.at[rows], raw.at[rows], tile_sem.at[c])

    @pl.loop(0, NCHUNK)
    def _(c):
        tile_copy(c).start()

    def there(dz, dy, dx):
        ok = True
        for d, at, n in ((dz, gz, GZ), (dy, gy, GY), (dx, gx, GX)):
            if d:
                near = at > 0 if d < 0 else at < n - 1
                ok = near if ok is True else jnp.logical_and(ok, near)
        return ok

    class Hub:
        def __init__(self, items):
            self.items = [
                (
                    there(*d),
                    there(*(-i for i in d)),
                    pltpu.make_async_remote_copy(
                        src, dst, ss, rs,
                        device_id=(gz + d[0], gy + d[1], gx + d[2]), device_id_type=MESH,
                    ),
                    dst,
                )
                for d, src, dst, ss, rs in items
            ]

        def clear(self):
            for _, arrives, _, dst in self.items:

                @pl.when(jnp.logical_not(arrives))
                def _():
                    dst[...] = jnp.zeros(dst.shape, dst.dtype)

        def start(self):
            for leaves, _, copy, _ in self.items:
                pl.when(leaves)(copy.start)

        def wait_recv(self):
            for _, arrives, copy, _ in self.items:
                pl.when(arrives)(copy.wait_recv)

        def wait_send(self):
            for leaves, _, copy, _ in self.items:
                pl.when(leaves)(copy.wait_send)

    def pair(axis, src, dst, send, recv):
        unit = [int(axis == a) for a in range(3)]
        return [
            ([-u for u in unit], src.at[0], dst.at[1], send.at[0], recv.at[0]),
            (unit, src.at[1], dst.at[0], send.at[1], recv.at[1]),
        ]

    def around(m, low, high, into_low, into_high):
        items = [
            ((0, -1, 0), low, into_high, yx_send.at[m, 0], yx_recv.at[m, 0]),
            ((0, 1, 0), high, into_low, yx_send.at[m, 1], yx_recv.at[m, 1]),
        ]
        k = 2
        for sy in (0, -1, 1):
            for side, sx in ((0, -1), (1, 1)):
                items.append((
                    (0, sy, sx), xs.at[m, side], xr.at[m, 1 - sy, 1 - side],
                    yx_send.at[m, k], yx_recv.at[m, k],
                ))
                k += 1
        return Hub(items)

    zhub = [Hub(pair(0, zs.at[n], zr.at[n], z_send.at[n], z_recv.at[n])) for n in range(3)]
    zhub2 = Hub(pair(0, zs2, zr2, z_send.at[3], z_recv.at[3]))
    yxhub = [around(n, ys.at[n, 0], ys.at[n, 1], yr.at[n, 0], yr.at[n, 1]) for n in range(4)]
    yxhub2 = around(4, ys2, ys2, yr2.at[0], yr2.at[1])
    fhub = [
        Hub(
            pair(0, fzs.at[n], fzr.at[n], f_send.at[n, 0], f_recv.at[n, 0])
            + pair(1, fys.at[n], fyr.at[n], f_send.at[n, 1], f_recv.at[n, 1])
            + pair(2, fxs.at[n], fxr.at[n], f_send.at[n, 2], f_recv.at[n, 2])
        )
        for n in range(3)
    ]
    hubs = zhub + [zhub2] + yxhub + [yxhub2] + fhub
    for h in hubs:
        h.clear()

    def gauss(d):
        df = d.astype(F32)
        w = jnp.exp(df * df * (-1.0 / 12.5)) * (1.0 / sum(RAW))
        return jnp.where(jnp.abs(d) <= R, w, 0.0)

    def iota(shape, axis):
        return lax.broadcasted_iota(jnp.int32, shape, axis)

    square = (CX, CX)
    bhi, blo = split(gauss(iota(square, 0) - iota(square, 1)))
    bx[0:CX] = bhi
    bx[CX : 2 * CX] = bhi
    bx[2 * CX : 3 * CX] = blo
    k0, k1 = iota((32, CX), 0), iota((32, CX), 1)
    pos = jnp.where(k0 < 16, lax.rem(k0, 8) - 8, CX + lax.rem(k0, 8))
    whi, wlo = split(gauss(pos - k1))
    wx[0:32] = whi
    wx[32:64] = wlo
    rim = ((k1 == 0) & ((k0 == 7) | (k0 == 15))) | ((k1 == CX - 1) & ((k0 == 16) | (k0 == 24)))
    wx[64:96] = jnp.where(rim, 1.0, 0.0).astype(BF16)
    s0, s1 = iota((32, 2 * CX), 0), iota((32, 2 * CX), 1)
    want = jnp.where(s0 < 16, lax.rem(s0, 8), CX - 8 + lax.rem(s0, 8)) + jnp.where(
        lax.rem(s0, 16) < 8, 0, CX
    )
    pick = jnp.where(s1 == want, 1.0, 0.0).astype(BF16)
    pick2 = jnp.where(k1 == jnp.where(k0 < 16, k0, CX - 32 + k0), 1.0, 0.0).astype(BF16)

    wide = (GX, GX * CX)
    spread = jnp.where(iota(wide, 0) == iota(wide, 1) // CX, 1.0, 0.0).astype(BF16)
    for b in range(GY):
        rows = dot(tb_ref[b].astype(F32).astype(BF16), spread, ((0,), (0,)))
        for c in range(GX):
            tbv[b * GX + c] = rows[:, c * CX : (c + 1) * CX]

    def relayout(low, high):
        @pl.loop(low, high)
        def _(c):
            tile_copy(c).wait()
            rows = pl.ds(pl.multiple_of(c * CHUNK, CHUNK), CHUNK)
            block = raw[rows].astype(F32).reshape(CHUNK * ANG, DW)
            for h in range(2):
                tmp[h] = block[:, h * 128 : (h + 1) * 128]
            for a in range(ANG):
                for h in range(2):
                    part = tmp[h, pl.ds(a, CHUNK, stride=ANG), :]
                    mat[rows, a * DW + h * 128 : a * DW + (h + 1) * 128] = part.astype(BF16)

    for c in ld:
        c.wait()
    for a in range(ANG):
        acc[pl.ds(a, 1), :] = obs[0, pl.ds(row_ref[a], 1), :]

    relayout(0, 6)
    with scope("wait_barrier"):
        pl.semaphore_wait(barrier, BRICKS - 1 + GZ - 1)

    def send_faces(n, src):
        fzs[n, 0] = src[0]
        fzs[n, 1] = src[CZ - 1]
        v = src[...]
        fys[n, 0] = v[:, 0, :]
        fys[n, 1] = v[:, CY - 1, :]
        hi, lo = split(v.reshape(ROWS, CX))
        f = dot(pick, jnp.concatenate([hi, lo], axis=1), ((1,), (1,))).astype(BF16)
        fxs[n, 0] = f[0:16]
        fxs[n, 1] = f[16:32]
        fhub[n].start()

    def send_z(n, src):
        zs[n, 0] = src[0:R].reshape(R * CY, CX).astype(BF16)
        zs[n, 1] = src[CZ - R : CZ].reshape(R * CY, CX).astype(BF16)
        zhub[n].start()

    def taps(at):
        t = TAPS[R] * at(R)
        for k in range(R):
            t += TAPS[k] * (at(k) + at(2 * R - k))
        return t

    def blur_z(n, src, out):
        zbuf[R : R + CZ] = src[...]
        with scope("wait_z"):
            zhub[n].wait_recv()
        zbuf[0:R] = zr[n, 0].astype(F32).reshape(R, CY, CX)
        zbuf[R + CZ : 2 * R + CZ] = zr[n, 1].astype(F32).reshape(R, CY, CX)

        @pl.loop(0, CZ, unroll=2)
        def _(z):
            out[z] = taps(lambda k: zbuf[z + k])

    def send_yx(n, w):
        v = w[...]
        ys[n, 0] = v[:, 0:R, :].reshape(CZ * R, CX).astype(BF16)
        ys[n, 1] = v[:, CY - R :, :].reshape(CZ * R, CX).astype(BF16)
        hi, lo = split(v.reshape(ROWS, CX))
        f = dot(pick, jnp.concatenate([hi, lo], axis=1), ((1,), (1,))).astype(BF16)
        xs[n, 0] = f[0:16]
        xs[n, 1] = f[16:32]
        yxhub[n].start()

    def rows_of(m, slot, weights):
        halo = xr[m, slot].reshape(32, ROWS)
        return dot(jnp.concatenate([halo, halo], axis=0), weights, ((0,), (0,)))

    def own_rows(w, mat3):
        hi, lo = split(w[...].reshape(ROWS, CX))
        both = jnp.concatenate([hi, lo], axis=1)
        return dot(both, mat3[0 : 2 * CX], ((1,), (0,))) + dot(hi, mat3[2 * CX :], ((1,), (0,)))

    def blur_yx(n, w, out):
        own = own_rows(w, bx)
        ybuf[:, R : R + CY, :] = own.reshape(CZ, CY, CX)
        with scope("wait_yx"):
            yxhub[n].wait_recv()
        ybuf[:, R : R + CY, :] += rows_of(n, 1, wx[0:64]).reshape(CZ, CY, CX)
        for side, at in ((0, slice(CY - R, CY)), (1, slice(0, R))):
            y = yr[n, side]
            rows = dot(jnp.concatenate([y, y], axis=1), bx[CX:], ((1,), (0,)))
            more = rows_of(n, 2 * side, wx[0:64]).reshape(CZ, CY, CX)[:, at, :]
            to = slice(0, R) if side == 0 else slice(R + CY, 2 * R + CY)
            ybuf[:, to, :] = rows.reshape(CZ, R, CX) + more

        @pl.loop(0, CZ, unroll=2)
        def _(z):
            out[z] = taps(lambda k: ybuf[z, k : k + CY, :])

    lane, sub = iota((CY, CX), 1), iota((CY, CX), 0)
    ends = ((gz == 0, gz == GZ - 1), (gy == 0, gy == GY - 1), (gx == 0, gx == GX - 1))

    def wait_faces(n):
        with scope("wait_faces"):
            fhub[n].wait_recv()
        xlr[...] = dot(fxr[n].reshape(32, ROWS), wx[64:96], ((0,), (0,))).reshape(CZ, CY, CX)
        xa[0] = fzr[n, 0]
        xa[CZ + 1] = fzr[n, 1]

    def diffs(n, z):
        v = xa[z + 1]
        up, low = xa[z + 2], xa[z]
        yield (
            jnp.where((z == CZ - 1) & ends[0][1], 0.0, up - v),
            jnp.where((z == 0) & ends[0][0], 0.0, v - low),
        )
        up = jnp.where(sub == CY - 1, fyr[n, 1, pl.ds(z, 1), :], pltpu.roll(v, CY - 1, 0))
        low = jnp.where(sub == 0, fyr[n, 0, pl.ds(z, 1), :], pltpu.roll(v, 1, 0))
        yield (
            jnp.where((sub == CY - 1) & ends[1][1], 0.0, up - v),
            jnp.where((sub == 0) & ends[1][0], 0.0, v - low),
        )
        edge = xlr[z]
        up = jnp.where(lane == CX - 1, edge, pltpu.roll(v, CX - 1, 1))
        low = jnp.where(lane == 0, edge, pltpu.roll(v, 1, 1))
        yield (
            jnp.where((lane == CX - 1) & ends[2][1], 0.0, up - v),
            jnp.where((lane == 0) & ends[2][0], 0.0, v - low),
        )

    def fold(p):
        return p[0:8] + p[8:16]

    def redz_copy(n, t):
        return pltpu.make_async_remote_copy(
            red0.at[n], redz.at[n, t], rz_send.at[n, t], rz_recv.at[n, t],
            device_id=(lax.rem(gz + t, GZ), gy, gx), device_id_type=MESH,
        )

    def redx_copy(n, t):
        return pltpu.make_async_remote_copy(
            red1.at[n], redx.at[n, t], rx_send.at[n], rx_recv.at[n],
            device_id=member(t)[1], device_id_type=MESH,
        )

    def send_sums(n, primal, dualres):
        p = jnp.sum(jnp.sum(primal, axis=0, keepdims=True), axis=1, keepdims=True)
        d = jnp.sum(jnp.sum(dualres, axis=0, keepdims=True), axis=1, keepdims=True)
        red0[n] = jnp.where(lane[0:1] < CX // 2, p, d)
        for t in range(1, GZ):
            redz_copy(n, t).start()

    def forward_sums(n):
        total = red0[n]
        for t in range(1, GZ):
            redz_copy(n, t).wait_recv()
            total += redz[n, t]
        red1[n] = total

        @pl.loop(1, BRICKS)
        def _(t):
            redx_copy(n, t).start()

    def factor_of(n, penalty):
        total = red1[n]
        got = redx.at[n, pl.ds(1, BRICKS - 1)]
        pltpu.make_async_copy(got, got, rx_recv.at[n]).wait()
        total += jnp.sum(redx[n, 1:BRICKS], axis=0)
        p = jnp.broadcast_to(total[:, 0:1], (8, CX)) * (1.0 / (3.0 * CELLS))
        d = jnp.broadcast_to(total[:, CX - 1 : CX], (8, CX)) * (1.0 / CELLS)
        d = penalty * penalty * d
        return jnp.sqrt(jnp.sqrt((p + EPS) / (d + EPS)))

    def arrivals(ref, sem):
        got = ref.at[pl.ds(0, BRICKS - 1)]
        pltpu.make_async_copy(got, got, sem).wait()

    def send_block(n, i, src, dst, d, dev):
        pltpu.make_async_remote_copy(
            src.at[n, d], dst.at[n, me], a_send.at[n, i], a_recv.at[n, i],
            device_id=dev, device_id_type=MESH,
        ).start()

    def project(n):
        for z0 in range(1):
            for y in range(CY):
                sl[:, y * CX : (y + 1) * CX] = res[pl.ds(y, CZ, stride=CY), :].astype(BF16)
        with scope("mm_fwd"):
            for a in range(ANG):
                c = dot(sl[...], mat[:, a * DW : (a + 1) * DW], ((1,), (0,)))
                for h in range(2):
                    stage[h, pl.ds(a, CZ, stride=ANG), :] = c[:, h * 128 : (h + 1) * 128]

        def block_of(d):
            rows = pl.ds(pl.multiple_of(d * ANG, ANG), ANG)
            return jnp.concatenate([stage[0, rows, :], stage[1, rows, :]], axis=1).astype(BF16)

        @pl.loop(1, BRICKS)
        def _(t):
            d, dev = member(t)
            snd1[n, d] = block_of(d)
            send_block(n, 0, snd1, rcv1, d, dev)

        rcv1[n, me] = block_of(me)

    def return_misfit(n):
        with scope("wait_a1"):
            arrivals(rcv1.at[n], a_recv.at[n, 0])

        def add(s, sums):
            x = rcv1[n, s].astype(F32)
            t = tbv[s]
            t = jnp.concatenate([t, t], axis=1)
            return tuple(sums[q] + jnp.where(t == float(q), x, 0.0) for q in range(NBLK))

        sums = lax.fori_loop(
            0, BRICKS, add, tuple(jnp.zeros((ANG, DW), F32) for _ in range(NBLK)), unroll=2
        )
        for q in range(NBLK):
            cols = slice(q * DW, (q + 1) * DW)
            mis[:, cols] = (sums[q] - acc[:, cols]).astype(BF16).astype(F32)

        def chosen(d):
            t = tbv[d]
            t = jnp.concatenate([t, t], axis=1)
            c = mis[:, 0:DW]
            for q in range(1, NBLK):
                c = jnp.where(t == float(q), mis[:, q * DW : (q + 1) * DW], c)
            return c.astype(BF16)

        @pl.loop(1, BRICKS)
        def _(t):
            d, dev = member(t)
            snd2[n, d] = chosen(d)
            send_block(n, 1, snd2, rcv2, d, dev)

        rcv2[n, me] = chosen(me)

    def backproject(n, out):
        with scope("wait_a2"):
            arrivals(rcv2.at[n], a_recv.at[n, 1])
        r = rcv2[n].astype(F32).reshape(CZ * ANG, DW)
        for h in range(2):
            stage[h] = r[:, h * 128 : (h + 1) * 128]
        for a in range(ANG):
            for h in range(2):
                sl[:, a * DW + h * 128 : a * DW + (h + 1) * 128] = stage[
                    h, pl.ds(a, CZ, stride=ANG), :
                ].astype(BF16)
        with scope("mm_bwd"):
            for c in range(ANG):
                b = dot(sl[...], mat[c * DW : (c + 1) * DW, :], ((1,), (1,)))
                for h in range(2):
                    res[pl.ds(2 * c + h, CZ, stride=CY), :] = b[:, h * 128 : (h + 1) * 128]
        out[...] = res[...].reshape(CZ, CY, CX)

    send_z(0, x0)
    send_faces(0, x0)
    relayout(6, 12)
    blur_z(0, x0, w1)
    send_yx(0, w1)
    relayout(12, NCHUNK)
    blur_yx(0, w1, w2)
    res[...] = w2[...].reshape(ROWS, CX)
    project(0)

    wait_faces(0)
    xa[1 : CZ + 1] = x0[...]
    cut = SHRINK

    @pl.loop(0, CZ, unroll=2)
    def _(z):
        smooth = jnp.zeros((CY, CX), F32)
        shrunk = jnp.zeros((CY, CX), F32)
        for j, jm in diffs(0, z):
            s = j - jnp.clip(j, -cut, cut)
            sm = jm - jnp.clip(jm, -cut, cut)
            smooth += jm - j
            shrunk += sm - s
        h = STEP * (smooth - shrunk)
        x0[z] = xa[z + 1] - h
        back[z] = shrunk

    send_z(1, x0)

    shape1, shape2 = (160, 256), (256, CX)
    i, m = iota(shape1, 0), iota(shape1, 1) - 8
    i = jnp.where(i < CX, i, jnp.where(i < CX + 16, i - CX - 16, i - 16))
    inside = ((m >= 0) | (gx > 0)) & ((m < CX) | (gx < GX - 1)) & (m < CX + 8)
    thi, tlo = split(jnp.where(inside, gauss(i - m), 0.0))
    m = iota(shape2, 0) - 8
    uhi, ulo = split(gauss(m - iota(shape2, 1)))
    twice = (
        dot(thi, uhi, ((1,), (0,))) + dot(thi, ulo, ((1,), (0,))) + dot(tlo, uhi, ((1,), (0,)))
    )
    bhi, blo = split(twice[0:CX])
    bx2[0:CX] = bhi
    bx2[CX : 2 * CX] = bhi
    bx2[2 * CX : 3 * CX] = blo
    whi, wlo = split(twice[CX : CX + 32])
    wx2[0:32] = whi
    wx2[32:64] = wlo

    return_misfit(0)
    blur_z(1, x0, w1)
    send_yx(1, w1)
    backproject(0, w2)

    zs2[0] = w2[0:16].reshape(16 * CY, CX).astype(BF16)
    zs2[1] = w2[CZ - 16 : CZ].reshape(16 * CY, CX).astype(BF16)
    zhub2.start()
    blur_yx(1, w1, qbuf)
    zbuf[16 : 16 + CZ] = w2[...]
    with scope("wait_z2"):
        zhub2.wait_recv()
    zbuf[0:16] = zr2[0].astype(F32).reshape(16, CY, CX)
    zbuf[16 + CZ : 32 + CZ] = zr2[1].astype(F32).reshape(16, CY, CX)

    @pl.loop(0, CZ + 16, unroll=2)
    def _(z):
        out = ((z < 8) & ends[0][0]) | ((z >= CZ + 8) & ends[0][1])
        zmid[z] = jnp.where(out, 0.0, taps(lambda k: zbuf[z + k]))

    @pl.loop(0, CZ, unroll=2)
    def _(z):
        w2[z] = taps(lambda k: zmid[z + k])

    hi = w2[...].reshape(ROWS, CX).astype(BF16)
    ys2[...] = hi
    f = dot(pick2, hi, ((1,), (1,))).astype(BF16)
    xs[4, 0] = f[0:16]
    xs[4, 1] = f[16:32]
    yxhub2.start()
    w1[...] = zmid[8 : 8 + CZ]
    send_yx(2, w1)

    ymid[:, 16 : 16 + CY, :] = own_rows(w2, bx2).reshape(CZ, CY, CX)
    with scope("wait_yx2"):
        yxhub2.wait_recv()
    ymid[:, 16 : 16 + CY, :] += rows_of(4, 1, wx2[...]).reshape(CZ, CY, CX)
    for side in range(2):
        y = yr2[side]
        rows = dot(jnp.concatenate([y, y], axis=1), bx2[CX:], ((1,), (0,)))
        rows = rows + rows_of(4, 2 * side, wx2[...])
        ymid[:, 32 * side : 32 * side + 16, :] = rows.reshape(CZ, CY, CX)
    sub2 = iota((CY + 16, CX), 0)
    outside = ((sub2 < 8) & ends[1][0]) | ((sub2 >= CY + 8) & ends[1][1])

    @pl.loop(0, CZ, unroll=2)
    def _(z):
        ybuf[z] = jnp.where(outside, 0.0, taps(lambda k: ymid[z, k : k + CY + 16, :]))

    @pl.loop(0, CZ, unroll=2)
    def _(z):
        rows = pl.ds(pl.multiple_of(z * CY, CY), CY)
        res[rows, :] = qbuf[z] - STEP * taps(lambda k: ybuf[z, k : k + CY, :])

    project(1)
    blur_yx(2, w1, w2)
    x0[...] = x0[...] - STEP * w2[...]
    send_faces(1, x0)
    xa[1 : CZ + 1] = x0[...]
    return_misfit(1)
    wait_faces(1)

    def one(z, sums):
        primal, dres = sums
        smooth = jnp.zeros((CY, CX), F32)
        shrunk = jnp.zeros((CY, CX), F32)
        bdual = jnp.zeros((CY, CX), F32)
        for axis, (j, jm) in enumerate(diffs(1, z)):
            s = j - jnp.clip(j, -cut, cut)
            sm = jm - jnp.clip(jm, -cut, cut)
            d = j - s
            dm = jm - sm
            smooth += jm - j
            shrunk += sm - s
            bdual += dm - d
            dl[axis, z] = d
            dlm[axis, z] = dm
            primal += fold(jnp.square(j - s))
        dres += fold(jnp.square(shrunk - back[z]))
        hterm[z] = smooth - shrunk
        back[z] = shrunk
        bdl[z] = bdual
        return primal, dres

    zero = jnp.zeros((8, CX), F32)
    primal, dres = lax.fori_loop(0, CZ, one, (zero, zero), unroll=2)
    send_sums(0, primal, dres)
    backproject(1, w2)
    send_z(2, w2)
    forward_sums(0)
    blur_z(2, w2, w1)
    send_yx(3, w1)
    penalty = factor_of(0, jnp.ones((8, CX), F32))
    inv1 = 1.0 / penalty
    pen3 = penalty[0:1].reshape(1, 1, CX)
    inv3 = inv1[0:1].reshape(1, 1, CX)
    x0[...] = x0[...] - STEP * pen3 * (hterm[...] + bdl[...] * inv3)
    blur_yx(3, w1, w2)
    x0[...] = x0[...] - STEP * w2[...]
    send_faces(2, x0)
    x_copy = pltpu.make_async_copy(x0, x_out, out_sem.at[0])
    x_copy.start()
    xa[1 : CZ + 1] = x0[...]
    wait_faces(2)
    cut2 = (SHRINK / penalty)[0:1]
    inv = inv1[0:1]

    def last(z, sums):
        primal, dres = sums
        shrunk = jnp.zeros((CY, CX), F32)
        for axis, (j, jm) in enumerate(diffs(2, z)):
            t = j + dl[axis, z] * inv
            tm = jm + dlm[axis, z] * inv
            s = t - jnp.clip(t, -cut2, cut2)
            sm = tm - jnp.clip(tm, -cut2, cut2)
            shrunk += sm - s
            dl[axis, z] = t - s
            primal += fold(jnp.square(j - s))
        dres += fold(jnp.square(shrunk - back[z]))
        return primal, dres

    with scope("last"):
        primal, dres = lax.fori_loop(0, CZ, last, (zero, zero), unroll=2)
    send_sums(1, primal, dres)
    with scope("sums_z"):
        forward_sums(1)
    with scope("sums_x"):
        factor2 = factor_of(1, penalty)
    scale = (1.0 / factor2)[0:1].reshape(1, 1, 1, CX)
    dl[...] = dl[...] * scale
    d_copy = pltpu.make_async_copy(dl, dual_out, out_sem.at[1])
    d_copy.start()

    with scope("wait_sends"):
        for h in hubs:
            h.wait_send()
        for n in range(2):
            for i, ref in enumerate((snd1, snd2)):
                arrivals(ref.at[n], a_send.at[n, i])
            for t in range(1, GZ):
                redz_copy(n, t).wait_send()
            got = redx.at[n, pl.ds(1, BRICKS - 1)]
            pltpu.make_async_copy(got, got, rx_send.at[n]).wait()
    x_copy.wait()
    d_copy.wait()


def body(start, measured, tiles, tile_block, angle_row):
    vm = pltpu.VMEM
    dma = pltpu.SemaphoreType.DMA
    block = vm((CZ, CY, CX), F32)
    return pl.pallas_call(
        kernel,
        out_shape=(
            jax.ShapeDtypeStruct((CZ, CY, CX), F32),
            jax.ShapeDtypeStruct((3, CZ, CY, CX), F32),
        ),
        in_specs=[
            pl.BlockSpec(memory_space=pl.ANY),
            pl.BlockSpec(memory_space=pl.ANY),
            pl.BlockSpec(memory_space=pl.ANY),
            pl.BlockSpec(memory_space=pltpu.VMEM),
            pl.BlockSpec(memory_space=pltpu.SMEM),
        ],
        out_specs=(pl.BlockSpec(memory_space=pl.ANY), pl.BlockSpec(memory_space=pl.ANY)),
        scratch_shapes=[
            vm((V, ANG, DW), BF16),
            vm((V, ANG * DW), BF16),
            vm((2, CHUNK * ANG, 128), F32),
            block, block, block,
            vm((ROWS, CX), F32),
            block,
            vm((CZ + 2, CY, CX), F32),
            vm((CZ + 32, CY, CX), F32),
            vm((CZ + 16, CY, CX), F32),
            vm((CZ, CY + 16, CX), F32),
            vm((CZ, CY + 32, CX), F32),
            vm((BRICKS, ANG, CX), F32),
            vm((1, ANG, NBLK * DW), F32),
            vm((ANG, NBLK * DW), F32),
            vm((ANG, NBLK * DW), F32),
            vm((3, 2, R * CY, CX), BF16),
            vm((3, 2, R * CY, CX), BF16),
            vm((2, 16 * CY, CX), BF16),
            vm((2, 16 * CY, CX), BF16),
            vm((4, 2, CZ * R, CX), BF16),
            vm((4, 2, CZ * R, CX), BF16),
            vm((ROWS, CX), BF16),
            vm((2, ROWS, CX), BF16),
            vm((5, 2, 16, ROWS), BF16),
            vm((5, 3, 2, 16, ROWS), BF16),
            vm((3, 2, CY, CX), F32),
            vm((3, 2, CY, CX), F32),
            vm((3, 2, CZ, CX), F32),
            vm((3, 2, CZ, CX), F32),
            vm((3, 2, 16, ROWS), BF16),
            vm((3, 2, 16, ROWS), BF16),
            vm((2, CZ * ANG, 128), F32),
            vm((CZ, V), BF16),
            vm((2, BRICKS, ANG, DW), BF16),
            vm((2, BRICKS, ANG, DW), BF16),
            vm((2, BRICKS, ANG, DW), BF16),
            vm((2, BRICKS, ANG, DW), BF16),
            block, block,
            vm((3, CZ, CY, CX), F32),
            vm((3, CZ, CY, CX), F32),
            block, block,
            vm((8, CX), F32),
            vm((2, 1, CX), F32),
            vm((2, GZ, 1, CX), F32),
            vm((2, 1, CX), F32),
            vm((2, BRICKS, 1, CX), F32),
            vm((3 * CX, CX), BF16),
            vm((96, CX), BF16),
            vm((3 * CX, CX), BF16),
            vm((64, CX), BF16),
            dma((2,)),
            dma((NCHUNK,)),
            dma((4, 2)),
            dma((4, 2)),
            dma((5, 8)),
            dma((5, 8)),
            dma((3, 3, 2)),
            dma((3, 3, 2)),
            dma((2, 2)),
            dma((2, 2)),
            dma((2, GZ)),
            dma((2, GZ)),
            dma((2,)),
            dma((2,)),
            dma((2,)),
        ],
        compiler_params=pltpu.CompilerParams(
            collective_id=0, has_side_effects=True, vmem_limit_bytes=60 * 1024 * 1024
        ),
    )(start, measured, tiles, tile_block, angle_row)


def solution(mesh):
    return jax.shard_map(
        body,
        mesh=mesh,
        in_specs=(
            P("gz", "gy", "gx"),
            P(("gz", "gy", "gx"), None, None),
            P("gy", None, "gx"),
            P(),
            P(),
        ),
        out_specs=(P("gz", "gy", "gx"), P(None, "gz", "gy", "gx")),
        check_vma=False,
    )
```

```python
import math

import jax
import jax.numpy as jnp
from jax import lax
from jax.experimental import pallas as pl
from jax.experimental.pallas import tpu as pltpu
from jax.sharding import PartitionSpec as P

CZ, CY, CX = 32, 16, 128
ROWS = CZ * CY
ANG, DW, NBLK = 8, 256, 4
V = CY * CX
R = 8
GZ, GY, GX = 4, 4, 8
BRICKS = GY * GX
CELLS = float(CZ * CY * CX * GZ * BRICKS)
MESH = pl.DeviceIdType.MESH
F32, BF16 = jnp.float32, jnp.bfloat16
STEP = 0.5
SHRINK = 0.2
EPS = 1e-6
CHUNK = 128
NCHUNK = V // CHUNK
ORDER = sorted(
    ((dx, dz, dc) for dz in range(4) for dx in range(4) for dc in range(2) if dx or dz or dc),
    key=lambda s: -(min(s[0], 4 - s[0]) + min(s[1], 4 - s[1])),
)
SPLIT = 5

RAW = [math.exp(-k * k / 12.5) for k in range(-R, R + 1)]
TAPS = [r / sum(RAW) for r in RAW]


def dot(a, b, dims):
    return lax.dot_general(a, b, (dims, ((), ())), preferred_element_type=F32)


def split(v):
    hi = v.astype(BF16)
    lo = (v - hi.astype(F32)).astype(BF16)
    return hi, lo


def kernel(
    start_ref, meas_ref, tiles_ref, tb_ref, row_ref,
    x_out, dual_out,
    raw, mat, tmp, x0, w1, w2, res, qbuf, xa, zbuf, zmid, ybuf, ymid, tbv, obs, mis, acc,
    zs, zr, zs2, zr2, ys, yr, ys2, yr2, xs, xr,
    fzs, fzr, fys, fyr, fxs, fxr,
    stage, sl, snd1, rcv1, snd2, rcv2,
    hterm, back, dl, dlm, xlr, bdl,
    red0, redz, red1, redx,
    bx, wx, bx2, wx2,
    load_sem, tile_sem, z_send, z_recv, yx_send, yx_recv, f_send, f_recv,
    a_send, a_recv, rz_send, rz_recv, rx_send, rx_recv,
):
    gz, gy, gx = lax.axis_index("gz"), lax.axis_index("gy"), lax.axis_index("gx")
    me = gy * GX + gx
    scope = jax.named_scope

    barrier = pltpu.get_barrier_semaphore()

    chip_x = 2 * (gy // 2) + lax.rem(gx, 2)
    chip_z, core = gx // 2, lax.rem(gy, 2)

    def member(t):
        dx, dz, dc = ORDER[t - 1]
        x = lax.rem(chip_x + dx, 4)
        z = lax.rem(chip_z + dz, 4)
        y = 2 * (x // 2) + lax.rem(core + dc, 2)
        x = 2 * z + lax.rem(x, 2)
        return y * GX + x, (gz, y, x)

    for t in range(1, BRICKS):
        pl.semaphore_signal(barrier, inc=1, device_id=member(t)[1], device_id_type=MESH)

    @pl.loop(1, GZ)
    def _(t):
        pl.semaphore_signal(
            barrier, inc=1, device_id=(lax.rem(gz + t, GZ), gy, gx), device_id_type=MESH
        )

    ld = [
        pltpu.make_async_copy(start_ref, x0, load_sem.at[0]),
        pltpu.make_async_copy(meas_ref, obs, load_sem.at[1]),
    ]
    for c in ld:
        c.start()

    def tile_copy(c):
        rows = pl.ds(pl.multiple_of(c * CHUNK, CHUNK), CHUNK)
        return pltpu.make_async_copy(tiles_ref.at[rows], raw.at[rows], tile_sem.at[c])

    @pl.loop(0, NCHUNK)
    def _(c):
        tile_copy(c).start()

    def there(dz, dy, dx):
        ok = True
        for d, at, n in ((dz, gz, GZ), (dy, gy, GY), (dx, gx, GX)):
            if d:
                near = at > 0 if d < 0 else at < n - 1
                ok = near if ok is True else jnp.logical_and(ok, near)
        return ok

    class Hub:
        def __init__(self, items):
            self.items = [
                (
                    there(*d),
                    there(*(-i for i in d)),
                    pltpu.make_async_remote_copy(
                        src, dst, ss, rs,
                        device_id=(gz + d[0], gy + d[1], gx + d[2]), device_id_type=MESH,
                    ),
                    dst,
                )
                for d, src, dst, ss, rs in items
            ]

        def clear(self):
            for _, arrives, _, dst in self.items:

                @pl.when(jnp.logical_not(arrives))
                def _():
                    dst[...] = jnp.zeros(dst.shape, dst.dtype)

        def start(self):
            for leaves, _, copy, _ in self.items:
                pl.when(leaves)(copy.start)

        def wait_recv(self):
            for _, arrives, copy, _ in self.items:
                pl.when(arrives)(copy.wait_recv)

        def wait_send(self):
            for leaves, _, copy, _ in self.items:
                pl.when(leaves)(copy.wait_send)

    def pair(axis, src, dst, send, recv):
        unit = [int(axis == a) for a in range(3)]
        return [
            ([-u for u in unit], src.at[0], dst.at[1], send.at[0], recv.at[0]),
            (unit, src.at[1], dst.at[0], send.at[1], recv.at[1]),
        ]

    def around(m, low, high, into_low, into_high):
        items = [
            ((0, -1, 0), low, into_high, yx_send.at[m, 0], yx_recv.at[m, 0]),
            ((0, 1, 0), high, into_low, yx_send.at[m, 1], yx_recv.at[m, 1]),
        ]
        k = 2
        for sy in (0, -1, 1):
            for side, sx in ((0, -1), (1, 1)):
                items.append((
                    (0, sy, sx), xs.at[m, side], xr.at[m, 1 - sy, 1 - side],
                    yx_send.at[m, k], yx_recv.at[m, k],
                ))
                k += 1
        return Hub(items)

    zhub = [Hub(pair(0, zs.at[n], zr.at[n], z_send.at[n], z_recv.at[n])) for n in range(3)]
    zhub2 = Hub(pair(0, zs2, zr2, z_send.at[3], z_recv.at[3]))
    yxhub = [around(n, ys.at[n, 0], ys.at[n, 1], yr.at[n, 0], yr.at[n, 1]) for n in range(4)]
    yxhub2 = around(4, ys2, ys2, yr2.at[0], yr2.at[1])
    fhub = [
        Hub(
            pair(0, fzs.at[n], fzr.at[n], f_send.at[n, 0], f_recv.at[n, 0])
            + pair(1, fys.at[n], fyr.at[n], f_send.at[n, 1], f_recv.at[n, 1])
            + pair(2, fxs.at[n], fxr.at[n], f_send.at[n, 2], f_recv.at[n, 2])
        )
        for n in range(3)
    ]
    hubs = zhub + [zhub2] + yxhub + [yxhub2] + fhub
    for h in hubs:
        h.clear()

    def gauss(d):
        df = d.astype(F32)
        w = jnp.exp(df * df * (-1.0 / 12.5)) * (1.0 / sum(RAW))
        return jnp.where(jnp.abs(d) <= R, w, 0.0)

    def iota(shape, axis):
        return lax.broadcasted_iota(jnp.int32, shape, axis)

    square = (CX, CX)
    bhi, blo = split(gauss(iota(square, 0) - iota(square, 1)))
    bx[0:CX] = bhi
    bx[CX : 2 * CX] = bhi
    bx[2 * CX : 3 * CX] = blo
    k0, k1 = iota((32, CX), 0), iota((32, CX), 1)
    pos = jnp.where(k0 < 16, lax.rem(k0, 8) - 8, CX + lax.rem(k0, 8))
    whi, wlo = split(gauss(pos - k1))
    wx[0:32] = whi
    wx[32:64] = wlo
    rim = ((k1 == 0) & ((k0 == 7) | (k0 == 15))) | ((k1 == CX - 1) & ((k0 == 16) | (k0 == 24)))
    wx[64:96] = jnp.where(rim, 1.0, 0.0).astype(BF16)
    s0, s1 = iota((32, 2 * CX), 0), iota((32, 2 * CX), 1)
    want = jnp.where(s0 < 16, lax.rem(s0, 8), CX - 8 + lax.rem(s0, 8)) + jnp.where(
        lax.rem(s0, 16) < 8, 0, CX
    )
    pick = jnp.where(s1 == want, 1.0, 0.0).astype(BF16)
    pick2 = jnp.where(k1 == jnp.where(k0 < 16, k0, CX - 32 + k0), 1.0, 0.0).astype(BF16)

    wide = (GX, GX * CX)
    spread = jnp.where(iota(wide, 0) == iota(wide, 1) // CX, 1.0, 0.0).astype(BF16)
    for b in range(GY):
        rows = dot(tb_ref[b].astype(F32).astype(BF16), spread, ((0,), (0,)))
        for c in range(GX):
            tbv[b * GX + c] = rows[:, c * CX : (c + 1) * CX]

    def relayout(low, high):
        @pl.loop(low, high)
        def _(c):
            tile_copy(c).wait()
            rows = pl.ds(pl.multiple_of(c * CHUNK, CHUNK), CHUNK)
            block = raw[rows].astype(F32).reshape(CHUNK * ANG, DW)
            for h in range(2):
                tmp[h] = block[:, h * 128 : (h + 1) * 128]
            for a in range(ANG):
                for h in range(2):
                    part = tmp[h, pl.ds(a, CHUNK, stride=ANG), :]
                    mat[rows, a * DW + h * 128 : a * DW + (h + 1) * 128] = part.astype(BF16)

    for c in ld:
        c.wait()
    for a in range(ANG):
        acc[pl.ds(a, 1), :] = obs[0, pl.ds(row_ref[a], 1), :]

    with scope("wait_barrier"):
        pl.semaphore_wait(barrier, BRICKS - 1 + GZ - 1)

    def send_faces(n, src):
        fzs[n, 0] = src[0]
        fzs[n, 1] = src[CZ - 1]
        v = src[...]
        fys[n, 0] = v[:, 0, :]
        fys[n, 1] = v[:, CY - 1, :]
        hi, lo = split(v.reshape(ROWS, CX))
        f = dot(pick, jnp.concatenate([hi, lo], axis=1), ((1,), (1,))).astype(BF16)
        fxs[n, 0] = f[0:16]
        fxs[n, 1] = f[16:32]
        fhub[n].start()

    def send_z(n, src):
        zs[n, 0] = src[0:R].reshape(R * CY, CX).astype(BF16)
        zs[n, 1] = src[CZ - R : CZ].reshape(R * CY, CX).astype(BF16)
        zhub[n].start()

    def taps(at):
        t = TAPS[R] * at(R)
        for k in range(R):
            t += TAPS[k] * (at(k) + at(2 * R - k))
        return t

    def blur_z(n, src, out):
        zbuf[R : R + CZ] = src[...]
        with scope("wait_z"):
            zhub[n].wait_recv()
        zbuf[0:R] = zr[n, 0].astype(F32).reshape(R, CY, CX)
        zbuf[R + CZ : 2 * R + CZ] = zr[n, 1].astype(F32).reshape(R, CY, CX)

        @pl.loop(0, CZ, unroll=2)
        def _(z):
            out[z] = taps(lambda k: zbuf[z + k])

    def send_yx(n, w):
        v = w[...]
        ys[n, 0] = v[:, 0:R, :].reshape(CZ * R, CX).astype(BF16)
        ys[n, 1] = v[:, CY - R :, :].reshape(CZ * R, CX).astype(BF16)
        hi, lo = split(v.reshape(ROWS, CX))
        f = dot(pick, jnp.concatenate([hi, lo], axis=1), ((1,), (1,))).astype(BF16)
        xs[n, 0] = f[0:16]
        xs[n, 1] = f[16:32]
        yxhub[n].start()

    def rows_of(m, slot, weights):
        halo = xr[m, slot].reshape(32, ROWS)
        return dot(jnp.concatenate([halo, halo], axis=0), weights, ((0,), (0,)))

    def own_rows(w, mat3):
        hi, lo = split(w[...].reshape(ROWS, CX))
        both = jnp.concatenate([hi, lo], axis=1)
        return dot(both, mat3[0 : 2 * CX], ((1,), (0,))) + dot(hi, mat3[2 * CX :], ((1,), (0,)))

    def blur_yx(n, w, out):
        own = own_rows(w, bx)
        ybuf[:, R : R + CY, :] = own.reshape(CZ, CY, CX)
        with scope("wait_yx"):
            yxhub[n].wait_recv()
        ybuf[:, R : R + CY, :] += rows_of(n, 1, wx[0:64]).reshape(CZ, CY, CX)
        for side, at in ((0, slice(CY - R, CY)), (1, slice(0, R))):
            y = yr[n, side]
            rows = dot(jnp.concatenate([y, y], axis=1), bx[CX:], ((1,), (0,)))
            more = rows_of(n, 2 * side, wx[0:64]).reshape(CZ, CY, CX)[:, at, :]
            to = slice(0, R) if side == 0 else slice(R + CY, 2 * R + CY)
            ybuf[:, to, :] = rows.reshape(CZ, R, CX) + more

        @pl.loop(0, CZ, unroll=2)
        def _(z):
            out[z] = taps(lambda k: ybuf[z, k : k + CY, :])

    lane, sub = iota((CY, CX), 1), iota((CY, CX), 0)
    ends = ((gz == 0, gz == GZ - 1), (gy == 0, gy == GY - 1), (gx == 0, gx == GX - 1))

    def wait_faces(n):
        with scope("wait_faces"):
            fhub[n].wait_recv()
        xlr[...] = dot(fxr[n].reshape(32, ROWS), wx[64:96], ((0,), (0,))).reshape(CZ, CY, CX)
        xa[0] = fzr[n, 0]
        xa[CZ + 1] = fzr[n, 1]

    def diffs(n, z):
        v = xa[z + 1]
        up, low = xa[z + 2], xa[z]
        yield (
            jnp.where((z == CZ - 1) & ends[0][1], 0.0, up - v),
            jnp.where((z == 0) & ends[0][0], 0.0, v - low),
        )
        up = jnp.where(sub == CY - 1, fyr[n, 1, pl.ds(z, 1), :], pltpu.roll(v, CY - 1, 0))
        low = jnp.where(sub == 0, fyr[n, 0, pl.ds(z, 1), :], pltpu.roll(v, 1, 0))
        yield (
            jnp.where((sub == CY - 1) & ends[1][1], 0.0, up - v),
            jnp.where((sub == 0) & ends[1][0], 0.0, v - low),
        )
        edge = xlr[z]
        up = jnp.where(lane == CX - 1, edge, pltpu.roll(v, CX - 1, 1))
        low = jnp.where(lane == 0, edge, pltpu.roll(v, 1, 1))
        yield (
            jnp.where((lane == CX - 1) & ends[2][1], 0.0, up - v),
            jnp.where((lane == 0) & ends[2][0], 0.0, v - low),
        )

    def fold(p):
        return p[0:8] + p[8:16]

    def redz_copy(n, t):
        return pltpu.make_async_remote_copy(
            red0.at[n], redz.at[n, t], rz_send.at[n, t], rz_recv.at[n, t],
            device_id=(lax.rem(gz + t, GZ), gy, gx), device_id_type=MESH,
        )

    def redx_copy(n, t):
        return pltpu.make_async_remote_copy(
            red1.at[n], redx.at[n, t], rx_send.at[n], rx_recv.at[n],
            device_id=member(t)[1], device_id_type=MESH,
        )

    def send_sums(n, primal, dualres):
        p = jnp.sum(jnp.sum(primal, axis=0, keepdims=True), axis=1, keepdims=True)
        d = jnp.sum(jnp.sum(dualres, axis=0, keepdims=True), axis=1, keepdims=True)
        red0[n] = jnp.where(lane[0:1] < CX // 2, p, d)
        for t in range(1, GZ):
            redz_copy(n, t).start()

    def forward_sums(n):
        total = red0[n]
        for t in range(1, GZ):
            redz_copy(n, t).wait_recv()
            total += redz[n, t]
        red1[n] = total

        for t in range(1, BRICKS):
            redx_copy(n, t).start()

    def factor_of(n, penalty):
        total = red1[n]
        got = redx.at[n, pl.ds(1, BRICKS - 1)]
        pltpu.make_async_copy(got, got, rx_recv.at[n]).wait()
        total += jnp.sum(redx[n, 1:BRICKS], axis=0)
        p = jnp.broadcast_to(total[:, 0:1], (8, CX)) * (1.0 / (3.0 * CELLS))
        d = jnp.broadcast_to(total[:, CX - 1 : CX], (8, CX)) * (1.0 / CELLS)
        d = penalty * penalty * d
        return jnp.sqrt(jnp.sqrt((p + EPS) / (d + EPS)))

    def arrivals(ref, sem):
        got = ref.at[pl.ds(0, BRICKS - 1)]
        pltpu.make_async_copy(got, got, sem).wait()

    def send_block(n, i, src, dst, d, dev):
        pltpu.make_async_remote_copy(
            src.at[n, d], dst.at[n, me], a_send.at[n, i], a_recv.at[n, i],
            device_id=dev, device_id_type=MESH,
        ).start()

    def project(n):
        for z0 in range(1):
            for y in range(CY):
                sl[:, y * CX : (y + 1) * CX] = res[pl.ds(y, CZ, stride=CY), :].astype(BF16)
        with scope("mm_fwd"):
            for a in range(ANG):
                c = dot(sl[...], mat[:, a * DW : (a + 1) * DW], ((1,), (0,)))
                for h in range(2):
                    stage[h, pl.ds(a, CZ, stride=ANG), :] = c[:, h * 128 : (h + 1) * 128]

        def block_of(d):
            rows = pl.ds(pl.multiple_of(d * ANG, ANG), ANG)
            return jnp.concatenate([stage[0, rows, :], stage[1, rows, :]], axis=1).astype(BF16)

        for t in range(1, BRICKS):
            d, dev = member(t)
            snd1[n, d] = block_of(d)
            send_block(n, 0, snd1, rcv1, d, dev)

        rcv1[n, me] = block_of(me)

    def return_misfit(n):
        with scope("wait_a1"):
            arrivals(rcv1.at[n], a_recv.at[n, 0])

        def add(s, sums):
            x = rcv1[n, s].astype(F32)
            t = tbv[s]
            t = jnp.concatenate([t, t], axis=1)
            return tuple(sums[q] + jnp.where(t == float(q), x, 0.0) for q in range(NBLK))

        sums = lax.fori_loop(
            0, BRICKS, add, tuple(jnp.zeros((ANG, DW), F32) for _ in range(NBLK)), unroll=2
        )
        for q in range(NBLK):
            cols = slice(q * DW, (q + 1) * DW)
            mis[:, cols] = (sums[q] - acc[:, cols]).astype(BF16).astype(F32)

        def chosen(d):
            t = tbv[d]
            t = jnp.concatenate([t, t], axis=1)
            c = mis[:, 0:DW]
            for q in range(1, NBLK):
                c = jnp.where(t == float(q), mis[:, q * DW : (q + 1) * DW], c)
            return c.astype(BF16)

        for t in range(1, BRICKS):
            d, dev = member(t)
            snd2[n, d] = chosen(d)
            send_block(n, 1, snd2, rcv2, d, dev)

        rcv2[n, me] = chosen(me)

    def backproject(n, out):
        with scope("wait_a2"):
            arrivals(rcv2.at[n], a_recv.at[n, 1])
        r = rcv2[n].astype(F32).reshape(CZ * ANG, DW)
        for h in range(2):
            stage[h] = r[:, h * 128 : (h + 1) * 128]
        for a in range(ANG):
            for h in range(2):
                sl[:, a * DW + h * 128 : a * DW + (h + 1) * 128] = stage[
                    h, pl.ds(a, CZ, stride=ANG), :
                ].astype(BF16)
        with scope("mm_bwd"):
            for c in range(ANG):
                b = dot(sl[...], mat[c * DW : (c + 1) * DW, :], ((1,), (1,)))
                for h in range(2):
                    res[pl.ds(2 * c + h, CZ, stride=CY), :] = b[:, h * 128 : (h + 1) * 128]
        out[...] = res[...].reshape(CZ, CY, CX)

    send_z(0, x0)
    send_faces(0, x0)
    relayout(0, SPLIT)
    blur_z(0, x0, w1)
    send_yx(0, w1)
    relayout(SPLIT, NCHUNK)
    blur_yx(0, w1, w2)
    res[...] = w2[...].reshape(ROWS, CX)
    project(0)

    wait_faces(0)
    xa[1 : CZ + 1] = x0[...]
    cut = SHRINK

    @pl.loop(0, CZ, unroll=2)
    def _(z):
        smooth = jnp.zeros((CY, CX), F32)
        shrunk = jnp.zeros((CY, CX), F32)
        for j, jm in diffs(0, z):
            s = j - jnp.clip(j, -cut, cut)
            sm = jm - jnp.clip(jm, -cut, cut)
            smooth += jm - j
            shrunk += sm - s
        h = STEP * (smooth - shrunk)
        x0[z] = xa[z + 1] - h
        back[z] = shrunk

    send_z(1, x0)

    shape1, shape2 = (160, 256), (256, CX)
    i, m = iota(shape1, 0), iota(shape1, 1) - 8
    i = jnp.where(i < CX, i, jnp.where(i < CX + 16, i - CX - 16, i - 16))
    inside = ((m >= 0) | (gx > 0)) & ((m < CX) | (gx < GX - 1)) & (m < CX + 8)
    thi, tlo = split(jnp.where(inside, gauss(i - m), 0.0))
    m = iota(shape2, 0) - 8
    uhi, ulo = split(gauss(m - iota(shape2, 1)))
    twice = (
        dot(thi, uhi, ((1,), (0,))) + dot(thi, ulo, ((1,), (0,))) + dot(tlo, uhi, ((1,), (0,)))
    )
    bhi, blo = split(twice[0:CX])
    bx2[0:CX] = bhi
    bx2[CX : 2 * CX] = bhi
    bx2[2 * CX : 3 * CX] = blo
    whi, wlo = split(twice[CX : CX + 32])
    wx2[0:32] = whi
    wx2[32:64] = wlo

    return_misfit(0)
    blur_z(1, x0, w1)
    send_yx(1, w1)
    backproject(0, w2)

    zs2[0] = w2[0:16].reshape(16 * CY, CX).astype(BF16)
    zs2[1] = w2[CZ - 16 : CZ].reshape(16 * CY, CX).astype(BF16)
    zhub2.start()
    blur_yx(1, w1, qbuf)
    zbuf[16 : 16 + CZ] = w2[...]
    with scope("wait_z2"):
        zhub2.wait_recv()
    zbuf[0:16] = zr2[0].astype(F32).reshape(16, CY, CX)
    zbuf[16 + CZ : 32 + CZ] = zr2[1].astype(F32).reshape(16, CY, CX)

    @pl.loop(0, CZ + 16, unroll=2)
    def _(z):
        out = ((z < 8) & ends[0][0]) | ((z >= CZ + 8) & ends[0][1])
        zmid[z] = jnp.where(out, 0.0, taps(lambda k: zbuf[z + k]))

    @pl.loop(0, CZ, unroll=2)
    def _(z):
        w2[z] = taps(lambda k: zmid[z + k])

    hi = w2[...].reshape(ROWS, CX).astype(BF16)
    ys2[...] = hi
    f = dot(pick2, hi, ((1,), (1,))).astype(BF16)
    xs[4, 0] = f[0:16]
    xs[4, 1] = f[16:32]
    yxhub2.start()
    w1[...] = zmid[8 : 8 + CZ]

    ymid[:, 16 : 16 + CY, :] = own_rows(w2, bx2).reshape(CZ, CY, CX)
    with scope("wait_yx2"):
        yxhub2.wait_recv()
    send_yx(2, w1)
    ymid[:, 16 : 16 + CY, :] += rows_of(4, 1, wx2[...]).reshape(CZ, CY, CX)
    for side in range(2):
        y = yr2[side]
        rows = dot(jnp.concatenate([y, y], axis=1), bx2[CX:], ((1,), (0,)))
        rows = rows + rows_of(4, 2 * side, wx2[...])
        ymid[:, 32 * side : 32 * side + 16, :] = rows.reshape(CZ, CY, CX)
    sub2 = iota((CY + 16, CX), 0)
    outside = ((sub2 < 8) & ends[1][0]) | ((sub2 >= CY + 8) & ends[1][1])

    @pl.loop(0, CZ, unroll=2)
    def _(z):
        ybuf[z] = jnp.where(outside, 0.0, taps(lambda k: ymid[z, k : k + CY + 16, :]))

    @pl.loop(0, CZ, unroll=2)
    def _(z):
        rows = pl.ds(pl.multiple_of(z * CY, CY), CY)
        res[rows, :] = qbuf[z] - STEP * taps(lambda k: ybuf[z, k : k + CY, :])

    project(1)
    blur_yx(2, w1, w2)
    x0[...] = x0[...] - STEP * w2[...]
    send_faces(1, x0)
    xa[1 : CZ + 1] = x0[...]
    return_misfit(1)
    wait_faces(1)

    def one(z, sums):
        primal, dres = sums
        smooth = jnp.zeros((CY, CX), F32)
        shrunk = jnp.zeros((CY, CX), F32)
        bdual = jnp.zeros((CY, CX), F32)
        for axis, (j, jm) in enumerate(diffs(1, z)):
            s = j - jnp.clip(j, -cut, cut)
            sm = jm - jnp.clip(jm, -cut, cut)
            d = j - s
            dm = jm - sm
            smooth += jm - j
            shrunk += sm - s
            bdual += dm - d
            dl[axis, z] = d
            dlm[axis, z] = dm
            primal += fold(jnp.square(j - s))
        dres += fold(jnp.square(shrunk - back[z]))
        hterm[z] = smooth - shrunk
        back[z] = shrunk
        bdl[z] = bdual
        return primal, dres

    zero = jnp.zeros((8, CX), F32)
    primal, dres = lax.fori_loop(0, CZ, one, (zero, zero), unroll=2)
    send_sums(0, primal, dres)
    backproject(1, w2)
    send_z(2, w2)
    forward_sums(0)
    blur_z(2, w2, w1)
    send_yx(3, w1)
    penalty = factor_of(0, jnp.ones((8, CX), F32))
    inv1 = 1.0 / penalty
    pen3 = penalty[0:1].reshape(1, 1, CX)
    inv3 = inv1[0:1].reshape(1, 1, CX)
    x0[...] = x0[...] - STEP * pen3 * (hterm[...] + bdl[...] * inv3)
    blur_yx(3, w1, w2)
    x0[...] = x0[...] - STEP * w2[...]
    send_faces(2, x0)
    x_out[...] = x0[...]
    xa[1 : CZ + 1] = x0[...]
    wait_faces(2)
    cut2 = (SHRINK / penalty)[0:1]
    inv = inv1[0:1]

    def last(z, sums):
        primal, dres = sums
        shrunk = jnp.zeros((CY, CX), F32)
        for axis, (j, jm) in enumerate(diffs(2, z)):
            t = j + dl[axis, z] * inv
            tm = jm + dlm[axis, z] * inv
            s = t - jnp.clip(t, -cut2, cut2)
            sm = tm - jnp.clip(tm, -cut2, cut2)
            shrunk += sm - s
            dl[axis, z] = t - s
            primal += fold(jnp.square(j - s))
        dres += fold(jnp.square(shrunk - back[z]))
        return primal, dres

    with scope("last"):
        primal, dres = lax.fori_loop(0, CZ, last, (zero, zero), unroll=2)
    send_sums(1, primal, dres)
    with scope("sums_z"):
        forward_sums(1)
    with scope("sums_x"):
        factor2 = factor_of(1, penalty)
    scale = (1.0 / factor2)[0:1].reshape(1, 1, 1, CX)
    dual_out[...] = dl[...] * scale

    with scope("wait_sends"):
        for h in hubs:
            h.wait_send()
        for n in range(2):
            for i, ref in enumerate((snd1, snd2)):
                arrivals(ref.at[n], a_send.at[n, i])
            for t in range(1, GZ):
                redz_copy(n, t).wait_send()
            got = redx.at[n, pl.ds(1, BRICKS - 1)]
            pltpu.make_async_copy(got, got, rx_send.at[n]).wait()


def body(start, measured, tiles, tile_block, angle_row):
    vm = pltpu.VMEM
    dma = pltpu.SemaphoreType.DMA
    block = vm((CZ, CY, CX), F32)
    return pl.pallas_call(
        kernel,
        out_shape=(
            pltpu.VMEM((CZ, CY, CX), F32),
            pltpu.VMEM((3, CZ, CY, CX), F32),
        ),
        in_specs=[
            pl.BlockSpec(memory_space=pltpu.HBM),
            pl.BlockSpec(memory_space=pltpu.HBM),
            pl.BlockSpec(memory_space=pltpu.HBM),
            pl.BlockSpec(memory_space=pltpu.VMEM),
            pl.BlockSpec(memory_space=pltpu.SMEM),
        ],
        out_specs=(pl.BlockSpec(memory_space=pltpu.VMEM), pl.BlockSpec(memory_space=pltpu.VMEM)),
        scratch_shapes=[
            vm((V, ANG, DW), BF16),
            vm((V, ANG * DW), BF16),
            vm((2, CHUNK * ANG, 128), F32),
            block, block, block,
            vm((ROWS, CX), F32),
            block,
            vm((CZ + 2, CY, CX), F32),
            vm((CZ + 32, CY, CX), F32),
            vm((CZ + 16, CY, CX), F32),
            vm((CZ, CY + 16, CX), F32),
            vm((CZ, CY + 32, CX), F32),
            vm((BRICKS, ANG, CX), F32),
            vm((1, ANG, NBLK * DW), F32),
            vm((ANG, NBLK * DW), F32),
            vm((ANG, NBLK * DW), F32),
            vm((3, 2, R * CY, CX), BF16),
            vm((3, 2, R * CY, CX), BF16),
            vm((2, 16 * CY, CX), BF16),
            vm((2, 16 * CY, CX), BF16),
            vm((4, 2, CZ * R, CX), BF16),
            vm((4, 2, CZ * R, CX), BF16),
            vm((ROWS, CX), BF16),
            vm((2, ROWS, CX), BF16),
            vm((5, 2, 16, ROWS), BF16),
            vm((5, 3, 2, 16, ROWS), BF16),
            vm((3, 2, CY, CX), F32),
            vm((3, 2, CY, CX), F32),
            vm((3, 2, CZ, CX), F32),
            vm((3, 2, CZ, CX), F32),
            vm((3, 2, 16, ROWS), BF16),
            vm((3, 2, 16, ROWS), BF16),
            vm((2, CZ * ANG, 128), F32),
            vm((CZ, V), BF16),
            vm((2, BRICKS, ANG, DW), BF16),
            vm((2, BRICKS, ANG, DW), BF16),
            vm((2, BRICKS, ANG, DW), BF16),
            vm((2, BRICKS, ANG, DW), BF16),
            block, block,
            vm((3, CZ, CY, CX), F32),
            vm((3, CZ, CY, CX), F32),
            block, block,
            vm((2, 1, CX), F32),
            vm((2, GZ, 1, CX), F32),
            vm((2, 1, CX), F32),
            vm((2, BRICKS, 1, CX), F32),
            vm((3 * CX, CX), BF16),
            vm((96, CX), BF16),
            vm((3 * CX, CX), BF16),
            vm((64, CX), BF16),
            dma((2,)),
            dma((NCHUNK,)),
            dma((4, 2)),
            dma((4, 2)),
            dma((5, 8)),
            dma((5, 8)),
            dma((3, 3, 2)),
            dma((3, 3, 2)),
            dma((2, 2)),
            dma((2, 2)),
            dma((2, GZ)),
            dma((2, GZ)),
            dma((2,)),
            dma((2,)),
        ],
        compiler_params=pltpu.CompilerParams(
            collective_id=0, has_side_effects=True, vmem_limit_bytes=60 * 1024 * 1024
        ),
    )(start, measured, tiles, tile_block, angle_row)


def solution(mesh):
    return jax.shard_map(
        body,
        mesh=mesh,
        in_specs=(
            P("gz", "gy", "gx"),
            P(("gz", "gy", "gx"), None, None),
            P("gy", None, "gx"),
            P(),
            P(),
        ),
        out_specs=(P("gz", "gy", "gx"), P(None, "gz", "gy", "gx")),
        check_vma=False,
    )
```

```python
import math

import jax
import jax.numpy as jnp
from jax import lax
from jax.experimental import pallas as pl
from jax.experimental.pallas import tpu as pltpu
from jax.sharding import PartitionSpec as P

CZ, CY, CX = 32, 16, 128
ROWS = CZ * CY
ANG, DW, NBLK = 8, 256, 4
V = CY * CX
R = 8
GZ, GY, GX = 4, 4, 8
BRICKS = GY * GX
CELLS = float(CZ * CY * CX * GZ * BRICKS)
MESH = pl.DeviceIdType.MESH
F32, BF16 = jnp.float32, jnp.bfloat16
STEP = 0.5
SHRINK = 0.2
EPS = 1e-6
CHUNK = 128
NCHUNK = V // CHUNK
ORDER = sorted(
    ((dx, dz, dc) for dz in range(4) for dx in range(4) for dc in range(2) if dx or dz or dc),
    key=lambda s: -(min(s[0], 4 - s[0]) + min(s[1], 4 - s[1])),
)
SPLIT = 5
ORDER_ALL = sorted(
    ((dy, t) for dy in range(GZ) for t in range(GY * GX) if dy or t),
    key=lambda s: -(
        min(s[0], 4 - s[0])
        + (sum(min(d, 4 - d) for d in ORDER[s[1] - 1][:2]) if s[1] else 0)
    ),
)

RAW = [math.exp(-k * k / 12.5) for k in range(-R, R + 1)]
TAPS = [r / sum(RAW) for r in RAW]


def dot(a, b, dims):
    return lax.dot_general(a, b, (dims, ((), ())), preferred_element_type=F32)


def split(v):
    hi = v.astype(BF16)
    lo = (v - hi.astype(F32)).astype(BF16)
    return hi, lo


def kernel(
    start_ref, meas_ref, tiles_ref, tb_ref, row_ref,
    x_out, dual_out,
    raw, mat, tmp, x0, w1, w2, res, qbuf, xa, zbuf, zmid, ybuf, ymid, tbv, obs, mis, acc,
    zs, zr, zs2, zr2, ys, yr, ys2, yr2, xs, xr,
    fzs, fzr, fys, fyr, fxs, fxr,
    stage, sl, snd1, rcv1, snd2, rcv2,
    hterm, back, dl, dlm, xlr, bdl,
    red0, redz, red1, redx, redall,
    bx, wx, bx2, wx2,
    load_sem, tile_sem, z_send, z_recv, yx_send, yx_recv, f_send, f_recv,
    a_send, a_recv, rz_send, rz_recv, rx_send, rx_recv, all_send, all_recv,
):
    gz, gy, gx = lax.axis_index("gz"), lax.axis_index("gy"), lax.axis_index("gx")
    me = gy * GX + gx
    scope = jax.named_scope

    barrier = pltpu.get_barrier_semaphore()

    chip_x = 2 * (gy // 2) + lax.rem(gx, 2)
    chip_z, core = gx // 2, lax.rem(gy, 2)

    def member(t):
        dx, dz, dc = ORDER[t - 1]
        x = lax.rem(chip_x + dx, 4)
        z = lax.rem(chip_z + dz, 4)
        y = 2 * (x // 2) + lax.rem(core + dc, 2)
        x = 2 * z + lax.rem(x, 2)
        return y * GX + x, (gz, y, x)

    for t in range(1, BRICKS):
        pl.semaphore_signal(barrier, inc=1, device_id=member(t)[1], device_id_type=MESH)

    @pl.loop(1, GZ)
    def _(t):
        pl.semaphore_signal(
            barrier, inc=1, device_id=(lax.rem(gz + t, GZ), gy, gx), device_id_type=MESH
        )

    ld = [
        pltpu.make_async_copy(start_ref, x0, load_sem.at[0]),
        pltpu.make_async_copy(meas_ref, obs, load_sem.at[1]),
    ]
    for c in ld:
        c.start()

    def tile_copy(c):
        rows = pl.ds(pl.multiple_of(c * CHUNK, CHUNK), CHUNK)
        return pltpu.make_async_copy(tiles_ref.at[rows], raw.at[rows], tile_sem.at[c])

    @pl.loop(0, NCHUNK)
    def _(c):
        tile_copy(c).start()

    def there(dz, dy, dx):
        ok = True
        for d, at, n in ((dz, gz, GZ), (dy, gy, GY), (dx, gx, GX)):
            if d:
                near = at > 0 if d < 0 else at < n - 1
                ok = near if ok is True else jnp.logical_and(ok, near)
        return ok

    class Hub:
        def __init__(self, items):
            self.items = [
                (
                    there(*d),
                    there(*(-i for i in d)),
                    pltpu.make_async_remote_copy(
                        src, dst, ss, rs,
                        device_id=(gz + d[0], gy + d[1], gx + d[2]), device_id_type=MESH,
                    ),
                    dst,
                )
                for d, src, dst, ss, rs in items
            ]

        def clear(self):
            for _, arrives, _, dst in self.items:

                @pl.when(jnp.logical_not(arrives))
                def _():
                    dst[...] = jnp.zeros(dst.shape, dst.dtype)

        def start(self):
            for leaves, _, copy, _ in self.items:
                pl.when(leaves)(copy.start)

        def wait_recv(self):
            for _, arrives, copy, _ in self.items:
                pl.when(arrives)(copy.wait_recv)

        def wait_send(self):
            for leaves, _, copy, _ in self.items:
                pl.when(leaves)(copy.wait_send)

    def pair(axis, src, dst, send, recv):
        unit = [int(axis == a) for a in range(3)]
        return [
            ([-u for u in unit], src.at[0], dst.at[1], send.at[0], recv.at[0]),
            (unit, src.at[1], dst.at[0], send.at[1], recv.at[1]),
        ]

    def around(m, low, high, into_low, into_high):
        items = [
            ((0, -1, 0), low, into_high, yx_send.at[m, 0], yx_recv.at[m, 0]),
            ((0, 1, 0), high, into_low, yx_send.at[m, 1], yx_recv.at[m, 1]),
        ]
        k = 2
        for sy in (0, -1, 1):
            for side, sx in ((0, -1), (1, 1)):
                items.append((
                    (0, sy, sx), xs.at[m, side], xr.at[m, 1 - sy, 1 - side],
                    yx_send.at[m, k], yx_recv.at[m, k],
                ))
                k += 1
        return Hub(items)

    zhub = [Hub(pair(0, zs.at[n], zr.at[n], z_send.at[n], z_recv.at[n])) for n in range(3)]
    zhub2 = Hub(pair(0, zs2, zr2, z_send.at[3], z_recv.at[3]))
    yxhub = [around(n, ys.at[n, 0], ys.at[n, 1], yr.at[n, 0], yr.at[n, 1]) for n in range(4)]
    yxhub2 = around(4, ys2, ys2, yr2.at[0], yr2.at[1])
    fhub = [
        Hub(
            pair(0, fzs.at[n], fzr.at[n], f_send.at[n, 0], f_recv.at[n, 0])
            + pair(1, fys.at[n], fyr.at[n], f_send.at[n, 1], f_recv.at[n, 1])
            + pair(2, fxs.at[n], fxr.at[n], f_send.at[n, 2], f_recv.at[n, 2])
        )
        for n in range(3)
    ]
    hubs = zhub + [zhub2] + yxhub + [yxhub2] + fhub
    for h in hubs:
        h.clear()

    def gauss(d):
        df = d.astype(F32)
        w = jnp.exp(df * df * (-1.0 / 12.5)) * (1.0 / sum(RAW))
        return jnp.where(jnp.abs(d) <= R, w, 0.0)

    def iota(shape, axis):
        return lax.broadcasted_iota(jnp.int32, shape, axis)

    square = (CX, CX)
    bhi, blo = split(gauss(iota(square, 0) - iota(square, 1)))
    bx[0:CX] = bhi
    bx[CX : 2 * CX] = bhi
    bx[2 * CX : 3 * CX] = blo
    k0, k1 = iota((32, CX), 0), iota((32, CX), 1)
    pos = jnp.where(k0 < 16, lax.rem(k0, 8) - 8, CX + lax.rem(k0, 8))
    whi, wlo = split(gauss(pos - k1))
    wx[0:32] = whi
    wx[32:64] = wlo
    rim = ((k1 == 0) & ((k0 == 7) | (k0 == 15))) | ((k1 == CX - 1) & ((k0 == 16) | (k0 == 24)))
    wx[64:96] = jnp.where(rim, 1.0, 0.0).astype(BF16)
    s0, s1 = iota((32, 2 * CX), 0), iota((32, 2 * CX), 1)
    want = jnp.where(s0 < 16, lax.rem(s0, 8), CX - 8 + lax.rem(s0, 8)) + jnp.where(
        lax.rem(s0, 16) < 8, 0, CX
    )
    pick = jnp.where(s1 == want, 1.0, 0.0).astype(BF16)
    pick2 = jnp.where(k1 == jnp.where(k0 < 16, k0, CX - 32 + k0), 1.0, 0.0).astype(BF16)

    wide = (GX, GX * CX)
    spread = jnp.where(iota(wide, 0) == iota(wide, 1) // CX, 1.0, 0.0).astype(BF16)
    for b in range(GY):
        rows = dot(tb_ref[b].astype(F32).astype(BF16), spread, ((0,), (0,)))
        for c in range(GX):
            tbv[b * GX + c] = rows[:, c * CX : (c + 1) * CX]

    def relayout(low, high):
        @pl.loop(low, high)
        def _(c):
            tile_copy(c).wait()
            rows = pl.ds(pl.multiple_of(c * CHUNK, CHUNK), CHUNK)
            block = raw[rows].astype(F32).reshape(CHUNK * ANG, DW)
            for h in range(2):
                tmp[h] = block[:, h * 128 : (h + 1) * 128]
            for a in range(ANG):
                for h in range(2):
                    part = tmp[h, pl.ds(a, CHUNK, stride=ANG), :]
                    mat[rows, a * DW + h * 128 : a * DW + (h + 1) * 128] = part.astype(BF16)

    for c in ld:
        c.wait()
    for a in range(ANG):
        acc[pl.ds(a, 1), :] = obs[0, pl.ds(row_ref[a], 1), :]

    with scope("wait_barrier"):
        pl.semaphore_wait(barrier, BRICKS - 1 + GZ - 1)

    def send_faces(n, src):
        fzs[n, 0] = src[0]
        fzs[n, 1] = src[CZ - 1]
        v = src[...]
        fys[n, 0] = v[:, 0, :]
        fys[n, 1] = v[:, CY - 1, :]
        hi, lo = split(v.reshape(ROWS, CX))
        f = dot(pick, jnp.concatenate([hi, lo], axis=1), ((1,), (1,))).astype(BF16)
        fxs[n, 0] = f[0:16]
        fxs[n, 1] = f[16:32]
        fhub[n].start()

    def send_z(n, src):
        zs[n, 0] = src[0:R].reshape(R * CY, CX).astype(BF16)
        zs[n, 1] = src[CZ - R : CZ].reshape(R * CY, CX).astype(BF16)
        zhub[n].start()

    def taps(at):
        t = TAPS[R] * at(R)
        for k in range(R):
            t += TAPS[k] * (at(k) + at(2 * R - k))
        return t

    def blur_z(n, src, out):
        zbuf[R : R + CZ] = src[...]
        with scope("wait_z"):
            zhub[n].wait_recv()
        zbuf[0:R] = zr[n, 0].astype(F32).reshape(R, CY, CX)
        zbuf[R + CZ : 2 * R + CZ] = zr[n, 1].astype(F32).reshape(R, CY, CX)

        @pl.loop(0, CZ, unroll=2)
        def _(z):
            out[z] = taps(lambda k: zbuf[z + k])

    def send_yx(n, w):
        v = w[...]
        ys[n, 0] = v[:, 0:R, :].reshape(CZ * R, CX).astype(BF16)
        ys[n, 1] = v[:, CY - R :, :].reshape(CZ * R, CX).astype(BF16)
        hi, lo = split(v.reshape(ROWS, CX))
        f = dot(pick, jnp.concatenate([hi, lo], axis=1), ((1,), (1,))).astype(BF16)
        xs[n, 0] = f[0:16]
        xs[n, 1] = f[16:32]
        yxhub[n].start()

    def rows_of(m, slot, weights):
        halo = xr[m, slot].reshape(32, ROWS)
        return dot(jnp.concatenate([halo, halo], axis=0), weights, ((0,), (0,)))

    def own_rows(w, mat3):
        hi, lo = split(w[...].reshape(ROWS, CX))
        both = jnp.concatenate([hi, lo], axis=1)
        return dot(both, mat3[0 : 2 * CX], ((1,), (0,))) + dot(hi, mat3[2 * CX :], ((1,), (0,)))

    def blur_yx(n, w, out):
        own = own_rows(w, bx)
        ybuf[:, R : R + CY, :] = own.reshape(CZ, CY, CX)
        with scope("wait_yx"):
            yxhub[n].wait_recv()
        ybuf[:, R : R + CY, :] += rows_of(n, 1, wx[0:64]).reshape(CZ, CY, CX)
        for side, at in ((0, slice(CY - R, CY)), (1, slice(0, R))):
            y = yr[n, side]
            rows = dot(jnp.concatenate([y, y], axis=1), bx[CX:], ((1,), (0,)))
            more = rows_of(n, 2 * side, wx[0:64]).reshape(CZ, CY, CX)[:, at, :]
            to = slice(0, R) if side == 0 else slice(R + CY, 2 * R + CY)
            ybuf[:, to, :] = rows.reshape(CZ, R, CX) + more

        @pl.loop(0, CZ, unroll=2)
        def _(z):
            out[z] = taps(lambda k: ybuf[z, k : k + CY, :])

    lane, sub = iota((CY, CX), 1), iota((CY, CX), 0)
    ends = ((gz == 0, gz == GZ - 1), (gy == 0, gy == GY - 1), (gx == 0, gx == GX - 1))

    def wait_faces(n):
        with scope("wait_faces"):
            fhub[n].wait_recv()
        xlr[...] = dot(fxr[n].reshape(32, ROWS), wx[64:96], ((0,), (0,))).reshape(CZ, CY, CX)
        xa[0] = fzr[n, 0]
        xa[CZ + 1] = fzr[n, 1]

    def diffs(n, z):
        v = xa[z + 1]
        up, low = xa[z + 2], xa[z]
        yield (
            jnp.where((z == CZ - 1) & ends[0][1], 0.0, up - v),
            jnp.where((z == 0) & ends[0][0], 0.0, v - low),
        )
        up = jnp.where(sub == CY - 1, fyr[n, 1, pl.ds(z, 1), :], pltpu.roll(v, CY - 1, 0))
        low = jnp.where(sub == 0, fyr[n, 0, pl.ds(z, 1), :], pltpu.roll(v, 1, 0))
        yield (
            jnp.where((sub == CY - 1) & ends[1][1], 0.0, up - v),
            jnp.where((sub == 0) & ends[1][0], 0.0, v - low),
        )
        edge = xlr[z]
        up = jnp.where(lane == CX - 1, edge, pltpu.roll(v, CX - 1, 1))
        low = jnp.where(lane == 0, edge, pltpu.roll(v, 1, 1))
        yield (
            jnp.where((lane == CX - 1) & ends[2][1], 0.0, up - v),
            jnp.where((lane == 0) & ends[2][0], 0.0, v - low),
        )

    def fold(p):
        return p[0:8] + p[8:16]

    def redz_copy(n, t):
        return pltpu.make_async_remote_copy(
            red0.at[n], redz.at[n, t], rz_send.at[n, t], rz_recv.at[n, t],
            device_id=(lax.rem(gz + t, GZ), gy, gx), device_id_type=MESH,
        )

    def redx_copy(n, t):
        return pltpu.make_async_remote_copy(
            red1.at[n], redx.at[n, t], rx_send.at[n], rx_recv.at[n],
            device_id=member(t)[1], device_id_type=MESH,
        )

    def put_sums(n, primal, dualres):
        p = jnp.sum(jnp.sum(primal, axis=0, keepdims=True), axis=1, keepdims=True)
        d = jnp.sum(jnp.sum(dualres, axis=0, keepdims=True), axis=1, keepdims=True)
        red0[n] = jnp.where(lane[0:1] < CX // 2, p, d)

    def send_all():
        for slot, (dy, t) in enumerate(ORDER_ALL):
            dev = (gy, gx) if t == 0 else member(t)[1][1:]
            pltpu.make_async_remote_copy(
                red0.at[1], redall.at[slot + 1], all_send, all_recv,
                device_id=(lax.rem(gz + dy, GZ), *dev), device_id_type=MESH,
            ).start()

    def forward_sums(n):
        total = red0[n]
        for t in range(1, GZ):
            redz_copy(n, t).wait_recv()
            total += redz[n, t]
        red1[n] = total

        for t in range(1, BRICKS):
            redx_copy(n, t).start()

    def factor_of(n, penalty):
        total = red1[n]
        got = redx.at[n, pl.ds(1, BRICKS - 1)]
        pltpu.make_async_copy(got, got, rx_recv.at[n]).wait()
        total += jnp.sum(redx[n, 1:BRICKS], axis=0)
        return factor_from(total, penalty)

    def factor_from(total, penalty):
        p = jnp.broadcast_to(total[:, 0:1], (8, CX)) * (1.0 / (3.0 * CELLS))
        d = jnp.broadcast_to(total[:, CX - 1 : CX], (8, CX)) * (1.0 / CELLS)
        d = penalty * penalty * d
        return jnp.sqrt(jnp.sqrt((p + EPS) / (d + EPS)))

    def arrivals(ref, sem):
        got = ref.at[pl.ds(0, BRICKS - 1)]
        pltpu.make_async_copy(got, got, sem).wait()

    def send_block(n, i, src, dst, d, dev):
        pltpu.make_async_remote_copy(
            src.at[n, d], dst.at[n, me], a_send.at[n, i], a_recv.at[n, i],
            device_id=dev, device_id_type=MESH,
        ).start()

    def project(n):
        for z0 in range(1):
            for y in range(CY):
                sl[:, y * CX : (y + 1) * CX] = res[pl.ds(y, CZ, stride=CY), :].astype(BF16)
        with scope("mm_fwd"):
            for a in range(ANG):
                c = dot(sl[...], mat[:, a * DW : (a + 1) * DW], ((1,), (0,)))
                for h in range(2):
                    stage[h, pl.ds(a, CZ, stride=ANG), :] = c[:, h * 128 : (h + 1) * 128]

        def block_of(d):
            rows = pl.ds(pl.multiple_of(d * ANG, ANG), ANG)
            return jnp.concatenate([stage[0, rows, :], stage[1, rows, :]], axis=1).astype(BF16)

        for t in range(1, BRICKS):
            d, dev = member(t)
            snd1[n, d] = block_of(d)
            send_block(n, 0, snd1, rcv1, d, dev)

        rcv1[n, me] = block_of(me)

    def return_misfit(n):
        with scope("wait_a1"):
            arrivals(rcv1.at[n], a_recv.at[n, 0])

        def add(s, sums):
            x = rcv1[n, s].astype(F32)
            t = tbv[s]
            t = jnp.concatenate([t, t], axis=1)
            return tuple(sums[q] + jnp.where(t == float(q), x, 0.0) for q in range(NBLK))

        sums = lax.fori_loop(
            0, BRICKS, add, tuple(jnp.zeros((ANG, DW), F32) for _ in range(NBLK)), unroll=2
        )
        for q in range(NBLK):
            cols = slice(q * DW, (q + 1) * DW)
            mis[:, cols] = (sums[q] - acc[:, cols]).astype(BF16).astype(F32)

        def chosen(d):
            t = tbv[d]
            t = jnp.concatenate([t, t], axis=1)
            c = mis[:, 0:DW]
            for q in range(1, NBLK):
                c = jnp.where(t == float(q), mis[:, q * DW : (q + 1) * DW], c)
            return c.astype(BF16)

        for t in range(1, BRICKS):
            d, dev = member(t)
            snd2[n, d] = chosen(d)
            send_block(n, 1, snd2, rcv2, d, dev)

        rcv2[n, me] = chosen(me)

    def backproject(n, out):
        with scope("wait_a2"):
            arrivals(rcv2.at[n], a_recv.at[n, 1])
        r = rcv2[n].astype(F32).reshape(CZ * ANG, DW)
        for h in range(2):
            stage[h] = r[:, h * 128 : (h + 1) * 128]
        for a in range(ANG):
            for h in range(2):
                sl[:, a * DW + h * 128 : a * DW + (h + 1) * 128] = stage[
                    h, pl.ds(a, CZ, stride=ANG), :
                ].astype(BF16)
        with scope("mm_bwd"):
            for c in range(ANG):
                b = dot(sl[...], mat[c * DW : (c + 1) * DW, :], ((1,), (1,)))
                for h in range(2):
                    res[pl.ds(2 * c + h, CZ, stride=CY), :] = b[:, h * 128 : (h + 1) * 128]
        out[...] = res[...].reshape(CZ, CY, CX)

    send_z(0, x0)
    send_faces(0, x0)
    relayout(0, SPLIT)
    blur_z(0, x0, w1)
    send_yx(0, w1)
    relayout(SPLIT, NCHUNK)
    blur_yx(0, w1, w2)
    res[...] = w2[...].reshape(ROWS, CX)
    project(0)

    wait_faces(0)
    xa[1 : CZ + 1] = x0[...]
    cut = SHRINK

    @pl.loop(0, CZ, unroll=2)
    def _(z):
        smooth = jnp.zeros((CY, CX), F32)
        shrunk = jnp.zeros((CY, CX), F32)
        for j, jm in diffs(0, z):
            s = j - jnp.clip(j, -cut, cut)
            sm = jm - jnp.clip(jm, -cut, cut)
            smooth += jm - j
            shrunk += sm - s
        h = STEP * (smooth - shrunk)
        x0[z] = xa[z + 1] - h
        back[z] = shrunk

    send_z(1, x0)

    shape1, shape2 = (160, 256), (256, CX)
    i, m = iota(shape1, 0), iota(shape1, 1) - 8
    i = jnp.where(i < CX, i, jnp.where(i < CX + 16, i - CX - 16, i - 16))
    inside = ((m >= 0) | (gx > 0)) & ((m < CX) | (gx < GX - 1)) & (m < CX + 8)
    thi, tlo = split(jnp.where(inside, gauss(i - m), 0.0))
    m = iota(shape2, 0) - 8
    uhi, ulo = split(gauss(m - iota(shape2, 1)))
    twice = (
        dot(thi, uhi, ((1,), (0,))) + dot(thi, ulo, ((1,), (0,))) + dot(tlo, uhi, ((1,), (0,)))
    )
    bhi, blo = split(twice[0:CX])
    bx2[0:CX] = bhi
    bx2[CX : 2 * CX] = bhi
    bx2[2 * CX : 3 * CX] = blo
    whi, wlo = split(twice[CX : CX + 32])
    wx2[0:32] = whi
    wx2[32:64] = wlo

    return_misfit(0)
    blur_z(1, x0, w1)
    send_yx(1, w1)
    backproject(0, w2)

    zs2[0] = w2[0:16].reshape(16 * CY, CX).astype(BF16)
    zs2[1] = w2[CZ - 16 : CZ].reshape(16 * CY, CX).astype(BF16)
    zhub2.start()
    blur_yx(1, w1, qbuf)
    zbuf[16 : 16 + CZ] = w2[...]
    with scope("wait_z2"):
        zhub2.wait_recv()
    zbuf[0:16] = zr2[0].astype(F32).reshape(16, CY, CX)
    zbuf[16 + CZ : 32 + CZ] = zr2[1].astype(F32).reshape(16, CY, CX)

    @pl.loop(0, CZ + 16, unroll=2)
    def _(z):
        out = ((z < 8) & ends[0][0]) | ((z >= CZ + 8) & ends[0][1])
        zmid[z] = jnp.where(out, 0.0, taps(lambda k: zbuf[z + k]))

    @pl.loop(0, CZ, unroll=2)
    def _(z):
        w2[z] = taps(lambda k: zmid[z + k])

    hi = w2[...].reshape(ROWS, CX).astype(BF16)
    ys2[...] = hi
    f = dot(pick2, hi, ((1,), (1,))).astype(BF16)
    xs[4, 0] = f[0:16]
    xs[4, 1] = f[16:32]
    yxhub2.start()
    w1[...] = zmid[8 : 8 + CZ]

    ymid[:, 16 : 16 + CY, :] = own_rows(w2, bx2).reshape(CZ, CY, CX)
    with scope("wait_yx2"):
        yxhub2.wait_recv()
    send_yx(2, w1)
    ymid[:, 16 : 16 + CY, :] += rows_of(4, 1, wx2[...]).reshape(CZ, CY, CX)
    for side in range(2):
        y = yr2[side]
        rows = dot(jnp.concatenate([y, y], axis=1), bx2[CX:], ((1,), (0,)))
        rows = rows + rows_of(4, 2 * side, wx2[...])
        ymid[:, 32 * side : 32 * side + 16, :] = rows.reshape(CZ, CY, CX)
    sub2 = iota((CY + 16, CX), 0)
    outside = ((sub2 < 8) & ends[1][0]) | ((sub2 >= CY + 8) & ends[1][1])

    @pl.loop(0, CZ, unroll=2)
    def _(z):
        ybuf[z] = jnp.where(outside, 0.0, taps(lambda k: ymid[z, k : k + CY + 16, :]))

    @pl.loop(0, CZ, unroll=2)
    def _(z):
        rows = pl.ds(pl.multiple_of(z * CY, CY), CY)
        res[rows, :] = qbuf[z] - STEP * taps(lambda k: ybuf[z, k : k + CY, :])

    project(1)
    blur_yx(2, w1, w2)
    x0[...] = x0[...] - STEP * w2[...]
    send_faces(1, x0)
    xa[1 : CZ + 1] = x0[...]
    return_misfit(1)
    wait_faces(1)

    def one(z, sums):
        primal, dres = sums
        smooth = jnp.zeros((CY, CX), F32)
        shrunk = jnp.zeros((CY, CX), F32)
        bdual = jnp.zeros((CY, CX), F32)
        for axis, (j, jm) in enumerate(diffs(1, z)):
            s = j - jnp.clip(j, -cut, cut)
            sm = jm - jnp.clip(jm, -cut, cut)
            d = j - s
            dm = jm - sm
            smooth += jm - j
            shrunk += sm - s
            bdual += dm - d
            dl[axis, z] = d
            dlm[axis, z] = dm
            primal += fold(jnp.square(j - s))
        dres += fold(jnp.square(shrunk - back[z]))
        hterm[z] = smooth - shrunk
        back[z] = shrunk
        bdl[z] = bdual
        return primal, dres

    zero = jnp.zeros((8, CX), F32)
    primal, dres = lax.fori_loop(0, CZ, one, (zero, zero), unroll=2)
    put_sums(0, primal, dres)
    for t in range(1, GZ):
        redz_copy(0, t).start()
    backproject(1, w2)
    send_z(2, w2)
    forward_sums(0)
    blur_z(2, w2, w1)
    send_yx(3, w1)
    penalty = factor_of(0, jnp.ones((8, CX), F32))
    inv1 = 1.0 / penalty
    pen3 = penalty[0:1].reshape(1, 1, CX)
    inv3 = inv1[0:1].reshape(1, 1, CX)
    x0[...] = x0[...] - STEP * pen3 * (hterm[...] + bdl[...] * inv3)
    dl[...] = dl[...] * inv3
    dlm[...] = dlm[...] * inv3
    blur_yx(3, w1, w2)
    x0[...] = x0[...] - STEP * w2[...]
    send_faces(2, x0)
    x_out[...] = x0[...]
    xa[1 : CZ + 1] = x0[...]
    wait_faces(2)
    cut2 = (SHRINK / penalty)[0:1]

    def last(z, sums):
        primal, dres = sums
        shrunk = jnp.zeros((CY, CX), F32)
        for axis, (j, jm) in enumerate(diffs(2, z)):
            t = j + dl[axis, z]
            tm = jm + dlm[axis, z]
            s = t - jnp.clip(t, -cut2, cut2)
            sm = tm - jnp.clip(tm, -cut2, cut2)
            shrunk += sm - s
            dl[axis, z] = t - s
            primal += fold(jnp.square(j - s))
        dres += fold(jnp.square(shrunk - back[z]))
        return primal, dres

    with scope("last"):
        primal, dres = lax.fori_loop(0, CZ, last, (zero, zero), unroll=4)
    put_sums(1, primal, dres)
    send_all()
    with scope("sums"):
        got = redall.at[pl.ds(1, GZ * BRICKS - 1)]
        pltpu.make_async_copy(got, got, all_recv).wait()
    factor2 = factor_from(red0[1] + jnp.sum(redall[1 : GZ * BRICKS], axis=0), penalty)
    scale = (1.0 / factor2)[0:1].reshape(1, 1, 1, CX)
    with scope("scale"):
        dual_out[...] = dl[...] * scale

    with scope("wait_sends"):
        for h in hubs:
            h.wait_send()
        for n in range(2):
            for i, ref in enumerate((snd1, snd2)):
                arrivals(ref.at[n], a_send.at[n, i])
        for t in range(1, GZ):
            redz_copy(0, t).wait_send()
        got = redx.at[0, pl.ds(1, BRICKS - 1)]
        pltpu.make_async_copy(got, got, rx_send.at[0]).wait()
        got = redall.at[pl.ds(1, GZ * BRICKS - 1)]
        pltpu.make_async_copy(got, got, all_send).wait()


def body(start, measured, tiles, tile_block, angle_row):
    vm = pltpu.VMEM
    dma = pltpu.SemaphoreType.DMA
    block = vm((CZ, CY, CX), F32)
    return pl.pallas_call(
        kernel,
        out_shape=(
            pltpu.VMEM((CZ, CY, CX), F32),
            pltpu.VMEM((3, CZ, CY, CX), F32),
        ),
        in_specs=[
            pl.BlockSpec(memory_space=pltpu.HBM),
            pl.BlockSpec(memory_space=pltpu.HBM),
            pl.BlockSpec(memory_space=pltpu.HBM),
            pl.BlockSpec(memory_space=pltpu.VMEM),
            pl.BlockSpec(memory_space=pltpu.SMEM),
        ],
        out_specs=(pl.BlockSpec(memory_space=pltpu.VMEM), pl.BlockSpec(memory_space=pltpu.VMEM)),
        scratch_shapes=[
            vm((V, ANG, DW), BF16),
            vm((V, ANG * DW), BF16),
            vm((2, CHUNK * ANG, 128), F32),
            block, block, block,
            vm((ROWS, CX), F32),
            block,
            vm((CZ + 2, CY, CX), F32),
            vm((CZ + 32, CY, CX), F32),
            vm((CZ + 16, CY, CX), F32),
            vm((CZ, CY + 16, CX), F32),
            vm((CZ, CY + 32, CX), F32),
            vm((BRICKS, ANG, CX), F32),
            vm((1, ANG, NBLK * DW), F32),
            vm((ANG, NBLK * DW), F32),
            vm((ANG, NBLK * DW), F32),
            vm((3, 2, R * CY, CX), BF16),
            vm((3, 2, R * CY, CX), BF16),
            vm((2, 16 * CY, CX), BF16),
            vm((2, 16 * CY, CX), BF16),
            vm((4, 2, CZ * R, CX), BF16),
            vm((4, 2, CZ * R, CX), BF16),
            vm((ROWS, CX), BF16),
            vm((2, ROWS, CX), BF16),
            vm((5, 2, 16, ROWS), BF16),
            vm((5, 3, 2, 16, ROWS), BF16),
            vm((3, 2, CY, CX), F32),
            vm((3, 2, CY, CX), F32),
            vm((3, 2, CZ, CX), F32),
            vm((3, 2, CZ, CX), F32),
            vm((3, 2, 16, ROWS), BF16),
            vm((3, 2, 16, ROWS), BF16),
            vm((2, CZ * ANG, 128), F32),
            vm((CZ, V), BF16),
            vm((2, BRICKS, ANG, DW), BF16),
            vm((2, BRICKS, ANG, DW), BF16),
            vm((2, BRICKS, ANG, DW), BF16),
            vm((2, BRICKS, ANG, DW), BF16),
            block, block,
            vm((3, CZ, CY, CX), F32),
            vm((3, CZ, CY, CX), F32),
            block, block,
            vm((2, 1, CX), F32),
            vm((2, GZ, 1, CX), F32),
            vm((2, 1, CX), F32),
            vm((2, BRICKS, 1, CX), F32),
            vm((GZ * BRICKS, 1, CX), F32),
            vm((3 * CX, CX), BF16),
            vm((96, CX), BF16),
            vm((3 * CX, CX), BF16),
            vm((64, CX), BF16),
            dma((2,)),
            dma((NCHUNK,)),
            dma((4, 2)),
            dma((4, 2)),
            dma((5, 8)),
            dma((5, 8)),
            dma((3, 3, 2)),
            dma((3, 3, 2)),
            dma((2, 2)),
            dma((2, 2)),
            dma((2, GZ)),
            dma((2, GZ)),
            dma((2,)),
            dma((2,)),
            dma,
            dma,
        ],
        compiler_params=pltpu.CompilerParams(
            collective_id=0, has_side_effects=True, vmem_limit_bytes=60 * 1024 * 1024
        ),
    )(start, measured, tiles, tile_block, angle_row)


def solution(mesh):
    return jax.shard_map(
        body,
        mesh=mesh,
        in_specs=(
            P("gz", "gy", "gx"),
            P(("gz", "gy", "gx"), None, None),
            P("gy", None, "gx"),
            P(),
            P(),
        ),
        out_specs=(P("gz", "gy", "gx"), P(None, "gz", "gy", "gx")),
        check_vma=False,
    )
```

```python
import math

import jax
import jax.numpy as jnp
from jax import lax
from jax.experimental import pallas as pl
from jax.experimental.pallas import tpu as pltpu
from jax.sharding import PartitionSpec as P

CZ, CY, CX = 32, 16, 128
ROWS = CZ * CY
ANG, DW, NBLK = 8, 256, 4
V = CY * CX
R = 8
GZ, GY, GX = 4, 4, 8
BRICKS = GY * GX
CELLS = float(CZ * CY * CX * GZ * BRICKS)
MESH = pl.DeviceIdType.MESH
F32, BF16 = jnp.float32, jnp.bfloat16
STEP = 0.5
SHRINK = 0.2
EPS = 1e-6
CHUNK = 128
NCHUNK = V // CHUNK
ORDER = sorted(
    ((dx, dz, dc) for dz in range(4) for dx in range(4) for dc in range(2) if dx or dz or dc),
    key=lambda s: -(min(s[0], 4 - s[0]) + min(s[1], 4 - s[1])),
)
LOAD = 512
PITCH = 9
SPLIT = 4
ORDER_ALL = sorted(
    ((dy, t) for dy in range(GZ) for t in range(GY * GX) if dy or t),
    key=lambda s: -(
        min(s[0], 4 - s[0])
        + (sum(min(d, 4 - d) for d in ORDER[s[1] - 1][:2]) if s[1] else 0)
    ),
)

RAW = [math.exp(-k * k / 12.5) for k in range(-R, R + 1)]
TAPS = [r / sum(RAW) for r in RAW]


def dot(a, b, dims):
    return lax.dot_general(a, b, (dims, ((), ())), preferred_element_type=F32)


def split(v):
    hi = v.astype(BF16)
    lo = (v - hi.astype(F32)).astype(BF16)
    return hi, lo


def kernel(
    start_ref, meas_ref, tiles_ref, tb_ref, row_ref,
    x_out, dual_out,
    raw, mat, tmp, x0, w1, w2, res, qbuf, xa, zbuf, zmid, ybuf, ymid, tbv, obs, mis, acc,
    zs, zr, zs2, zr2, ys, yr, ys2, yr2, xs, xr,
    fzs, fzr, fys, fyr, fxs, fxr,
    stage, sl, snd1, rcv1, snd2, rcv2,
    hterm, back, dl, dlm, xlr, bdl,
    red0, redz, red1, redx, redall,
    bx, wx, bx2, wx2,
    load_sem, tile_sem, z_send, z_recv, yx_send, yx_recv, f_send, f_recv,
    a_send, a_recv, rz_send, rz_recv, rx_send, rx_recv, all_send, all_recv,
):
    gz, gy, gx = lax.axis_index("gz"), lax.axis_index("gy"), lax.axis_index("gx")
    me = gy * GX + gx
    scope = jax.named_scope

    barrier = pltpu.get_barrier_semaphore()

    chip_x = 2 * (gy // 2) + lax.rem(gx, 2)
    chip_z, core = gx // 2, lax.rem(gy, 2)

    def member(t):
        dx, dz, dc = ORDER[t - 1]
        x = lax.rem(chip_x + dx, 4)
        z = lax.rem(chip_z + dz, 4)
        y = 2 * (x // 2) + lax.rem(core + dc, 2)
        x = 2 * z + lax.rem(x, 2)
        return y * GX + x, (gz, y, x)

    for t in range(1, BRICKS):
        pl.semaphore_signal(barrier, inc=1, device_id=member(t)[1], device_id_type=MESH)

    @pl.loop(1, GZ)
    def _(t):
        pl.semaphore_signal(
            barrier, inc=1, device_id=(lax.rem(gz + t, GZ), gy, gx), device_id_type=MESH
        )

    ld = [
        pltpu.make_async_copy(start_ref, x0, load_sem.at[0]),
        pltpu.make_async_copy(meas_ref, obs, load_sem.at[1]),
    ]
    for c in ld:
        c.start()

    def tile_copy(c):
        rows = pl.ds(c * LOAD, LOAD)
        return pltpu.make_async_copy(tiles_ref.at[rows], raw.at[rows], tile_sem.at[c])


    def there(dz, dy, dx):
        ok = True
        for d, at, n in ((dz, gz, GZ), (dy, gy, GY), (dx, gx, GX)):
            if d:
                near = at > 0 if d < 0 else at < n - 1
                ok = near if ok is True else jnp.logical_and(ok, near)
        return ok

    class Hub:
        def __init__(self, items, before=None):
            self.before = before
            self.items = [
                (
                    there(*d),
                    there(*(-i for i in d)),
                    pltpu.make_async_remote_copy(
                        src, dst, ss, rs,
                        device_id=(gz + d[0], gy + d[1], gx + d[2]), device_id_type=MESH,
                    ),
                    dst,
                )
                for d, src, dst, ss, rs in items
            ]

        def clear(self):
            for _, arrives, _, dst in self.items:

                @pl.when(jnp.logical_not(arrives))
                def _():
                    dst[...] = jnp.zeros(dst.shape, dst.dtype)

        def start(self):
            if self.before is not None:
                self.before.wait_send()
            for leaves, _, copy, _ in self.items:
                pl.when(leaves)(copy.start)

        def wait_recv(self):
            for _, arrives, copy, _ in self.items:
                pl.when(arrives)(copy.wait_recv)

        def wait_send(self):
            for leaves, _, copy, _ in self.items:
                pl.when(leaves)(copy.wait_send)

    def pair(axis, src, dst, send, recv):
        unit = [int(axis == a) for a in range(3)]
        return [
            ([-u for u in unit], src.at[0], dst.at[1], send.at[0], recv.at[0]),
            (unit, src.at[1], dst.at[0], send.at[1], recv.at[1]),
        ]

    def around(m, k, low, high, into_low, into_high, before):
        items = [
            ((0, -1, 0), low, into_high, yx_send.at[0], yx_recv.at[k, 0]),
            ((0, 1, 0), high, into_low, yx_send.at[1], yx_recv.at[k, 1]),
        ]
        i = 2
        for sy in (0, -1, 1):
            for side, sx in ((0, -1), (1, 1)):
                items.append((
                    (0, sy, sx), xs.at[m, side], xr.at[m, 1 - sy, 1 - side],
                    yx_send.at[i], yx_recv.at[k, i],
                ))
                i += 1
        return Hub(items, before)

    def zswap(k, src, dst, before):
        return Hub(pair(0, src, dst, z_send, z_recv.at[k]), before)

    zhub = [zswap(0, zs.at[0], zr.at[0], None)]
    zhub.append(zswap(1, zs.at[1], zr.at[1], zhub[0]))
    zhub2 = zswap(0, zs2, zr2, zhub[1])
    zhub.append(zswap(1, zs.at[2], zr.at[2], zhub2))

    def yxswap(n, k, before):
        return around(n, k, ys.at[n, 0], ys.at[n, 1], yr.at[n, 0], yr.at[n, 1], before)

    yxhub = [yxswap(0, 0, None)]
    yxhub.append(yxswap(1, 1, yxhub[0]))
    yxhub2 = around(4, 0, ys2, ys2, yr2.at[0], yr2.at[1], yxhub[1])
    yxhub.append(yxswap(2, 1, yxhub2))
    yxhub.append(yxswap(3, 0, yxhub[2]))
    fhub = []
    for n in range(3):
        k = n % 2
        fhub.append(
            Hub(
                pair(0, fzs.at[n], fzr.at[n], f_send.at[0], f_recv.at[k, 0])
                + pair(1, fys.at[n], fyr.at[n], f_send.at[1], f_recv.at[k, 1])
                + pair(2, fxs.at[n], fxr.at[n], f_send.at[2], f_recv.at[k, 2]),
                fhub[-1] if n else None,
            )
        )
    hubs = zhub + [zhub2] + yxhub + [yxhub2] + fhub
    for h in hubs:
        h.clear()

    def gauss(d):
        df = d.astype(F32)
        w = jnp.exp(df * df * (-1.0 / 12.5)) * (1.0 / sum(RAW))
        return jnp.where(jnp.abs(d) <= R, w, 0.0)

    def iota(shape, axis):
        return lax.broadcasted_iota(jnp.int32, shape, axis)

    square = (CX, CX)
    bhi, blo = split(gauss(iota(square, 0) - iota(square, 1)))
    bx[0:CX] = bhi
    bx[CX : 2 * CX] = bhi
    bx[2 * CX : 3 * CX] = blo
    k0, k1 = iota((32, CX), 0), iota((32, CX), 1)
    pos = jnp.where(k0 < 16, lax.rem(k0, 8) - 8, CX + lax.rem(k0, 8))
    whi, wlo = split(gauss(pos - k1))
    wx[0:32] = whi
    wx[32:64] = wlo
    rim = ((k1 == 0) & ((k0 == 7) | (k0 == 15))) | ((k1 == CX - 1) & ((k0 == 16) | (k0 == 24)))
    wx[64:96] = jnp.where(rim, 1.0, 0.0).astype(BF16)
    s0, s1 = iota((32, 2 * CX), 0), iota((32, 2 * CX), 1)
    want = jnp.where(s0 < 16, lax.rem(s0, 8), CX - 8 + lax.rem(s0, 8)) + jnp.where(
        lax.rem(s0, 16) < 8, 0, CX
    )
    pick = jnp.where(s1 == want, 1.0, 0.0).astype(BF16)
    pick2 = jnp.where(k1 == jnp.where(k0 < 16, k0, CX - 32 + k0), 1.0, 0.0).astype(BF16)

    wide = (GX, GX * CX)
    spread = jnp.where(iota(wide, 0) == iota(wide, 1) // CX, 1.0, 0.0).astype(BF16)
    for b in range(GY):
        rows = dot(tb_ref[b].astype(F32).astype(BF16), spread, ((0,), (0,)))
        for c in range(GX):
            tbv[b * GX + c] = rows[:, c * CX : (c + 1) * CX]

    def relayout(low, high):
        for c in range(V // LOAD):
            if low * CHUNK <= c * LOAD < high * CHUNK:
                tile_copy(c).wait()

        @pl.loop(low, high)
        def _(c):
            rows = pl.ds(pl.multiple_of(c * CHUNK, CHUNK), CHUNK)
            block = raw[rows].astype(F32)
            for h in range(2):
                for j in range(CHUNK):
                    tmp[h, PITCH * j : PITCH * j + ANG, :] = block[j, :, h * 128 : (h + 1) * 128]
            for a in range(ANG):
                for h in range(2):
                    part = tmp[h, pl.ds(a, CHUNK, stride=PITCH), :]
                    mat[rows, a * DW + h * 128 : a * DW + (h + 1) * 128] = part.astype(BF16)

    ld[0].wait()
    for c in range(V // LOAD):
        tile_copy(c).start()
    ld[1].wait()
    for a in range(ANG):
        acc[pl.ds(a, 1), :] = obs[0, pl.ds(row_ref[a], 1), :]

    with scope("wait_barrier"):
        pl.semaphore_wait(barrier, BRICKS - 1 + GZ - 1)

    def send_faces(n, src):
        fzs[n, 0] = src[0]
        fzs[n, 1] = src[CZ - 1]
        v = src[...]
        fys[n, 0] = v[:, 0, :]
        fys[n, 1] = v[:, CY - 1, :]
        hi, lo = split(v.reshape(ROWS, CX))
        f = dot(pick, jnp.concatenate([hi, lo], axis=1), ((1,), (1,))).astype(BF16)
        fxs[n, 0] = f[0:16]
        fxs[n, 1] = f[16:32]
        fhub[n].start()

    def send_z(n, src):
        zs[n, 0] = src[0:R].reshape(R * CY, CX).astype(BF16)
        zs[n, 1] = src[CZ - R : CZ].reshape(R * CY, CX).astype(BF16)
        zhub[n].start()

    def taps(at):
        t = TAPS[R] * at(R)
        for k in range(R):
            t += TAPS[k] * (at(k) + at(2 * R - k))
        return t

    def blur_z(n, src, out):
        zbuf[R : R + CZ] = src[...]
        with scope("wait_z"):
            zhub[n].wait_recv()
        zbuf[0:R] = zr[n, 0].astype(F32).reshape(R, CY, CX)
        zbuf[R + CZ : 2 * R + CZ] = zr[n, 1].astype(F32).reshape(R, CY, CX)

        @pl.loop(0, CZ, unroll=2)
        def _(z):
            out[z] = taps(lambda k: zbuf[z + k])

    def send_yx(n, w):
        v = w[...]
        ys[n, 0] = v[:, 0:R, :].reshape(CZ * R, CX).astype(BF16)
        ys[n, 1] = v[:, CY - R :, :].reshape(CZ * R, CX).astype(BF16)
        hi, lo = split(v.reshape(ROWS, CX))
        f = dot(pick, jnp.concatenate([hi, lo], axis=1), ((1,), (1,))).astype(BF16)
        xs[n, 0] = f[0:16]
        xs[n, 1] = f[16:32]
        yxhub[n].start()

    def rows_of(m, slot, weights):
        halo = xr[m, slot].reshape(32, ROWS)
        return dot(jnp.concatenate([halo, halo], axis=0), weights, ((0,), (0,)))

    def own_rows(w, mat3):
        hi, lo = split(w[...].reshape(ROWS, CX))
        both = jnp.concatenate([hi, lo], axis=1)
        return dot(both, mat3[0 : 2 * CX], ((1,), (0,))) + dot(hi, mat3[2 * CX :], ((1,), (0,)))

    def blur_yx(n, w, out):
        own = own_rows(w, bx)
        ybuf[:, R : R + CY, :] = own.reshape(CZ, CY, CX)
        with scope("wait_yx"):
            yxhub[n].wait_recv()
        ybuf[:, R : R + CY, :] += rows_of(n, 1, wx[0:64]).reshape(CZ, CY, CX)
        for side, at in ((0, slice(CY - R, CY)), (1, slice(0, R))):
            y = yr[n, side]
            rows = dot(jnp.concatenate([y, y], axis=1), bx[CX:], ((1,), (0,)))
            more = rows_of(n, 2 * side, wx[0:64]).reshape(CZ, CY, CX)[:, at, :]
            to = slice(0, R) if side == 0 else slice(R + CY, 2 * R + CY)
            ybuf[:, to, :] = rows.reshape(CZ, R, CX) + more

        @pl.loop(0, CZ, unroll=2)
        def _(z):
            out[z] = taps(lambda k: ybuf[z, k : k + CY, :])

    lane, sub = iota((CY, CX), 1), iota((CY, CX), 0)
    ends = ((gz == 0, gz == GZ - 1), (gy == 0, gy == GY - 1), (gx == 0, gx == GX - 1))

    def wait_faces(n):
        with scope("wait_faces"):
            fhub[n].wait_recv()
        xlr[...] = dot(fxr[n].reshape(32, ROWS), wx[64:96], ((0,), (0,))).reshape(CZ, CY, CX)
        xa[0] = fzr[n, 0]
        xa[CZ + 1] = fzr[n, 1]

    def diffs(n, z):
        v = xa[z + 1]
        up, low = xa[z + 2], xa[z]
        yield (
            jnp.where((z == CZ - 1) & ends[0][1], 0.0, up - v),
            jnp.where((z == 0) & ends[0][0], 0.0, v - low),
        )
        up = jnp.where(sub == CY - 1, fyr[n, 1, pl.ds(z, 1), :], pltpu.roll(v, CY - 1, 0))
        low = jnp.where(sub == 0, fyr[n, 0, pl.ds(z, 1), :], pltpu.roll(v, 1, 0))
        yield (
            jnp.where((sub == CY - 1) & ends[1][1], 0.0, up - v),
            jnp.where((sub == 0) & ends[1][0], 0.0, v - low),
        )
        edge = xlr[z]
        up = jnp.where(lane == CX - 1, edge, pltpu.roll(v, CX - 1, 1))
        low = jnp.where(lane == 0, edge, pltpu.roll(v, 1, 1))
        yield (
            jnp.where((lane == CX - 1) & ends[2][1], 0.0, up - v),
            jnp.where((lane == 0) & ends[2][0], 0.0, v - low),
        )

    def fold(p):
        return p[0:8] + p[8:16]

    def redz_copy(n, t):
        return pltpu.make_async_remote_copy(
            red0.at[n], redz.at[n, t], rz_send, rz_recv,
            device_id=(lax.rem(gz + t, GZ), gy, gx), device_id_type=MESH,
        )

    def redx_copy(n, t):
        return pltpu.make_async_remote_copy(
            red1.at[n], redx.at[n, t], rx_send, rx_recv,
            device_id=member(t)[1], device_id_type=MESH,
        )

    def put_sums(n, primal, dualres):
        p = jnp.sum(jnp.sum(primal, axis=0, keepdims=True), axis=1, keepdims=True)
        d = jnp.sum(jnp.sum(dualres, axis=0, keepdims=True), axis=1, keepdims=True)
        red0[n] = jnp.where(lane[0:1] < CX // 2, p, d)

    def send_all():
        for slot, (dy, t) in enumerate(ORDER_ALL):
            dev = (gy, gx) if t == 0 else member(t)[1][1:]
            pltpu.make_async_remote_copy(
                red0.at[1], redall.at[slot + 1], all_send, all_recv,
                device_id=(lax.rem(gz + dy, GZ), *dev), device_id_type=MESH,
            ).start()

    def forward_sums(n):
        got = redz.at[n, pl.ds(1, GZ - 1)]
        pltpu.make_async_copy(got, got, rz_recv).wait()
        red1[n] = red0[n] + jnp.sum(redz[n, 1:GZ], axis=0)

        for t in range(1, BRICKS):
            redx_copy(n, t).start()

    def factor_of(n, penalty):
        total = red1[n]
        got = redx.at[n, pl.ds(1, BRICKS - 1)]
        pltpu.make_async_copy(got, got, rx_recv).wait()
        total += jnp.sum(redx[n, 1:BRICKS], axis=0)
        return factor_from(total, penalty)

    def factor_from(total, penalty):
        p = jnp.broadcast_to(total[:, 0:1], (8, CX)) * (1.0 / (3.0 * CELLS))
        d = jnp.broadcast_to(total[:, CX - 1 : CX], (8, CX)) * (1.0 / CELLS)
        d = penalty * penalty * d
        return jnp.sqrt(jnp.sqrt((p + EPS) / (d + EPS)))

    def arrivals(ref, sem):
        got = ref.at[pl.ds(0, BRICKS - 1)]
        pltpu.make_async_copy(got, got, sem).wait()

    def sent(n, ref):
        arrivals(ref.at[n], a_send)

    def send_block(n, i, src, dst, d, dev):
        pltpu.make_async_remote_copy(
            src.at[n, d], dst.at[n, me], a_send, a_recv.at[n, i],
            device_id=dev, device_id_type=MESH,
        ).start()

    def project(n):
        for z0 in range(1):
            for y in range(CY):
                sl[:, y * CX : (y + 1) * CX] = res[pl.ds(y, CZ, stride=CY), :].astype(BF16)
        with scope("mm_fwd"):
            for a in range(ANG):
                c = dot(sl[...], mat[:, a * DW : (a + 1) * DW], ((1,), (0,)))
                for h in range(2):
                    stage[h, pl.ds(a, CZ, stride=ANG), :] = c[:, h * 128 : (h + 1) * 128]

        def block_of(d):
            rows = pl.ds(pl.multiple_of(d * ANG, ANG), ANG)
            return jnp.concatenate([stage[0, rows, :], stage[1, rows, :]], axis=1).astype(BF16)

        if n:
            sent(0, snd2)
        for t in range(1, BRICKS):
            d, dev = member(t)
            snd1[n, d] = block_of(d)
            send_block(n, 0, snd1, rcv1, d, dev)

        rcv1[n, me] = block_of(me)

    def return_misfit(n):
        with scope("wait_a1"):
            arrivals(rcv1.at[n], a_recv.at[n, 0])

        def add(s, sums):
            x = rcv1[n, s].astype(F32)
            t = tbv[s]
            t = jnp.concatenate([t, t], axis=1)
            return tuple(sums[q] + jnp.where(t == float(q), x, 0.0) for q in range(NBLK))

        sums = lax.fori_loop(
            0, BRICKS, add, tuple(jnp.zeros((ANG, DW), F32) for _ in range(NBLK)), unroll=2
        )
        for q in range(NBLK):
            cols = slice(q * DW, (q + 1) * DW)
            mis[:, cols] = (sums[q] - acc[:, cols]).astype(BF16).astype(F32)

        def chosen(d):
            t = tbv[d]
            t = jnp.concatenate([t, t], axis=1)
            c = mis[:, 0:DW]
            for q in range(1, NBLK):
                c = jnp.where(t == float(q), mis[:, q * DW : (q + 1) * DW], c)
            return c.astype(BF16)

        sent(n, snd1)
        for t in range(1, BRICKS):
            d, dev = member(t)
            snd2[n, d] = chosen(d)
            send_block(n, 1, snd2, rcv2, d, dev)

        rcv2[n, me] = chosen(me)

    def backproject(n, out):
        with scope("wait_a2"):
            arrivals(rcv2.at[n], a_recv.at[n, 1])
        r = rcv2[n].astype(F32).reshape(CZ * ANG, DW)
        for h in range(2):
            stage[h] = r[:, h * 128 : (h + 1) * 128]
        for a in range(ANG):
            for h in range(2):
                sl[:, a * DW + h * 128 : a * DW + (h + 1) * 128] = stage[
                    h, pl.ds(a, CZ, stride=ANG), :
                ].astype(BF16)
        with scope("mm_bwd"):
            for c in range(ANG):
                b = dot(sl[...], mat[c * DW : (c + 1) * DW, :], ((1,), (1,)))
                for h in range(2):
                    res[pl.ds(2 * c + h, CZ, stride=CY), :] = b[:, h * 128 : (h + 1) * 128]
        out[...] = res[...].reshape(CZ, CY, CX)

    send_z(0, x0)
    send_faces(0, x0)
    relayout(0, SPLIT)
    blur_z(0, x0, w1)
    send_yx(0, w1)
    relayout(SPLIT, NCHUNK)
    blur_yx(0, w1, w2)
    res[...] = w2[...].reshape(ROWS, CX)
    project(0)

    wait_faces(0)
    xa[1 : CZ + 1] = x0[...]
    cut = SHRINK

    @pl.loop(0, CZ, unroll=2)
    def _(z):
        smooth = jnp.zeros((CY, CX), F32)
        shrunk = jnp.zeros((CY, CX), F32)
        for j, jm in diffs(0, z):
            s = j - jnp.clip(j, -cut, cut)
            sm = jm - jnp.clip(jm, -cut, cut)
            smooth += jm - j
            shrunk += sm - s
        h = STEP * (smooth - shrunk)
        x0[z] = xa[z + 1] - h
        back[z] = shrunk

    send_z(1, x0)

    shape1, shape2 = (160, 256), (256, CX)
    i, m = iota(shape1, 0), iota(shape1, 1) - 8
    i = jnp.where(i < CX, i, jnp.where(i < CX + 16, i - CX - 16, i - 16))
    inside = ((m >= 0) | (gx > 0)) & ((m < CX) | (gx < GX - 1)) & (m < CX + 8)
    thi, tlo = split(jnp.where(inside, gauss(i - m), 0.0))
    m = iota(shape2, 0) - 8
    uhi, ulo = split(gauss(m - iota(shape2, 1)))
    twice = (
        dot(thi, uhi, ((1,), (0,))) + dot(thi, ulo, ((1,), (0,))) + dot(tlo, uhi, ((1,), (0,)))
    )
    bhi, blo = split(twice[0:CX])
    bx2[0:CX] = bhi
    bx2[CX : 2 * CX] = bhi
    bx2[2 * CX : 3 * CX] = blo
    whi, wlo = split(twice[CX : CX + 32])
    wx2[0:32] = whi
    wx2[32:64] = wlo

    return_misfit(0)
    blur_z(1, x0, w1)
    send_yx(1, w1)
    backproject(0, w2)

    zs2[0] = w2[0:16].reshape(16 * CY, CX).astype(BF16)
    zs2[1] = w2[CZ - 16 : CZ].reshape(16 * CY, CX).astype(BF16)
    zhub2.start()
    blur_yx(1, w1, qbuf)
    zbuf[16 : 16 + CZ] = w2[...]
    with scope("wait_z2"):
        zhub2.wait_recv()
    zbuf[0:16] = zr2[0].astype(F32).reshape(16, CY, CX)
    zbuf[16 + CZ : 32 + CZ] = zr2[1].astype(F32).reshape(16, CY, CX)

    @pl.loop(0, CZ + 16, unroll=2)
    def _(z):
        out = ((z < 8) & ends[0][0]) | ((z >= CZ + 8) & ends[0][1])
        zmid[z] = jnp.where(out, 0.0, taps(lambda k: zbuf[z + k]))

    @pl.loop(0, CZ, unroll=2)
    def _(z):
        w2[z] = taps(lambda k: zmid[z + k])

    hi = w2[...].reshape(ROWS, CX).astype(BF16)
    ys2[...] = hi
    f = dot(pick2, hi, ((1,), (1,))).astype(BF16)
    xs[4, 0] = f[0:16]
    xs[4, 1] = f[16:32]
    yxhub2.start()
    w1[...] = zmid[8 : 8 + CZ]

    ymid[:, 16 : 16 + CY, :] = own_rows(w2, bx2).reshape(CZ, CY, CX)
    with scope("wait_yx2"):
        yxhub2.wait_recv()
    send_yx(2, w1)
    ymid[:, 16 : 16 + CY, :] += rows_of(4, 1, wx2[...]).reshape(CZ, CY, CX)
    for side in range(2):
        y = yr2[side]
        rows = dot(jnp.concatenate([y, y], axis=1), bx2[CX:], ((1,), (0,)))
        rows = rows + rows_of(4, 2 * side, wx2[...])
        ymid[:, 32 * side : 32 * side + 16, :] = rows.reshape(CZ, CY, CX)
    sub2 = iota((CY + 16, CX), 0)
    outside = ((sub2 < 8) & ends[1][0]) | ((sub2 >= CY + 8) & ends[1][1])

    @pl.loop(0, CZ, unroll=2)
    def _(z):
        ybuf[z] = jnp.where(outside, 0.0, taps(lambda k: ymid[z, k : k + CY + 16, :]))

    @pl.loop(0, CZ, unroll=2)
    def _(z):
        rows = pl.ds(pl.multiple_of(z * CY, CY), CY)
        res[rows, :] = qbuf[z] - STEP * taps(lambda k: ybuf[z, k : k + CY, :])

    project(1)
    blur_yx(2, w1, w2)
    x0[...] = x0[...] - STEP * w2[...]
    send_faces(1, x0)
    xa[1 : CZ + 1] = x0[...]
    return_misfit(1)
    wait_faces(1)

    def one(z, sums):
        primal, dres = sums
        smooth = jnp.zeros((CY, CX), F32)
        shrunk = jnp.zeros((CY, CX), F32)
        bdual = jnp.zeros((CY, CX), F32)
        for axis, (j, jm) in enumerate(diffs(1, z)):
            s = j - jnp.clip(j, -cut, cut)
            sm = jm - jnp.clip(jm, -cut, cut)
            d = j - s
            dm = jm - sm
            smooth += jm - j
            shrunk += sm - s
            bdual += dm - d
            dl[axis, z] = d
            dlm[axis, z] = dm
            primal += fold(jnp.square(j - s))
        dres += fold(jnp.square(shrunk - back[z]))
        hterm[z] = smooth - shrunk
        back[z] = shrunk
        bdl[z] = bdual
        return primal, dres

    zero = jnp.zeros((8, CX), F32)
    primal, dres = lax.fori_loop(0, CZ, one, (zero, zero), unroll=2)
    put_sums(0, primal, dres)
    for t in range(1, GZ):
        redz_copy(0, t).start()
    backproject(1, w2)
    send_z(2, w2)
    forward_sums(0)
    blur_z(2, w2, w1)
    send_yx(3, w1)
    penalty = factor_of(0, jnp.ones((8, CX), F32))
    inv1 = 1.0 / penalty
    pen3 = penalty[0:1].reshape(1, 1, CX)
    inv3 = inv1[0:1].reshape(1, 1, CX)
    x0[...] = x0[...] - STEP * pen3 * (hterm[...] + bdl[...] * inv3)
    dl[...] = dl[...] * inv3
    dlm[...] = dlm[...] * inv3
    blur_yx(3, w1, w2)
    x0[...] = x0[...] - STEP * w2[...]
    send_faces(2, x0)
    x_out[...] = x0[...]
    xa[1 : CZ + 1] = x0[...]
    wait_faces(2)
    cut2 = (SHRINK / penalty)[0:1]

    def last(z, sums):
        primal, dres = sums
        shrunk = jnp.zeros((CY, CX), F32)
        for axis, (j, jm) in enumerate(diffs(2, z)):
            t = j + dl[axis, z]
            tm = jm + dlm[axis, z]
            s = t - jnp.clip(t, -cut2, cut2)
            sm = tm - jnp.clip(tm, -cut2, cut2)
            shrunk += sm - s
            dl[axis, z] = t - s
            primal += fold(jnp.square(j - s))
        dres += fold(jnp.square(shrunk - back[z]))
        return primal, dres

    with scope("last"):
        primal, dres = lax.fori_loop(0, CZ, last, (zero, zero), unroll=4)
    put_sums(1, primal, dres)
    send_all()
    with scope("sums"):
        got = redall.at[pl.ds(1, GZ * BRICKS - 1)]
        pltpu.make_async_copy(got, got, all_recv).wait()
    factor2 = factor_from(red0[1] + jnp.sum(redall[1 : GZ * BRICKS], axis=0), penalty)
    scale = (1.0 / factor2)[0:1].reshape(1, 1, 1, CX)
    with scope("scale"):
        dual_out[...] = dl[...] * scale

    with scope("wait_sends"):
        for h in (zhub[2], yxhub[3], fhub[2]):
            h.wait_send()
        sent(1, snd2)
        got = redz.at[0, pl.ds(1, GZ - 1)]
        pltpu.make_async_copy(got, got, rz_send).wait()
        got = redx.at[0, pl.ds(1, BRICKS - 1)]
        pltpu.make_async_copy(got, got, rx_send).wait()
        got = redall.at[pl.ds(1, GZ * BRICKS - 1)]
        pltpu.make_async_copy(got, got, all_send).wait()


def body(start, measured, tiles, tile_block, angle_row):
    vm = pltpu.VMEM
    dma = pltpu.SemaphoreType.DMA
    block = vm((CZ, CY, CX), F32)
    return pl.pallas_call(
        kernel,
        out_shape=(
            pltpu.VMEM((CZ, CY, CX), F32),
            pltpu.VMEM((3, CZ, CY, CX), F32),
        ),
        in_specs=[
            pl.BlockSpec(memory_space=pltpu.HBM),
            pl.BlockSpec(memory_space=pltpu.HBM),
            pl.BlockSpec(memory_space=pltpu.HBM),
            pl.BlockSpec(memory_space=pltpu.VMEM),
            pl.BlockSpec(memory_space=pltpu.SMEM),
        ],
        out_specs=(pl.BlockSpec(memory_space=pltpu.VMEM), pl.BlockSpec(memory_space=pltpu.VMEM)),
        scratch_shapes=[
            vm((V, ANG, DW), BF16),
            vm((V, ANG * DW), BF16),
            vm((2, CHUNK * PITCH, 128), F32),
            block, block, block,
            vm((ROWS, CX), F32),
            block,
            vm((CZ + 2, CY, CX), F32),
            vm((CZ + 32, CY, CX), F32),
            vm((CZ + 16, CY, CX), F32),
            vm((CZ, CY + 16, CX), F32),
            vm((CZ, CY + 32, CX), F32),
            vm((BRICKS, ANG, CX), F32),
            vm((1, ANG, NBLK * DW), F32),
            vm((ANG, NBLK * DW), F32),
            vm((ANG, NBLK * DW), F32),
            vm((3, 2, R * CY, CX), BF16),
            vm((3, 2, R * CY, CX), BF16),
            vm((2, 16 * CY, CX), BF16),
            vm((2, 16 * CY, CX), BF16),
            vm((4, 2, CZ * R, CX), BF16),
            vm((4, 2, CZ * R, CX), BF16),
            vm((ROWS, CX), BF16),
            vm((2, ROWS, CX), BF16),
            vm((5, 2, 16, ROWS), BF16),
            vm((5, 3, 2, 16, ROWS), BF16),
            vm((3, 2, CY, CX), F32),
            vm((3, 2, CY, CX), F32),
            vm((3, 2, CZ, CX), F32),
            vm((3, 2, CZ, CX), F32),
            vm((3, 2, 16, ROWS), BF16),
            vm((3, 2, 16, ROWS), BF16),
            vm((2, CZ * ANG, 128), F32),
            vm((CZ, V), BF16),
            vm((2, BRICKS, ANG, DW), BF16),
            vm((2, BRICKS, ANG, DW), BF16),
            vm((2, BRICKS, ANG, DW), BF16),
            vm((2, BRICKS, ANG, DW), BF16),
            block, block,
            vm((3, CZ, CY, CX), F32),
            vm((3, CZ, CY, CX), F32),
            block, block,
            vm((2, 1, CX), F32),
            vm((2, GZ, 1, CX), F32),
            vm((2, 1, CX), F32),
            vm((2, BRICKS, 1, CX), F32),
            vm((GZ * BRICKS, 1, CX), F32),
            vm((3 * CX, CX), BF16),
            vm((96, CX), BF16),
            vm((3 * CX, CX), BF16),
            vm((64, CX), BF16),
            dma((2,)),
            dma((V // LOAD,)),
            dma((2,)),
            dma((2, 2)),
            dma((8,)),
            dma((2, 8)),
            dma((3, 2)),
            dma((2, 3, 2)),
            dma,
            dma((2, 2)),
            dma,
            dma,
            dma,
            dma,
            dma,
            dma,
        ],
        compiler_params=pltpu.CompilerParams(
            collective_id=0, has_side_effects=True, vmem_limit_bytes=60 * 1024 * 1024
        ),
    )(start, measured, tiles, tile_block, angle_row)


def solution(mesh):
    return jax.shard_map(
        body,
        mesh=mesh,
        in_specs=(
            P("gz", "gy", "gx"),
            P(("gz", "gy", "gx"), None, None),
            P("gy", None, "gx"),
            P(),
            P(),
        ),
        out_specs=(P("gz", "gy", "gx"), P(None, "gz", "gy", "gx")),
        check_vma=False,
    )
```

```python
import math

import jax
import jax.numpy as jnp
from jax import lax
from jax.experimental import pallas as pl
from jax.experimental.pallas import tpu as pltpu
from jax.sharding import PartitionSpec as P

CZ, CY, CX = 32, 16, 128
ROWS = CZ * CY
ANG, DW, NBLK = 8, 256, 4
V = CY * CX
R = 8
GZ, GY, GX = 4, 4, 8
BRICKS = GY * GX
CELLS = float(CZ * CY * CX * GZ * BRICKS)
MESH = pl.DeviceIdType.MESH
F32, BF16 = jnp.float32, jnp.bfloat16
STEP = 0.5
SHRINK = 0.2
EPS = 1e-6
CHUNK = 128
NCHUNK = V // CHUNK
ORDER = sorted(
    ((dx, dz, dc) for dz in range(4) for dx in range(4) for dc in range(2) if dx or dz or dc),
    key=lambda s: -(min(s[0], 4 - s[0]) + min(s[1], 4 - s[1])),
)
LOAD = 512
ROWS9 = (CZ + 2) * CY
ROWS9P = -(-ROWS9 // 128) * 128
PITCH = 9
SPLIT = 4
ORDER_ALL = sorted(
    ((dy, t) for dy in range(GZ) for t in range(GY * GX) if dy or t),
    key=lambda s: -(
        min(s[0], 4 - s[0])
        + (sum(min(d, 4 - d) for d in ORDER[s[1] - 1][:2]) if s[1] else 0)
    ),
)

RAW = [math.exp(-k * k / 12.5) for k in range(-R, R + 1)]
TAPS = [r / sum(RAW) for r in RAW]


def dot(a, b, dims):
    return lax.dot_general(a, b, (dims, ((), ())), preferred_element_type=F32)


def split(v):
    hi = v.astype(BF16)
    lo = (v - hi.astype(F32)).astype(BF16)
    return hi, lo


def kernel(
    start_ref, meas_ref, tiles_ref, tb_ref, row_ref,
    x_out, dual_out,
    raw, mat, tmp, x0, w1, w2, res, qbuf, xa, zbuf, zmid, ybuf, ymid, tbv, obs, mis, acc,
    zs, zr, zs2, zr2, ys, yr, ys2, yr2, xs, xr,
    zs9, zr9, ys9, yr9, xs9, xr9,
    fzs, fzr, fys, fyr, fxs, fxr, fzs2, fzr2, fys2, fyr2, fxs2, fxr2, fz2, fy2,
    stage, sl, snd1, rcv1, snd2, rcv2,
    hterm, back, dl, dlm, xlr, bdl,
    red0, redz, red1, redx, redall,
    bx, wx, bx2, wx2, bx9, wx9,
    load_sem, tile_sem, z_send, z_recv, yx_send, yx_recv, f_send, f_recv,
    a_send, a_recv, rz_send, rz_recv, rx_send, rx_recv, all_send, all_recv,
):
    gz, gy, gx = lax.axis_index("gz"), lax.axis_index("gy"), lax.axis_index("gx")
    me = gy * GX + gx
    scope = jax.named_scope

    barrier = pltpu.get_barrier_semaphore()

    chip_x = 2 * (gy // 2) + lax.rem(gx, 2)
    chip_z, core = gx // 2, lax.rem(gy, 2)

    def member(t):
        dx, dz, dc = ORDER[t - 1]
        x = lax.rem(chip_x + dx, 4)
        z = lax.rem(chip_z + dz, 4)
        y = 2 * (x // 2) + lax.rem(core + dc, 2)
        x = 2 * z + lax.rem(x, 2)
        return y * GX + x, (gz, y, x)

    for t in range(1, BRICKS):
        pl.semaphore_signal(barrier, inc=1, device_id=member(t)[1], device_id_type=MESH)

    @pl.loop(1, GZ)
    def _(t):
        pl.semaphore_signal(
            barrier, inc=1, device_id=(lax.rem(gz + t, GZ), gy, gx), device_id_type=MESH
        )

    ld = [
        pltpu.make_async_copy(start_ref, x0, load_sem.at[0]),
        pltpu.make_async_copy(meas_ref, obs, load_sem.at[1]),
    ]
    for c in ld:
        c.start()

    def tile_copy(c):
        rows = pl.ds(c * LOAD, LOAD)
        return pltpu.make_async_copy(tiles_ref.at[rows], raw.at[rows], tile_sem.at[c])


    def there(dz, dy, dx):
        ok = True
        for d, at, n in ((dz, gz, GZ), (dy, gy, GY), (dx, gx, GX)):
            if d:
                near = at > 0 if d < 0 else at < n - 1
                ok = near if ok is True else jnp.logical_and(ok, near)
        return ok

    class Hub:
        def __init__(self, items, before=None):
            self.before = before
            self.items = [
                (
                    there(*d),
                    there(*(-i for i in d)),
                    pltpu.make_async_remote_copy(
                        src, dst, ss, rs,
                        device_id=(gz + d[0], gy + d[1], gx + d[2]), device_id_type=MESH,
                    ),
                    dst,
                )
                for d, src, dst, ss, rs in items
            ]

        def clear(self):
            for _, arrives, _, dst in self.items:

                @pl.when(jnp.logical_not(arrives))
                def _():
                    dst[...] = jnp.zeros(dst.shape, dst.dtype)

        def start(self):
            if self.before is not None:
                self.before.wait_send()
            for leaves, _, copy, _ in self.items:
                pl.when(leaves)(copy.start)

        def wait_recv(self):
            for _, arrives, copy, _ in self.items:
                pl.when(arrives)(copy.wait_recv)

        def wait_send(self):
            for leaves, _, copy, _ in self.items:
                pl.when(leaves)(copy.wait_send)

    def pair(axis, src, dst, send, recv):
        unit = [int(axis == a) for a in range(3)]
        return [
            ([-u for u in unit], src.at[0], dst.at[1], send.at[0], recv.at[0]),
            (unit, src.at[1], dst.at[0], send.at[1], recv.at[1]),
        ]

    def around(k, low, high, into_low, into_high, faces, halos, before):
        items = [
            ((0, -1, 0), low, into_high, yx_send.at[0], yx_recv.at[k, 0]),
            ((0, 1, 0), high, into_low, yx_send.at[1], yx_recv.at[k, 1]),
        ]
        i = 2
        for sy in (0, -1, 1):
            for side, sx in ((0, -1), (1, 1)):
                items.append((
                    (0, sy, sx), faces.at[side], halos.at[1 - sy, 1 - side],
                    yx_send.at[i], yx_recv.at[k, i],
                ))
                i += 1
        return Hub(items, before)

    def zswap(k, src, dst, before):
        return Hub(pair(0, src, dst, z_send, z_recv.at[k]), before)

    zhub = [zswap(0, zs.at[0], zr.at[0], None)]
    zhub.append(zswap(1, zs.at[1], zr.at[1], zhub[0]))
    zhub2 = zswap(0, zs2, zr2, zhub[1])
    zhub.append(zswap(1, zs9, zr9, zhub2))

    def yxswap(n, k, before):
        low, high = yr.at[n, 0], yr.at[n, 1]
        return around(k, ys.at[n, 0], ys.at[n, 1], low, high, xs.at[n], xr.at[n], before)

    yxhub = [yxswap(0, 0, None)]
    yxhub.append(yxswap(1, 1, yxhub[0]))
    yxhub2 = around(0, ys2, ys2, yr2.at[0], yr2.at[1], xs.at[3], xr.at[3], yxhub[1])
    yxhub.append(yxswap(2, 1, yxhub2))
    yxhub.append(
        around(0, ys9.at[0], ys9.at[1], yr9.at[0], yr9.at[1], xs9, xr9, yxhub[2])
    )
    fhub = []
    for k, z, y, x in (
        (0, (fzs.at[0], fzr.at[0]), (fys.at[0], fyr.at[0]), (fxs.at[0], fxr.at[0])),
        (1, (fzs.at[1], fzr.at[1]), (fys.at[1], fyr.at[1]), (fxs.at[1], fxr.at[1])),
        (0, (fzs2, fzr2), (fys2, fyr2), (fxs2, fxr2)),
    ):
        fhub.append(
            Hub(
                pair(0, *z, f_send.at[0], f_recv.at[k, 0])
                + pair(1, *y, f_send.at[1], f_recv.at[k, 1])
                + pair(2, *x, f_send.at[2], f_recv.at[k, 2]),
                fhub[-1] if fhub else None,
            )
        )
    xs9[...] = jnp.zeros_like(xs9)
    hubs = zhub + [zhub2] + yxhub + [yxhub2] + fhub
    for h in hubs:
        h.clear()

    def gauss(d):
        df = d.astype(F32)
        w = jnp.exp(df * df * (-1.0 / 12.5)) * (1.0 / sum(RAW))
        return jnp.where(jnp.abs(d) <= R, w, 0.0)

    def iota(shape, axis):
        return lax.broadcasted_iota(jnp.int32, shape, axis)

    square = (CX, CX)
    bhi, blo = split(gauss(iota(square, 0) - iota(square, 1)))
    bx[0:CX] = bhi
    bx[CX : 2 * CX] = bhi
    bx[2 * CX : 3 * CX] = blo
    k0, k1 = iota((32, CX), 0), iota((32, CX), 1)
    pos = jnp.where(k0 < 16, lax.rem(k0, 8) - 8, CX + lax.rem(k0, 8))
    whi, wlo = split(gauss(pos - k1))
    wx[0:32] = whi
    wx[32:64] = wlo
    rim = ((k1 == 0) & ((k0 == 7) | (k0 == 15))) | ((k1 == CX - 1) & ((k0 == 16) | (k0 == 24)))
    wx[64:96] = jnp.where(rim, 1.0, 0.0).astype(BF16)
    s0, s1 = iota((32, 2 * CX), 0), iota((32, 2 * CX), 1)
    want = jnp.where(s0 < 16, lax.rem(s0, 8), CX - 8 + lax.rem(s0, 8)) + jnp.where(
        lax.rem(s0, 16) < 8, 0, CX
    )
    pick = jnp.where(s1 == want, 1.0, 0.0).astype(BF16)
    pick2 = jnp.where(k1 == jnp.where(k0 < 16, k0, CX - 32 + k0), 1.0, 0.0).astype(BF16)

    def place(c):
        edge = jnp.where(c == CX, -1, jnp.where(c == 2 * CX - 1, CX, 4 * CX))
        return jnp.where(c < CX, c, edge)

    def last_weights():
        shape = (CX, 2 * CX)
        hi, lo = split(gauss(iota(shape, 0) - place(iota(shape, 1))))
        bx9[0:CX] = hi
        bx9[CX : 2 * CX] = hi
        bx9[2 * CX : 3 * CX] = lo
        shape = (32, 2 * CX)
        k = iota(shape, 0)
        hi, lo = split(gauss(jnp.where(k < 16, k - 16, CX - 16 + k) - place(iota(shape, 1))))
        wx9[0:32] = hi
        wx9[32:64] = lo

    wide = (GX, GX * CX)
    spread = jnp.where(iota(wide, 0) == iota(wide, 1) // CX, 1.0, 0.0).astype(BF16)
    for b in range(GY):
        rows = dot(tb_ref[b].astype(F32).astype(BF16), spread, ((0,), (0,)))
        for c in range(GX):
            tbv[b * GX + c] = rows[:, c * CX : (c + 1) * CX]

    def relayout(low, high):
        for c in range(V // LOAD):
            if low * CHUNK <= c * LOAD < high * CHUNK:
                tile_copy(c).wait()

        @pl.loop(low, high)
        def _(c):
            rows = pl.ds(pl.multiple_of(c * CHUNK, CHUNK), CHUNK)
            block = raw[rows].astype(F32)
            for h in range(2):
                for j in range(CHUNK):
                    tmp[h, PITCH * j : PITCH * j + ANG, :] = block[j, :, h * 128 : (h + 1) * 128]
            for a in range(ANG):
                for h in range(2):
                    part = tmp[h, pl.ds(a, CHUNK, stride=PITCH), :]
                    mat[rows, a * DW + h * 128 : a * DW + (h + 1) * 128] = part.astype(BF16)

    ld[0].wait()
    for c in range(V // LOAD):
        tile_copy(c).start()
    ld[1].wait()
    for a in range(ANG):
        acc[pl.ds(a, 1), :] = obs[0, pl.ds(row_ref[a], 1), :]

    with scope("wait_barrier"):
        pl.semaphore_wait(barrier, BRICKS - 1 + GZ - 1)

    def send_faces(n, src):
        fzs[n, 0] = src[0]
        fzs[n, 1] = src[CZ - 1]
        v = src[...]
        fys[n, 0] = v[:, 0, :]
        fys[n, 1] = v[:, CY - 1, :]
        hi, lo = split(v.reshape(ROWS, CX))
        f = dot(pick, jnp.concatenate([hi, lo], axis=1), ((1,), (1,))).astype(BF16)
        fxs[n, 0] = f[0:16]
        fxs[n, 1] = f[16:32]
        fhub[n].start()

    def send_terms():
        for i, src in enumerate((hterm, bdl)):
            fzs2[0, i] = src[0]
            fzs2[1, i] = src[CZ - 1]
            v = src[...]
            fys2[0, i] = v[:, 0, :]
            fys2[1, i] = v[:, CY - 1, :]
            hi, lo = split(v.reshape(ROWS, CX))
            f = dot(pick, jnp.concatenate([hi, lo], axis=1), ((1,), (1,))).astype(BF16)
            fxs2[0, i] = f[0:16]
            fxs2[1, i] = f[16:32]
        fhub[2].start()

    def send_z(n, src):
        zs[n, 0] = src[0:R].reshape(R * CY, CX).astype(BF16)
        zs[n, 1] = src[CZ - R : CZ].reshape(R * CY, CX).astype(BF16)
        zhub[n].start()

    def taps(at):
        t = TAPS[R] * at(R)
        for k in range(R):
            t += TAPS[k] * (at(k) + at(2 * R - k))
        return t

    def blur_z(n, src, out):
        zbuf[R : R + CZ] = src[...]
        with scope("wait_z"):
            zhub[n].wait_recv()
        zbuf[0:R] = zr[n, 0].astype(F32).reshape(R, CY, CX)
        zbuf[R + CZ : 2 * R + CZ] = zr[n, 1].astype(F32).reshape(R, CY, CX)

        @pl.loop(0, CZ, unroll=2)
        def _(z):
            out[z] = taps(lambda k: zbuf[z + k])

    def send_yx(n, w):
        v = w[...]
        ys[n, 0] = v[:, 0:R, :].reshape(CZ * R, CX).astype(BF16)
        ys[n, 1] = v[:, CY - R :, :].reshape(CZ * R, CX).astype(BF16)
        hi, lo = split(v.reshape(ROWS, CX))
        f = dot(pick, jnp.concatenate([hi, lo], axis=1), ((1,), (1,))).astype(BF16)
        xs[n, 0] = f[0:16]
        xs[n, 1] = f[16:32]
        yxhub[n].start()

    def rows_of(m, slot, weights):
        halo = xr[m, slot].reshape(32, ROWS)
        return dot(jnp.concatenate([halo, halo], axis=0), weights, ((0,), (0,)))

    def own_rows(w, mat3):
        hi, lo = split(w[...].reshape(ROWS, CX))
        both = jnp.concatenate([hi, lo], axis=1)
        return dot(both, mat3[0 : 2 * CX], ((1,), (0,))) + dot(hi, mat3[2 * CX :], ((1,), (0,)))

    def blur_yx(n, w, out):
        own = own_rows(w, bx)
        ybuf[:, R : R + CY, :] = own.reshape(CZ, CY, CX)
        with scope("wait_yx"):
            yxhub[n].wait_recv()
        ybuf[:, R : R + CY, :] += rows_of(n, 1, wx[0:64]).reshape(CZ, CY, CX)
        for side, at in ((0, slice(CY - R, CY)), (1, slice(0, R))):
            y = yr[n, side]
            rows = dot(jnp.concatenate([y, y], axis=1), bx[CX:], ((1,), (0,)))
            more = rows_of(n, 2 * side, wx[0:64]).reshape(CZ, CY, CX)[:, at, :]
            to = slice(0, R) if side == 0 else slice(R + CY, 2 * R + CY)
            ybuf[:, to, :] = rows.reshape(CZ, R, CX) + more

        @pl.loop(0, CZ, unroll=2)
        def _(z):
            out[z] = taps(lambda k: ybuf[z, k : k + CY, :])

    lane, sub = iota((CY, CX), 1), iota((CY, CX), 0)
    ends = ((gz == 0, gz == GZ - 1), (gy == 0, gy == GY - 1), (gx == 0, gx == GX - 1))

    def wait_faces(n):
        with scope("wait_faces"):
            fhub[n].wait_recv()
        xlr[...] = dot(fxr[n].reshape(32, ROWS), wx[64:96], ((0,), (0,))).reshape(CZ, CY, CX)
        xa[0] = fzr[n, 0]
        xa[CZ + 1] = fzr[n, 1]

    def diffs(fy, z):
        v = xa[z + 1]
        up, low = xa[z + 2], xa[z]
        yield (
            jnp.where((z == CZ - 1) & ends[0][1], 0.0, up - v),
            jnp.where((z == 0) & ends[0][0], 0.0, v - low),
        )
        up = jnp.where(sub == CY - 1, fy[1, pl.ds(z, 1), :], pltpu.roll(v, CY - 1, 0))
        low = jnp.where(sub == 0, fy[0, pl.ds(z, 1), :], pltpu.roll(v, 1, 0))
        yield (
            jnp.where((sub == CY - 1) & ends[1][1], 0.0, up - v),
            jnp.where((sub == 0) & ends[1][0], 0.0, v - low),
        )
        edge = xlr[z]
        up = jnp.where(lane == CX - 1, edge, pltpu.roll(v, CX - 1, 1))
        low = jnp.where(lane == 0, edge, pltpu.roll(v, 1, 1))
        yield (
            jnp.where((lane == CX - 1) & ends[2][1], 0.0, up - v),
            jnp.where((lane == 0) & ends[2][0], 0.0, v - low),
        )

    def fold(p):
        return p[0:8] + p[8:16]

    def redz_copy(n, t):
        return pltpu.make_async_remote_copy(
            red0.at[n], redz.at[n, t], rz_send, rz_recv,
            device_id=(lax.rem(gz + t, GZ), gy, gx), device_id_type=MESH,
        )

    def redx_copy(n, t):
        return pltpu.make_async_remote_copy(
            red1.at[n], redx.at[n, t], rx_send, rx_recv,
            device_id=member(t)[1], device_id_type=MESH,
        )

    def put_sums(n, primal, dualres):
        p = jnp.sum(jnp.sum(primal, axis=0, keepdims=True), axis=1, keepdims=True)
        d = jnp.sum(jnp.sum(dualres, axis=0, keepdims=True), axis=1, keepdims=True)
        red0[n] = jnp.where(lane[0:1] < CX // 2, p, d)

    def send_all():
        for slot, (dy, t) in enumerate(ORDER_ALL):
            dev = (gy, gx) if t == 0 else member(t)[1][1:]
            pltpu.make_async_remote_copy(
                red0.at[1], redall.at[slot + 1], all_send, all_recv,
                device_id=(lax.rem(gz + dy, GZ), *dev), device_id_type=MESH,
            ).start()

    def forward_sums(n):
        got = redz.at[n, pl.ds(1, GZ - 1)]
        pltpu.make_async_copy(got, got, rz_recv).wait()
        red1[n] = red0[n] + jnp.sum(redz[n, 1:GZ], axis=0)

        for t in range(1, BRICKS):
            redx_copy(n, t).start()

    def factor_of(n, penalty):
        total = red1[n]
        got = redx.at[n, pl.ds(1, BRICKS - 1)]
        pltpu.make_async_copy(got, got, rx_recv).wait()
        total += jnp.sum(redx[n, 1:BRICKS], axis=0)
        return factor_from(total, penalty)

    def factor_from(total, penalty):
        p = jnp.broadcast_to(total[:, 0:1], (8, CX)) * (1.0 / (3.0 * CELLS))
        d = jnp.broadcast_to(total[:, CX - 1 : CX], (8, CX)) * (1.0 / CELLS)
        d = penalty * penalty * d
        return jnp.sqrt(jnp.sqrt((p + EPS) / (d + EPS)))

    def arrivals(ref, sem):
        got = ref.at[pl.ds(0, BRICKS - 1)]
        pltpu.make_async_copy(got, got, sem).wait()

    def sent(n, ref):
        arrivals(ref.at[n], a_send)

    def send_block(n, i, src, dst, d, dev):
        pltpu.make_async_remote_copy(
            src.at[n, d], dst.at[n, me], a_send, a_recv.at[n, i],
            device_id=dev, device_id_type=MESH,
        ).start()

    def project(n):
        for z0 in range(1):
            for y in range(CY):
                sl[:, y * CX : (y + 1) * CX] = res[pl.ds(y, CZ, stride=CY), :].astype(BF16)
        with scope("mm_fwd"):
            for a in range(ANG):
                c = dot(sl[...], mat[:, a * DW : (a + 1) * DW], ((1,), (0,)))
                for h in range(2):
                    stage[h, pl.ds(a, CZ, stride=ANG), :] = c[:, h * 128 : (h + 1) * 128]

        def block_of(d):
            rows = pl.ds(pl.multiple_of(d * ANG, ANG), ANG)
            return jnp.concatenate([stage[0, rows, :], stage[1, rows, :]], axis=1).astype(BF16)

        if n:
            sent(0, snd2)
        for t in range(1, BRICKS):
            d, dev = member(t)
            snd1[n, d] = block_of(d)
            send_block(n, 0, snd1, rcv1, d, dev)

        rcv1[n, me] = block_of(me)

    def return_misfit(n):
        with scope("wait_a1"):
            arrivals(rcv1.at[n], a_recv.at[n, 0])

        def add(s, sums):
            x = rcv1[n, s].astype(F32)
            t = tbv[s]
            t = jnp.concatenate([t, t], axis=1)
            return tuple(sums[q] + jnp.where(t == float(q), x, 0.0) for q in range(NBLK))

        sums = lax.fori_loop(
            0, BRICKS, add, tuple(jnp.zeros((ANG, DW), F32) for _ in range(NBLK)), unroll=2
        )
        for q in range(NBLK):
            cols = slice(q * DW, (q + 1) * DW)
            mis[:, cols] = (sums[q] - acc[:, cols]).astype(BF16).astype(F32)

        def chosen(d):
            t = tbv[d]
            t = jnp.concatenate([t, t], axis=1)
            c = mis[:, 0:DW]
            for q in range(1, NBLK):
                c = jnp.where(t == float(q), mis[:, q * DW : (q + 1) * DW], c)
            return c.astype(BF16)

        sent(n, snd1)
        for t in range(1, BRICKS):
            d, dev = member(t)
            snd2[n, d] = chosen(d)
            send_block(n, 1, snd2, rcv2, d, dev)

        rcv2[n, me] = chosen(me)

    def backproject(n, out):
        with scope("wait_a2"):
            arrivals(rcv2.at[n], a_recv.at[n, 1])
        r = rcv2[n].astype(F32).reshape(CZ * ANG, DW)
        for h in range(2):
            stage[h] = r[:, h * 128 : (h + 1) * 128]
        for a in range(ANG):
            for h in range(2):
                sl[:, a * DW + h * 128 : a * DW + (h + 1) * 128] = stage[
                    h, pl.ds(a, CZ, stride=ANG), :
                ].astype(BF16)
        with scope("mm_bwd"):
            for c in range(ANG):
                b = dot(sl[...], mat[c * DW : (c + 1) * DW, :], ((1,), (1,)))
                for h in range(2):
                    res[pl.ds(2 * c + h, CZ, stride=CY), :] = b[:, h * 128 : (h + 1) * 128]
        out[...] = res[...].reshape(CZ, CY, CX)

    send_z(0, x0)
    send_faces(0, x0)
    relayout(0, SPLIT)
    blur_z(0, x0, w1)
    send_yx(0, w1)
    relayout(SPLIT, NCHUNK)
    blur_yx(0, w1, w2)
    res[...] = w2[...].reshape(ROWS, CX)
    project(0)

    wait_faces(0)
    xa[1 : CZ + 1] = x0[...]
    cut = SHRINK

    @pl.loop(0, CZ, unroll=2)
    def _(z):
        smooth = jnp.zeros((CY, CX), F32)
        shrunk = jnp.zeros((CY, CX), F32)
        for j, jm in diffs(fyr.at[0], z):
            s = j - jnp.clip(j, -cut, cut)
            sm = jm - jnp.clip(jm, -cut, cut)
            smooth += jm - j
            shrunk += sm - s
        h = STEP * (smooth - shrunk)
        x0[z] = xa[z + 1] - h
        back[z] = shrunk

    send_z(1, x0)

    shape1, shape2 = (160, 256), (256, CX)
    i, m = iota(shape1, 0), iota(shape1, 1) - 8
    i = jnp.where(i < CX, i, jnp.where(i < CX + 16, i - CX - 16, i - 16))
    inside = ((m >= 0) | (gx > 0)) & ((m < CX) | (gx < GX - 1)) & (m < CX + 8)
    thi, tlo = split(jnp.where(inside, gauss(i - m), 0.0))
    m = iota(shape2, 0) - 8
    uhi, ulo = split(gauss(m - iota(shape2, 1)))
    twice = (
        dot(thi, uhi, ((1,), (0,))) + dot(thi, ulo, ((1,), (0,))) + dot(tlo, uhi, ((1,), (0,)))
    )
    bhi, blo = split(twice[0:CX])
    bx2[0:CX] = bhi
    bx2[CX : 2 * CX] = bhi
    bx2[2 * CX : 3 * CX] = blo
    whi, wlo = split(twice[CX : CX + 32])
    wx2[0:32] = whi
    wx2[32:64] = wlo
    last_weights()

    return_misfit(0)
    blur_z(1, x0, w1)
    send_yx(1, w1)
    backproject(0, w2)

    zs2[0] = w2[0:16].reshape(16 * CY, CX).astype(BF16)
    zs2[1] = w2[CZ - 16 : CZ].reshape(16 * CY, CX).astype(BF16)
    zhub2.start()
    blur_yx(1, w1, qbuf)
    zbuf[16 : 16 + CZ] = w2[...]
    with scope("wait_z2"):
        zhub2.wait_recv()
    zbuf[0:16] = zr2[0].astype(F32).reshape(16, CY, CX)
    zbuf[16 + CZ : 32 + CZ] = zr2[1].astype(F32).reshape(16, CY, CX)

    @pl.loop(0, CZ + 16, unroll=2)
    def _(z):
        out = ((z < 8) & ends[0][0]) | ((z >= CZ + 8) & ends[0][1])
        zmid[z] = jnp.where(out, 0.0, taps(lambda k: zbuf[z + k]))

    @pl.loop(0, CZ, unroll=2)
    def _(z):
        w2[z] = taps(lambda k: zmid[z + k])

    hi = w2[...].reshape(ROWS, CX).astype(BF16)
    ys2[...] = hi
    f = dot(pick2, hi, ((1,), (1,))).astype(BF16)
    xs[3, 0] = f[0:16]
    xs[3, 1] = f[16:32]
    yxhub2.start()
    w1[...] = zmid[8 : 8 + CZ]

    ymid[0:CZ, 16 : 16 + CY, :] = own_rows(w2, bx2).reshape(CZ, CY, CX)
    with scope("wait_yx2"):
        yxhub2.wait_recv()
    send_yx(2, w1)
    ymid[0:CZ, 16 : 16 + CY, :] += rows_of(3, 1, wx2[...]).reshape(CZ, CY, CX)
    for side in range(2):
        y = yr2[side]
        rows = dot(jnp.concatenate([y, y], axis=1), bx2[CX:], ((1,), (0,)))
        rows = rows + rows_of(3, 2 * side, wx2[...])
        ymid[0:CZ, 32 * side : 32 * side + 16, :] = rows.reshape(CZ, CY, CX)
    sub2 = iota((CY + 16, CX), 0)
    outside = ((sub2 < 8) & ends[1][0]) | ((sub2 >= CY + 8) & ends[1][1])

    @pl.loop(0, CZ, unroll=2)
    def _(z):
        ybuf[z] = jnp.where(outside, 0.0, taps(lambda k: ymid[z, k : k + CY + 16, :]))

    @pl.loop(0, CZ, unroll=2)
    def _(z):
        rows = pl.ds(pl.multiple_of(z * CY, CY), CY)
        res[rows, :] = qbuf[z] - STEP * taps(lambda k: ybuf[z, k : k + CY, :])

    project(1)
    blur_yx(2, w1, w2)
    x0[...] = x0[...] - STEP * w2[...]
    send_faces(1, x0)
    xa[1 : CZ + 1] = x0[...]
    return_misfit(1)
    wait_faces(1)

    def one(z, sums):
        primal, dres = sums
        smooth = jnp.zeros((CY, CX), F32)
        shrunk = jnp.zeros((CY, CX), F32)
        bdual = jnp.zeros((CY, CX), F32)
        for axis, (j, jm) in enumerate(diffs(fyr.at[1], z)):
            s = j - jnp.clip(j, -cut, cut)
            sm = jm - jnp.clip(jm, -cut, cut)
            d = j - s
            dm = jm - sm
            smooth += jm - j
            shrunk += sm - s
            bdual += dm - d
            dl[axis, z] = d
            dlm[axis, z] = dm
            primal += fold(jnp.square(j - s))
        dres += fold(jnp.square(shrunk - back[z]))
        hterm[z] = smooth - shrunk
        back[z] = shrunk
        bdl[z] = bdual
        return primal, dres

    zero = jnp.zeros((8, CX), F32)
    primal, dres = lax.fori_loop(0, CZ, one, (zero, zero), unroll=2)
    put_sums(0, primal, dres)
    for t in range(1, GZ):
        redz_copy(0, t).start()
    send_terms()
    backproject(1, w2)
    zs9[0] = w2[0 : R + 1].reshape((R + 1) * CY, CX).astype(BF16)
    zs9[1] = w2[CZ - R - 1 : CZ].reshape((R + 1) * CY, CX).astype(BF16)
    zhub[2].start()
    forward_sums(0)
    zbuf[R + 1 : R + 1 + CZ] = w2[...]
    with scope("wait_z"):
        zhub[2].wait_recv()
    zbuf[0 : R + 1] = zr9[0].astype(F32).reshape(R + 1, CY, CX)
    zbuf[R + 1 + CZ : 2 * R + 2 + CZ] = zr9[1].astype(F32).reshape(R + 1, CY, CX)

    @pl.loop(0, CZ + 2, unroll=2)
    def _(z):
        zmid[z] = taps(lambda k: zbuf[z + k])

    outer = zmid[0 : CZ + 2]
    n9 = (CZ + 2) * R
    for side, at, ninth in ((0, slice(0, R), R), (1, slice(CY - R, CY), CY - R - 1)):
        ys9[side, 0:n9] = outer[:, at, :].reshape(n9, CX).astype(BF16)
        ys9[side, n9:] = outer[1 : CZ + 1, ninth, :].astype(BF16)
    hi, lo = split(outer.reshape(ROWS9, CX))
    f = dot(pick2, hi, ((1,), (1,))).astype(BF16)
    xs9[0, :, 0:ROWS9] = f[0:16]
    xs9[1, :, 0:ROWS9] = f[16:32]
    yxhub[3].start()
    both = jnp.concatenate([hi, lo], axis=1)
    own = dot(both, bx9[0 : 2 * CX], ((1,), (0,))) + dot(hi, bx9[2 * CX :], ((1,), (0,)))
    own = own.reshape(CZ + 2, CY, 2 * CX)
    ymid[0 : CZ + 2, 16 : 16 + CY, :] = own[:, :, 0:CX]
    ybuf[:, R : R + CY, :] = own[1 : CZ + 1, :, CX:]
    penalty = factor_of(0, jnp.ones((8, CX), F32))
    inv1 = 1.0 / penalty
    pen3 = penalty[0:1].reshape(1, 1, CX)
    inv3 = inv1[0:1].reshape(1, 1, CX)
    spen = STEP * pen3
    x0[...] = x0[...] - spen * (hterm[...] + bdl[...] * inv3)
    dl[...] = dl[...] * inv3
    dlm[...] = dlm[...] * inv3
    with scope("wait_terms"):
        fhub[2].wait_recv()
    for side in range(2):
        fz2[side] = fzr[1, side] - spen[0] * (fzr2[side, 0] + fzr2[side, 1] * inv3[0])
        fy2[side] = fyr[1, side] - spen[0] * (fyr2[side, 0] + fyr2[side, 1] * inv3[0])
    rims = [
        dot(
            jnp.concatenate([fxr2[0, i], fxr2[1, i]], axis=0), wx[64:96], ((0,), (0,))
        ).reshape(CZ, CY, CX)
        for i in range(2)
    ]
    xlr[...] = xlr[...] - spen * (rims[0] + rims[1] * inv3)

    def halo_rows(slot):
        h = xr9[slot].reshape(32, ROWS9P)[:, 0:ROWS9]
        h = dot(jnp.concatenate([h, h], axis=0), wx9[...], ((0,), (0,)))
        return h.reshape(CZ + 2, CY, 2 * CX)

    with scope("wait_yx"):
        yxhub[3].wait_recv()
    more = halo_rows(1)
    ymid[0 : CZ + 2, 16 : 16 + CY, :] += more[:, :, 0:CX]
    ybuf[:, R : R + CY, :] += more[1 : CZ + 1, :, CX:]
    for side, at, ninth in ((0, slice(CY - R, CY), CY - R - 1), (1, slice(0, R), R)):
        y = yr9[side]
        rows = dot(jnp.concatenate([y, y], axis=1), bx9[CX:], ((1,), (0,)))
        more = halo_rows(2 * side)
        near = rows[0:n9].reshape(CZ + 2, R, 2 * CX) + more[:, at, :]
        far = rows[n9:, 0:CX] + more[1 : CZ + 1, ninth, 0:CX]
        to = slice(16 - R, 16) if side == 0 else slice(16 + CY, 16 + CY + R)
        ymid[0 : CZ + 2, to, :] = near[:, :, 0:CX]
        ymid[1 : CZ + 1, (15 - R if side == 0 else 16 + CY + R), :] = far
        to = slice(0, R) if side == 0 else slice(R + CY, 2 * R + CY)
        ybuf[:, to, :] = near[1 : CZ + 1, :, CX:]

    @pl.loop(0, CZ, unroll=2)
    def _(z):
        v = x0[z] - STEP * taps(lambda k: ymid[z + 1, 16 - R + k : 16 - R + CY + k, :])
        xa[z + 1] = v
        x_out[z] = v
        xlr[z] = xlr[z] - STEP * taps(lambda k: ybuf[z, k : k + CY, :])
        low = taps(lambda k: ymid[z + 1, k : k + R, :])[R - 1 : R]
        fy2[0, pl.ds(z, 1), :] = fy2[0, pl.ds(z, 1), :] - STEP * low
        high = taps(lambda k: ymid[z + 1, 16 + R + k : 16 + 2 * R + k, :])[0:1]
        fy2[1, pl.ds(z, 1), :] = fy2[1, pl.ds(z, 1), :] - STEP * high

    for side, at in ((0, 0), (1, CZ + 1)):
        xa[at] = fz2[side] - STEP * taps(lambda k: ymid[at, 16 - R + k : 16 - R + CY + k, :])
    cut2 = (SHRINK / penalty)[0:1]

    def last(z, sums):
        primal, dres = sums
        shrunk = jnp.zeros((CY, CX), F32)
        for axis, (j, jm) in enumerate(diffs(fy2, z)):
            t = j + dl[axis, z]
            tm = jm + dlm[axis, z]
            s = t - jnp.clip(t, -cut2, cut2)
            sm = tm - jnp.clip(tm, -cut2, cut2)
            shrunk += sm - s
            dl[axis, z] = t - s
            primal += fold(jnp.square(j - s))
        dres += fold(jnp.square(shrunk - back[z]))
        return primal, dres

    with scope("last"):
        primal, dres = lax.fori_loop(0, CZ, last, (zero, zero), unroll=4)
    put_sums(1, primal, dres)
    send_all()
    with scope("sums"):
        got = redall.at[pl.ds(1, GZ * BRICKS - 1)]
        pltpu.make_async_copy(got, got, all_recv).wait()
    factor2 = factor_from(red0[1] + jnp.sum(redall[1 : GZ * BRICKS], axis=0), penalty)
    scale = (1.0 / factor2)[0:1].reshape(1, 1, 1, CX)
    with scope("scale"):
        dual_out[...] = dl[...] * scale

    with scope("wait_sends"):
        for h in (zhub[2], yxhub[3], fhub[2]):
            h.wait_send()
        sent(1, snd2)
        got = redz.at[0, pl.ds(1, GZ - 1)]
        pltpu.make_async_copy(got, got, rz_send).wait()
        got = redx.at[0, pl.ds(1, BRICKS - 1)]
        pltpu.make_async_copy(got, got, rx_send).wait()
        got = redall.at[pl.ds(1, GZ * BRICKS - 1)]
        pltpu.make_async_copy(got, got, all_send).wait()


def body(start, measured, tiles, tile_block, angle_row):
    vm = pltpu.VMEM
    dma = pltpu.SemaphoreType.DMA
    block = vm((CZ, CY, CX), F32)
    return pl.pallas_call(
        kernel,
        out_shape=(
            pltpu.VMEM((CZ, CY, CX), F32),
            pltpu.VMEM((3, CZ, CY, CX), F32),
        ),
        in_specs=[
            pl.BlockSpec(memory_space=pltpu.HBM),
            pl.BlockSpec(memory_space=pltpu.HBM),
            pl.BlockSpec(memory_space=pltpu.HBM),
            pl.BlockSpec(memory_space=pltpu.VMEM),
            pl.BlockSpec(memory_space=pltpu.SMEM),
        ],
        out_specs=(pl.BlockSpec(memory_space=pltpu.VMEM), pl.BlockSpec(memory_space=pltpu.VMEM)),
        scratch_shapes=[
            vm((V, ANG, DW), BF16),
            vm((V, ANG * DW), BF16),
            vm((2, CHUNK * PITCH, 128), F32),
            block, block, block,
            vm((ROWS, CX), F32),
            block,
            vm((CZ + 2, CY, CX), F32),
            vm((CZ + 32, CY, CX), F32),
            vm((CZ + 16, CY, CX), F32),
            vm((CZ, CY + 16, CX), F32),
            vm((CZ + 2, CY + 32, CX), F32),
            vm((BRICKS, ANG, CX), F32),
            vm((1, ANG, NBLK * DW), F32),
            vm((ANG, NBLK * DW), F32),
            vm((ANG, NBLK * DW), F32),
            vm((2, 2, R * CY, CX), BF16),
            vm((2, 2, R * CY, CX), BF16),
            vm((2, 16 * CY, CX), BF16),
            vm((2, 16 * CY, CX), BF16),
            vm((3, 2, CZ * R, CX), BF16),
            vm((3, 2, CZ * R, CX), BF16),
            vm((ROWS, CX), BF16),
            vm((2, ROWS, CX), BF16),
            vm((4, 2, 16, ROWS), BF16),
            vm((4, 3, 2, 16, ROWS), BF16),
            vm((2, (R + 1) * CY, CX), BF16),
            vm((2, (R + 1) * CY, CX), BF16),
            vm((2, (CZ + 2) * R + CZ, CX), BF16),
            vm((2, (CZ + 2) * R + CZ, CX), BF16),
            vm((2, 16, ROWS9P), BF16),
            vm((3, 2, 16, ROWS9P), BF16),
            vm((2, 2, CY, CX), F32),
            vm((2, 2, CY, CX), F32),
            vm((2, 2, CZ, CX), F32),
            vm((2, 2, CZ, CX), F32),
            vm((2, 2, 16, ROWS), BF16),
            vm((2, 2, 16, ROWS), BF16),
            vm((2, 2, CY, CX), F32),
            vm((2, 2, CY, CX), F32),
            vm((2, 2, CZ, CX), F32),
            vm((2, 2, CZ, CX), F32),
            vm((2, 2, 16, ROWS), BF16),
            vm((2, 2, 16, ROWS), BF16),
            vm((2, CY, CX), F32),
            vm((2, CZ, CX), F32),
            vm((2, CZ * ANG, 128), F32),
            vm((CZ, V), BF16),
            vm((2, BRICKS, ANG, DW), BF16),
            vm((2, BRICKS, ANG, DW), BF16),
            vm((2, BRICKS, ANG, DW), BF16),
            vm((2, BRICKS, ANG, DW), BF16),
            block, block,
            vm((3, CZ, CY, CX), F32),
            vm((3, CZ, CY, CX), F32),
            block, block,
            vm((2, 1, CX), F32),
            vm((2, GZ, 1, CX), F32),
            vm((2, 1, CX), F32),
            vm((2, BRICKS, 1, CX), F32),
            vm((GZ * BRICKS, 1, CX), F32),
            vm((3 * CX, CX), BF16),
            vm((96, CX), BF16),
            vm((3 * CX, CX), BF16),
            vm((64, CX), BF16),
            vm((3 * CX, 2 * CX), BF16),
            vm((64, 2 * CX), BF16),
            dma((2,)),
            dma((V // LOAD,)),
            dma((2,)),
            dma((2, 2)),
            dma((8,)),
            dma((2, 8)),
            dma((3, 2)),
            dma((2, 3, 2)),
            dma,
            dma((2, 2)),
            dma,
            dma,
            dma,
            dma,
            dma,
            dma,
        ],
        compiler_params=pltpu.CompilerParams(
            collective_id=0, has_side_effects=True, vmem_limit_bytes=60 * 1024 * 1024
        ),
    )(start, measured, tiles, tile_block, angle_row)


def solution(mesh):
    return jax.shard_map(
        body,
        mesh=mesh,
        in_specs=(
            P("gz", "gy", "gx"),
            P(("gz", "gy", "gx"), None, None),
            P("gy", None, "gx"),
            P(),
            P(),
        ),
        out_specs=(P("gz", "gy", "gx"), P(None, "gz", "gy", "gx")),
        check_vma=False,
    )
```

```python
import math

import jax
import jax.numpy as jnp
from jax import lax
from jax.experimental import pallas as pl
from jax.experimental.pallas import tpu as pltpu
from jax.sharding import PartitionSpec as P

CZ, CY, CX = 32, 16, 128
ROWS = CZ * CY
ANG, DW, NBLK = 8, 256, 4
V = CY * CX
R = 8
GZ, GY, GX = 4, 4, 8
BRICKS = GY * GX
CELLS = float(CZ * CY * CX * GZ * BRICKS)
MESH = pl.DeviceIdType.MESH
F32, BF16 = jnp.float32, jnp.bfloat16
STEP = 0.5
SHRINK = 0.2
EPS = 1e-6
CHUNK = 128
NCHUNK = V // CHUNK
ORDER = sorted(
    ((dx, dz, dc) for dz in range(4) for dx in range(4) for dc in range(2) if dx or dz or dc),
    key=lambda s: -(min(s[0], 4 - s[0]) + min(s[1], 4 - s[1])),
)
LOAD = 512
ROWS9 = (CZ + 2) * CY
ROWS9P = -(-ROWS9 // 128) * 128
PITCH = 9
SPLIT = 4
ORDER_ALL = sorted(
    ((dy, t) for dy in range(GZ) for t in range(GY * GX) if dy or t),
    key=lambda s: -(
        min(s[0], 4 - s[0])
        + (sum(min(d, 4 - d) for d in ORDER[s[1] - 1][:2]) if s[1] else 0)
    ),
)

RAW = [math.exp(-k * k / 12.5) for k in range(-R, R + 1)]
TAPS = [r / sum(RAW) for r in RAW]


def dot(a, b, dims):
    return lax.dot_general(a, b, (dims, ((), ())), preferred_element_type=F32)


def split(v):
    hi = v.astype(BF16)
    lo = (v - hi.astype(F32)).astype(BF16)
    return hi, lo


def kernel(
    start_ref, meas_ref, tiles_ref, tb_ref, row_ref,
    x_out, dual_out,
    raw, mat, tmp, x0, w1, w2, res, qbuf, xa, zbuf, zmid, ybuf, ymid, tbv, obs, mis, acc,
    zs, zr, zst, tz, v1z, umid, ytwo, ys, yr, ys2, yr2, xs, xr,
    zs9, zr9, ys9, yr9, xs9, xr9,
    fzs, fzr, fys, fyr, fxs, fxr, fzs2, fzr2, fys2, fyr2, fxs2, fxr2, fz2, fy2,
    stage, sl, snd1, rcv1, snd2, rcv2,
    hterm, back, dl, dlm, xlr, bdl,
    red0, redz, red1, redx, redall,
    bx, wx, bx2, wx2, bx9, wx9,
    load_sem, tile_sem, z_send, z_recv, yx_send, yx_recv, f_send, f_recv,
    a_send, a_recv, rz_send, rz_recv, rx_send, rx_recv, all_send, all_recv,
):
    gz, gy, gx = lax.axis_index("gz"), lax.axis_index("gy"), lax.axis_index("gx")
    me = gy * GX + gx
    scope = jax.named_scope

    barrier = pltpu.get_barrier_semaphore()

    chip_x = 2 * (gy // 2) + lax.rem(gx, 2)
    chip_z, core = gx // 2, lax.rem(gy, 2)

    def member(t):
        dx, dz, dc = ORDER[t - 1]
        x = lax.rem(chip_x + dx, 4)
        z = lax.rem(chip_z + dz, 4)
        y = 2 * (x // 2) + lax.rem(core + dc, 2)
        x = 2 * z + lax.rem(x, 2)
        return y * GX + x, (gz, y, x)

    for t in range(1, BRICKS):
        pl.semaphore_signal(barrier, inc=1, device_id=member(t)[1], device_id_type=MESH)

    @pl.loop(1, GZ)
    def _(t):
        pl.semaphore_signal(
            barrier, inc=1, device_id=(lax.rem(gz + t, GZ), gy, gx), device_id_type=MESH
        )

    ld = [
        pltpu.make_async_copy(start_ref, x0, load_sem.at[0]),
        pltpu.make_async_copy(meas_ref, obs, load_sem.at[1]),
    ]
    for c in ld:
        c.start()

    def tile_copy(c):
        rows = pl.ds(c * LOAD, LOAD)
        return pltpu.make_async_copy(tiles_ref.at[rows], raw.at[rows], tile_sem.at[c])


    def there(dz, dy, dx):
        ok = True
        for d, at, n in ((dz, gz, GZ), (dy, gy, GY), (dx, gx, GX)):
            if d:
                near = at > 0 if d < 0 else at < n - 1
                ok = near if ok is True else jnp.logical_and(ok, near)
        return ok

    class Hub:
        def __init__(self, items, before=None):
            self.before = before
            self.items = [
                (
                    there(*d),
                    there(*(-i for i in d)),
                    pltpu.make_async_remote_copy(
                        src, dst, ss, rs,
                        device_id=(gz + d[0], gy + d[1], gx + d[2]), device_id_type=MESH,
                    ),
                    dst,
                )
                for d, src, dst, ss, rs in items
            ]

        def clear(self):
            for _, arrives, _, dst in self.items:

                @pl.when(jnp.logical_not(arrives))
                def _():
                    dst[...] = jnp.zeros(dst.shape, dst.dtype)

        def start(self):
            if self.before is not None:
                self.before.wait_send()
            for leaves, _, copy, _ in self.items:
                pl.when(leaves)(copy.start)

        def wait_recv(self, part=slice(None)):
            for _, arrives, copy, _ in self.items[part]:
                pl.when(arrives)(copy.wait_recv)

        def wait_send(self):
            for leaves, _, copy, _ in self.items:
                pl.when(leaves)(copy.wait_send)

    def pair(axis, src, dst, send, recv):
        unit = [int(axis == a) for a in range(3)]
        return [
            ([-u for u in unit], src.at[0], dst.at[1], send.at[0], recv.at[0]),
            (unit, src.at[1], dst.at[0], send.at[1], recv.at[1]),
        ]

    def around(k, low, high, into_low, into_high, faces, halos, before):
        items = []
        i = 2
        for sy in (-1, 1, 0):
            for side, sx in ((0, -1), (1, 1)):
                items.append((
                    (0, sy, sx), faces.at[side], halos.at[1 - sy, 1 - side],
                    yx_send.at[i], yx_recv.at[k, i],
                ))
                i += 1
        items += [
            ((0, -1, 0), low, into_high, yx_send.at[0], yx_recv.at[k, 0]),
            ((0, 1, 0), high, into_low, yx_send.at[1], yx_recv.at[k, 1]),
        ]
        return Hub(items, before)

    def zswap(k, src, dst, before):
        return Hub(pair(0, src, dst, z_send, z_recv.at[k]), before)

    zhub = [zswap(0, zs.at[0], zr.at[0], None)]
    zhub.append(zswap(1, zs.at[1], zr.at[1], zhub[0]))
    zhub2 = Hub(
        [
            ((-1, 0, 0), zst.at[0:16], zst.at[80:96], z_send.at[0], z_recv.at[0, 0]),
            ((1, 0, 0), zst.at[16:32], zst.at[64:80], z_send.at[1], z_recv.at[0, 1]),
        ],
        zhub[1],
    )
    zhub.append(zswap(1, zs9, zr9, zhub2))

    def yxswap(n, k, before):
        low, high = yr.at[n, 0], yr.at[n, 1]
        return around(k, ys.at[n, 0], ys.at[n, 1], low, high, xs.at[n], xr.at[n], before)

    yxhub = [yxswap(0, 0, None)]
    yxhub.append(yxswap(1, 1, yxhub[0]))
    yxhub2 = around(0, ys2, ys2, yr2.at[0], yr2.at[1], xs.at[3], xr.at[3], yxhub[1])
    yxhub.append(yxswap(2, 1, yxhub2))
    yxhub.append(
        around(0, ys9.at[0], ys9.at[1], yr9.at[0], yr9.at[1], xs9, xr9, yxhub[2])
    )
    fhub = []
    for k, z, y, x in (
        (0, (fzs.at[0], fzr.at[0]), (fys.at[0], fyr.at[0]), (fxs.at[0], fxr.at[0])),
        (1, (fzs.at[1], fzr.at[1]), (fys.at[1], fyr.at[1]), (fxs.at[1], fxr.at[1])),
        (0, (fzs2, fzr2), (fys2, fyr2), (fxs2, fxr2)),
    ):
        fhub.append(
            Hub(
                pair(0, *z, f_send.at[0], f_recv.at[k, 0])
                + pair(1, *y, f_send.at[1], f_recv.at[k, 1])
                + pair(2, *x, f_send.at[2], f_recv.at[k, 2]),
                fhub[-1] if fhub else None,
            )
        )
    xs9[...] = jnp.zeros_like(xs9)
    hubs = zhub + [zhub2] + yxhub + [yxhub2] + fhub
    for h in hubs:
        h.clear()

    def gauss(d):
        df = d.astype(F32)
        w = jnp.exp(df * df * (-1.0 / 12.5)) * (1.0 / sum(RAW))
        return jnp.where(jnp.abs(d) <= R, w, 0.0)

    def iota(shape, axis):
        return lax.broadcasted_iota(jnp.int32, shape, axis)

    square = (CX, CX)
    bhi, blo = split(gauss(iota(square, 0) - iota(square, 1)))
    bx[0:CX] = bhi
    bx[CX : 2 * CX] = bhi
    bx[2 * CX : 3 * CX] = blo
    k0, k1 = iota((32, CX), 0), iota((32, CX), 1)
    pos = jnp.where(k0 < 16, lax.rem(k0, 8) - 8, CX + lax.rem(k0, 8))
    whi, wlo = split(gauss(pos - k1))
    wx[0:32] = whi
    wx[32:64] = wlo
    rim = ((k1 == 0) & ((k0 == 7) | (k0 == 15))) | ((k1 == CX - 1) & ((k0 == 16) | (k0 == 24)))
    wx[64:96] = jnp.where(rim, 1.0, 0.0).astype(BF16)
    s0, s1 = iota((32, 2 * CX), 0), iota((32, 2 * CX), 1)
    want = jnp.where(s0 < 16, lax.rem(s0, 8), CX - 8 + lax.rem(s0, 8)) + jnp.where(
        lax.rem(s0, 16) < 8, 0, CX
    )
    pick = jnp.where(s1 == want, 1.0, 0.0).astype(BF16)
    pick2 = jnp.where(k1 == jnp.where(k0 < 16, k0, CX - 32 + k0), 1.0, 0.0).astype(BF16)

    def place(c):
        edge = jnp.where(c == CX, -1, jnp.where(c == 2 * CX - 1, CX, 4 * CX))
        return jnp.where(c < CX, c, edge)

    def last_weights():
        shape = (CX, 2 * CX)
        hi, lo = split(gauss(iota(shape, 0) - place(iota(shape, 1))))
        bx9[0:CX] = hi
        bx9[CX : 2 * CX] = hi
        bx9[2 * CX : 3 * CX] = lo
        shape = (32, 2 * CX)
        k = iota(shape, 0)
        hi, lo = split(gauss(jnp.where(k < 16, k - 16, CX - 16 + k) - place(iota(shape, 1))))
        wx9[0:32] = hi
        wx9[32:64] = lo

    wide = (GX, GX * CX)
    spread = jnp.where(iota(wide, 0) == iota(wide, 1) // CX, 1.0, 0.0).astype(BF16)
    for b in range(GY):
        rows = dot(tb_ref[b].astype(F32).astype(BF16), spread, ((0,), (0,)))
        for c in range(GX):
            tbv[b * GX + c] = rows[:, c * CX : (c + 1) * CX]

    def relayout(low, high):
        for c in range(V // LOAD):
            if low * CHUNK <= c * LOAD < high * CHUNK:
                tile_copy(c).wait()

        @pl.loop(low, high)
        def _(c):
            rows = pl.ds(pl.multiple_of(c * CHUNK, CHUNK), CHUNK)
            block = raw[rows].astype(F32)
            for h in range(2):
                for j in range(CHUNK):
                    tmp[h, PITCH * j : PITCH * j + ANG, :] = block[j, :, h * 128 : (h + 1) * 128]
            for a in range(ANG):
                for h in range(2):
                    part = tmp[h, pl.ds(a, CHUNK, stride=PITCH), :]
                    mat[rows, a * DW + h * 128 : a * DW + (h + 1) * 128] = part.astype(BF16)

    ld[0].wait()
    for c in range(V // LOAD):
        tile_copy(c).start()
    ld[1].wait()
    for a in range(ANG):
        acc[pl.ds(a, 1), :] = obs[0, pl.ds(row_ref[a], 1), :]

    with scope("wait_barrier"):
        pl.semaphore_wait(barrier, BRICKS - 1 + GZ - 1)

    def send_faces(n, src):
        fzs[n, 0] = src[0]
        fzs[n, 1] = src[CZ - 1]
        v = src[...]
        fys[n, 0] = v[:, 0, :]
        fys[n, 1] = v[:, CY - 1, :]
        hi, lo = split(v.reshape(ROWS, CX))
        f = dot(pick, jnp.concatenate([hi, lo], axis=1), ((1,), (1,))).astype(BF16)
        fxs[n, 0] = f[0:16]
        fxs[n, 1] = f[16:32]
        fhub[n].start()

    def send_terms():
        for i, src in enumerate((hterm, bdl)):
            fzs2[0, i] = src[0]
            fzs2[1, i] = src[CZ - 1]
            v = src[...]
            fys2[0, i] = v[:, 0, :]
            fys2[1, i] = v[:, CY - 1, :]
            hi, lo = split(v.reshape(ROWS, CX))
            f = dot(pick, jnp.concatenate([hi, lo], axis=1), ((1,), (1,))).astype(BF16)
            fxs2[0, i] = f[0:16]
            fxs2[1, i] = f[16:32]
        fhub[2].start()

    def send_z(n, src):
        zs[n, 0] = src[0:R].reshape(R * CY, CX).astype(BF16)
        zs[n, 1] = src[CZ - R : CZ].reshape(R * CY, CX).astype(BF16)
        zhub[n].start()

    def taps(at):
        t = TAPS[R] * at(R)
        for k in range(R):
            t += TAPS[k] * (at(k) + at(2 * R - k))
        return t

    def blur_z(n, src, out):
        zbuf[R : R + CZ] = src[...]
        with scope("wait_z"):
            zhub[n].wait_recv()
        zbuf[0:R] = zr[n, 0].astype(F32).reshape(R, CY, CX)
        zbuf[R + CZ : 2 * R + CZ] = zr[n, 1].astype(F32).reshape(R, CY, CX)

        @pl.loop(0, CZ, unroll=2)
        def _(z):
            out[z] = taps(lambda k: zbuf[z + k])

    def send_yx(n, w):
        v = w[...]
        ys[n, 0] = v[:, 0:R, :].reshape(CZ * R, CX).astype(BF16)
        ys[n, 1] = v[:, CY - R :, :].reshape(CZ * R, CX).astype(BF16)
        hi, lo = split(v.reshape(ROWS, CX))
        f = dot(pick, jnp.concatenate([hi, lo], axis=1), ((1,), (1,))).astype(BF16)
        xs[n, 0] = f[0:16]
        xs[n, 1] = f[16:32]
        yxhub[n].start()

    def rows_of(m, slot, weights):
        halo = xr[m, slot].reshape(32, ROWS)
        return dot(jnp.concatenate([halo, halo], axis=0), weights, ((0,), (0,)))

    def own_rows(w, mat3):
        hi, lo = split(w[...].reshape(ROWS, CX))
        both = jnp.concatenate([hi, lo], axis=1)
        return dot(both, mat3[0 : 2 * CX], ((1,), (0,))) + dot(hi, mat3[2 * CX :], ((1,), (0,)))

    def blur_yx(n, w, put):
        own = own_rows(w, bx)
        ybuf[:, R : R + CY, :] = own.reshape(CZ, CY, CX)
        with scope("wait_yx"):
            yxhub[n].wait_recv(slice(0, 6))
        ybuf[:, R : R + CY, :] += rows_of(n, 1, wx[0:64]).reshape(CZ, CY, CX)
        sides = (
            (0, slice(CY - R, CY), slice(0, R)),
            (1, slice(0, R), slice(R + CY, 2 * R + CY)),
        )
        for side, at, to in sides:
            ybuf[:, to, :] = rows_of(n, 2 * side, wx[0:64]).reshape(CZ, CY, CX)[:, at, :]
        with scope("wait_yx"):
            yxhub[n].wait_recv(slice(6, 8))
        for side, at, to in sides:
            y = yr[n, side]
            rows = dot(jnp.concatenate([y, y], axis=1), bx[CX:], ((1,), (0,)))
            ybuf[:, to, :] += rows.reshape(CZ, R, CX)

        @pl.loop(0, CZ, unroll=2)
        def _(z):
            put(z, taps(lambda k: ybuf[z, k : k + CY, :]))

    lane, sub = iota((CY, CX), 1), iota((CY, CX), 0)
    ends = ((gz == 0, gz == GZ - 1), (gy == 0, gy == GY - 1), (gx == 0, gx == GX - 1))

    def wait_faces(n):
        with scope("wait_faces"):
            fhub[n].wait_recv()
        xlr[...] = dot(fxr[n].reshape(32, ROWS), wx[64:96], ((0,), (0,))).reshape(CZ, CY, CX)
        xa[0] = fzr[n, 0]
        xa[CZ + 1] = fzr[n, 1]

    def diffs(fy, z):
        v = xa[z + 1]
        up, low = xa[z + 2], xa[z]
        yield (
            jnp.where((z == CZ - 1) & ends[0][1], 0.0, up - v),
            jnp.where((z == 0) & ends[0][0], 0.0, v - low),
        )
        up = jnp.where(sub == CY - 1, fy[1, pl.ds(z, 1), :], pltpu.roll(v, CY - 1, 0))
        low = jnp.where(sub == 0, fy[0, pl.ds(z, 1), :], pltpu.roll(v, 1, 0))
        yield (
            jnp.where((sub == CY - 1) & ends[1][1], 0.0, up - v),
            jnp.where((sub == 0) & ends[1][0], 0.0, v - low),
        )
        edge = xlr[z]
        up = jnp.where(lane == CX - 1, edge, pltpu.roll(v, CX - 1, 1))
        low = jnp.where(lane == 0, edge, pltpu.roll(v, 1, 1))
        yield (
            jnp.where((lane == CX - 1) & ends[2][1], 0.0, up - v),
            jnp.where((lane == 0) & ends[2][0], 0.0, v - low),
        )

    def fold(p):
        return p[0:8] + p[8:16]

    def redz_copy(n, t):
        return pltpu.make_async_remote_copy(
            red0.at[n], redz.at[n, t], rz_send, rz_recv,
            device_id=(lax.rem(gz + t, GZ), gy, gx), device_id_type=MESH,
        )

    def redx_copy(n, t):
        return pltpu.make_async_remote_copy(
            red1.at[n], redx.at[n, t], rx_send, rx_recv,
            device_id=member(t)[1], device_id_type=MESH,
        )

    def put_sums(n, primal, dualres):
        p = jnp.sum(jnp.sum(primal, axis=0, keepdims=True), axis=1, keepdims=True)
        d = jnp.sum(jnp.sum(dualres, axis=0, keepdims=True), axis=1, keepdims=True)
        red0[n] = jnp.where(lane[0:1] < CX // 2, p, d)

    def send_all():
        for slot, (dy, t) in enumerate(ORDER_ALL):
            dev = (gy, gx) if t == 0 else member(t)[1][1:]
            pltpu.make_async_remote_copy(
                red0.at[1], redall.at[slot + 1], all_send, all_recv,
                device_id=(lax.rem(gz + dy, GZ), *dev), device_id_type=MESH,
            ).start()

    def forward_sums(n):
        got = redz.at[n, pl.ds(1, GZ - 1)]
        pltpu.make_async_copy(got, got, rz_recv).wait()
        red1[n] = red0[n] + jnp.sum(redz[n, 1:GZ], axis=0)

        for t in range(1, BRICKS):
            redx_copy(n, t).start()

    def factor_of(n, penalty):
        total = red1[n]
        got = redx.at[n, pl.ds(1, BRICKS - 1)]
        pltpu.make_async_copy(got, got, rx_recv).wait()
        total += jnp.sum(redx[n, 1:BRICKS], axis=0)
        return factor_from(total, penalty)

    def factor_from(total, penalty):
        p = jnp.broadcast_to(total[:, 0:1], (8, CX)) * (1.0 / (3.0 * CELLS))
        d = jnp.broadcast_to(total[:, CX - 1 : CX], (8, CX)) * (1.0 / CELLS)
        d = penalty * penalty * d
        return jnp.sqrt(jnp.sqrt((p + EPS) / (d + EPS)))

    def arrivals(ref, sem):
        got = ref.at[pl.ds(0, BRICKS - 1)]
        pltpu.make_async_copy(got, got, sem).wait()

    def sent(n, ref):
        arrivals(ref.at[n], a_send)

    def send_block(n, i, src, dst, d, dev):
        pltpu.make_async_remote_copy(
            src.at[n, d], dst.at[n, me], a_send, a_recv.at[n, i],
            device_id=dev, device_id_type=MESH,
        ).start()

    def project(n):
        with scope("mm_fwd"):
            for a in range(ANG):
                c = dot(sl[...], mat[:, a * DW : (a + 1) * DW], ((1,), (0,)))
                for h in range(2):
                    stage[h, pl.ds(a, CZ, stride=ANG), :] = c[:, h * 128 : (h + 1) * 128]

        def block_of(d):
            rows = pl.ds(pl.multiple_of(d * ANG, ANG), ANG)
            return jnp.concatenate([stage[0, rows, :], stage[1, rows, :]], axis=1).astype(BF16)

        if n:
            sent(0, snd2)
        for t in range(1, BRICKS):
            d, dev = member(t)
            snd1[n, d] = block_of(d)
            send_block(n, 0, snd1, rcv1, d, dev)

        rcv1[n, me] = block_of(me)

    def return_misfit(n):
        with scope("wait_a1"):
            arrivals(rcv1.at[n], a_recv.at[n, 0])

        def add(s, sums):
            x = rcv1[n, s].astype(F32)
            t = tbv[s]
            t = jnp.concatenate([t, t], axis=1)
            return tuple(sums[q] + jnp.where(t == float(q), x, 0.0) for q in range(NBLK))

        sums = lax.fori_loop(
            0, BRICKS, add, tuple(jnp.zeros((ANG, DW), F32) for _ in range(NBLK)), unroll=2
        )
        for q in range(NBLK):
            cols = slice(q * DW, (q + 1) * DW)
            mis[:, cols] = (sums[q] - acc[:, cols]).astype(BF16).astype(F32)

        def chosen(d):
            t = tbv[d]
            t = jnp.concatenate([t, t], axis=1)
            c = mis[:, 0:DW]
            for q in range(1, NBLK):
                c = jnp.where(t == float(q), mis[:, q * DW : (q + 1) * DW], c)
            return c.astype(BF16)

        sent(n, snd1)
        for t in range(1, BRICKS):
            d, dev = member(t)
            snd2[n, d] = chosen(d)
            send_block(n, 1, snd2, rcv2, d, dev)

        rcv2[n, me] = chosen(me)

    def backproject(n, put):
        with scope("wait_a2"):
            arrivals(rcv2.at[n], a_recv.at[n, 1])
        r = rcv2[n].astype(F32).reshape(CZ * ANG, DW)
        for h in range(2):
            stage[h] = r[:, h * 128 : (h + 1) * 128]
        for a in range(ANG):
            for h in range(2):
                sl[:, a * DW + h * 128 : a * DW + (h + 1) * 128] = stage[
                    h, pl.ds(a, CZ, stride=ANG), :
                ].astype(BF16)
        with scope("mm_bwd"):
            for c in range(ANG):
                put(c, dot(sl[...], mat[c * DW : (c + 1) * DW, :], ((1,), (1,))))

    send_z(0, x0)
    send_faces(0, x0)
    relayout(0, SPLIT)
    blur_z(0, x0, w1)
    send_yx(0, w1)
    relayout(SPLIT, NCHUNK)

    def to_res(z, v):
        res[pl.ds(pl.multiple_of(z * CY, CY), CY), :] = v

    blur_yx(0, w1, to_res)
    for y in range(CY):
        sl[:, y * CX : (y + 1) * CX] = res[pl.ds(y, CZ, stride=CY), :].astype(BF16)
    project(0)

    wait_faces(0)
    xa[1 : CZ + 1] = x0[...]
    cut = SHRINK

    @pl.loop(0, CZ, unroll=2)
    def _(z):
        smooth = jnp.zeros((CY, CX), F32)
        shrunk = jnp.zeros((CY, CX), F32)
        for j, jm in diffs(fyr.at[0], z):
            s = j - jnp.clip(j, -cut, cut)
            sm = jm - jnp.clip(jm, -cut, cut)
            smooth += jm - j
            shrunk += sm - s
        h = STEP * (smooth - shrunk)
        x0[z] = xa[z + 1] - h
        back[z] = shrunk

    send_z(1, x0)

    shape1, shape2 = (160, 256), (256, CX)
    i, m = iota(shape1, 0), iota(shape1, 1) - 8
    i = jnp.where(i < CX, i, jnp.where(i < CX + 16, i - CX - 16, i - 16))
    inside = ((m >= 0) | (gx > 0)) & ((m < CX) | (gx < GX - 1)) & (m < CX + 8)
    thi, tlo = split(jnp.where(inside, gauss(i - m), 0.0))
    m = iota(shape2, 0) - 8
    uhi, ulo = split(gauss(m - iota(shape2, 1)))
    twice = (
        dot(thi, uhi, ((1,), (0,))) + dot(thi, ulo, ((1,), (0,))) + dot(tlo, uhi, ((1,), (0,)))
    )
    bhi, blo = split(twice[0:CX])
    bx2[0:CX] = bhi
    bx2[CX : 2 * CX] = bhi
    bx2[2 * CX : 3 * CX] = blo
    whi, wlo = split(twice[CX : CX + 32])
    wx2[0:32] = whi
    wx2[32:64] = wlo
    last_weights()

    zst[96:128] = jnp.zeros((32, V), BF16)
    shape1, shape2 = (CZ, CX), (CX, CX)
    m = iota(shape1, 1) - 8
    inside = ((m >= 0) | (gz > 0)) & ((m < CZ) | (gz < GZ - 1)) & (m < CZ + 8)
    thi, tlo = split(jnp.where(inside, gauss(iota(shape1, 0) - m), 0.0))

    def from_place(k):
        halo = jnp.where(k < 80, k - 80, jnp.where(k < 96, k - 80 + CZ, 4 * CX))
        return jnp.where(k < 64, lax.rem(k, CZ), halo)

    uhi, ulo = split(gauss(iota(shape2, 0) - 8 - from_place(iota(shape2, 1))))
    twice = (
        dot(thi, uhi, ((1,), (0,))) + dot(thi, ulo, ((1,), (0,))) + dot(tlo, uhi, ((1,), (0,)))
    )
    once = gauss(iota(shape1, 0) - from_place(iota(shape1, 1)))
    for i, t in enumerate((twice, once)):
        hi, lo = split(t)
        tz[32 * i : 32 * i + 32] = hi
        tz[64 + 32 * i : 96 + 32 * i] = lo

    return_misfit(0)
    blur_z(1, x0, w1)
    send_yx(1, w1)

    def to_stack(c, b):
        cols = slice(c * DW, (c + 1) * DW)
        hi, lo = split(b)
        zst[0:32, cols] = hi
        zst[32:64, cols] = lo

    backproject(0, to_stack)
    zhub2.start()

    def to_q(z, v):
        qbuf[pl.ds(z, CY, stride=CZ), :] = v

    blur_yx(1, w1, to_q)
    with scope("wait_z2"):
        zhub2.wait_recv()
    for c in range(ANG):
        cols = slice(c * DW, (c + 1) * DW)
        o = dot(tz[...], zst[:, cols], ((1,), (0,)))
        o = o[0:64] + o[64:128]
        for h in range(2):
            w2[ROWS // 16 * (2 * c + h) : ROWS // 16 * (2 * c + h + 1)] = o[
                0:32, h * 128 : (h + 1) * 128
            ]
        v1z[:, cols] = o[32:64]

    hi, lo = split(w2[...])
    ys2[...] = hi
    f = dot(pick2, hi, ((1,), (1,))).astype(BF16)
    xs[3, 0] = f[0:16]
    xs[3, 1] = f[16:32]
    yxhub2.start()
    slab = (CY, CZ, CX)
    both = jnp.concatenate([hi, lo], axis=1)
    own = dot(both, bx2[0 : 2 * CX], ((1,), (0,))) + dot(hi, bx2[2 * CX :], ((1,), (0,)))
    umid[16:32] = own.reshape(slab)
    for y in range(CY):
        res[pl.ds(y, CZ, stride=CY), :] = v1z[:, y * CX : (y + 1) * CX]
    w1[...] = res[...].reshape(CZ, CY, CX)
    with scope("wait_yx2"):
        yxhub2.wait_recv(slice(0, 6))
    umid[16:32] += rows_of(3, 1, wx2[...]).reshape(slab)
    for side in range(2):
        umid[32 * side : 32 * side + 16] = rows_of(3, 2 * side, wx2[...]).reshape(slab)
    with scope("wait_yx2"):
        yxhub2.wait_recv(slice(6, 8))
    send_yx(2, w1)
    for side in range(2):
        y = yr2[side]
        rows = dot(jnp.concatenate([y, y], axis=1), bx2[CX:], ((1,), (0,)))
        umid[32 * side : 32 * side + 16] += rows.reshape(slab)

    @pl.loop(0, CY + 16)
    def _(y):
        out = ((y < 8) & ends[1][0]) | ((y >= CY + 8) & ends[1][1])
        ytwo[y] = jnp.where(out, 0.0, taps(lambda k: umid[y + k]))

    for y in range(CY):
        q = qbuf[y * CZ : (y + 1) * CZ, :]
        v = q - STEP * taps(lambda k: ytwo[y + k])
        sl[:, y * CX : (y + 1) * CX] = v.astype(BF16)

    project(1)

    def to_x(z, v):
        x = x0[z] - STEP * v
        x0[z] = x
        xa[z + 1] = x

    blur_yx(2, w1, to_x)
    send_faces(1, x0)
    return_misfit(1)
    wait_faces(1)

    def one(z, sums):
        primal, dres = sums
        smooth = jnp.zeros((CY, CX), F32)
        shrunk = jnp.zeros((CY, CX), F32)
        bdual = jnp.zeros((CY, CX), F32)
        for axis, (j, jm) in enumerate(diffs(fyr.at[1], z)):
            s = j - jnp.clip(j, -cut, cut)
            sm = jm - jnp.clip(jm, -cut, cut)
            d = j - s
            dm = jm - sm
            smooth += jm - j
            shrunk += sm - s
            bdual += dm - d
            dl[axis, z] = d
            dlm[axis, z] = dm
            primal += fold(jnp.square(j - s))
        dres += fold(jnp.square(shrunk - back[z]))
        hterm[z] = smooth - shrunk
        back[z] = shrunk
        bdl[z] = bdual
        return primal, dres

    zero = jnp.zeros((8, CX), F32)
    primal, dres = lax.fori_loop(0, CZ, one, (zero, zero), unroll=2)
    put_sums(0, primal, dres)
    for t in range(1, GZ):
        redz_copy(0, t).start()
    send_terms()

    def spread_rows(c, b):
        for h in range(2):
            res[pl.ds(2 * c + h, CZ, stride=CY), :] = b[:, h * 128 : (h + 1) * 128]

    backproject(1, spread_rows)
    zs9[0] = res[0 : (R + 1) * CY].astype(BF16)
    zs9[1] = res[(CZ - R - 1) * CY :].astype(BF16)
    zhub[2].start()
    forward_sums(0)
    zbuf[R + 1 : R + 1 + CZ] = res[...].reshape(CZ, CY, CX)
    with scope("wait_z"):
        zhub[2].wait_recv()
    zbuf[0 : R + 1] = zr9[0].astype(F32).reshape(R + 1, CY, CX)
    zbuf[R + 1 + CZ : 2 * R + 2 + CZ] = zr9[1].astype(F32).reshape(R + 1, CY, CX)

    @pl.loop(0, CZ + 2, unroll=2)
    def _(z):
        zmid[z] = taps(lambda k: zbuf[z + k])

    outer = zmid[0 : CZ + 2]
    n9 = (CZ + 2) * R
    for side, at, ninth in ((0, slice(0, R), R), (1, slice(CY - R, CY), CY - R - 1)):
        ys9[side, 0:n9] = outer[:, at, :].reshape(n9, CX).astype(BF16)
        ys9[side, n9:] = outer[1 : CZ + 1, ninth, :].astype(BF16)
    hi, lo = split(outer.reshape(ROWS9, CX))
    f = dot(pick2, hi, ((1,), (1,))).astype(BF16)
    xs9[0, :, 0:ROWS9] = f[0:16]
    xs9[1, :, 0:ROWS9] = f[16:32]
    yxhub[3].start()
    both = jnp.concatenate([hi, lo], axis=1)
    own = dot(both, bx9[0 : 2 * CX], ((1,), (0,))) + dot(hi, bx9[2 * CX :], ((1,), (0,)))
    own = own.reshape(CZ + 2, CY, 2 * CX)
    ymid[0 : CZ + 2, 16 : 16 + CY, :] = own[:, :, 0:CX]
    ybuf[:, R : R + CY, :] = own[1 : CZ + 1, :, CX:]
    penalty = factor_of(0, jnp.ones((8, CX), F32))
    inv1 = 1.0 / penalty
    pen3 = penalty[0:1].reshape(1, 1, CX)
    inv3 = inv1[0:1].reshape(1, 1, CX)
    spen = STEP * pen3
    x0[...] = x0[...] - spen * (hterm[...] + bdl[...] * inv3)
    dl[...] = dl[...] * inv3
    dlm[...] = dlm[...] * inv3
    with scope("wait_terms"):
        fhub[2].wait_recv()
    for side in range(2):
        fz2[side] = fzr[1, side] - spen[0] * (fzr2[side, 0] + fzr2[side, 1] * inv3[0])
        fy2[side] = fyr[1, side] - spen[0] * (fyr2[side, 0] + fyr2[side, 1] * inv3[0])
    rims = [
        dot(
            jnp.concatenate([fxr2[0, i], fxr2[1, i]], axis=0), wx[64:96], ((0,), (0,))
        ).reshape(CZ, CY, CX)
        for i in range(2)
    ]
    xlr[...] = xlr[...] - spen * (rims[0] + rims[1] * inv3)

    def halo_rows(slot):
        h = xr9[slot].reshape(32, ROWS9P)[:, 0:ROWS9]
        h = dot(jnp.concatenate([h, h], axis=0), wx9[...], ((0,), (0,)))
        return h.reshape(CZ + 2, CY, 2 * CX)

    with scope("wait_yx"):
        yxhub[3].wait_recv(slice(0, 6))
    more = halo_rows(1)
    ymid[0 : CZ + 2, 16 : 16 + CY, :] += more[:, :, 0:CX]
    ybuf[:, R : R + CY, :] += more[1 : CZ + 1, :, CX:]
    sides = ((0, slice(0, 16)), (1, slice(16 + CY, 32 + CY)))
    for side, to in sides:
        more = halo_rows(2 * side)
        ymid[0 : CZ + 2, to, :] = more[:, :, 0:CX]
        if side == 0:
            ybuf[:, 0:R, :] = more[1 : CZ + 1, CY - R :, CX:]
        else:
            ybuf[:, R + CY :, :] = more[1 : CZ + 1, 0:R, CX:]
    with scope("wait_yx"):
        yxhub[3].wait_recv(slice(6, 8))
    for side in range(2):
        y = yr9[side]
        rows = dot(jnp.concatenate([y, y], axis=1), bx9[CX:], ((1,), (0,)))
        near = rows[0:n9].reshape(CZ + 2, R, 2 * CX)
        to = slice(16 - R, 16) if side == 0 else slice(16 + CY, 16 + CY + R)
        ymid[0 : CZ + 2, to, :] += near[:, :, 0:CX]
        ymid[1 : CZ + 1, (15 - R if side == 0 else 16 + CY + R), :] += rows[n9:, 0:CX]
        to = slice(0, R) if side == 0 else slice(R + CY, 2 * R + CY)
        ybuf[:, to, :] += near[1 : CZ + 1, :, CX:]

    @pl.loop(0, CZ, unroll=2)
    def _(z):
        v = x0[z] - STEP * taps(lambda k: ymid[z + 1, 16 - R + k : 16 - R + CY + k, :])
        xa[z + 1] = v
        x_out[z] = v
        xlr[z] = xlr[z] - STEP * taps(lambda k: ybuf[z, k : k + CY, :])
        low = taps(lambda k: ymid[z + 1, k : k + R, :])[R - 1 : R]
        fy2[0, pl.ds(z, 1), :] = fy2[0, pl.ds(z, 1), :] - STEP * low
        high = taps(lambda k: ymid[z + 1, 16 + R + k : 16 + 2 * R + k, :])[0:1]
        fy2[1, pl.ds(z, 1), :] = fy2[1, pl.ds(z, 1), :] - STEP * high

    for side, at in ((0, 0), (1, CZ + 1)):
        xa[at] = fz2[side] - STEP * taps(lambda k: ymid[at, 16 - R + k : 16 - R + CY + k, :])
    cut2 = (SHRINK / penalty)[0:1]

    def last(z, sums):
        primal, dres = sums
        shrunk = jnp.zeros((CY, CX), F32)
        for axis, (j, jm) in enumerate(diffs(fy2, z)):
            t = j + dl[axis, z]
            tm = jm + dlm[axis, z]
            s = t - jnp.clip(t, -cut2, cut2)
            sm = tm - jnp.clip(tm, -cut2, cut2)
            shrunk += sm - s
            dl[axis, z] = t - s
            primal += fold(jnp.square(j - s))
        dres += fold(jnp.square(shrunk - back[z]))
        return primal, dres

    with scope("last"):
        primal, dres = lax.fori_loop(0, CZ, last, (zero, zero), unroll=4)
    put_sums(1, primal, dres)
    send_all()
    with scope("sums"):
        got = redall.at[pl.ds(1, GZ * BRICKS - 1)]
        pltpu.make_async_copy(got, got, all_recv).wait()
    factor2 = factor_from(red0[1] + jnp.sum(redall[1 : GZ * BRICKS], axis=0), penalty)
    scale = (1.0 / factor2)[0:1].reshape(1, 1, 1, CX)
    with scope("scale"):
        dual_out[...] = dl[...] * scale

    with scope("wait_sends"):
        for h in (zhub[2], yxhub[3], fhub[2]):
            h.wait_send()
        sent(1, snd2)
        got = redz.at[0, pl.ds(1, GZ - 1)]
        pltpu.make_async_copy(got, got, rz_send).wait()
        got = redx.at[0, pl.ds(1, BRICKS - 1)]
        pltpu.make_async_copy(got, got, rx_send).wait()
        got = redall.at[pl.ds(1, GZ * BRICKS - 1)]
        pltpu.make_async_copy(got, got, all_send).wait()


def body(start, measured, tiles, tile_block, angle_row):
    vm = pltpu.VMEM
    dma = pltpu.SemaphoreType.DMA
    block = vm((CZ, CY, CX), F32)
    return pl.pallas_call(
        kernel,
        out_shape=(
            pltpu.VMEM((CZ, CY, CX), F32),
            pltpu.VMEM((3, CZ, CY, CX), F32),
        ),
        in_specs=[
            pl.BlockSpec(memory_space=pltpu.HBM),
            pl.BlockSpec(memory_space=pltpu.HBM),
            pl.BlockSpec(memory_space=pltpu.HBM),
            pl.BlockSpec(memory_space=pltpu.VMEM),
            pl.BlockSpec(memory_space=pltpu.SMEM),
        ],
        out_specs=(pl.BlockSpec(memory_space=pltpu.VMEM), pl.BlockSpec(memory_space=pltpu.VMEM)),
        scratch_shapes=[
            vm((V, ANG, DW), BF16),
            vm((V, ANG * DW), BF16),
            vm((2, CHUNK * PITCH, 128), F32),
            block, block,
            vm((ROWS, CX), F32),
            vm((ROWS, CX), F32),
            vm((ROWS, CX), F32),
            vm((CZ + 2, CY, CX), F32),
            vm((CZ + 32, CY, CX), F32),
            vm((CZ + 16, CY, CX), F32),
            vm((CZ, CY + 16, CX), F32),
            vm((CZ + 2, CY + 32, CX), F32),
            vm((BRICKS, ANG, CX), F32),
            vm((1, ANG, NBLK * DW), F32),
            vm((ANG, NBLK * DW), F32),
            vm((ANG, NBLK * DW), F32),
            vm((2, 2, R * CY, CX), BF16),
            vm((2, 2, R * CY, CX), BF16),
            vm((128, V), BF16),
            vm((128, 128), BF16),
            vm((CZ, V), F32),
            vm((CY + 32, CZ, CX), F32),
            vm((CY + 16, CZ, CX), F32),
            vm((3, 2, CZ * R, CX), BF16),
            vm((3, 2, CZ * R, CX), BF16),
            vm((ROWS, CX), BF16),
            vm((2, ROWS, CX), BF16),
            vm((4, 2, 16, ROWS), BF16),
            vm((4, 3, 2, 16, ROWS), BF16),
            vm((2, (R + 1) * CY, CX), BF16),
            vm((2, (R + 1) * CY, CX), BF16),
            vm((2, (CZ + 2) * R + CZ, CX), BF16),
            vm((2, (CZ + 2) * R + CZ, CX), BF16),
            vm((2, 16, ROWS9P), BF16),
            vm((3, 2, 16, ROWS9P), BF16),
            vm((2, 2, CY, CX), F32),
            vm((2, 2, CY, CX), F32),
            vm((2, 2, CZ, CX), F32),
            vm((2, 2, CZ, CX), F32),
            vm((2, 2, 16, ROWS), BF16),
            vm((2, 2, 16, ROWS), BF16),
            vm((2, 2, CY, CX), F32),
            vm((2, 2, CY, CX), F32),
            vm((2, 2, CZ, CX), F32),
            vm((2, 2, CZ, CX), F32),
            vm((2, 2, 16, ROWS), BF16),
            vm((2, 2, 16, ROWS), BF16),
            vm((2, CY, CX), F32),
            vm((2, CZ, CX), F32),
            vm((2, CZ * ANG, 128), F32),
            vm((CZ, V), BF16),
            vm((2, BRICKS, ANG, DW), BF16),
            vm((2, BRICKS, ANG, DW), BF16),
            vm((2, BRICKS, ANG, DW), BF16),
            vm((2, BRICKS, ANG, DW), BF16),
            block, block,
            vm((3, CZ, CY, CX), F32),
            vm((3, CZ, CY, CX), F32),
            block, block,
            vm((2, 1, CX), F32),
            vm((2, GZ, 1, CX), F32),
            vm((2, 1, CX), F32),
            vm((2, BRICKS, 1, CX), F32),
            vm((GZ * BRICKS, 1, CX), F32),
            vm((3 * CX, CX), BF16),
            vm((96, CX), BF16),
            vm((3 * CX, CX), BF16),
            vm((64, CX), BF16),
            vm((3 * CX, 2 * CX), BF16),
            vm((64, 2 * CX), BF16),
            dma((2,)),
            dma((V // LOAD,)),
            dma((2,)),
            dma((2, 2)),
            dma((8,)),
            dma((2, 8)),
            dma((3, 2)),
            dma((2, 3, 2)),
            dma,
            dma((2, 2)),
            dma,
            dma,
            dma,
            dma,
            dma,
            dma,
        ],
        compiler_params=pltpu.CompilerParams(
            collective_id=0, has_side_effects=True, vmem_limit_bytes=60 * 1024 * 1024
        ),
    )(start, measured, tiles, tile_block, angle_row)


def solution(mesh):
    return jax.shard_map(
        body,
        mesh=mesh,
        in_specs=(
            P("gz", "gy", "gx"),
            P(("gz", "gy", "gx"), None, None),
            P("gy", None, "gx"),
            P(),
            P(),
        ),
        out_specs=(P("gz", "gy", "gx"), P(None, "gz", "gy", "gx")),
        check_vma=False,
    )
```

```python
import math

import jax
import jax.numpy as jnp
from jax import lax
from jax.experimental import pallas as pl
from jax.experimental.pallas import tpu as pltpu
from jax.sharding import PartitionSpec as P

CZ, CY, CX = 32, 16, 128
ROWS = CZ * CY
ANG, DW, NBLK = 8, 256, 4
V = CY * CX
R = 8
GZ, GY, GX = 4, 4, 8
BRICKS = GY * GX
CELLS = float(CZ * CY * CX * GZ * BRICKS)
MESH = pl.DeviceIdType.MESH
F32, BF16 = jnp.float32, jnp.bfloat16
STEP = 0.5
SHRINK = 0.2
EPS = 1e-6
CHUNK = 128
NCHUNK = V // CHUNK
ORDER = sorted(
    ((dx, dz, dc) for dz in range(4) for dx in range(4) for dc in range(2) if dx or dz or dc),
    key=lambda s: -(min(s[0], 4 - s[0]) + min(s[1], 4 - s[1])),
)
LOAD = 512
ROWS9 = (CZ + 2) * CY
ROWS9P = -(-ROWS9 // 128) * 128
PITCH = 9
SPLIT = 4
TURN = 3
ORDER_ALL = sorted(
    ((dy, t) for dy in range(GZ) for t in range(GY * GX) if dy or t),
    key=lambda s: -(
        min(s[0], 4 - s[0])
        + (sum(min(d, 4 - d) for d in ORDER[s[1] - 1][:2]) if s[1] else 0)
    ),
)

RAW = [math.exp(-k * k / 12.5) for k in range(-R, R + 1)]
TAPS = [r / sum(RAW) for r in RAW]
TWICE = [
    sum(TAPS[k] * TAPS[d + 2 * R - k] for k in range(2 * R + 1) if 0 <= d + 2 * R - k <= 2 * R)
    for d in range(2 * R + 1)
]


def dot(a, b, dims):
    return lax.dot_general(a, b, (dims, ((), ())), preferred_element_type=F32)


def split(v):
    hi = v.astype(BF16)
    lo = (v - hi.astype(F32)).astype(BF16)
    return hi, lo


def kernel(
    start_ref, meas_ref, tiles_ref, tb_ref, row_ref,
    x_out, dual_out,
    raw, mat, turned, tmp, x0, w1, w2, res, qbuf, xa, zbuf, zmid, ybuf, ymid, tbv, obs, mis, acc,
    zs, zr, zst, tz, tz9, v1z, umid, ytwo, ys, yr, ys2, yr2, xs, xr,
    ys9, yr9, xs9, xr9,
    fzs, fzr, fys, fyr, fxs, fxr, fzs2, fzr2, fys2, fyr2, fxs2, fxr2, fz2, fy2,
    stage, sl, snd1, rcv1, snd2, rcv2,
    hterm, back, dl, dlm, xlr, bdl,
    red0, redz, red1, redx, redall,
    bx, wx, bx2, wx2, bx9, wx9,
    load_sem, tile_sem, z_send, z_recv, yx_send, yx_recv, f_send, f_recv,
    a_send, a_recv, rz_send, rz_recv, rx_send, rx_recv, all_send, all_recv,
):
    gz, gy, gx = lax.axis_index("gz"), lax.axis_index("gy"), lax.axis_index("gx")
    me = gy * GX + gx
    scope = jax.named_scope

    barrier = pltpu.get_barrier_semaphore()

    chip_x = 2 * (gy // 2) + lax.rem(gx, 2)
    chip_z, core = gx // 2, lax.rem(gy, 2)

    def member(t):
        dx, dz, dc = ORDER[t - 1]
        x = lax.rem(chip_x + dx, 4)
        z = lax.rem(chip_z + dz, 4)
        y = 2 * (x // 2) + lax.rem(core + dc, 2)
        x = 2 * z + lax.rem(x, 2)
        return y * GX + x, (gz, y, x)

    for t in range(1, BRICKS):
        pl.semaphore_signal(barrier, inc=1, device_id=member(t)[1], device_id_type=MESH)

    @pl.loop(1, GZ)
    def _(t):
        pl.semaphore_signal(
            barrier, inc=1, device_id=(lax.rem(gz + t, GZ), gy, gx), device_id_type=MESH
        )

    ld = [
        pltpu.make_async_copy(start_ref, x0, load_sem.at[0]),
        pltpu.make_async_copy(meas_ref, obs, load_sem.at[1]),
    ]
    for c in ld:
        c.start()

    def turn(low, high):
        @pl.loop(low, high)
        def _(c):
            rows = pl.ds(pl.multiple_of(c * DW, DW), DW)
            for a in range(ANG):
                turned[a * DW : (a + 1) * DW, rows] = mat[rows, a * DW : (a + 1) * DW].T

    def tile_copy(c):
        rows = pl.ds(c * LOAD, LOAD)
        return pltpu.make_async_copy(tiles_ref.at[rows], raw.at[rows], tile_sem.at[c])


    def there(dz, dy, dx):
        ok = True
        for d, at, n in ((dz, gz, GZ), (dy, gy, GY), (dx, gx, GX)):
            if d:
                near = at > 0 if d < 0 else at < n - 1
                ok = near if ok is True else jnp.logical_and(ok, near)
        return ok

    class Hub:
        def __init__(self, items, before=None):
            self.before = before
            self.items = [
                (
                    there(*d),
                    there(*(-i for i in d)),
                    pltpu.make_async_remote_copy(
                        src, dst, ss, rs,
                        device_id=(gz + d[0], gy + d[1], gx + d[2]), device_id_type=MESH,
                    ),
                    dst,
                )
                for d, src, dst, ss, rs in items
            ]

        def clear(self):
            for _, arrives, _, dst in self.items:

                @pl.when(jnp.logical_not(arrives))
                def _():
                    dst[...] = jnp.zeros(dst.shape, dst.dtype)

        def start(self):
            if self.before is not None:
                self.before.wait_send()
            for leaves, _, copy, _ in self.items:
                pl.when(leaves)(copy.start)

        def wait_recv(self, part=slice(None)):
            for _, arrives, copy, _ in self.items[part]:
                pl.when(arrives)(copy.wait_recv)

        def wait_send(self):
            for leaves, _, copy, _ in self.items:
                pl.when(leaves)(copy.wait_send)

    def pair(axis, src, dst, send, recv):
        unit = [int(axis == a) for a in range(3)]
        return [
            ([-u for u in unit], src.at[0], dst.at[1], send.at[0], recv.at[0]),
            (unit, src.at[1], dst.at[0], send.at[1], recv.at[1]),
        ]

    def around(k, low, high, into_low, into_high, faces, halos, before):
        items = []
        i = 2
        for sy in (-1, 1, 0):
            for side, sx in ((0, -1), (1, 1)):
                items.append((
                    (0, sy, sx), faces.at[side], halos.at[1 - sy, 1 - side],
                    yx_send.at[i], yx_recv.at[k, i],
                ))
                i += 1
        items += [
            ((0, -1, 0), low, into_high, yx_send.at[0], yx_recv.at[k, 0]),
            ((0, 1, 0), high, into_low, yx_send.at[1], yx_recv.at[k, 1]),
        ]
        return Hub(items, before)

    def zswap(k, src, dst, before):
        return Hub(pair(0, src, dst, z_send, z_recv.at[k]), before)

    zhub = [zswap(0, zs.at[0], zr.at[0], None)]
    zhub.append(zswap(1, zs.at[1], zr.at[1], zhub[0]))
    def zstack(k, before):
        return Hub(
            [
                ((-1, 0, 0), zst.at[0:16], zst.at[80:96], z_send.at[0], z_recv.at[k, 0]),
                ((1, 0, 0), zst.at[16:32], zst.at[64:80], z_send.at[1], z_recv.at[k, 1]),
            ],
            before,
        )

    zhub2 = zstack(0, zhub[1])
    zhub.append(zstack(1, None))

    def yxswap(n, k, before):
        low, high = yr.at[n, 0], yr.at[n, 1]
        return around(k, ys.at[n, 0], ys.at[n, 1], low, high, xs.at[n], xr.at[n], before)

    yxhub = [yxswap(0, 0, None)]
    yxhub.append(yxswap(1, 1, yxhub[0]))
    yxhub2 = around(0, ys2, ys2, yr2.at[0], yr2.at[1], xs.at[3], xr.at[3], yxhub[1])
    yxhub.append(yxswap(2, 1, yxhub2))
    yxhub.append(
        around(0, ys9.at[0], ys9.at[1], yr9.at[0], yr9.at[1], xs9, xr9, yxhub[2])
    )
    fhub = []
    for k, z, y, x in (
        (0, (fzs.at[0], fzr.at[0]), (fys.at[0], fyr.at[0]), (fxs.at[0], fxr.at[0])),
        (1, (fzs.at[1], fzr.at[1]), (fys.at[1], fyr.at[1]), (fxs.at[1], fxr.at[1])),
        (0, (fzs2, fzr2), (fys2, fyr2), (fxs2, fxr2)),
    ):
        fhub.append(
            Hub(
                pair(0, *z, f_send.at[0], f_recv.at[k, 0])
                + pair(1, *y, f_send.at[1], f_recv.at[k, 1])
                + pair(2, *x, f_send.at[2], f_recv.at[k, 2]),
                fhub[-1] if fhub else None,
            )
        )
    xs9[...] = jnp.zeros_like(xs9)
    hubs = zhub + [zhub2] + yxhub + [yxhub2] + fhub
    for h in hubs:
        h.clear()

    def gauss(d):
        df = d.astype(F32)
        w = jnp.exp(df * df * (-1.0 / 12.5)) * (1.0 / sum(RAW))
        return jnp.where(jnp.abs(d) <= R, w, 0.0)

    def iota(shape, axis):
        return lax.broadcasted_iota(jnp.int32, shape, axis)

    square = (CX, CX)
    bhi, blo = split(gauss(iota(square, 0) - iota(square, 1)))
    bx[0:CX] = bhi
    bx[CX : 2 * CX] = bhi
    bx[2 * CX : 3 * CX] = blo
    k0, k1 = iota((32, CX), 0), iota((32, CX), 1)
    pos = jnp.where(k0 < 16, lax.rem(k0, 8) - 8, CX + lax.rem(k0, 8))
    whi, wlo = split(gauss(pos - k1))
    wx[0:32] = whi
    wx[32:64] = wlo
    rim = ((k1 == 0) & ((k0 == 7) | (k0 == 15))) | ((k1 == CX - 1) & ((k0 == 16) | (k0 == 24)))
    wx[64:96] = jnp.where(rim, 1.0, 0.0).astype(BF16)
    s0, s1 = iota((32, 2 * CX), 0), iota((32, 2 * CX), 1)
    want = jnp.where(s0 < 16, lax.rem(s0, 8), CX - 8 + lax.rem(s0, 8)) + jnp.where(
        lax.rem(s0, 16) < 8, 0, CX
    )
    pick = jnp.where(s1 == want, 1.0, 0.0).astype(BF16)
    pick2 = jnp.where(k1 == jnp.where(k0 < 16, k0, CX - 32 + k0), 1.0, 0.0).astype(BF16)

    def place(c):
        edge = jnp.where(c == CX, -1, jnp.where(c == 2 * CX - 1, CX, 4 * CX))
        return jnp.where(c < CX, c, edge)

    def last_weights():
        shape = (CX, 2 * CX)
        hi, lo = split(gauss(iota(shape, 0) - place(iota(shape, 1))))
        bx9[0:CX] = hi
        bx9[CX : 2 * CX] = hi
        bx9[2 * CX : 3 * CX] = lo
        shape = (32, 2 * CX)
        k = iota(shape, 0)
        hi, lo = split(gauss(jnp.where(k < 16, k - 16, CX - 16 + k) - place(iota(shape, 1))))
        wx9[0:32] = hi
        wx9[32:64] = lo

    wide = (GX, GX * CX)
    spread = jnp.where(iota(wide, 0) == iota(wide, 1) // CX, 1.0, 0.0).astype(BF16)
    for b in range(GY):
        rows = dot(tb_ref[b].astype(F32).astype(BF16), spread, ((0,), (0,)))
        for c in range(GX):
            tbv[b * GX + c] = rows[:, c * CX : (c + 1) * CX]

    def relayout(low, high):
        for c in range(V // LOAD):
            if low * CHUNK <= c * LOAD < high * CHUNK:
                tile_copy(c).wait()

        @pl.loop(low, high)
        def _(c):
            rows = pl.ds(pl.multiple_of(c * CHUNK, CHUNK), CHUNK)
            block = raw[rows].astype(F32)
            for h in range(2):
                for j in range(CHUNK):
                    tmp[h, PITCH * j : PITCH * j + ANG, :] = block[j, :, h * 128 : (h + 1) * 128]
            for a in range(ANG):
                for h in range(2):
                    part = tmp[h, pl.ds(a, CHUNK, stride=PITCH), :]
                    mat[rows, a * DW + h * 128 : a * DW + (h + 1) * 128] = part.astype(BF16)

    ld[0].wait()
    for c in range(V // LOAD):
        tile_copy(c).start()
    ld[1].wait()
    for a in range(ANG):
        acc[pl.ds(a, 1), :] = obs[0, pl.ds(row_ref[a], 1), :]

    with scope("wait_barrier"):
        pl.semaphore_wait(barrier, BRICKS - 1 + GZ - 1)

    def send_faces(n, src):
        fzs[n, 0] = src[0]
        fzs[n, 1] = src[CZ - 1]
        v = src[...]
        fys[n, 0] = v[:, 0, :]
        fys[n, 1] = v[:, CY - 1, :]
        hi, lo = split(v.reshape(ROWS, CX))
        f = dot(pick, jnp.concatenate([hi, lo], axis=1), ((1,), (1,))).astype(BF16)
        fxs[n, 0] = f[0:16]
        fxs[n, 1] = f[16:32]
        fhub[n].start()

    def send_terms():
        for i, src in enumerate((hterm, bdl)):
            fzs2[0, i] = src[0]
            fzs2[1, i] = src[CZ - 1]
            v = src[...]
            fys2[0, i] = v[:, 0, :]
            fys2[1, i] = v[:, CY - 1, :]
            hi, lo = split(v.reshape(ROWS, CX))
            f = dot(pick, jnp.concatenate([hi, lo], axis=1), ((1,), (1,))).astype(BF16)
            fxs2[0, i] = f[0:16]
            fxs2[1, i] = f[16:32]
        fhub[2].start()

    def send_z(n, src):
        zs[n, 0] = src[0:R].reshape(R * CY, CX).astype(BF16)
        zs[n, 1] = src[CZ - R : CZ].reshape(R * CY, CX).astype(BF16)
        zhub[n].start()

    def taps(at):
        t = TAPS[R] * at(R)
        for k in range(R):
            t += TAPS[k] * (at(k) + at(2 * R - k))
        return t

    def blur_z(n, src, out):
        zbuf[R : R + CZ] = src[...]
        with scope("wait_z"):
            zhub[n].wait_recv()
        zbuf[0:R] = zr[n, 0].astype(F32).reshape(R, CY, CX)
        zbuf[R + CZ : 2 * R + CZ] = zr[n, 1].astype(F32).reshape(R, CY, CX)

        @pl.loop(0, CZ, unroll=2)
        def _(z):
            out[z] = taps(lambda k: zbuf[z + k])

    def send_yx(n, w, now=True):
        v = w[...]
        ys[n, 0] = v[:, 0:R, :].reshape(CZ * R, CX).astype(BF16)
        ys[n, 1] = v[:, CY - R :, :].reshape(CZ * R, CX).astype(BF16)
        hi, lo = split(v.reshape(ROWS, CX))
        f = dot(pick, jnp.concatenate([hi, lo], axis=1), ((1,), (1,))).astype(BF16)
        xs[n, 0] = f[0:16]
        xs[n, 1] = f[16:32]
        if now:
            yxhub[n].start()

    def rows_of(m, slot, weights):
        halo = xr[m, slot].reshape(32, ROWS)
        return dot(jnp.concatenate([halo, halo], axis=0), weights, ((0,), (0,)))

    def own_rows(w, mat3):
        hi, lo = split(w[...].reshape(ROWS, CX))
        both = jnp.concatenate([hi, lo], axis=1)
        return dot(both, mat3[0 : 2 * CX], ((1,), (0,))) + dot(hi, mat3[2 * CX :], ((1,), (0,)))

    def blur_yx(n, w, put):
        own = own_rows(w, bx)
        ybuf[:, R : R + CY, :] = own.reshape(CZ, CY, CX)
        with scope("wait_yx"):
            yxhub[n].wait_recv(slice(0, 6))
        ybuf[:, R : R + CY, :] += rows_of(n, 1, wx[0:64]).reshape(CZ, CY, CX)
        sides = (
            (0, slice(CY - R, CY), slice(0, R)),
            (1, slice(0, R), slice(R + CY, 2 * R + CY)),
        )
        for side, at, to in sides:
            ybuf[:, to, :] = rows_of(n, 2 * side, wx[0:64]).reshape(CZ, CY, CX)[:, at, :]
        with scope("wait_yx"):
            yxhub[n].wait_recv(slice(6, 8))
        for side, at, to in sides:
            y = yr[n, side]
            rows = dot(jnp.concatenate([y, y], axis=1), bx[CX:], ((1,), (0,)))
            ybuf[:, to, :] += rows.reshape(CZ, R, CX)

        @pl.loop(0, CZ, unroll=2)
        def _(z):
            put(z, taps(lambda k: ybuf[z, k : k + CY, :]))

    lane, sub = iota((CY, CX), 1), iota((CY, CX), 0)
    ends = ((gz == 0, gz == GZ - 1), (gy == 0, gy == GY - 1), (gx == 0, gx == GX - 1))

    def wait_faces(n):
        with scope("wait_faces"):
            fhub[n].wait_recv()
        xlr[...] = dot(fxr[n].reshape(32, ROWS), wx[64:96], ((0,), (0,))).reshape(CZ, CY, CX)
        xa[0] = fzr[n, 0]
        xa[CZ + 1] = fzr[n, 1]

    def diffs(fy, z):
        v = xa[z + 1]
        up, low = xa[z + 2], xa[z]
        yield (
            jnp.where((z == CZ - 1) & ends[0][1], 0.0, up - v),
            jnp.where((z == 0) & ends[0][0], 0.0, v - low),
        )
        up = jnp.where(sub == CY - 1, fy[1, pl.ds(z, 1), :], pltpu.roll(v, CY - 1, 0))
        low = jnp.where(sub == 0, fy[0, pl.ds(z, 1), :], pltpu.roll(v, 1, 0))
        yield (
            jnp.where((sub == CY - 1) & ends[1][1], 0.0, up - v),
            jnp.where((sub == 0) & ends[1][0], 0.0, v - low),
        )
        edge = xlr[z]
        up = jnp.where(lane == CX - 1, edge, pltpu.roll(v, CX - 1, 1))
        low = jnp.where(lane == 0, edge, pltpu.roll(v, 1, 1))
        yield (
            jnp.where((lane == CX - 1) & ends[2][1], 0.0, up - v),
            jnp.where((lane == 0) & ends[2][0], 0.0, v - low),
        )

    def fold(p):
        return p[0:8] + p[8:16]

    def redz_copy(n, t):
        return pltpu.make_async_remote_copy(
            red0.at[n], redz.at[n, t], rz_send, rz_recv,
            device_id=(lax.rem(gz + t, GZ), gy, gx), device_id_type=MESH,
        )

    def redx_copy(n, t):
        return pltpu.make_async_remote_copy(
            red1.at[n], redx.at[n, t], rx_send, rx_recv,
            device_id=member(t)[1], device_id_type=MESH,
        )

    def put_sums(n, primal, dualres):
        p = jnp.sum(jnp.sum(primal, axis=0, keepdims=True), axis=1, keepdims=True)
        d = jnp.sum(jnp.sum(dualres, axis=0, keepdims=True), axis=1, keepdims=True)
        red0[n] = jnp.where(lane[0:1] < CX // 2, p, d)

    def send_all():
        for slot, (dy, t) in enumerate(ORDER_ALL):
            dev = (gy, gx) if t == 0 else member(t)[1][1:]
            pltpu.make_async_remote_copy(
                red0.at[1], redall.at[slot + 1], all_send, all_recv,
                device_id=(lax.rem(gz + dy, GZ), *dev), device_id_type=MESH,
            ).start()

    def forward_sums(n):
        got = redz.at[n, pl.ds(1, GZ - 1)]
        pltpu.make_async_copy(got, got, rz_recv).wait()
        red1[n] = red0[n] + jnp.sum(redz[n, 1:GZ], axis=0)

        for t in range(1, BRICKS):
            redx_copy(n, t).start()

    def factor_of(n, penalty):
        total = red1[n]
        got = redx.at[n, pl.ds(1, BRICKS - 1)]
        pltpu.make_async_copy(got, got, rx_recv).wait()
        total += jnp.sum(redx[n, 1:BRICKS], axis=0)
        return factor_from(total, penalty)

    def factor_from(total, penalty):
        p = jnp.broadcast_to(total[:, 0:1], (8, CX)) * (1.0 / (3.0 * CELLS))
        d = jnp.broadcast_to(total[:, CX - 1 : CX], (8, CX)) * (1.0 / CELLS)
        d = penalty * penalty * d
        return jnp.sqrt(jnp.sqrt((p + EPS) / (d + EPS)))

    def arrivals(ref, sem):
        got = ref.at[pl.ds(0, BRICKS - 1)]
        pltpu.make_async_copy(got, got, sem).wait()

    def sent(n, ref):
        arrivals(ref.at[n], a_send)

    def send_block(n, i, src, dst, d, dev):
        pltpu.make_async_remote_copy(
            src.at[n, d], dst.at[n, me], a_send, a_recv.at[n, i],
            device_id=dev, device_id_type=MESH,
        ).start()

    def project(n):
        with scope("mm_fwd"):
            for a in range(ANG):
                c = dot(sl[...], mat[:, a * DW : (a + 1) * DW], ((1,), (0,)))
                for h in range(2):
                    stage[h, pl.ds(a, CZ, stride=ANG), :] = c[:, h * 128 : (h + 1) * 128]

        def block_of(d):
            rows = pl.ds(pl.multiple_of(d * ANG, ANG), ANG)
            return jnp.concatenate([stage[0, rows, :], stage[1, rows, :]], axis=1).astype(BF16)

        if n:
            sent(0, snd2)
        for t in range(1, BRICKS):
            d, dev = member(t)
            snd1[n, d] = block_of(d)
            send_block(n, 0, snd1, rcv1, d, dev)

        rcv1[n, me] = block_of(me)

    def return_misfit(n):
        with scope("wait_a1"):
            arrivals(rcv1.at[n], a_recv.at[n, 0])

        def add(s, sums):
            x = rcv1[n, s].astype(F32)
            t = tbv[s]
            t = jnp.concatenate([t, t], axis=1)
            return tuple(sums[q] + jnp.where(t == float(q), x, 0.0) for q in range(NBLK))

        sums = lax.fori_loop(
            0, BRICKS, add, tuple(jnp.zeros((ANG, DW), F32) for _ in range(NBLK)), unroll=2
        )
        for q in range(NBLK):
            cols = slice(q * DW, (q + 1) * DW)
            mis[:, cols] = (sums[q] - acc[:, cols]).astype(BF16).astype(F32)

        def chosen(d):
            t = tbv[d]
            t = jnp.concatenate([t, t], axis=1)
            c = mis[:, 0:DW]
            for q in range(1, NBLK):
                c = jnp.where(t == float(q), mis[:, q * DW : (q + 1) * DW], c)
            return c.astype(BF16)

        sent(n, snd1)
        for t in range(1, BRICKS):
            d, dev = member(t)
            snd2[n, d] = chosen(d)
            send_block(n, 1, snd2, rcv2, d, dev)

        rcv2[n, me] = chosen(me)

    def backproject(n, put):
        with scope("wait_a2"):
            arrivals(rcv2.at[n], a_recv.at[n, 1])
        r = rcv2[n].astype(F32).reshape(CZ * ANG, DW)
        for h in range(2):
            stage[h] = r[:, h * 128 : (h + 1) * 128]
        for a in range(ANG):
            for h in range(2):
                sl[:, a * DW + h * 128 : a * DW + (h + 1) * 128] = stage[
                    h, pl.ds(a, CZ, stride=ANG), :
                ].astype(BF16)
        with scope("mm_bwd"):
            for c in range(ANG):
                put(c, dot(sl[...], turned[:, c * DW : (c + 1) * DW], ((1,), (0,))))

    send_z(0, x0)
    send_faces(0, x0)
    relayout(0, SPLIT)
    blur_z(0, x0, w1)
    send_yx(0, w1)
    relayout(SPLIT, NCHUNK)

    def to_res(z, v):
        res[pl.ds(pl.multiple_of(z * CY, CY), CY), :] = v

    blur_yx(0, w1, to_res)
    for y in range(CY):
        sl[:, y * CX : (y + 1) * CX] = res[pl.ds(y, CZ, stride=CY), :].astype(BF16)
    project(0)

    wait_faces(0)
    xa[1 : CZ + 1] = x0[...]
    cut = SHRINK

    @pl.loop(0, CZ, unroll=2)
    def _(z):
        smooth = jnp.zeros((CY, CX), F32)
        shrunk = jnp.zeros((CY, CX), F32)
        for j, jm in diffs(fyr.at[0], z):
            s = j - jnp.clip(j, -cut, cut)
            sm = jm - jnp.clip(jm, -cut, cut)
            smooth += jm - j
            shrunk += sm - s
        h = STEP * (smooth - shrunk)
        x0[z] = xa[z + 1] - h
        back[z] = shrunk

    send_z(1, x0)

    shape1, shape2 = (160, 256), (256, CX)
    i, m = iota(shape1, 0), iota(shape1, 1) - 8
    i = jnp.where(i < CX, i, jnp.where(i < CX + 16, i - CX - 16, i - 16))
    inside = ((m >= 0) | (gx > 0)) & ((m < CX) | (gx < GX - 1)) & (m < CX + 8)
    thi, tlo = split(jnp.where(inside, gauss(i - m), 0.0))
    m = iota(shape2, 0) - 8
    uhi, ulo = split(gauss(m - iota(shape2, 1)))
    twice = (
        dot(thi, uhi, ((1,), (0,))) + dot(thi, ulo, ((1,), (0,))) + dot(tlo, uhi, ((1,), (0,)))
    )
    bhi, blo = split(twice[0:CX])
    bx2[0:CX] = bhi
    bx2[CX : 2 * CX] = bhi
    bx2[2 * CX : 3 * CX] = blo
    whi, wlo = split(twice[CX : CX + 32])
    wx2[0:32] = whi
    wx2[32:64] = wlo
    last_weights()

    zst[96:128] = jnp.zeros((32, V), BF16)
    shape1, shape2 = (CZ, CX), (CX, CX)
    m = iota(shape1, 1) - 8
    inside = ((m >= 0) | (gz > 0)) & ((m < CZ) | (gz < GZ - 1)) & (m < CZ + 8)
    thi, tlo = split(jnp.where(inside, gauss(iota(shape1, 0) - m), 0.0))

    def from_place(k):
        halo = jnp.where(k < 80, k - 80, jnp.where(k < 96, k - 80 + CZ, 4 * CX))
        return jnp.where(k < 64, lax.rem(k, CZ), halo)

    uhi, ulo = split(gauss(iota(shape2, 0) - 8 - from_place(iota(shape2, 1))))
    twice = (
        dot(thi, uhi, ((1,), (0,))) + dot(thi, ulo, ((1,), (0,))) + dot(tlo, uhi, ((1,), (0,)))
    )
    hi, lo = split(gauss(iota((48, CX), 0) - 1 - from_place(iota((48, CX), 1))))
    tz9[0:48] = hi
    tz9[48:96] = lo
    once = gauss(iota(shape1, 0) - from_place(iota(shape1, 1)))
    for i, t in enumerate((twice, once)):
        hi, lo = split(t)
        tz[32 * i : 32 * i + 32] = hi
        tz[64 + 32 * i : 96 + 32 * i] = lo

    with scope("turn"):
        turn(0, TURN)
    return_misfit(0)
    with scope("turn"):
        turn(TURN, ANG)
    blur_z(1, x0, w1)
    send_yx(1, w1)

    def to_stack(c, b):
        cols = slice(c * DW, (c + 1) * DW)
        hi, lo = split(b)
        zst[0:32, cols] = hi
        zst[32:64, cols] = lo

    backproject(0, to_stack)
    zhub2.start()

    def to_q(z, v):
        qbuf[pl.ds(z, CY, stride=CZ), :] = v

    blur_yx(1, w1, to_q)
    with scope("wait_z2"):
        zhub2.wait_recv()
    for c in range(ANG):
        cols = slice(c * DW, (c + 1) * DW)
        o = dot(tz[...], zst[:, cols], ((1,), (0,)))
        o = o[0:64] + o[64:128]
        for h in range(2):
            w2[ROWS // 16 * (2 * c + h) : ROWS // 16 * (2 * c + h + 1)] = o[
                0:32, h * 128 : (h + 1) * 128
            ]
        v1z[:, cols] = o[32:64]

    hi, lo = split(w2[...])
    ys2[...] = hi
    f = dot(pick2, hi, ((1,), (1,))).astype(BF16)
    xs[3, 0] = f[0:16]
    xs[3, 1] = f[16:32]
    yxhub2.start()
    slab = (CY, CZ, CX)
    both = jnp.concatenate([hi, lo], axis=1)
    own = dot(both, bx2[0 : 2 * CX], ((1,), (0,))) + dot(hi, bx2[2 * CX :], ((1,), (0,)))
    umid[16:32] = own.reshape(slab)
    for y in range(CY):
        res[pl.ds(y, CZ, stride=CY), :] = v1z[:, y * CX : (y + 1) * CX]
    w1[...] = res[...].reshape(CZ, CY, CX)
    with scope("wait_yx2"):
        yxhub2.wait_recv(slice(0, 6))
    umid[16:32] += rows_of(3, 1, wx2[...]).reshape(slab)
    for side in range(2):
        umid[32 * side : 32 * side + 16] = rows_of(3, 2 * side, wx2[...]).reshape(slab)

    @pl.loop(0, CY + 16)
    def _(y):
        out = ((y < 8) & ends[1][0]) | ((y >= CY + 8) & ends[1][1])
        ytwo[y] = jnp.where(out, 0.0, taps(lambda k: umid[y + k]))

    for y in range(CY):
        rows = slice(y * CZ, (y + 1) * CZ)
        qbuf[rows, :] = qbuf[rows, :] - STEP * taps(lambda k: ytwo[y + k])
    send_yx(2, w1, now=False)
    with scope("wait_yx2"):
        yxhub2.wait_recv(slice(6, 8))
    yxhub[2].start()
    for side in range(2):
        y = yr2[side]
        rows = dot(jnp.concatenate([y, y], axis=1), bx2[CX:], ((1,), (0,)))
        umid[32 * side : 32 * side + 16] = rows.reshape(slab)
    for y in range(CY):
        t = TWICE[16] * (umid[y] + umid[32 + y])
        for r in range(y + 1, CY):
            t += TWICE[y + 16 - r] * umid[r]
        for r in range(y):
            t += TWICE[16 + r - y] * umid[32 + r]
        v = qbuf[y * CZ : (y + 1) * CZ, :] - STEP * t
        sl[:, y * CX : (y + 1) * CX] = v.astype(BF16)

    project(1)

    def to_x(z, v):
        x = x0[z] - STEP * v
        x0[z] = x
        xa[z + 1] = x

    blur_yx(2, w1, to_x)
    send_faces(1, x0)
    return_misfit(1)
    wait_faces(1)

    def one(z, sums):
        primal, dres = sums
        smooth = jnp.zeros((CY, CX), F32)
        shrunk = jnp.zeros((CY, CX), F32)
        bdual = jnp.zeros((CY, CX), F32)
        for axis, (j, jm) in enumerate(diffs(fyr.at[1], z)):
            s = j - jnp.clip(j, -cut, cut)
            sm = jm - jnp.clip(jm, -cut, cut)
            d = j - s
            dm = jm - sm
            smooth += jm - j
            shrunk += sm - s
            bdual += dm - d
            dl[axis, z] = d
            dlm[axis, z] = dm
            primal += fold(jnp.square(j - s))
        dres += fold(jnp.square(shrunk - back[z]))
        hterm[z] = smooth - shrunk
        back[z] = shrunk
        bdl[z] = bdual
        return primal, dres

    zero = jnp.zeros((8, CX), F32)
    primal, dres = lax.fori_loop(0, CZ, one, (zero, zero), unroll=2)
    put_sums(0, primal, dres)
    for t in range(1, GZ):
        redz_copy(0, t).start()
    send_terms()

    zhub2.wait_send()
    backproject(1, to_stack)
    zhub[2].start()
    forward_sums(0)
    with scope("wait_z"):
        zhub[2].wait_recv()
    for c in range(ANG):
        o = dot(tz9[...], zst[:, c * DW : (c + 1) * DW], ((1,), (0,)))
        o = o[0:40] + o[48:88]
        for h in range(2):
            zmid[pl.ds(2 * c + h, 40, stride=CY), :] = o[:, h * 128 : (h + 1) * 128]
    outer = zmid[0:ROWS9].reshape(CZ + 2, CY, CX)
    n9 = (CZ + 2) * R
    for side, at, ninth in ((0, slice(0, R), R), (1, slice(CY - R, CY), CY - R - 1)):
        ys9[side, 0:n9] = outer[:, at, :].reshape(n9, CX).astype(BF16)
        ys9[side, n9:] = zmid[pl.ds(CY + ninth, CZ, stride=CY), :].astype(BF16)
    hi, lo = split(outer.reshape(ROWS9, CX))
    f = dot(pick2, hi, ((1,), (1,))).astype(BF16)
    xs9[0, :, 0:ROWS9] = f[0:16]
    xs9[1, :, 0:ROWS9] = f[16:32]
    yxhub[3].start()
    both = jnp.concatenate([hi, lo], axis=1)
    own = dot(both, bx9[0 : 2 * CX], ((1,), (0,))) + dot(hi, bx9[2 * CX :], ((1,), (0,)))
    own = own.reshape(CZ + 2, CY, 2 * CX)
    ymid[0 : CZ + 2, 16 : 16 + CY, :] = own[:, :, 0:CX]
    ybuf[:, R : R + CY, :] = own[1 : CZ + 1, :, CX:]
    penalty = factor_of(0, jnp.ones((8, CX), F32))
    inv1 = 1.0 / penalty
    pen3 = penalty[0:1].reshape(1, 1, CX)
    inv3 = inv1[0:1].reshape(1, 1, CX)
    spen = STEP * pen3
    x0[...] = x0[...] - spen * (hterm[...] + bdl[...] * inv3)
    dl[...] = dl[...] * inv3
    dlm[...] = dlm[...] * inv3
    with scope("wait_terms"):
        fhub[2].wait_recv()
    for side in range(2):
        fz2[side] = fzr[1, side] - spen[0] * (fzr2[side, 0] + fzr2[side, 1] * inv3[0])
        fy2[side] = fyr[1, side] - spen[0] * (fyr2[side, 0] + fyr2[side, 1] * inv3[0])
    rims = [
        dot(
            jnp.concatenate([fxr2[0, i], fxr2[1, i]], axis=0), wx[64:96], ((0,), (0,))
        ).reshape(CZ, CY, CX)
        for i in range(2)
    ]
    xlr[...] = xlr[...] - spen * (rims[0] + rims[1] * inv3)

    def halo_rows(slot):
        h = xr9[slot].reshape(32, ROWS9P)[:, 0:ROWS9]
        h = dot(jnp.concatenate([h, h], axis=0), wx9[...], ((0,), (0,)))
        return h.reshape(CZ + 2, CY, 2 * CX)

    with scope("wait_yx"):
        yxhub[3].wait_recv(slice(0, 6))
    more = halo_rows(1)
    ymid[0 : CZ + 2, 16 : 16 + CY, :] += more[:, :, 0:CX]
    ybuf[:, R : R + CY, :] += more[1 : CZ + 1, :, CX:]
    sides = ((0, slice(0, 16)), (1, slice(16 + CY, 32 + CY)))
    for side, to in sides:
        more = halo_rows(2 * side)
        ymid[0 : CZ + 2, to, :] = more[:, :, 0:CX]
        if side == 0:
            ybuf[:, 0:R, :] = more[1 : CZ + 1, CY - R :, CX:]
        else:
            ybuf[:, R + CY :, :] = more[1 : CZ + 1, 0:R, CX:]
    with scope("wait_yx"):
        yxhub[3].wait_recv(slice(6, 8))
    for side in range(2):
        y = yr9[side]
        rows = dot(jnp.concatenate([y, y], axis=1), bx9[CX:], ((1,), (0,)))
        near = rows[0:n9].reshape(CZ + 2, R, 2 * CX)
        to = slice(16 - R, 16) if side == 0 else slice(16 + CY, 16 + CY + R)
        ymid[0 : CZ + 2, to, :] += near[:, :, 0:CX]
        fy2[side] = fy2[side] - STEP * TAPS[0] * rows[n9:, 0:CX]
        to = slice(0, R) if side == 0 else slice(R + CY, 2 * R + CY)
        ybuf[:, to, :] += near[1 : CZ + 1, :, CX:]

    @pl.loop(0, CZ, unroll=2)
    def _(z):
        v = x0[z] - STEP * taps(lambda k: ymid[z + 1, 16 - R + k : 16 - R + CY + k, :])
        xa[z + 1] = v
        x_out[z] = v
        xlr[z] = xlr[z] - STEP * taps(lambda k: ybuf[z, k : k + CY, :])
        low = taps(lambda k: ymid[z + 1, k : k + R, :])[R - 1 : R]
        fy2[0, pl.ds(z, 1), :] = fy2[0, pl.ds(z, 1), :] - STEP * low
        high = taps(lambda k: ymid[z + 1, 16 + R + k : 16 + 2 * R + k, :])[0:1]
        fy2[1, pl.ds(z, 1), :] = fy2[1, pl.ds(z, 1), :] - STEP * high

    for side, at in ((0, 0), (1, CZ + 1)):
        xa[at] = fz2[side] - STEP * taps(lambda k: ymid[at, 16 - R + k : 16 - R + CY + k, :])
    cut2 = (SHRINK / penalty)[0:1]

    def last(z, sums):
        primal, dres = sums
        shrunk = jnp.zeros((CY, CX), F32)
        for axis, (j, jm) in enumerate(diffs(fy2, z)):
            t = j + dl[axis, z]
            tm = jm + dlm[axis, z]
            s = t - jnp.clip(t, -cut2, cut2)
            sm = tm - jnp.clip(tm, -cut2, cut2)
            shrunk += sm - s
            dl[axis, z] = t - s
            primal += fold(jnp.square(j - s))
        dres += fold(jnp.square(shrunk - back[z]))
        return primal, dres

    with scope("last"):
        primal, dres = lax.fori_loop(0, CZ, last, (zero, zero), unroll=4)
    put_sums(1, primal, dres)
    send_all()
    with scope("sums"):
        got = redall.at[pl.ds(1, GZ * BRICKS - 1)]
        pltpu.make_async_copy(got, got, all_recv).wait()
    factor2 = factor_from(red0[1] + jnp.sum(redall[1 : GZ * BRICKS], axis=0), penalty)
    scale = (1.0 / factor2)[0:1].reshape(1, 1, 1, CX)
    with scope("scale"):
        dual_out[...] = dl[...] * scale

    with scope("wait_sends"):
        for h in (zhub[2], yxhub[3], fhub[2]):
            h.wait_send()
        sent(1, snd2)
        got = redz.at[0, pl.ds(1, GZ - 1)]
        pltpu.make_async_copy(got, got, rz_send).wait()
        got = redx.at[0, pl.ds(1, BRICKS - 1)]
        pltpu.make_async_copy(got, got, rx_send).wait()
        got = redall.at[pl.ds(1, GZ * BRICKS - 1)]
        pltpu.make_async_copy(got, got, all_send).wait()


def body(start, measured, tiles, tile_block, angle_row):
    vm = pltpu.VMEM
    dma = pltpu.SemaphoreType.DMA
    block = vm((CZ, CY, CX), F32)
    return pl.pallas_call(
        kernel,
        out_shape=(
            pltpu.VMEM((CZ, CY, CX), F32),
            pltpu.VMEM((3, CZ, CY, CX), F32),
        ),
        in_specs=[
            pl.BlockSpec(memory_space=pltpu.HBM),
            pl.BlockSpec(memory_space=pltpu.HBM),
            pl.BlockSpec(memory_space=pltpu.HBM),
            pl.BlockSpec(memory_space=pltpu.VMEM),
            pl.BlockSpec(memory_space=pltpu.SMEM),
        ],
        out_specs=(pl.BlockSpec(memory_space=pltpu.VMEM), pl.BlockSpec(memory_space=pltpu.VMEM)),
        scratch_shapes=[
            vm((V, ANG, DW), BF16),
            vm((V, ANG * DW), BF16),
            vm((ANG * DW, V), BF16),
            vm((2, CHUNK * PITCH, 128), F32),
            block, block,
            vm((ROWS, CX), F32),
            vm((ROWS, CX), F32),
            vm((ROWS, CX), F32),
            vm((CZ + 2, CY, CX), F32),
            vm((CZ + 32, CY, CX), F32),
            vm((40 * CY, CX), F32),
            vm((CZ, CY + 16, CX), F32),
            vm((CZ + 2, CY + 32, CX), F32),
            vm((BRICKS, ANG, CX), F32),
            vm((1, ANG, NBLK * DW), F32),
            vm((ANG, NBLK * DW), F32),
            vm((ANG, NBLK * DW), F32),
            vm((2, 2, R * CY, CX), BF16),
            vm((2, 2, R * CY, CX), BF16),
            vm((128, V), BF16),
            vm((128, 128), BF16),
            vm((96, 128), BF16),
            vm((CZ, V), F32),
            vm((CY + 32, CZ, CX), F32),
            vm((CY + 16, CZ, CX), F32),
            vm((3, 2, CZ * R, CX), BF16),
            vm((3, 2, CZ * R, CX), BF16),
            vm((ROWS, CX), BF16),
            vm((2, ROWS, CX), BF16),
            vm((4, 2, 16, ROWS), BF16),
            vm((4, 3, 2, 16, ROWS), BF16),
            vm((2, (CZ + 2) * R + CZ, CX), BF16),
            vm((2, (CZ + 2) * R + CZ, CX), BF16),
            vm((2, 16, ROWS9P), BF16),
            vm((3, 2, 16, ROWS9P), BF16),
            vm((2, 2, CY, CX), F32),
            vm((2, 2, CY, CX), F32),
            vm((2, 2, CZ, CX), F32),
            vm((2, 2, CZ, CX), F32),
            vm((2, 2, 16, ROWS), BF16),
            vm((2, 2, 16, ROWS), BF16),
            vm((2, 2, CY, CX), F32),
            vm((2, 2, CY, CX), F32),
            vm((2, 2, CZ, CX), F32),
            vm((2, 2, CZ, CX), F32),
            vm((2, 2, 16, ROWS), BF16),
            vm((2, 2, 16, ROWS), BF16),
            vm((2, CY, CX), F32),
            vm((2, CZ, CX), F32),
            vm((2, CZ * ANG, 128), F32),
            vm((CZ, V), BF16),
            vm((2, BRICKS, ANG, DW), BF16),
            vm((2, BRICKS, ANG, DW), BF16),
            vm((2, BRICKS, ANG, DW), BF16),
            vm((2, BRICKS, ANG, DW), BF16),
            block, block,
            vm((3, CZ, CY, CX), F32),
            vm((3, CZ, CY, CX), F32),
            block, block,
            vm((2, 1, CX), F32),
            vm((2, GZ, 1, CX), F32),
            vm((2, 1, CX), F32),
            vm((2, BRICKS, 1, CX), F32),
            vm((GZ * BRICKS, 1, CX), F32),
            vm((3 * CX, CX), BF16),
            vm((96, CX), BF16),
            vm((3 * CX, CX), BF16),
            vm((64, CX), BF16),
            vm((3 * CX, 2 * CX), BF16),
            vm((64, 2 * CX), BF16),
            dma((2,)),
            dma((V // LOAD,)),
            dma((2,)),
            dma((2, 2)),
            dma((8,)),
            dma((2, 8)),
            dma((3, 2)),
            dma((2, 3, 2)),
            dma,
            dma((2, 2)),
            dma,
            dma,
            dma,
            dma,
            dma,
            dma,
        ],
        compiler_params=pltpu.CompilerParams(
            collective_id=0, has_side_effects=True, vmem_limit_bytes=60 * 1024 * 1024
        ),
    )(start, measured, tiles, tile_block, angle_row)


def solution(mesh):
    return jax.shard_map(
        body,
        mesh=mesh,
        in_specs=(
            P("gz", "gy", "gx"),
            P(("gz", "gy", "gx"), None, None),
            P("gy", None, "gx"),
            P(),
            P(),
        ),
        out_specs=(P("gz", "gy", "gx"), P(None, "gz", "gy", "gx")),
        check_vma=False,
    )
```

```python
import math

import jax
import jax.numpy as jnp
from jax import lax
from jax.experimental import pallas as pl
from jax.experimental.pallas import tpu as pltpu
from jax.sharding import PartitionSpec as P

CZ, CY, CX = 32, 16, 128
ROWS = CZ * CY
ANG, DW, NBLK = 8, 256, 4
V = CY * CX
R = 8
GZ, GY, GX = 4, 4, 8
BRICKS = GY * GX
CELLS = float(CZ * CY * CX * GZ * BRICKS)
MESH = pl.DeviceIdType.MESH
F32, BF16 = jnp.float32, jnp.bfloat16
STEP = 0.5
SHRINK = 0.2
EPS = 1e-6
CHUNK = 128
NCHUNK = V // CHUNK
ORDER = sorted(
    ((dx, dz, dc) for dz in range(4) for dx in range(4) for dc in range(2) if dx or dz or dc),
    key=lambda s: -(min(s[0], 4 - s[0]) + min(s[1], 4 - s[1])),
)
LOAD = 512
ROWS9 = (CZ + 2) * CY
ROWS9P = -(-ROWS9 // 128) * 128
PITCH = 9
SPLIT = 4
TURN = 3
ORDER_ALL = sorted(
    ((dy, t) for dy in range(GZ) for t in range(GY * GX) if dy or t),
    key=lambda s: -(
        min(s[0], 4 - s[0])
        + (sum(min(d, 4 - d) for d in ORDER[s[1] - 1][:2]) if s[1] else 0)
    ),
)

RAW = [math.exp(-k * k / 12.5) for k in range(-R, R + 1)]
TAPS = [r / sum(RAW) for r in RAW]
TWICE = [
    sum(TAPS[k] * TAPS[d + 2 * R - k] for k in range(2 * R + 1) if 0 <= d + 2 * R - k <= 2 * R)
    for d in range(2 * R + 1)
]


def dot(a, b, dims):
    return lax.dot_general(a, b, (dims, ((), ())), preferred_element_type=F32)


def split(v):
    hi = v.astype(BF16)
    lo = (v - hi.astype(F32)).astype(BF16)
    return hi, lo


def kernel(
    start_ref, meas_ref, tiles_ref, tb_ref, row_ref,
    x_out, dual_out,
    raw, mat, turned, tmp, x0, w1, w2, res, qbuf, xa, zbuf, zmid, ybuf, ymid, tbv, obs, mis, acc,
    zs, zr, zst, tz, tz9, v1z, umid, ytwo, ys, yr, ys2, yr2, xs, xr,
    ys9, yr9, xs9, xr9,
    fzs, fzr, fys, fyr, fxs, fxr, fzs2, fzr2, fys2, fyr2, fxs2, fxr2, fz2, fy2,
    stage, sl, snd1, rcv1, snd2, rcv2,
    hterm, back, dl, dlm, xlr, bdl,
    red0, redz, red1, redx, redall,
    bx, wx, bx2, wx2, bx9, wx9,
    load_sem, tile_sem, z_send, z_recv, yx_send, yx_recv, f_send, f_recv,
    a_send, a_recv, rz_send, rz_recv, rx_send, rx_recv, all_send, all_recv, meet,
):
    gz, gy, gx = lax.axis_index("gz"), lax.axis_index("gy"), lax.axis_index("gx")
    me = gy * GX + gx
    scope = jax.named_scope

    barrier = pltpu.get_barrier_semaphore()

    chip_x = 2 * (gy // 2) + lax.rem(gx, 2)
    chip_z, core = gx // 2, lax.rem(gy, 2)

    def member(t):
        dx, dz, dc = ORDER[t - 1]
        x = lax.rem(chip_x + dx, 4)
        z = lax.rem(chip_z + dz, 4)
        y = 2 * (x // 2) + lax.rem(core + dc, 2)
        x = 2 * z + lax.rem(x, 2)
        return y * GX + x, (gz, y, x)

    def there(dz, dy, dx):
        ok = True
        for d, at, n in ((dz, gz, GZ), (dy, gy, GY), (dx, gx, GX)):
            if d:
                near = at >= -d if d < 0 else at < n - d
                ok = near if ok is True else jnp.logical_and(ok, near)
        return ok

    def greet(sem, stride):
        steps = (-stride, 0, stride)
        places = [(0, dy, dx) for dy in steps for dx in steps if dy or dx]
        places += [(-stride, 0, 0), (stride, 0, 0)]
        if stride == 4:
            places = [(0, 0, -stride), (0, 0, stride)]
        heard = 0
        for dz, dy, dx in places:
            ok = there(dz, dy, dx)
            heard = heard + ok.astype(jnp.int32)

            @pl.when(ok)
            def _():
                pl.semaphore_signal(
                    sem, inc=1, device_id=(gz + dz, gy + dy, gx + dx), device_id_type=MESH
                )

        return lambda: pl.semaphore_wait(sem, heard)

    wait_near = greet(barrier, 1)

    ld = [
        pltpu.make_async_copy(start_ref, x0, load_sem.at[0]),
        pltpu.make_async_copy(meas_ref, obs, load_sem.at[1]),
    ]
    for c in ld:
        c.start()

    def turn(low, high):
        @pl.loop(low, high)
        def _(c):
            rows = pl.ds(pl.multiple_of(c * DW, DW), DW)
            for a in range(ANG):
                turned[a * DW : (a + 1) * DW, rows] = mat[rows, a * DW : (a + 1) * DW].T

    def tile_copy(c):
        rows = pl.ds(c * LOAD, LOAD)
        return pltpu.make_async_copy(tiles_ref.at[rows], raw.at[rows], tile_sem.at[c])


    class Hub:
        def __init__(self, items, before=None):
            self.before = before
            self.items = [
                (
                    there(*d),
                    there(*(-i for i in d)),
                    pltpu.make_async_remote_copy(
                        src, dst, ss, rs,
                        device_id=(gz + d[0], gy + d[1], gx + d[2]), device_id_type=MESH,
                    ),
                    dst,
                )
                for d, src, dst, ss, rs in items
            ]

        def clear(self):
            for _, arrives, _, dst in self.items:

                @pl.when(jnp.logical_not(arrives))
                def _():
                    dst[...] = jnp.zeros(dst.shape, dst.dtype)

        def start(self):
            if self.before is not None:
                self.before.wait_send()
            for leaves, _, copy, _ in self.items:
                pl.when(leaves)(copy.start)

        def wait_recv(self, part=slice(None)):
            for _, arrives, copy, _ in self.items[part]:
                pl.when(arrives)(copy.wait_recv)

        def wait_send(self):
            for leaves, _, copy, _ in self.items:
                pl.when(leaves)(copy.wait_send)

    def pair(axis, src, dst, send, recv):
        unit = [int(axis == a) for a in range(3)]
        return [
            ([-u for u in unit], src.at[0], dst.at[1], send.at[0], recv.at[0]),
            (unit, src.at[1], dst.at[0], send.at[1], recv.at[1]),
        ]

    def around(k, low, high, into_low, into_high, faces, halos, before):
        items = []
        i = 2
        for sy in (-1, 1, 0):
            for side, sx in ((0, -1), (1, 1)):
                items.append((
                    (0, sy, sx), faces.at[side], halos.at[1 - sy, 1 - side],
                    yx_send.at[i], yx_recv.at[k, i],
                ))
                i += 1
        items += [
            ((0, -1, 0), low, into_high, yx_send.at[0], yx_recv.at[k, 0]),
            ((0, 1, 0), high, into_low, yx_send.at[1], yx_recv.at[k, 1]),
        ]
        return Hub(items, before)

    def zswap(k, src, dst, before):
        return Hub(pair(0, src, dst, z_send, z_recv.at[k]), before)

    zhub = [zswap(0, zs.at[0], zr.at[0], None)]
    zhub.append(zswap(1, zs.at[1], zr.at[1], zhub[0]))
    def zstack(k, before):
        return Hub(
            [
                ((-1, 0, 0), zst.at[0:16], zst.at[80:96], z_send.at[0], z_recv.at[k, 0]),
                ((1, 0, 0), zst.at[16:32], zst.at[64:80], z_send.at[1], z_recv.at[k, 1]),
            ],
            before,
        )

    zhub2 = zstack(0, zhub[1])
    zhub.append(zstack(1, None))

    def yxswap(n, k, before):
        low, high = yr.at[n, 0], yr.at[n, 1]
        return around(k, ys.at[n, 0], ys.at[n, 1], low, high, xs.at[n], xr.at[n], before)

    yxhub = [yxswap(0, 0, None)]
    yxhub.append(yxswap(1, 1, yxhub[0]))
    yxhub2 = around(0, ys2, ys2, yr2.at[0], yr2.at[1], xs.at[3], xr.at[3], yxhub[1])
    yxhub.append(yxswap(2, 1, yxhub2))
    yxhub.append(
        around(0, ys9.at[0], ys9.at[1], yr9.at[0], yr9.at[1], xs9, xr9, yxhub[2])
    )
    fhub = []
    for k, z, y, x in (
        (0, (fzs.at[0], fzr.at[0]), (fys.at[0], fyr.at[0]), (fxs.at[0], fxr.at[0])),
        (1, (fzs.at[1], fzr.at[1]), (fys.at[1], fyr.at[1]), (fxs.at[1], fxr.at[1])),
        (0, (fzs2, fzr2), (fys2, fyr2), (fxs2, fxr2)),
    ):
        fhub.append(
            Hub(
                pair(0, *z, f_send.at[0], f_recv.at[k, 0])
                + pair(1, *y, f_send.at[1], f_recv.at[k, 1])
                + pair(2, *x, f_send.at[2], f_recv.at[k, 2]),
                fhub[-1] if fhub else None,
            )
        )
    xs9[...] = jnp.zeros_like(xs9)
    hubs = zhub + [zhub2] + yxhub + [yxhub2] + fhub
    for h in hubs:
        h.clear()

    def gauss(d):
        df = d.astype(F32)
        w = jnp.exp(df * df * (-1.0 / 12.5)) * (1.0 / sum(RAW))
        return jnp.where(jnp.abs(d) <= R, w, 0.0)

    def iota(shape, axis):
        return lax.broadcasted_iota(jnp.int32, shape, axis)

    square = (CX, CX)
    bhi, blo = split(gauss(iota(square, 0) - iota(square, 1)))
    bx[0:CX] = bhi
    bx[CX : 2 * CX] = bhi
    bx[2 * CX : 3 * CX] = blo
    k0, k1 = iota((32, CX), 0), iota((32, CX), 1)
    pos = jnp.where(k0 < 16, lax.rem(k0, 8) - 8, CX + lax.rem(k0, 8))
    whi, wlo = split(gauss(pos - k1))
    wx[0:32] = whi
    wx[32:64] = wlo
    rim = ((k1 == 0) & ((k0 == 7) | (k0 == 15))) | ((k1 == CX - 1) & ((k0 == 16) | (k0 == 24)))
    wx[64:96] = jnp.where(rim, 1.0, 0.0).astype(BF16)
    s0, s1 = iota((32, 2 * CX), 0), iota((32, 2 * CX), 1)
    want = jnp.where(s0 < 16, lax.rem(s0, 8), CX - 8 + lax.rem(s0, 8)) + jnp.where(
        lax.rem(s0, 16) < 8, 0, CX
    )
    pick = jnp.where(s1 == want, 1.0, 0.0).astype(BF16)
    pick2 = jnp.where(k1 == jnp.where(k0 < 16, k0, CX - 32 + k0), 1.0, 0.0).astype(BF16)

    def place(c):
        edge = jnp.where(c == CX, -1, jnp.where(c == 2 * CX - 1, CX, 4 * CX))
        return jnp.where(c < CX, c, edge)

    def last_weights():
        shape = (CX, 2 * CX)
        hi, lo = split(gauss(iota(shape, 0) - place(iota(shape, 1))))
        bx9[0:CX] = hi
        bx9[CX : 2 * CX] = hi
        bx9[2 * CX : 3 * CX] = lo
        shape = (32, 2 * CX)
        k = iota(shape, 0)
        hi, lo = split(gauss(jnp.where(k < 16, k - 16, CX - 16 + k) - place(iota(shape, 1))))
        wx9[0:32] = hi
        wx9[32:64] = lo

    wide = (GX, GX * CX)
    spread = jnp.where(iota(wide, 0) == iota(wide, 1) // CX, 1.0, 0.0).astype(BF16)
    for b in range(GY):
        rows = dot(tb_ref[b].astype(F32).astype(BF16), spread, ((0,), (0,)))
        for c in range(GX):
            tbv[b * GX + c] = rows[:, c * CX : (c + 1) * CX]

    def relayout(low, high):
        for c in range(V // LOAD):
            if low * CHUNK <= c * LOAD < high * CHUNK:
                tile_copy(c).wait()

        @pl.loop(low, high)
        def _(c):
            rows = pl.ds(pl.multiple_of(c * CHUNK, CHUNK), CHUNK)
            block = raw[rows].astype(F32)
            for h in range(2):
                for j in range(CHUNK):
                    tmp[h, PITCH * j : PITCH * j + ANG, :] = block[j, :, h * 128 : (h + 1) * 128]
            for a in range(ANG):
                for h in range(2):
                    part = tmp[h, pl.ds(a, CHUNK, stride=PITCH), :]
                    mat[rows, a * DW + h * 128 : a * DW + (h + 1) * 128] = part.astype(BF16)

    ld[0].wait()
    for c in range(V // LOAD):
        tile_copy(c).start()
    ld[1].wait()
    for a in range(ANG):
        acc[pl.ds(a, 1), :] = obs[0, pl.ds(row_ref[a], 1), :]

    def stage_z(n, src):
        zs[n, 0] = src[0:R].reshape(R * CY, CX).astype(BF16)
        zs[n, 1] = src[CZ - R : CZ].reshape(R * CY, CX).astype(BF16)

    stage_z(0, x0)
    with scope("wait_barrier"):
        wait_near()

    def send_faces(n, src):
        fzs[n, 0] = src[0]
        fzs[n, 1] = src[CZ - 1]
        v = src[...]
        fys[n, 0] = v[:, 0, :]
        fys[n, 1] = v[:, CY - 1, :]
        hi, lo = split(v.reshape(ROWS, CX))
        f = dot(pick, jnp.concatenate([hi, lo], axis=1), ((1,), (1,))).astype(BF16)
        fxs[n, 0] = f[0:16]
        fxs[n, 1] = f[16:32]
        fhub[n].start()

    def send_terms():
        for i, src in enumerate((hterm, bdl)):
            fzs2[0, i] = src[0]
            fzs2[1, i] = src[CZ - 1]
            v = src[...]
            fys2[0, i] = v[:, 0, :]
            fys2[1, i] = v[:, CY - 1, :]
            hi, lo = split(v.reshape(ROWS, CX))
            f = dot(pick, jnp.concatenate([hi, lo], axis=1), ((1,), (1,))).astype(BF16)
            fxs2[0, i] = f[0:16]
            fxs2[1, i] = f[16:32]
        fhub[2].start()

    def taps(at):
        t = TAPS[R] * at(R)
        for k in range(R):
            t += TAPS[k] * (at(k) + at(2 * R - k))
        return t

    def blur_z(n, src, out):
        zbuf[R : R + CZ] = src[...]
        with scope("wait_z"):
            zhub[n].wait_recv()
        zbuf[0:R] = zr[n, 0].astype(F32).reshape(R, CY, CX)
        zbuf[R + CZ : 2 * R + CZ] = zr[n, 1].astype(F32).reshape(R, CY, CX)

        @pl.loop(0, CZ, unroll=2)
        def _(z):
            out[z] = taps(lambda k: zbuf[z + k])

    def send_yx(n, w, now=True):
        v = w[...]
        ys[n, 0] = v[:, 0:R, :].reshape(CZ * R, CX).astype(BF16)
        ys[n, 1] = v[:, CY - R :, :].reshape(CZ * R, CX).astype(BF16)
        hi, lo = split(v.reshape(ROWS, CX))
        f = dot(pick, jnp.concatenate([hi, lo], axis=1), ((1,), (1,))).astype(BF16)
        xs[n, 0] = f[0:16]
        xs[n, 1] = f[16:32]
        if now:
            yxhub[n].start()

    def rows_of(m, slot, weights):
        halo = xr[m, slot].reshape(32, ROWS)
        return dot(jnp.concatenate([halo, halo], axis=0), weights, ((0,), (0,)))

    def own_rows(w, mat3):
        hi, lo = split(w[...].reshape(ROWS, CX))
        both = jnp.concatenate([hi, lo], axis=1)
        return dot(both, mat3[0 : 2 * CX], ((1,), (0,))) + dot(hi, mat3[2 * CX :], ((1,), (0,)))

    def blur_yx(n, w, put):
        own = own_rows(w, bx)
        ybuf[:, R : R + CY, :] = own.reshape(CZ, CY, CX)
        with scope("wait_yx"):
            yxhub[n].wait_recv(slice(0, 6))
        ybuf[:, R : R + CY, :] += rows_of(n, 1, wx[0:64]).reshape(CZ, CY, CX)
        sides = (
            (0, slice(CY - R, CY), slice(0, R)),
            (1, slice(0, R), slice(R + CY, 2 * R + CY)),
        )
        for side, at, to in sides:
            ybuf[:, to, :] = rows_of(n, 2 * side, wx[0:64]).reshape(CZ, CY, CX)[:, at, :]
        with scope("wait_yx"):
            yxhub[n].wait_recv(slice(6, 8))
        for side, at, to in sides:
            y = yr[n, side]
            rows = dot(jnp.concatenate([y, y], axis=1), bx[CX:], ((1,), (0,)))
            ybuf[:, to, :] += rows.reshape(CZ, R, CX)

        @pl.loop(0, CZ, unroll=2)
        def _(z):
            put(z, taps(lambda k: ybuf[z, k : k + CY, :]))

    lane, sub = iota((CY, CX), 1), iota((CY, CX), 0)
    ends = ((gz == 0, gz == GZ - 1), (gy == 0, gy == GY - 1), (gx == 0, gx == GX - 1))

    def wait_faces(n):
        with scope("wait_faces"):
            fhub[n].wait_recv()
        xlr[...] = dot(fxr[n].reshape(32, ROWS), wx[64:96], ((0,), (0,))).reshape(CZ, CY, CX)
        xa[0] = fzr[n, 0]
        xa[CZ + 1] = fzr[n, 1]

    def diffs(fy, z):
        v = xa[z + 1]
        up, low = xa[z + 2], xa[z]
        yield (
            jnp.where((z == CZ - 1) & ends[0][1], 0.0, up - v),
            jnp.where((z == 0) & ends[0][0], 0.0, v - low),
        )
        up = jnp.where(sub == CY - 1, fy[1, pl.ds(z, 1), :], pltpu.roll(v, CY - 1, 0))
        low = jnp.where(sub == 0, fy[0, pl.ds(z, 1), :], pltpu.roll(v, 1, 0))
        yield (
            jnp.where((sub == CY - 1) & ends[1][1], 0.0, up - v),
            jnp.where((sub == 0) & ends[1][0], 0.0, v - low),
        )
        edge = xlr[z]
        up = jnp.where(lane == CX - 1, edge, pltpu.roll(v, CX - 1, 1))
        low = jnp.where(lane == 0, edge, pltpu.roll(v, 1, 1))
        yield (
            jnp.where((lane == CX - 1) & ends[2][1], 0.0, up - v),
            jnp.where((lane == 0) & ends[2][0], 0.0, v - low),
        )

    def fold(p):
        return p[0:8] + p[8:16]

    def redz_copy(n, t):
        return pltpu.make_async_remote_copy(
            red0.at[n], redz.at[n, t], rz_send, rz_recv,
            device_id=(lax.rem(gz + t, GZ), gy, gx), device_id_type=MESH,
        )

    def redx_copy(n, t):
        return pltpu.make_async_remote_copy(
            red1.at[n], redx.at[n, t], rx_send, rx_recv,
            device_id=member(t)[1], device_id_type=MESH,
        )

    def put_sums(n, primal, dualres):
        p = jnp.sum(jnp.sum(primal, axis=0, keepdims=True), axis=1, keepdims=True)
        d = jnp.sum(jnp.sum(dualres, axis=0, keepdims=True), axis=1, keepdims=True)
        red0[n] = jnp.where(lane[0:1] < CX // 2, p, d)

    def send_all():
        for slot, (dy, t) in enumerate(ORDER_ALL):
            dev = (gy, gx) if t == 0 else member(t)[1][1:]
            pltpu.make_async_remote_copy(
                red0.at[1], redall.at[slot + 1], all_send, all_recv,
                device_id=(lax.rem(gz + dy, GZ), *dev), device_id_type=MESH,
            ).start()

    def forward_sums(n):
        got = redz.at[n, pl.ds(1, GZ - 1)]
        pltpu.make_async_copy(got, got, rz_recv).wait()
        red1[n] = red0[n] + jnp.sum(redz[n, 1:GZ], axis=0)

        for t in range(1, BRICKS):
            redx_copy(n, t).start()

    def factor_of(n, penalty):
        total = red1[n]
        got = redx.at[n, pl.ds(1, BRICKS - 1)]
        pltpu.make_async_copy(got, got, rx_recv).wait()
        total += jnp.sum(redx[n, 1:BRICKS], axis=0)
        return factor_from(total, penalty)

    def factor_from(total, penalty):
        p = jnp.broadcast_to(total[:, 0:1], (8, CX)) * (1.0 / (3.0 * CELLS))
        d = jnp.broadcast_to(total[:, CX - 1 : CX], (8, CX)) * (1.0 / CELLS)
        d = penalty * penalty * d
        return jnp.sqrt(jnp.sqrt((p + EPS) / (d + EPS)))

    def arrivals(ref, sem):
        got = ref.at[pl.ds(0, BRICKS - 1)]
        pltpu.make_async_copy(got, got, sem).wait()

    def sent(n, ref):
        arrivals(ref.at[n], a_send)

    def send_block(n, i, src, dst, d, dev):
        pltpu.make_async_remote_copy(
            src.at[n, d], dst.at[n, me], a_send, a_recv.at[n, i],
            device_id=dev, device_id_type=MESH,
        ).start()

    def project(n):
        with scope("mm_fwd"):
            for a in range(ANG):
                c = dot(sl[...], mat[:, a * DW : (a + 1) * DW], ((1,), (0,)))
                for h in range(2):
                    stage[h, pl.ds(a, CZ, stride=ANG), :] = c[:, h * 128 : (h + 1) * 128]

        def block_of(d):
            rows = pl.ds(pl.multiple_of(d * ANG, ANG), ANG)
            return jnp.concatenate([stage[0, rows, :], stage[1, rows, :]], axis=1).astype(BF16)

        if n:
            sent(0, snd2)
        else:
            wait_round()
        for t in range(1, BRICKS):
            d, dev = member(t)
            snd1[n, d] = block_of(d)
            send_block(n, 0, snd1, rcv1, d, dev)

        rcv1[n, me] = block_of(me)

    def return_misfit(n):
        with scope("wait_a1"):
            arrivals(rcv1.at[n], a_recv.at[n, 0])

        def add(s, sums):
            x = rcv1[n, s].astype(F32)
            t = tbv[s]
            t = jnp.concatenate([t, t], axis=1)
            return tuple(sums[q] + jnp.where(t == float(q), x, 0.0) for q in range(NBLK))

        sums = lax.fori_loop(
            0, BRICKS, add, tuple(jnp.zeros((ANG, DW), F32) for _ in range(NBLK)), unroll=2
        )
        for q in range(NBLK):
            cols = slice(q * DW, (q + 1) * DW)
            mis[:, cols] = (sums[q] - acc[:, cols]).astype(BF16).astype(F32)

        def chosen(d):
            t = tbv[d]
            t = jnp.concatenate([t, t], axis=1)
            c = mis[:, 0:DW]
            for q in range(1, NBLK):
                c = jnp.where(t == float(q), mis[:, q * DW : (q + 1) * DW], c)
            return c.astype(BF16)

        sent(n, snd1)
        for t in range(1, BRICKS):
            d, dev = member(t)
            snd2[n, d] = chosen(d)
            send_block(n, 1, snd2, rcv2, d, dev)

        rcv2[n, me] = chosen(me)

    def backproject(n, put):
        with scope("wait_a2"):
            arrivals(rcv2.at[n], a_recv.at[n, 1])
        r = rcv2[n].astype(F32).reshape(CZ * ANG, DW)
        for h in range(2):
            stage[h] = r[:, h * 128 : (h + 1) * 128]
        for a in range(ANG):
            for h in range(2):
                sl[:, a * DW + h * 128 : a * DW + (h + 1) * 128] = stage[
                    h, pl.ds(a, CZ, stride=ANG), :
                ].astype(BF16)
        with scope("mm_bwd"):
            for c in range(ANG):
                put(c, dot(sl[...], turned[:, c * DW : (c + 1) * DW], ((1,), (0,))))

    zhub[0].start()
    wait_round = greet(meet.at[0], 1)
    send_faces(0, x0)
    relayout(0, SPLIT)
    blur_z(0, x0, w1)
    send_yx(0, w1)
    wait_round()
    wait_round = greet(meet.at[1], 2)
    relayout(SPLIT, NCHUNK)

    def to_res(z, v):
        res[pl.ds(pl.multiple_of(z * CY, CY), CY), :] = v

    wait_round()
    wait_round = greet(meet.at[2], 4)
    blur_yx(0, w1, to_res)
    for y in range(CY):
        sl[:, y * CX : (y + 1) * CX] = res[pl.ds(y, CZ, stride=CY), :].astype(BF16)
    project(0)

    wait_faces(0)
    xa[1 : CZ + 1] = x0[...]
    cut = SHRINK

    @pl.loop(0, CZ, unroll=2)
    def _(z):
        smooth = jnp.zeros((CY, CX), F32)
        shrunk = jnp.zeros((CY, CX), F32)
        for j, jm in diffs(fyr.at[0], z):
            s = j - jnp.clip(j, -cut, cut)
            sm = jm - jnp.clip(jm, -cut, cut)
            smooth += jm - j
            shrunk += sm - s
        h = STEP * (smooth - shrunk)
        x0[z] = xa[z + 1] - h
        back[z] = shrunk

    stage_z(1, x0)
    zhub[1].start()

    shape1, shape2 = (160, 256), (256, CX)
    i, m = iota(shape1, 0), iota(shape1, 1) - 8
    i = jnp.where(i < CX, i, jnp.where(i < CX + 16, i - CX - 16, i - 16))
    inside = ((m >= 0) | (gx > 0)) & ((m < CX) | (gx < GX - 1)) & (m < CX + 8)
    thi, tlo = split(jnp.where(inside, gauss(i - m), 0.0))
    m = iota(shape2, 0) - 8
    uhi, ulo = split(gauss(m - iota(shape2, 1)))
    twice = (
        dot(thi, uhi, ((1,), (0,))) + dot(thi, ulo, ((1,), (0,))) + dot(tlo, uhi, ((1,), (0,)))
    )
    bhi, blo = split(twice[0:CX])
    bx2[0:CX] = bhi
    bx2[CX : 2 * CX] = bhi
    bx2[2 * CX : 3 * CX] = blo
    whi, wlo = split(twice[CX : CX + 32])
    wx2[0:32] = whi
    wx2[32:64] = wlo
    last_weights()

    zst[96:128] = jnp.zeros((32, V), BF16)
    shape1, shape2 = (CZ, CX), (CX, CX)
    m = iota(shape1, 1) - 8
    inside = ((m >= 0) | (gz > 0)) & ((m < CZ) | (gz < GZ - 1)) & (m < CZ + 8)
    thi, tlo = split(jnp.where(inside, gauss(iota(shape1, 0) - m), 0.0))

    def from_place(k):
        halo = jnp.where(k < 80, k - 80, jnp.where(k < 96, k - 80 + CZ, 4 * CX))
        return jnp.where(k < 64, lax.rem(k, CZ), halo)

    uhi, ulo = split(gauss(iota(shape2, 0) - 8 - from_place(iota(shape2, 1))))
    twice = (
        dot(thi, uhi, ((1,), (0,))) + dot(thi, ulo, ((1,), (0,))) + dot(tlo, uhi, ((1,), (0,)))
    )
    hi, lo = split(gauss(iota((48, CX), 0) - 1 - from_place(iota((48, CX), 1))))
    tz9[0:48] = hi
    tz9[48:96] = lo
    once = gauss(iota(shape1, 0) - from_place(iota(shape1, 1)))
    for i, t in enumerate((twice, once)):
        hi, lo = split(t)
        tz[32 * i : 32 * i + 32] = hi
        tz[64 + 32 * i : 96 + 32 * i] = lo

    with scope("turn"):
        turn(0, TURN)
    return_misfit(0)
    with scope("turn"):
        turn(TURN, ANG)
    blur_z(1, x0, w1)
    send_yx(1, w1)

    def to_stack(c, b):
        cols = slice(c * DW, (c + 1) * DW)
        hi, lo = split(b)
        zst[0:32, cols] = hi
        zst[32:64, cols] = lo

    backproject(0, to_stack)
    zhub2.start()

    def to_q(z, v):
        qbuf[pl.ds(z, CY, stride=CZ), :] = v

    blur_yx(1, w1, to_q)
    with scope("wait_z2"):
        zhub2.wait_recv()
    for c in range(ANG):
        cols = slice(c * DW, (c + 1) * DW)
        o = dot(tz[...], zst[:, cols], ((1,), (0,)))
        o = o[0:64] + o[64:128]
        for h in range(2):
            w2[ROWS // 16 * (2 * c + h) : ROWS // 16 * (2 * c + h + 1)] = o[
                0:32, h * 128 : (h + 1) * 128
            ]
        v1z[:, cols] = o[32:64]

    hi, lo = split(w2[...])
    ys2[...] = hi
    f = dot(pick2, hi, ((1,), (1,))).astype(BF16)
    xs[3, 0] = f[0:16]
    xs[3, 1] = f[16:32]
    yxhub2.start()
    slab = (CY, CZ, CX)
    both = jnp.concatenate([hi, lo], axis=1)
    own = dot(both, bx2[0 : 2 * CX], ((1,), (0,))) + dot(hi, bx2[2 * CX :], ((1,), (0,)))
    umid[16:32] = own.reshape(slab)
    for y in range(CY):
        res[pl.ds(y, CZ, stride=CY), :] = v1z[:, y * CX : (y + 1) * CX]
    w1[...] = res[...].reshape(CZ, CY, CX)
    with scope("wait_yx2"):
        yxhub2.wait_recv(slice(0, 6))
    umid[16:32] += rows_of(3, 1, wx2[...]).reshape(slab)
    for side in range(2):
        umid[32 * side : 32 * side + 16] = rows_of(3, 2 * side, wx2[...]).reshape(slab)

    @pl.loop(0, CY + 16)
    def _(y):
        out = ((y < 8) & ends[1][0]) | ((y >= CY + 8) & ends[1][1])
        ytwo[y] = jnp.where(out, 0.0, taps(lambda k: umid[y + k]))

    for y in range(CY):
        rows = slice(y * CZ, (y + 1) * CZ)
        qbuf[rows, :] = qbuf[rows, :] - STEP * taps(lambda k: ytwo[y + k])
    send_yx(2, w1, now=False)
    with scope("wait_yx2"):
        yxhub2.wait_recv(slice(6, 8))
    yxhub[2].start()
    for side in range(2):
        y = yr2[side]
        rows = dot(jnp.concatenate([y, y], axis=1), bx2[CX:], ((1,), (0,)))
        umid[32 * side : 32 * side + 16] = rows.reshape(slab)
    for y in range(CY):
        t = TWICE[16] * (umid[y] + umid[32 + y])
        for r in range(y + 1, CY):
            t += TWICE[y + 16 - r] * umid[r]
        for r in range(y):
            t += TWICE[16 + r - y] * umid[32 + r]
        v = qbuf[y * CZ : (y + 1) * CZ, :] - STEP * t
        sl[:, y * CX : (y + 1) * CX] = v.astype(BF16)

    project(1)

    def to_x(z, v):
        x = x0[z] - STEP * v
        x0[z] = x
        xa[z + 1] = x

    blur_yx(2, w1, to_x)
    send_faces(1, x0)
    return_misfit(1)
    wait_faces(1)

    def one(z, sums):
        primal, dres = sums
        smooth = jnp.zeros((CY, CX), F32)
        shrunk = jnp.zeros((CY, CX), F32)
        bdual = jnp.zeros((CY, CX), F32)
        for axis, (j, jm) in enumerate(diffs(fyr.at[1], z)):
            s = j - jnp.clip(j, -cut, cut)
            sm = jm - jnp.clip(jm, -cut, cut)
            d = j - s
            dm = jm - sm
            smooth += jm - j
            shrunk += sm - s
            bdual += dm - d
            dl[axis, z] = d
            dlm[axis, z] = dm
            primal += fold(jnp.square(j - s))
        dres += fold(jnp.square(shrunk - back[z]))
        hterm[z] = smooth - shrunk
        back[z] = shrunk
        bdl[z] = bdual
        return primal, dres

    zero = jnp.zeros((8, CX), F32)
    primal, dres = lax.fori_loop(0, CZ, one, (zero, zero), unroll=2)
    put_sums(0, primal, dres)
    for t in range(1, GZ):
        redz_copy(0, t).start()
    send_terms()

    zhub2.wait_send()
    backproject(1, to_stack)
    zhub[2].start()
    forward_sums(0)
    with scope("wait_z"):
        zhub[2].wait_recv()
    for c in range(ANG):
        o = dot(tz9[...], zst[:, c * DW : (c + 1) * DW], ((1,), (0,)))
        o = o[0:40] + o[48:88]
        for h in range(2):
            zmid[pl.ds(2 * c + h, 40, stride=CY), :] = o[:, h * 128 : (h + 1) * 128]
    outer = zmid[0:ROWS9].reshape(CZ + 2, CY, CX)
    n9 = (CZ + 2) * R
    for side, at, ninth in ((0, slice(0, R), R), (1, slice(CY - R, CY), CY - R - 1)):
        ys9[side, 0:n9] = outer[:, at, :].reshape(n9, CX).astype(BF16)
        ys9[side, n9:] = zmid[pl.ds(CY + ninth, CZ, stride=CY), :].astype(BF16)
    hi, lo = split(outer.reshape(ROWS9, CX))
    f = dot(pick2, hi, ((1,), (1,))).astype(BF16)
    xs9[0, :, 0:ROWS9] = f[0:16]
    xs9[1, :, 0:ROWS9] = f[16:32]
    yxhub[3].start()
    both = jnp.concatenate([hi, lo], axis=1)
    own = dot(both, bx9[0 : 2 * CX], ((1,), (0,))) + dot(hi, bx9[2 * CX :], ((1,), (0,)))
    own = own.reshape(CZ + 2, CY, 2 * CX)
    ymid[0 : CZ + 2, 16 : 16 + CY, :] = own[:, :, 0:CX]
    ybuf[:, R : R + CY, :] = own[1 : CZ + 1, :, CX:]
    penalty = factor_of(0, jnp.ones((8, CX), F32))
    inv1 = 1.0 / penalty
    pen3 = penalty[0:1].reshape(1, 1, CX)
    inv3 = inv1[0:1].reshape(1, 1, CX)
    spen = STEP * pen3
    x0[...] = x0[...] - spen * (hterm[...] + bdl[...] * inv3)
    dl[...] = dl[...] * inv3
    dlm[...] = dlm[...] * inv3
    with scope("wait_terms"):
        fhub[2].wait_recv()
    for side in range(2):
        fz2[side] = fzr[1, side] - spen[0] * (fzr2[side, 0] + fzr2[side, 1] * inv3[0])
        fy2[side] = fyr[1, side] - spen[0] * (fyr2[side, 0] + fyr2[side, 1] * inv3[0])
    rims = [
        dot(
            jnp.concatenate([fxr2[0, i], fxr2[1, i]], axis=0), wx[64:96], ((0,), (0,))
        ).reshape(CZ, CY, CX)
        for i in range(2)
    ]
    xlr[...] = xlr[...] - spen * (rims[0] + rims[1] * inv3)

    def halo_rows(slot):
        h = xr9[slot].reshape(32, ROWS9P)[:, 0:ROWS9]
        h = dot(jnp.concatenate([h, h], axis=0), wx9[...], ((0,), (0,)))
        return h.reshape(CZ + 2, CY, 2 * CX)

    with scope("wait_yx"):
        yxhub[3].wait_recv(slice(0, 6))
    more = halo_rows(1)
    ymid[0 : CZ + 2, 16 : 16 + CY, :] += more[:, :, 0:CX]
    ybuf[:, R : R + CY, :] += more[1 : CZ + 1, :, CX:]
    sides = ((0, slice(0, 16)), (1, slice(16 + CY, 32 + CY)))
    for side, to in sides:
        more = halo_rows(2 * side)
        ymid[0 : CZ + 2, to, :] = more[:, :, 0:CX]
        if side == 0:
            ybuf[:, 0:R, :] = more[1 : CZ + 1, CY - R :, CX:]
        else:
            ybuf[:, R + CY :, :] = more[1 : CZ + 1, 0:R, CX:]
    with scope("wait_yx"):
        yxhub[3].wait_recv(slice(6, 8))
    for side in range(2):
        y = yr9[side]
        rows = dot(jnp.concatenate([y, y], axis=1), bx9[CX:], ((1,), (0,)))
        near = rows[0:n9].reshape(CZ + 2, R, 2 * CX)
        to = slice(16 - R, 16) if side == 0 else slice(16 + CY, 16 + CY + R)
        ymid[0 : CZ + 2, to, :] += near[:, :, 0:CX]
        fy2[side] = fy2[side] - STEP * TAPS[0] * rows[n9:, 0:CX]
        to = slice(0, R) if side == 0 else slice(R + CY, 2 * R + CY)
        ybuf[:, to, :] += near[1 : CZ + 1, :, CX:]

    @pl.loop(0, CZ, unroll=2)
    def _(z):
        v = x0[z] - STEP * taps(lambda k: ymid[z + 1, 16 - R + k : 16 - R + CY + k, :])
        xa[z + 1] = v
        x_out[z] = v
        xlr[z] = xlr[z] - STEP * taps(lambda k: ybuf[z, k : k + CY, :])
        low = taps(lambda k: ymid[z + 1, k : k + R, :])[R - 1 : R]
        fy2[0, pl.ds(z, 1), :] = fy2[0, pl.ds(z, 1), :] - STEP * low
        high = taps(lambda k: ymid[z + 1, 16 + R + k : 16 + 2 * R + k, :])[0:1]
        fy2[1, pl.ds(z, 1), :] = fy2[1, pl.ds(z, 1), :] - STEP * high

    for side, at in ((0, 0), (1, CZ + 1)):
        xa[at] = fz2[side] - STEP * taps(lambda k: ymid[at, 16 - R + k : 16 - R + CY + k, :])
    cut2 = (SHRINK / penalty)[0:1]

    def last(z, sums):
        primal, dres = sums
        shrunk = jnp.zeros((CY, CX), F32)
        for axis, (j, jm) in enumerate(diffs(fy2, z)):
            t = j + dl[axis, z]
            tm = jm + dlm[axis, z]
            s = t - jnp.clip(t, -cut2, cut2)
            sm = tm - jnp.clip(tm, -cut2, cut2)
            shrunk += sm - s
            dl[axis, z] = t - s
            primal += fold(jnp.square(j - s))
        dres += fold(jnp.square(shrunk - back[z]))
        return primal, dres

    with scope("last"):
        primal, dres = lax.fori_loop(0, CZ, last, (zero, zero), unroll=4)
    put_sums(1, primal, dres)
    send_all()
    with scope("sums"):
        got = redall.at[pl.ds(1, GZ * BRICKS - 1)]
        pltpu.make_async_copy(got, got, all_recv).wait()
    factor2 = factor_from(red0[1] + jnp.sum(redall[1 : GZ * BRICKS], axis=0), penalty)
    scale = (1.0 / factor2)[0:1].reshape(1, 1, 1, CX)
    with scope("scale"):
        dual_out[...] = dl[...] * scale

    with scope("wait_sends"):
        for h in (zhub[2], yxhub[3], fhub[2]):
            h.wait_send()
        sent(1, snd2)
        got = redz.at[0, pl.ds(1, GZ - 1)]
        pltpu.make_async_copy(got, got, rz_send).wait()
        got = redx.at[0, pl.ds(1, BRICKS - 1)]
        pltpu.make_async_copy(got, got, rx_send).wait()
        got = redall.at[pl.ds(1, GZ * BRICKS - 1)]
        pltpu.make_async_copy(got, got, all_send).wait()


def body(start, measured, tiles, tile_block, angle_row):
    vm = pltpu.VMEM
    dma = pltpu.SemaphoreType.DMA
    block = vm((CZ, CY, CX), F32)
    return pl.pallas_call(
        kernel,
        out_shape=(
            pltpu.VMEM((CZ, CY, CX), F32),
            pltpu.VMEM((3, CZ, CY, CX), F32),
        ),
        in_specs=[
            pl.BlockSpec(memory_space=pltpu.HBM),
            pl.BlockSpec(memory_space=pltpu.HBM),
            pl.BlockSpec(memory_space=pltpu.HBM),
            pl.BlockSpec(memory_space=pltpu.VMEM),
            pl.BlockSpec(memory_space=pltpu.SMEM),
        ],
        out_specs=(pl.BlockSpec(memory_space=pltpu.VMEM), pl.BlockSpec(memory_space=pltpu.VMEM)),
        scratch_shapes=[
            vm((V, ANG, DW), BF16),
            vm((V, ANG * DW), BF16),
            vm((ANG * DW, V), BF16),
            vm((2, CHUNK * PITCH, 128), F32),
            block, block,
            vm((ROWS, CX), F32),
            vm((ROWS, CX), F32),
            vm((ROWS, CX), F32),
            vm((CZ + 2, CY, CX), F32),
            vm((CZ + 32, CY, CX), F32),
            vm((40 * CY, CX), F32),
            vm((CZ, CY + 16, CX), F32),
            vm((CZ + 2, CY + 32, CX), F32),
            vm((BRICKS, ANG, CX), F32),
            vm((1, ANG, NBLK * DW), F32),
            vm((ANG, NBLK * DW), F32),
            vm((ANG, NBLK * DW), F32),
            vm((2, 2, R * CY, CX), BF16),
            vm((2, 2, R * CY, CX), BF16),
            vm((128, V), BF16),
            vm((128, 128), BF16),
            vm((96, 128), BF16),
            vm((CZ, V), F32),
            vm((CY + 32, CZ, CX), F32),
            vm((CY + 16, CZ, CX), F32),
            vm((3, 2, CZ * R, CX), BF16),
            vm((3, 2, CZ * R, CX), BF16),
            vm((ROWS, CX), BF16),
            vm((2, ROWS, CX), BF16),
            vm((4, 2, 16, ROWS), BF16),
            vm((4, 3, 2, 16, ROWS), BF16),
            vm((2, (CZ + 2) * R + CZ, CX), BF16),
            vm((2, (CZ + 2) * R + CZ, CX), BF16),
            vm((2, 16, ROWS9P), BF16),
            vm((3, 2, 16, ROWS9P), BF16),
            vm((2, 2, CY, CX), F32),
            vm((2, 2, CY, CX), F32),
            vm((2, 2, CZ, CX), F32),
            vm((2, 2, CZ, CX), F32),
            vm((2, 2, 16, ROWS), BF16),
            vm((2, 2, 16, ROWS), BF16),
            vm((2, 2, CY, CX), F32),
            vm((2, 2, CY, CX), F32),
            vm((2, 2, CZ, CX), F32),
            vm((2, 2, CZ, CX), F32),
            vm((2, 2, 16, ROWS), BF16),
            vm((2, 2, 16, ROWS), BF16),
            vm((2, CY, CX), F32),
            vm((2, CZ, CX), F32),
            vm((2, CZ * ANG, 128), F32),
            vm((CZ, V), BF16),
            vm((2, BRICKS, ANG, DW), BF16),
            vm((2, BRICKS, ANG, DW), BF16),
            vm((2, BRICKS, ANG, DW), BF16),
            vm((2, BRICKS, ANG, DW), BF16),
            block, block,
            vm((3, CZ, CY, CX), F32),
            vm((3, CZ, CY, CX), F32),
            block, block,
            vm((2, 1, CX), F32),
            vm((2, GZ, 1, CX), F32),
            vm((2, 1, CX), F32),
            vm((2, BRICKS, 1, CX), F32),
            vm((GZ * BRICKS, 1, CX), F32),
            vm((3 * CX, CX), BF16),
            vm((96, CX), BF16),
            vm((3 * CX, CX), BF16),
            vm((64, CX), BF16),
            vm((3 * CX, 2 * CX), BF16),
            vm((64, 2 * CX), BF16),
            dma((2,)),
            dma((V // LOAD,)),
            dma((2,)),
            dma((2, 2)),
            dma((8,)),
            dma((2, 8)),
            dma((3, 2)),
            dma((2, 3, 2)),
            dma,
            dma((2, 2)),
            dma,
            dma,
            dma,
            dma,
            dma,
            dma,
            pltpu.SemaphoreType.REGULAR((3,)),
        ],
        compiler_params=pltpu.CompilerParams(
            collective_id=0, has_side_effects=True, vmem_limit_bytes=60 * 1024 * 1024
        ),
    )(start, measured, tiles, tile_block, angle_row)


def solution(mesh):
    return jax.shard_map(
        body,
        mesh=mesh,
        in_specs=(
            P("gz", "gy", "gx"),
            P(("gz", "gy", "gx"), None, None),
            P("gy", None, "gx"),
            P(),
            P(),
        ),
        out_specs=(P("gz", "gy", "gx"), P(None, "gz", "gy", "gx")),
        check_vma=False,
    )
```

```python
import math

import jax
import jax.numpy as jnp
from jax import lax
from jax.experimental import pallas as pl
from jax.experimental.pallas import tpu as pltpu
from jax.sharding import PartitionSpec as P

CZ, CY, CX = 32, 16, 128
ROWS = CZ * CY
ANG, DW, NBLK = 8, 256, 4
V = CY * CX
R = 8
GZ, GY, GX = 4, 4, 8
BRICKS = GY * GX
CELLS = float(CZ * CY * CX * GZ * BRICKS)
MESH = pl.DeviceIdType.MESH
F32, BF16 = jnp.float32, jnp.bfloat16
STEP = 0.5
SHRINK = 0.2
EPS = 1e-6
CHUNK = 128
NCHUNK = V // CHUNK
ORDER = sorted(
    ((dx, dz, dc) for dz in range(4) for dx in range(4) for dc in range(2) if dx or dz or dc),
    key=lambda s: -(min(s[0], 4 - s[0]) + min(s[1], 4 - s[1])),
)
LOAD = 512
ROWS9 = (CZ + 2) * CY
ROWS9P = -(-ROWS9 // 128) * 128
PITCH = 9
SPLIT = 4
NEAR = 16
TURN = 3
ORDER_ALL = sorted(
    ((dy, t) for dy in range(GZ) for t in range(GY * GX) if dy or t),
    key=lambda s: -(
        min(s[0], 4 - s[0])
        + (sum(min(d, 4 - d) for d in ORDER[s[1] - 1][:2]) if s[1] else 0)
    ),
)

RAW = [math.exp(-k * k / 12.5) for k in range(-R, R + 1)]
TAPS = [r / sum(RAW) for r in RAW]
TWICE = [
    sum(TAPS[k] * TAPS[d + 2 * R - k] for k in range(2 * R + 1) if 0 <= d + 2 * R - k <= 2 * R)
    for d in range(2 * R + 1)
]


def dot(a, b, dims):
    return lax.dot_general(a, b, (dims, ((), ())), preferred_element_type=F32)


def split(v):
    hi = v.astype(BF16)
    lo = (v - hi.astype(F32)).astype(BF16)
    return hi, lo


def kernel(
    start_ref, meas_ref, tiles_ref, tb_ref, row_ref,
    x_out, dual_out,
    raw, mat, turned, tmp, x0, w1, w2, res, qbuf, xa, zbuf, zmid, ybuf, ymid, tbv, obs, mis, acc,
    zs, zr, zst, tz, tz9, v1z, umid, ytwo, ys, yr, ys2, yr2, xs, xr,
    ys9, yr9, xs9, xr9,
    fzs, fzr, fys, fyr, fxs, fxr, fzs2, fzr2, fys2, fyr2, fxs2, fxr2, fz2, fy2,
    stage, sl, snd1, rcv1, snd2, rcv2,
    hterm, back, dl, dlm, xlr, bdl,
    red0, redz, red1, redx, redall,
    bx, wx, bx2, wx2, bx9, wx9,
    load_sem, tile_sem, z_send, z_recv, yx_send, yx_recv, f_send, f_recv,
    a_send, a_recv, rz_send, rz_recv, rx_send, rx_recv, all_send, all_recv, meet, near_recv,
):
    gz, gy, gx = lax.axis_index("gz"), lax.axis_index("gy"), lax.axis_index("gx")
    me = gy * GX + gx
    scope = jax.named_scope

    barrier = pltpu.get_barrier_semaphore()

    chip_x = 2 * (gy // 2) + lax.rem(gx, 2)
    chip_z, core = gx // 2, lax.rem(gy, 2)

    def member(t):
        dx, dz, dc = ORDER[t - 1]
        x = lax.rem(chip_x + dx, 4)
        z = lax.rem(chip_z + dz, 4)
        y = 2 * (x // 2) + lax.rem(core + dc, 2)
        x = 2 * z + lax.rem(x, 2)
        return y * GX + x, (gz, y, x)

    def there(dz, dy, dx):
        ok = True
        for d, at, n in ((dz, gz, GZ), (dy, gy, GY), (dx, gx, GX)):
            if d:
                near = at >= -d if d < 0 else at < n - d
                ok = near if ok is True else jnp.logical_and(ok, near)
        return ok

    def greet(sem, stride):
        steps = (-stride, 0, stride)
        places = [(0, dy, dx) for dy in steps for dx in steps if dy or dx]
        places += [(-stride, 0, 0), (stride, 0, 0)]
        if stride == 4:
            places = [(0, 0, -stride), (0, 0, stride)]
        heard = 0
        for dz, dy, dx in places:
            ok = there(dz, dy, dx)
            heard = heard + ok.astype(jnp.int32)

            @pl.when(ok)
            def _():
                pl.semaphore_signal(
                    sem, inc=1, device_id=(gz + dz, gy + dy, gx + dx), device_id_type=MESH
                )

        return lambda: pl.semaphore_wait(sem, heard)

    wait_near = greet(barrier, 1)

    ld = [
        pltpu.make_async_copy(start_ref, x0, load_sem.at[0]),
        pltpu.make_async_copy(meas_ref, obs, load_sem.at[1]),
    ]
    for c in ld:
        c.start()

    def turn(low, high):
        @pl.loop(low, high)
        def _(c):
            rows = pl.ds(pl.multiple_of(c * DW, DW), DW)
            for a in range(ANG):
                turned[a * DW : (a + 1) * DW, rows] = mat[rows, a * DW : (a + 1) * DW].T

    def tile_copy(c):
        rows = pl.ds(c * LOAD, LOAD)
        return pltpu.make_async_copy(tiles_ref.at[rows], raw.at[rows], tile_sem.at[c])


    class Hub:
        def __init__(self, items, before=None):
            self.before = before
            self.items = [
                (
                    there(*d),
                    there(*(-i for i in d)),
                    pltpu.make_async_remote_copy(
                        src, dst, ss, rs,
                        device_id=(gz + d[0], gy + d[1], gx + d[2]), device_id_type=MESH,
                    ),
                    dst,
                )
                for d, src, dst, ss, rs in items
            ]

        def clear(self):
            for _, arrives, _, dst in self.items:

                @pl.when(jnp.logical_not(arrives))
                def _():
                    dst[...] = jnp.zeros(dst.shape, dst.dtype)

        def start(self):
            if self.before is not None:
                self.before.wait_send()
            for leaves, _, copy, _ in self.items:
                pl.when(leaves)(copy.start)

        def wait_recv(self, part=slice(None)):
            for _, arrives, copy, _ in self.items[part]:
                pl.when(arrives)(copy.wait_recv)

        def wait_send(self):
            for leaves, _, copy, _ in self.items:
                pl.when(leaves)(copy.wait_send)

    def pair(axis, src, dst, send, recv):
        unit = [int(axis == a) for a in range(3)]
        return [
            ([-u for u in unit], src.at[0], dst.at[1], send.at[0], recv.at[0]),
            (unit, src.at[1], dst.at[0], send.at[1], recv.at[1]),
        ]

    def around(k, low, high, into_low, into_high, faces, halos, before):
        items = []
        i = 2
        for sy in (-1, 1, 0):
            for side, sx in ((0, -1), (1, 1)):
                items.append((
                    (0, sy, sx), faces.at[side], halos.at[1 - sy, 1 - side],
                    yx_send.at[i], yx_recv.at[k, i],
                ))
                i += 1
        items += [
            ((0, -1, 0), low, into_high, yx_send.at[0], yx_recv.at[k, 0]),
            ((0, 1, 0), high, into_low, yx_send.at[1], yx_recv.at[k, 1]),
        ]
        return Hub(items, before)

    def zswap(k, src, dst, before):
        return Hub(pair(0, src, dst, z_send, z_recv.at[k]), before)

    zhub = [zswap(0, zs.at[0], zr.at[0], None)]
    zhub.append(zswap(1, zs.at[1], zr.at[1], zhub[0]))
    def zstack(k, before):
        return Hub(
            [
                ((-1, 0, 0), zst.at[0:16], zst.at[80:96], z_send.at[0], z_recv.at[k, 0]),
                ((1, 0, 0), zst.at[16:32], zst.at[64:80], z_send.at[1], z_recv.at[k, 1]),
            ],
            before,
        )

    zhub2 = zstack(0, zhub[1])
    zhub.append(zstack(1, None))

    def yxswap(n, k, before):
        low, high = yr.at[n, 0], yr.at[n, 1]
        return around(k, ys.at[n, 0], ys.at[n, 1], low, high, xs.at[n], xr.at[n], before)

    yxhub = [yxswap(0, 0, None)]
    yxhub.append(yxswap(1, 1, yxhub[0]))
    yxhub2 = around(0, ys2, ys2, yr2.at[0], yr2.at[1], xs.at[3], xr.at[3], yxhub[1])
    yxhub.append(yxswap(2, 1, yxhub2))
    yxhub.append(
        around(0, ys9.at[0], ys9.at[1], yr9.at[0], yr9.at[1], xs9, xr9, yxhub[2])
    )
    fhub = []
    for k, z, y, x in (
        (0, (fzs.at[0], fzr.at[0]), (fys.at[0], fyr.at[0]), (fxs.at[0], fxr.at[0])),
        (1, (fzs.at[1], fzr.at[1]), (fys.at[1], fyr.at[1]), (fxs.at[1], fxr.at[1])),
        (0, (fzs2, fzr2), (fys2, fyr2), (fxs2, fxr2)),
    ):
        fhub.append(
            Hub(
                pair(0, *z, f_send.at[0], f_recv.at[k, 0])
                + pair(1, *y, f_send.at[1], f_recv.at[k, 1])
                + pair(2, *x, f_send.at[2], f_recv.at[k, 2]),
                fhub[-1] if fhub else None,
            )
        )
    xs9[...] = jnp.zeros_like(xs9)
    hubs = zhub + [zhub2] + yxhub + [yxhub2] + fhub
    for h in hubs:
        h.clear()

    def gauss(d):
        df = d.astype(F32)
        w = jnp.exp(df * df * (-1.0 / 12.5)) * (1.0 / sum(RAW))
        return jnp.where(jnp.abs(d) <= R, w, 0.0)

    def iota(shape, axis):
        return lax.broadcasted_iota(jnp.int32, shape, axis)

    square = (CX, CX)
    bhi, blo = split(gauss(iota(square, 0) - iota(square, 1)))
    bx[0:CX] = bhi
    bx[CX : 2 * CX] = bhi
    bx[2 * CX : 3 * CX] = blo
    k0, k1 = iota((32, CX), 0), iota((32, CX), 1)
    pos = jnp.where(k0 < 16, lax.rem(k0, 8) - 8, CX + lax.rem(k0, 8))
    whi, wlo = split(gauss(pos - k1))
    wx[0:32] = whi
    wx[32:64] = wlo
    rim = ((k1 == 0) & ((k0 == 7) | (k0 == 15))) | ((k1 == CX - 1) & ((k0 == 16) | (k0 == 24)))
    wx[64:96] = jnp.where(rim, 1.0, 0.0).astype(BF16)
    s0, s1 = iota((32, 2 * CX), 0), iota((32, 2 * CX), 1)
    want = jnp.where(s0 < 16, lax.rem(s0, 8), CX - 8 + lax.rem(s0, 8)) + jnp.where(
        lax.rem(s0, 16) < 8, 0, CX
    )
    pick = jnp.where(s1 == want, 1.0, 0.0).astype(BF16)
    pick2 = jnp.where(k1 == jnp.where(k0 < 16, k0, CX - 32 + k0), 1.0, 0.0).astype(BF16)

    def place(c):
        edge = jnp.where(c == CX, -1, jnp.where(c == 2 * CX - 1, CX, 4 * CX))
        return jnp.where(c < CX, c, edge)

    def last_weights():
        shape = (CX, 2 * CX)
        hi, lo = split(gauss(iota(shape, 0) - place(iota(shape, 1))))
        bx9[0:CX] = hi
        bx9[CX : 2 * CX] = hi
        bx9[2 * CX : 3 * CX] = lo
        shape = (32, 2 * CX)
        k = iota(shape, 0)
        hi, lo = split(gauss(jnp.where(k < 16, k - 16, CX - 16 + k) - place(iota(shape, 1))))
        wx9[0:32] = hi
        wx9[32:64] = lo

    wide = (GX, GX * CX)
    spread = jnp.where(iota(wide, 0) == iota(wide, 1) // CX, 1.0, 0.0).astype(BF16)
    for b in range(GY):
        rows = dot(tb_ref[b].astype(F32).astype(BF16), spread, ((0,), (0,)))
        for c in range(GX):
            tbv[b * GX + c] = rows[:, c * CX : (c + 1) * CX]

    def relayout(low, high):
        for c in range(V // LOAD):
            if low * CHUNK <= c * LOAD < high * CHUNK:
                tile_copy(c).wait()

        @pl.loop(low, high)
        def _(c):
            rows = pl.ds(pl.multiple_of(c * CHUNK, CHUNK), CHUNK)
            block = raw[rows].astype(F32)
            for h in range(2):
                for j in range(CHUNK):
                    tmp[h, PITCH * j : PITCH * j + ANG, :] = block[j, :, h * 128 : (h + 1) * 128]
            for a in range(ANG):
                for h in range(2):
                    part = tmp[h, pl.ds(a, CHUNK, stride=PITCH), :]
                    mat[rows, a * DW + h * 128 : a * DW + (h + 1) * 128] = part.astype(BF16)

    ld[0].wait()
    for c in range(V // LOAD):
        tile_copy(c).start()
    ld[1].wait()
    for a in range(ANG):
        acc[pl.ds(a, 1), :] = obs[0, pl.ds(row_ref[a], 1), :]

    def stage_z(n, src):
        zs[n, 0] = src[0:R].reshape(R * CY, CX).astype(BF16)
        zs[n, 1] = src[CZ - R : CZ].reshape(R * CY, CX).astype(BF16)

    stage_z(0, x0)
    with scope("wait_barrier"):
        wait_near()

    def send_faces(n, src):
        fzs[n, 0] = src[0]
        fzs[n, 1] = src[CZ - 1]
        v = src[...]
        fys[n, 0] = v[:, 0, :]
        fys[n, 1] = v[:, CY - 1, :]
        hi, lo = split(v.reshape(ROWS, CX))
        f = dot(pick, jnp.concatenate([hi, lo], axis=1), ((1,), (1,))).astype(BF16)
        fxs[n, 0] = f[0:16]
        fxs[n, 1] = f[16:32]
        fhub[n].start()

    def send_terms():
        for i, src in enumerate((hterm, bdl)):
            fzs2[0, i] = src[0]
            fzs2[1, i] = src[CZ - 1]
            v = src[...]
            fys2[0, i] = v[:, 0, :]
            fys2[1, i] = v[:, CY - 1, :]
            hi, lo = split(v.reshape(ROWS, CX))
            f = dot(pick, jnp.concatenate([hi, lo], axis=1), ((1,), (1,))).astype(BF16)
            fxs2[0, i] = f[0:16]
            fxs2[1, i] = f[16:32]
        fhub[2].start()

    def taps(at):
        t = TAPS[R] * at(R)
        for k in range(R):
            t += TAPS[k] * (at(k) + at(2 * R - k))
        return t

    def blur_z(n, src, out):
        zbuf[R : R + CZ] = src[...]
        with scope("wait_z"):
            zhub[n].wait_recv()
        zbuf[0:R] = zr[n, 0].astype(F32).reshape(R, CY, CX)
        zbuf[R + CZ : 2 * R + CZ] = zr[n, 1].astype(F32).reshape(R, CY, CX)

        @pl.loop(0, CZ, unroll=2)
        def _(z):
            out[z] = taps(lambda k: zbuf[z + k])

    def send_yx(n, w, now=True):
        v = w[...]
        ys[n, 0] = v[:, 0:R, :].reshape(CZ * R, CX).astype(BF16)
        ys[n, 1] = v[:, CY - R :, :].reshape(CZ * R, CX).astype(BF16)
        hi, lo = split(v.reshape(ROWS, CX))
        f = dot(pick, jnp.concatenate([hi, lo], axis=1), ((1,), (1,))).astype(BF16)
        xs[n, 0] = f[0:16]
        xs[n, 1] = f[16:32]
        if now:
            yxhub[n].start()

    def rows_of(m, slot, weights):
        halo = xr[m, slot].reshape(32, ROWS)
        return dot(jnp.concatenate([halo, halo], axis=0), weights, ((0,), (0,)))

    def own_rows(w, mat3):
        hi, lo = split(w[...].reshape(ROWS, CX))
        both = jnp.concatenate([hi, lo], axis=1)
        return dot(both, mat3[0 : 2 * CX], ((1,), (0,))) + dot(hi, mat3[2 * CX :], ((1,), (0,)))

    def blur_yx(n, w, put):
        own = own_rows(w, bx)
        ybuf[:, R : R + CY, :] = own.reshape(CZ, CY, CX)
        with scope("wait_yx"):
            yxhub[n].wait_recv(slice(0, 6))
        ybuf[:, R : R + CY, :] += rows_of(n, 1, wx[0:64]).reshape(CZ, CY, CX)
        sides = (
            (0, slice(CY - R, CY), slice(0, R)),
            (1, slice(0, R), slice(R + CY, 2 * R + CY)),
        )
        for side, at, to in sides:
            ybuf[:, to, :] = rows_of(n, 2 * side, wx[0:64]).reshape(CZ, CY, CX)[:, at, :]
        with scope("wait_yx"):
            yxhub[n].wait_recv(slice(6, 8))
        for side, at, to in sides:
            y = yr[n, side]
            rows = dot(jnp.concatenate([y, y], axis=1), bx[CX:], ((1,), (0,)))
            ybuf[:, to, :] += rows.reshape(CZ, R, CX)

        @pl.loop(0, CZ, unroll=2)
        def _(z):
            put(z, taps(lambda k: ybuf[z, k : k + CY, :]))

    lane, sub = iota((CY, CX), 1), iota((CY, CX), 0)
    ends = ((gz == 0, gz == GZ - 1), (gy == 0, gy == GY - 1), (gx == 0, gx == GX - 1))

    def wait_faces(n):
        with scope("wait_faces"):
            fhub[n].wait_recv()
        xlr[...] = dot(fxr[n].reshape(32, ROWS), wx[64:96], ((0,), (0,))).reshape(CZ, CY, CX)
        xa[0] = fzr[n, 0]
        xa[CZ + 1] = fzr[n, 1]

    def diffs(fy, z):
        v = xa[z + 1]
        up, low = xa[z + 2], xa[z]
        yield (
            jnp.where((z == CZ - 1) & ends[0][1], 0.0, up - v),
            jnp.where((z == 0) & ends[0][0], 0.0, v - low),
        )
        up = jnp.where(sub == CY - 1, fy[1, pl.ds(z, 1), :], pltpu.roll(v, CY - 1, 0))
        low = jnp.where(sub == 0, fy[0, pl.ds(z, 1), :], pltpu.roll(v, 1, 0))
        yield (
            jnp.where((sub == CY - 1) & ends[1][1], 0.0, up - v),
            jnp.where((sub == 0) & ends[1][0], 0.0, v - low),
        )
        edge = xlr[z]
        up = jnp.where(lane == CX - 1, edge, pltpu.roll(v, CX - 1, 1))
        low = jnp.where(lane == 0, edge, pltpu.roll(v, 1, 1))
        yield (
            jnp.where((lane == CX - 1) & ends[2][1], 0.0, up - v),
            jnp.where((lane == 0) & ends[2][0], 0.0, v - low),
        )

    def fold(p):
        return p[0:8] + p[8:16]

    def redz_copy(n, t):
        return pltpu.make_async_remote_copy(
            red0.at[n], redz.at[n, t], rz_send, rz_recv,
            device_id=(lax.rem(gz + t, GZ), gy, gx), device_id_type=MESH,
        )

    def redx_copy(n, t):
        return pltpu.make_async_remote_copy(
            red1.at[n], redx.at[n, t], rx_send, rx_recv,
            device_id=member(t)[1], device_id_type=MESH,
        )

    def put_sums(n, primal, dualres):
        p = jnp.sum(jnp.sum(primal, axis=0, keepdims=True), axis=1, keepdims=True)
        d = jnp.sum(jnp.sum(dualres, axis=0, keepdims=True), axis=1, keepdims=True)
        red0[n] = jnp.where(lane[0:1] < CX // 2, p, d)

    def send_all():
        for slot, (dy, t) in enumerate(ORDER_ALL):
            dev = (gy, gx) if t == 0 else member(t)[1][1:]
            pltpu.make_async_remote_copy(
                red0.at[1], redall.at[slot + 1], all_send, all_recv,
                device_id=(lax.rem(gz + dy, GZ), *dev), device_id_type=MESH,
            ).start()

    def forward_sums(n):
        got = redz.at[n, pl.ds(1, GZ - 1)]
        pltpu.make_async_copy(got, got, rz_recv).wait()
        red1[n] = red0[n] + jnp.sum(redz[n, 1:GZ], axis=0)

        for t in range(1, BRICKS):
            redx_copy(n, t).start()

    def factor_of(n, penalty):
        total = red1[n]
        got = redx.at[n, pl.ds(1, BRICKS - 1)]
        pltpu.make_async_copy(got, got, rx_recv).wait()
        total += jnp.sum(redx[n, 1:BRICKS], axis=0)
        return factor_from(total, penalty)

    def factor_from(total, penalty):
        p = jnp.broadcast_to(total[:, 0:1], (8, CX)) * (1.0 / (3.0 * CELLS))
        d = jnp.broadcast_to(total[:, CX - 1 : CX], (8, CX)) * (1.0 / CELLS)
        d = penalty * penalty * d
        return jnp.sqrt(jnp.sqrt((p + EPS) / (d + EPS)))

    def arrivals(ref, sem):
        got = ref.at[pl.ds(0, BRICKS - 1)]
        pltpu.make_async_copy(got, got, sem).wait()

    def sent(n, ref):
        arrivals(ref.at[n], a_send)

    def send_block(n, i, src, dst, d, dev):
        pltpu.make_async_remote_copy(
            src.at[n, d], dst.at[n, me], a_send, a_recv.at[n, i],
            device_id=dev, device_id_type=MESH,
        ).start()

    def project(n):
        with scope("mm_fwd"):
            for a in range(ANG):
                c = dot(sl[...], mat[:, a * DW : (a + 1) * DW], ((1,), (0,)))
                for h in range(2):
                    stage[h, pl.ds(a, CZ, stride=ANG), :] = c[:, h * 128 : (h + 1) * 128]

        def block_of(d):
            rows = pl.ds(pl.multiple_of(d * ANG, ANG), ANG)
            return jnp.concatenate([stage[0, rows, :], stage[1, rows, :]], axis=1).astype(BF16)

        if n:
            sent(0, snd2)
        else:
            wait_round()
        for t in range(1, BRICKS):
            d, dev = member(t)
            snd1[n, d] = block_of(d)
            pltpu.make_async_remote_copy(
                snd1.at[n, d], rcv1.at[n, t], a_send,
                a_recv.at[n, 0] if t < NEAR else near_recv.at[n],
                device_id=dev, device_id_type=MESH,
            ).start()

        rcv1[n, 0] = block_of(me)

    def return_misfit(n):
        def sender(t):
            if t == 0:
                return me
            dx, dz, dc = ORDER[t - 1]
            x = lax.rem(chip_x + 4 - dx, 4)
            z = lax.rem(chip_z + 4 - dz, 4)
            y = 2 * (x // 2) + lax.rem(core + dc, 2)
            return y * GX + 2 * z + lax.rem(x, 2)

        def add(slots, sums):
            for t in slots:
                x = rcv1[n, t].astype(F32)
                b = tbv[sender(t)]
                b = jnp.concatenate([b, b], axis=1)
                sums = [sums[q] + jnp.where(b == float(q), x, 0.0) for q in range(NBLK)]
            return sums

        with scope("wait_a1"):
            got = rcv1.at[n, pl.ds(NEAR, BRICKS - NEAR)]
            pltpu.make_async_copy(got, got, near_recv.at[n]).wait()
        sums = [jnp.zeros((ANG, DW), F32) for _ in range(NBLK)]
        sums = add([0, *range(NEAR, BRICKS)], sums)
        with scope("wait_a1"):
            got = rcv1.at[n, pl.ds(1, NEAR - 1)]
            pltpu.make_async_copy(got, got, a_recv.at[n, 0]).wait()
        sums = add(range(1, NEAR), sums)
        for q in range(NBLK):
            cols = slice(q * DW, (q + 1) * DW)
            mis[:, cols] = (sums[q] - acc[:, cols]).astype(BF16).astype(F32)

        def chosen(d):
            t = tbv[d]
            t = jnp.concatenate([t, t], axis=1)
            c = mis[:, 0:DW]
            for q in range(1, NBLK):
                c = jnp.where(t == float(q), mis[:, q * DW : (q + 1) * DW], c)
            return c.astype(BF16)

        sent(n, snd1)
        for t in range(1, BRICKS):
            d, dev = member(t)
            snd2[n, d] = chosen(d)
            send_block(n, 1, snd2, rcv2, d, dev)

        rcv2[n, me] = chosen(me)

    def backproject(n, put):
        with scope("wait_a2"):
            arrivals(rcv2.at[n], a_recv.at[n, 1])
        r = rcv2[n].astype(F32).reshape(CZ * ANG, DW)
        for h in range(2):
            stage[h] = r[:, h * 128 : (h + 1) * 128]
        for a in range(ANG):
            for h in range(2):
                sl[:, a * DW + h * 128 : a * DW + (h + 1) * 128] = stage[
                    h, pl.ds(a, CZ, stride=ANG), :
                ].astype(BF16)
        with scope("mm_bwd"):
            for c in range(ANG):
                put(c, dot(sl[...], turned[:, c * DW : (c + 1) * DW], ((1,), (0,))))

    zhub[0].start()
    wait_round = greet(meet.at[0], 1)
    send_faces(0, x0)
    relayout(0, SPLIT)
    blur_z(0, x0, w1)
    send_yx(0, w1)
    wait_round()
    wait_round = greet(meet.at[1], 2)
    relayout(SPLIT, NCHUNK)

    def to_res(z, v):
        res[pl.ds(pl.multiple_of(z * CY, CY), CY), :] = v

    wait_round()
    wait_round = greet(meet.at[2], 4)
    blur_yx(0, w1, to_res)
    for y in range(CY):
        sl[:, y * CX : (y + 1) * CX] = res[pl.ds(y, CZ, stride=CY), :].astype(BF16)
    project(0)

    wait_faces(0)
    xa[1 : CZ + 1] = x0[...]
    cut = SHRINK

    @pl.loop(0, CZ, unroll=2)
    def _(z):
        smooth = jnp.zeros((CY, CX), F32)
        shrunk = jnp.zeros((CY, CX), F32)
        for j, jm in diffs(fyr.at[0], z):
            s = j - jnp.clip(j, -cut, cut)
            sm = jm - jnp.clip(jm, -cut, cut)
            smooth += jm - j
            shrunk += sm - s
        h = STEP * (smooth - shrunk)
        x0[z] = xa[z + 1] - h
        back[z] = shrunk

    stage_z(1, x0)
    zhub[1].start()

    shape1, shape2 = (160, 256), (256, CX)
    i, m = iota(shape1, 0), iota(shape1, 1) - 8
    i = jnp.where(i < CX, i, jnp.where(i < CX + 16, i - CX - 16, i - 16))
    inside = ((m >= 0) | (gx > 0)) & ((m < CX) | (gx < GX - 1)) & (m < CX + 8)
    thi, tlo = split(jnp.where(inside, gauss(i - m), 0.0))
    m = iota(shape2, 0) - 8
    uhi, ulo = split(gauss(m - iota(shape2, 1)))
    twice = (
        dot(thi, uhi, ((1,), (0,))) + dot(thi, ulo, ((1,), (0,))) + dot(tlo, uhi, ((1,), (0,)))
    )
    bhi, blo = split(twice[0:CX])
    bx2[0:CX] = bhi
    bx2[CX : 2 * CX] = bhi
    bx2[2 * CX : 3 * CX] = blo
    whi, wlo = split(twice[CX : CX + 32])
    wx2[0:32] = whi
    wx2[32:64] = wlo
    last_weights()

    zst[96:128] = jnp.zeros((32, V), BF16)
    shape1, shape2 = (CZ, CX), (CX, CX)
    m = iota(shape1, 1) - 8
    inside = ((m >= 0) | (gz > 0)) & ((m < CZ) | (gz < GZ - 1)) & (m < CZ + 8)
    thi, tlo = split(jnp.where(inside, gauss(iota(shape1, 0) - m), 0.0))

    def from_place(k):
        halo = jnp.where(k < 80, k - 80, jnp.where(k < 96, k - 80 + CZ, 4 * CX))
        return jnp.where(k < 64, lax.rem(k, CZ), halo)

    uhi, ulo = split(gauss(iota(shape2, 0) - 8 - from_place(iota(shape2, 1))))
    twice = (
        dot(thi, uhi, ((1,), (0,))) + dot(thi, ulo, ((1,), (0,))) + dot(tlo, uhi, ((1,), (0,)))
    )
    hi, lo = split(gauss(iota((48, CX), 0) - 1 - from_place(iota((48, CX), 1))))
    tz9[0:48] = hi
    tz9[48:96] = lo
    once = gauss(iota(shape1, 0) - from_place(iota(shape1, 1)))
    for i, t in enumerate((twice, once)):
        hi, lo = split(t)
        tz[32 * i : 32 * i + 32] = hi
        tz[64 + 32 * i : 96 + 32 * i] = lo

    with scope("turn"):
        turn(0, TURN)
    return_misfit(0)
    with scope("turn"):
        turn(TURN, ANG)
    blur_z(1, x0, w1)
    send_yx(1, w1)

    def to_stack(c, b):
        cols = slice(c * DW, (c + 1) * DW)
        hi, lo = split(b)
        zst[0:32, cols] = hi
        zst[32:64, cols] = lo

    backproject(0, to_stack)
    zhub2.start()

    def to_q(z, v):
        qbuf[pl.ds(z, CY, stride=CZ), :] = v

    blur_yx(1, w1, to_q)
    with scope("wait_z2"):
        zhub2.wait_recv()
    for c in range(ANG):
        cols = slice(c * DW, (c + 1) * DW)
        o = dot(tz[...], zst[:, cols], ((1,), (0,)))
        o = o[0:64] + o[64:128]
        for h in range(2):
            w2[ROWS // 16 * (2 * c + h) : ROWS // 16 * (2 * c + h + 1)] = o[
                0:32, h * 128 : (h + 1) * 128
            ]
        v1z[:, cols] = o[32:64]

    hi, lo = split(w2[...])
    ys2[...] = hi
    f = dot(pick2, hi, ((1,), (1,))).astype(BF16)
    xs[3, 0] = f[0:16]
    xs[3, 1] = f[16:32]
    yxhub2.start()
    slab = (CY, CZ, CX)
    both = jnp.concatenate([hi, lo], axis=1)
    own = dot(both, bx2[0 : 2 * CX], ((1,), (0,))) + dot(hi, bx2[2 * CX :], ((1,), (0,)))
    umid[16:32] = own.reshape(slab)
    for y in range(CY):
        res[pl.ds(y, CZ, stride=CY), :] = v1z[:, y * CX : (y + 1) * CX]
    w1[...] = res[...].reshape(CZ, CY, CX)
    with scope("wait_yx2"):
        yxhub2.wait_recv(slice(0, 6))
    umid[16:32] += rows_of(3, 1, wx2[...]).reshape(slab)
    for side in range(2):
        umid[32 * side : 32 * side + 16] = rows_of(3, 2 * side, wx2[...]).reshape(slab)

    @pl.loop(0, CY + 16)
    def _(y):
        out = ((y < 8) & ends[1][0]) | ((y >= CY + 8) & ends[1][1])
        ytwo[y] = jnp.where(out, 0.0, taps(lambda k: umid[y + k]))

    for y in range(CY):
        rows = slice(y * CZ, (y + 1) * CZ)
        qbuf[rows, :] = qbuf[rows, :] - STEP * taps(lambda k: ytwo[y + k])
    send_yx(2, w1, now=False)
    with scope("wait_yx2"):
        yxhub2.wait_recv(slice(6, 8))
    yxhub[2].start()
    for side in range(2):
        y = yr2[side]
        rows = dot(jnp.concatenate([y, y], axis=1), bx2[CX:], ((1,), (0,)))
        umid[32 * side : 32 * side + 16] = rows.reshape(slab)
    for y in range(CY):
        t = TWICE[16] * (umid[y] + umid[32 + y])
        for r in range(y + 1, CY):
            t += TWICE[y + 16 - r] * umid[r]
        for r in range(y):
            t += TWICE[16 + r - y] * umid[32 + r]
        v = qbuf[y * CZ : (y + 1) * CZ, :] - STEP * t
        sl[:, y * CX : (y + 1) * CX] = v.astype(BF16)

    project(1)

    def to_x(z, v):
        x = x0[z] - STEP * v
        x0[z] = x
        xa[z + 1] = x

    blur_yx(2, w1, to_x)
    send_faces(1, x0)
    return_misfit(1)
    wait_faces(1)

    def one(z, sums):
        primal, dres = sums
        smooth = jnp.zeros((CY, CX), F32)
        shrunk = jnp.zeros((CY, CX), F32)
        bdual = jnp.zeros((CY, CX), F32)
        for axis, (j, jm) in enumerate(diffs(fyr.at[1], z)):
            s = j - jnp.clip(j, -cut, cut)
            sm = jm - jnp.clip(jm, -cut, cut)
            d = j - s
            dm = jm - sm
            smooth += jm - j
            shrunk += sm - s
            bdual += dm - d
            dl[axis, z] = d
            dlm[axis, z] = dm
            primal += fold(jnp.square(j - s))
        dres += fold(jnp.square(shrunk - back[z]))
        hterm[z] = smooth - shrunk
        back[z] = shrunk
        bdl[z] = bdual
        return primal, dres

    zero = jnp.zeros((8, CX), F32)
    primal, dres = lax.fori_loop(0, CZ, one, (zero, zero), unroll=2)
    put_sums(0, primal, dres)
    for t in range(1, GZ):
        redz_copy(0, t).start()
    send_terms()

    zhub2.wait_send()
    backproject(1, to_stack)
    zhub[2].start()
    forward_sums(0)
    with scope("wait_z"):
        zhub[2].wait_recv()
    for c in range(ANG):
        o = dot(tz9[...], zst[:, c * DW : (c + 1) * DW], ((1,), (0,)))
        o = o[0:40] + o[48:88]
        for h in range(2):
            zmid[pl.ds(2 * c + h, 40, stride=CY), :] = o[:, h * 128 : (h + 1) * 128]
    outer = zmid[0:ROWS9].reshape(CZ + 2, CY, CX)
    n9 = (CZ + 2) * R
    for side, at, ninth in ((0, slice(0, R), R), (1, slice(CY - R, CY), CY - R - 1)):
        ys9[side, 0:n9] = outer[:, at, :].reshape(n9, CX).astype(BF16)
        ys9[side, n9:] = zmid[pl.ds(CY + ninth, CZ, stride=CY), :].astype(BF16)
    hi, lo = split(outer.reshape(ROWS9, CX))
    f = dot(pick2, hi, ((1,), (1,))).astype(BF16)
    xs9[0, :, 0:ROWS9] = f[0:16]
    xs9[1, :, 0:ROWS9] = f[16:32]
    yxhub[3].start()
    both = jnp.concatenate([hi, lo], axis=1)
    own = dot(both, bx9[0 : 2 * CX], ((1,), (0,))) + dot(hi, bx9[2 * CX :], ((1,), (0,)))
    own = own.reshape(CZ + 2, CY, 2 * CX)
    ymid[0 : CZ + 2, 16 : 16 + CY, :] = own[:, :, 0:CX]
    ybuf[:, R : R + CY, :] = own[1 : CZ + 1, :, CX:]
    penalty = factor_of(0, jnp.ones((8, CX), F32))
    inv1 = 1.0 / penalty
    pen3 = penalty[0:1].reshape(1, 1, CX)
    inv3 = inv1[0:1].reshape(1, 1, CX)
    spen = STEP * pen3
    x0[...] = x0[...] - spen * (hterm[...] + bdl[...] * inv3)
    dl[...] = dl[...] * inv3
    dlm[...] = dlm[...] * inv3
    with scope("wait_terms"):
        fhub[2].wait_recv()
    for side in range(2):
        fz2[side] = fzr[1, side] - spen[0] * (fzr2[side, 0] + fzr2[side, 1] * inv3[0])
        fy2[side] = fyr[1, side] - spen[0] * (fyr2[side, 0] + fyr2[side, 1] * inv3[0])
    rims = [
        dot(
            jnp.concatenate([fxr2[0, i], fxr2[1, i]], axis=0), wx[64:96], ((0,), (0,))
        ).reshape(CZ, CY, CX)
        for i in range(2)
    ]
    xlr[...] = xlr[...] - spen * (rims[0] + rims[1] * inv3)

    def halo_rows(slot):
        h = xr9[slot].reshape(32, ROWS9P)[:, 0:ROWS9]
        h = dot(jnp.concatenate([h, h], axis=0), wx9[...], ((0,), (0,)))
        return h.reshape(CZ + 2, CY, 2 * CX)

    with scope("wait_yx"):
        yxhub[3].wait_recv(slice(0, 6))
    more = halo_rows(1)
    ymid[0 : CZ + 2, 16 : 16 + CY, :] += more[:, :, 0:CX]
    ybuf[:, R : R + CY, :] += more[1 : CZ + 1, :, CX:]
    sides = ((0, slice(0, 16)), (1, slice(16 + CY, 32 + CY)))
    for side, to in sides:
        more = halo_rows(2 * side)
        ymid[0 : CZ + 2, to, :] = more[:, :, 0:CX]
        if side == 0:
            ybuf[:, 0:R, :] = more[1 : CZ + 1, CY - R :, CX:]
        else:
            ybuf[:, R + CY :, :] = more[1 : CZ + 1, 0:R, CX:]
    with scope("wait_yx"):
        yxhub[3].wait_recv(slice(6, 8))
    for side in range(2):
        y = yr9[side]
        rows = dot(jnp.concatenate([y, y], axis=1), bx9[CX:], ((1,), (0,)))
        near = rows[0:n9].reshape(CZ + 2, R, 2 * CX)
        to = slice(16 - R, 16) if side == 0 else slice(16 + CY, 16 + CY + R)
        ymid[0 : CZ + 2, to, :] += near[:, :, 0:CX]
        fy2[side] = fy2[side] - STEP * TAPS[0] * rows[n9:, 0:CX]
        to = slice(0, R) if side == 0 else slice(R + CY, 2 * R + CY)
        ybuf[:, to, :] += near[1 : CZ + 1, :, CX:]

    @pl.loop(0, CZ, unroll=2)
    def _(z):
        v = x0[z] - STEP * taps(lambda k: ymid[z + 1, 16 - R + k : 16 - R + CY + k, :])
        xa[z + 1] = v
        x_out[z] = v
        xlr[z] = xlr[z] - STEP * taps(lambda k: ybuf[z, k : k + CY, :])
        low = taps(lambda k: ymid[z + 1, k : k + R, :])[R - 1 : R]
        fy2[0, pl.ds(z, 1), :] = fy2[0, pl.ds(z, 1), :] - STEP * low
        high = taps(lambda k: ymid[z + 1, 16 + R + k : 16 + 2 * R + k, :])[0:1]
        fy2[1, pl.ds(z, 1), :] = fy2[1, pl.ds(z, 1), :] - STEP * high

    for side, at in ((0, 0), (1, CZ + 1)):
        xa[at] = fz2[side] - STEP * taps(lambda k: ymid[at, 16 - R + k : 16 - R + CY + k, :])
    cut2 = (SHRINK / penalty)[0:1]

    def last(z, sums):
        primal, dres = sums
        shrunk = jnp.zeros((CY, CX), F32)
        for axis, (j, jm) in enumerate(diffs(fy2, z)):
            t = j + dl[axis, z]
            tm = jm + dlm[axis, z]
            s = t - jnp.clip(t, -cut2, cut2)
            sm = tm - jnp.clip(tm, -cut2, cut2)
            shrunk += sm - s
            dl[axis, z] = t - s
            primal += fold(jnp.square(j - s))
        dres += fold(jnp.square(shrunk - back[z]))
        return primal, dres

    with scope("last"):
        primal, dres = lax.fori_loop(0, CZ, last, (zero, zero), unroll=4)
    put_sums(1, primal, dres)
    send_all()
    with scope("sums"):
        got = redall.at[pl.ds(1, GZ * BRICKS - 1)]
        pltpu.make_async_copy(got, got, all_recv).wait()
    factor2 = factor_from(red0[1] + jnp.sum(redall[1 : GZ * BRICKS], axis=0), penalty)
    scale = (1.0 / factor2)[0:1].reshape(1, 1, 1, CX)
    with scope("scale"):
        dual_out[...] = dl[...] * scale

    with scope("wait_sends"):
        for h in (zhub[2], yxhub[3], fhub[2]):
            h.wait_send()
        sent(1, snd2)
        got = redz.at[0, pl.ds(1, GZ - 1)]
        pltpu.make_async_copy(got, got, rz_send).wait()
        got = redx.at[0, pl.ds(1, BRICKS - 1)]
        pltpu.make_async_copy(got, got, rx_send).wait()
        got = redall.at[pl.ds(1, GZ * BRICKS - 1)]
        pltpu.make_async_copy(got, got, all_send).wait()


def body(start, measured, tiles, tile_block, angle_row):
    vm = pltpu.VMEM
    dma = pltpu.SemaphoreType.DMA
    block = vm((CZ, CY, CX), F32)
    return pl.pallas_call(
        kernel,
        out_shape=(
            pltpu.VMEM((CZ, CY, CX), F32),
            pltpu.VMEM((3, CZ, CY, CX), F32),
        ),
        in_specs=[
            pl.BlockSpec(memory_space=pltpu.HBM),
            pl.BlockSpec(memory_space=pltpu.HBM),
            pl.BlockSpec(memory_space=pltpu.HBM),
            pl.BlockSpec(memory_space=pltpu.VMEM),
            pl.BlockSpec(memory_space=pltpu.SMEM),
        ],
        out_specs=(pl.BlockSpec(memory_space=pltpu.VMEM), pl.BlockSpec(memory_space=pltpu.VMEM)),
        scratch_shapes=[
            vm((V, ANG, DW), BF16),
            vm((V, ANG * DW), BF16),
            vm((ANG * DW, V), BF16),
            vm((2, CHUNK * PITCH, 128), F32),
            block, block,
            vm((ROWS, CX), F32),
            vm((ROWS, CX), F32),
            vm((ROWS, CX), F32),
            vm((CZ + 2, CY, CX), F32),
            vm((CZ + 32, CY, CX), F32),
            vm((40 * CY, CX), F32),
            vm((CZ, CY + 16, CX), F32),
            vm((CZ + 2, CY + 32, CX), F32),
            vm((BRICKS, ANG, CX), F32),
            vm((1, ANG, NBLK * DW), F32),
            vm((ANG, NBLK * DW), F32),
            vm((ANG, NBLK * DW), F32),
            vm((2, 2, R * CY, CX), BF16),
            vm((2, 2, R * CY, CX), BF16),
            vm((128, V), BF16),
            vm((128, 128), BF16),
            vm((96, 128), BF16),
            vm((CZ, V), F32),
            vm((CY + 32, CZ, CX), F32),
            vm((CY + 16, CZ, CX), F32),
            vm((3, 2, CZ * R, CX), BF16),
            vm((3, 2, CZ * R, CX), BF16),
            vm((ROWS, CX), BF16),
            vm((2, ROWS, CX), BF16),
            vm((4, 2, 16, ROWS), BF16),
            vm((4, 3, 2, 16, ROWS), BF16),
            vm((2, (CZ + 2) * R + CZ, CX), BF16),
            vm((2, (CZ + 2) * R + CZ, CX), BF16),
            vm((2, 16, ROWS9P), BF16),
            vm((3, 2, 16, ROWS9P), BF16),
            vm((2, 2, CY, CX), F32),
            vm((2, 2, CY, CX), F32),
            vm((2, 2, CZ, CX), F32),
            vm((2, 2, CZ, CX), F32),
            vm((2, 2, 16, ROWS), BF16),
            vm((2, 2, 16, ROWS), BF16),
            vm((2, 2, CY, CX), F32),
            vm((2, 2, CY, CX), F32),
            vm((2, 2, CZ, CX), F32),
            vm((2, 2, CZ, CX), F32),
            vm((2, 2, 16, ROWS), BF16),
            vm((2, 2, 16, ROWS), BF16),
            vm((2, CY, CX), F32),
            vm((2, CZ, CX), F32),
            vm((2, CZ * ANG, 128), F32),
            vm((CZ, V), BF16),
            vm((2, BRICKS, ANG, DW), BF16),
            vm((2, BRICKS, ANG, DW), BF16),
            vm((2, BRICKS, ANG, DW), BF16),
            vm((2, BRICKS, ANG, DW), BF16),
            block, block,
            vm((3, CZ, CY, CX), F32),
            vm((3, CZ, CY, CX), F32),
            block, block,
            vm((2, 1, CX), F32),
            vm((2, GZ, 1, CX), F32),
            vm((2, 1, CX), F32),
            vm((2, BRICKS, 1, CX), F32),
            vm((GZ * BRICKS, 1, CX), F32),
            vm((3 * CX, CX), BF16),
            vm((96, CX), BF16),
            vm((3 * CX, CX), BF16),
            vm((64, CX), BF16),
            vm((3 * CX, 2 * CX), BF16),
            vm((64, 2 * CX), BF16),
            dma((2,)),
            dma((V // LOAD,)),
            dma((2,)),
            dma((2, 2)),
            dma((8,)),
            dma((2, 8)),
            dma((3, 2)),
            dma((2, 3, 2)),
            dma,
            dma((2, 2)),
            dma,
            dma,
            dma,
            dma,
            dma,
            dma,
            pltpu.SemaphoreType.REGULAR((3,)),
            dma((2,)),
        ],
        compiler_params=pltpu.CompilerParams(
            collective_id=0, has_side_effects=True, vmem_limit_bytes=60 * 1024 * 1024
        ),
    )(start, measured, tiles, tile_block, angle_row)


def solution(mesh):
    return jax.shard_map(
        body,
        mesh=mesh,
        in_specs=(
            P("gz", "gy", "gx"),
            P(("gz", "gy", "gx"), None, None),
            P("gy", None, "gx"),
            P(),
            P(),
        ),
        out_specs=(P("gz", "gy", "gx"), P(None, "gz", "gy", "gx")),
        check_vma=False,
    )
```
